32 devices in a mesh: dp: 8 (over z, y), row: 2 (over core), col: 2 (over x).
Axes of the slice: x: 2, y: 2, z: 4, core: 2. Of those that a mesh axis runs over, the one named last changes fastest.
Arguments:
- hidden: bfloat16 [16384, 768], P('dp', 'row'), may hold values from -6 to 6
- gate_proj: bfloat16 [768, 1536], P('row', 'col'), may hold values from -0.21875 to 0.21875
- value_proj: bfloat16 [768, 1536], P('row', 'col'), may hold values from -0.21875 to 0.21875
- step_proj: bfloat16 [768, 24], P('row', 'col'), may hold values from -0.21875 to 0.21875
- state_proj: bfloat16 [768, 256], P('row'), may hold values from -0.21875 to 0.21875
- value_filter: float32 [4, 1536], P(None, ('col', 'row')), may hold values from -3 to 3
- value_shift: float32 [1536], P(('col', 'row')), may hold values from -0.5 to 0.5
- shared_kernel: float32 [4, 256], replicated, may hold values from -3 to 3
- shared_offset: float32 [256], replicated, may hold values from -0.5 to 0.5
- decay_log: float32 [24], P(('col', 'row')), may hold values from 0 to 2.77
- step_bias: float32 [24], P(('col', 'row')), may hold values from -6.9 to -2.3
- skip_gain: float32 [24], P(('col', 'row')), may hold values from 0.5 to 1.5
- input_gain: float32 [768], P('row'), may hold values from 0.5 to 1.5
- gated_gain: bfloat16 [1536], P(('col', 'row')), may hold values from 0.5 to 1.5
- output_proj: bfloat16 [1536, 768], P('col', 'row'), may hold values from -0.15625 to 0.15625
- cotangent: bfloat16 [16384, 768], P('dp', 'row'), may hold values from -6 to 6
Outputs:
- result: bfloat16 [16384, 768], P('dp', 'row')
- hidden_grad: float32 [16384, 768], P('dp', 'row')
- gate_grad: float32 [768, 1536], P('row', 'col')
- value_grad: float32 [768, 1536], P('row', 'col')
- step_grad: float32 [768, 24], P('row', 'col')
- state_grad: float32 [768, 256], P('row')
- filter_grad: float32 [4, 1536], P(None, ('col', 'row'))
- shift_grad: float32 [1536], P(('col', 'row'))
- kernel_grad: float32 [4, 256], replicated
- offset_grad: float32 [256], replicated
- decay_grad: float32 [24], P(('col', 'row'))
- bias_grad: float32 [24], P(('col', 'row'))
- skip_grad: float32 [24], P(('col', 'row'))
- norm_grad: float32 [768], P('row')
- gated_grad: float32 [1536], P(('col', 'row'))
- output_grad: float32 [1536, 768], P('col', 'row')
The draws below stay inside these ranges and needn't reach their ends.
All inputs are finite; a program needn't handle non-finite values.
Results may differ from the reference program's by a relative error of at most 0.012.
Values may be sent and summed in bfloat16 or wider, within the bound.
A program may use at most 320 MiB of HBM per device.

```python
import functools
import jax
import jax.numpy as jnp
from jax import lax

D = 768
HEADS = 24
STATE = 128
CONV = 4
GROUP = 256
LEN = 2048
INNER = 1536
SEQS = 8
TOKENS = 16384


def level_of(own_key, extent, cuts, smallest, top_value):
    def one(dim, shards_of):
        draws = jax.random.uniform(jax.random.fold_in(jax.random.fold_in(own_key, 6), dim), (shards_of,), jnp.float32, smallest / len(cuts), top_value / len(cuts))
        return jnp.repeat(jnp.exp(draws), extent[dim] // shards_of).reshape((-1,) + (1,) * (len(extent) - dim - 1))

    loudness = one(*cuts[0])
    for cut in cuts[1:]:
        loudness = loudness * one(*cut)
    return loudness


def bell_draw(own_key, extent, deviation, bound, cuts=(), kind=jnp.bfloat16):
    values = jax.random.normal(own_key, extent, jnp.float32) * deviation
    if len(cuts) > 0:
        values = level_of(own_key, extent, cuts, -0.22, 0.18) * values
    return jnp.clip(values, min=-bound, max=bound).astype(kind)


def setup_inputs(seed: int = 0) -> dict:
    splits = jax.random.split(jax.random.key(seed), 17)
    hidden = bell_draw(splits[0], (TOKENS, D), 1.0, 6.0, ((0, 8), (1, 2)))
    gate_proj = bell_draw(splits[1], (D, INNER), D ** -0.5, 0.21875, ((0, 2), (1, 2)))
    value_proj = bell_draw(splits[2], (D, INNER), D ** -0.5, 0.21875, ((0, 2), (1, 2)))
    step_proj = bell_draw(splits[3], (D, HEADS), D ** -0.5, 0.21875, ((0, 2), (1, 2)))
    state_proj = bell_draw(splits[4], (D, 2 * STATE), D ** -0.5, 0.21875, ((0, 2),))
    value_filter = bell_draw(splits[5], (CONV, INNER), CONV ** -0.5, 3.0, ((1, 4),), jnp.float32)
    value_shift = jnp.clip(jax.random.uniform(splits[6], (INNER,), jnp.float32, -0.5, 0.5) * level_of(splits[6], (INNER,), ((0, 4),), -0.4, 0.0), -0.5, 0.5)
    shared_kernel = bell_draw(splits[7], (CONV, 2 * STATE), CONV ** -0.5, 3.0, (), jnp.float32)
    shared_offset = jnp.clip(jax.random.uniform(splits[8], (2 * STATE,), jnp.float32, -0.5, 0.5), -0.5, 0.5)
    decay_log = jnp.clip(2.77 * jax.random.uniform(splits[9], (HEADS,), jnp.float32) ** level_of(splits[9], (HEADS,), ((0, 4),), -0.2, 0.2), 0.0, 2.77)
    step_bias = jnp.clip(-6.9 + 4.6000001430511475 * jax.random.uniform(splits[10], (HEADS,), jnp.float32) ** level_of(splits[10], (HEADS,), ((0, 4),), -0.2, 0.2), -6.9, -2.3)
    skip_gain = jnp.clip(0.5 + 1.0 * jax.random.uniform(splits[11], (HEADS,), jnp.float32) ** level_of(splits[11], (HEADS,), ((0, 4),), -0.2, 0.2), 0.5, 1.5)
    input_gain = jnp.clip(1.0 + 0.1 * jax.random.normal(splits[12], (D,), jnp.float32), 0.5, 1.5)
    gated_gain = jnp.clip(1.0 + 0.1 * jax.random.normal(splits[13], (INNER,), jnp.float32), 0.5, 1.5).astype(jnp.bfloat16)
    output_proj = bell_draw(splits[14], (INNER, D), INNER ** -0.5, 0.15625, ((0, 2), (1, 2)))
    cotangent = bell_draw(splits[15], (TOKENS, D), 1.0, 6.0, ((0, 8), (1, 2)))
    return dict(hidden=hidden, gate_proj=gate_proj, value_proj=value_proj, step_proj=step_proj, state_proj=state_proj, value_filter=value_filter, value_shift=value_shift, shared_kernel=shared_kernel, shared_offset=shared_offset, decay_log=decay_log, step_bias=step_bias, skip_gain=skip_gain, input_gain=input_gain, gated_gain=gated_gain, output_proj=output_proj, cotangent=cotangent)


EPSILON = 1e-05
HIGHEST = lax.Precision.HIGHEST

def causal_filter(signal, kernel, offset, seq_count):
    channels = signal.shape[-1]
    taps = kernel.shape[0]
    seq_view = signal.reshape(seq_count, -1, channels)
    length = seq_view.shape[1]
    padded = jnp.pad(seq_view, ((0, 0), (taps - 1, 0), (0, 0)))
    total = jnp.zeros_like(seq_view) + offset
    for position in range(taps):
        total = total + padded[:, position:position + length] * kernel[position]
    return jax.nn.silu(total).reshape(signal.shape)

def state_scan(values, inputs_b, reads_c, steps, logdecay, block_len):
    seq_count, length, heads, channels = values.shape
    width = inputs_b.shape[-1]
    blocks = length // block_len

    def split(array):
        shaped = array.reshape((seq_count, blocks, block_len) + array.shape[2:])
        return jnp.moveaxis(shaped, 1, 0)
    positions = jnp.arange(block_len)
    lower = (positions[:, None] >= positions[None, :])[None, :, :, None]

    def advance(carried, pieces):
        vals, b_in, c_in, step_in, log_in = pieces
        cumul = jnp.cumsum(log_in, axis=1)
        gaps = cumul[:, :, None, :] - cumul[:, None, :, :]
        decays = jnp.where(lower, jnp.exp(jnp.where(lower, gaps, 0.0)), 0.0)
        scores = jnp.einsum('sqn,skn->sqk', c_in, b_in, precision=HIGHEST)
        weights = scores[..., None] * decays * step_in[:, None, :, :]
        inside = jnp.einsum('sqkh,skhp->sqhp', weights, vals, precision=HIGHEST)
        carried_out = jnp.einsum('sqn,shpn->sqhp', c_in, carried, precision=HIGHEST)
        outputs = inside + carried_out * jnp.exp(cumul)[..., None]
        final = cumul[:, -1, :]
        tails = jnp.exp(final[:, None, :] - cumul) * step_in
        fresh = jnp.einsum('skh,skhp,skn->shpn', tails, vals, b_in, precision=HIGHEST)
        carried = carried * jnp.exp(final)[:, :, None, None] + fresh
        return (carried, outputs)
    start = jnp.zeros((seq_count, heads, channels, width), jnp.float32)
    _, outputs = lax.scan(advance, start, (split(values), split(inputs_b), split(reads_c), split(steps), split(logdecay)))
    return jnp.moveaxis(outputs, 0, 1).reshape(seq_count, length, heads, channels)

def mixer_core(pre_value, pre_shared, pre_step, pre_gate, value_filter, value_shift, shared_kernel, shared_offset, decay_log, step_bias, skip_gain, seq_count, block_len):
    heads = pre_step.shape[1]
    channels = pre_value.shape[1] // heads
    width = pre_shared.shape[1] // 2
    token_count = pre_value.shape[0]
    filtered = causal_filter(pre_value, value_filter, value_shift, seq_count)
    shared = causal_filter(pre_shared, shared_kernel, shared_offset, seq_count)
    steps = jax.nn.softplus(pre_step + step_bias)
    logdecay = -jnp.exp(decay_log) * steps
    values = filtered.reshape(seq_count, -1, heads, channels)
    inputs_b = shared[:, :width].reshape(seq_count, -1, width)
    reads_c = shared[:, width:].reshape(seq_count, -1, width)
    outputs = state_scan(values, inputs_b, reads_c, steps.reshape(seq_count, -1, heads), logdecay.reshape(seq_count, -1, heads), block_len)
    outputs = outputs + skip_gain[:, None] * values
    return outputs.reshape(token_count, heads * channels) * jax.nn.silu(pre_gate)

def reference(hidden, gate_proj, value_proj, step_proj, state_proj, value_filter, value_shift, shared_kernel, shared_offset, decay_log, step_bias, skip_gain, input_gain, gated_gain, output_proj, cotangent):
    inner_width = gate_proj.shape[1]
    width = hidden.shape[1]
    gain_out = gated_gain.astype(jnp.float32)

    def one_sequence(totals, pair):
        seq_in, seq_cot = pair
        hidden32 = seq_in.astype(jnp.float32)
        recip = lax.rsqrt(lax.optimization_barrier(jnp.mean(hidden32 * hidden32, axis=1, keepdims=True)) + EPSILON)
        normed = (hidden32 * input_gain).astype(jnp.bfloat16)
        q_gate = jnp.dot(normed, gate_proj, preferred_element_type=jnp.float32)
        q_value = jnp.dot(normed, value_proj, preferred_element_type=jnp.float32)
        q_step = jnp.dot(normed, step_proj, preferred_element_type=jnp.float32)
        q_shared = jnp.dot(normed, state_proj, preferred_element_type=jnp.float32)
        local_mixer = functools.partial(mixer_core, seq_count=1, block_len=GROUP)
        mixed32, pullback = jax.vjp(local_mixer, recip * q_value, recip * q_shared, recip * q_step, recip * q_gate, value_filter, value_shift, shared_kernel, shared_offset, decay_log, step_bias, skip_gain)
        mixed = mixed32.astype(jnp.bfloat16).astype(jnp.float32)
        scale = lax.rsqrt(lax.optimization_barrier(jnp.mean(mixed * mixed, axis=1, keepdims=True)) + EPSILON)
        weighted = (mixed * gain_out).astype(jnp.bfloat16)
        proj = jnp.dot(weighted, output_proj, preferred_element_type=jnp.float32)
        out_seq = (hidden32 + scale * proj).astype(jnp.bfloat16)
        cot = seq_cot.astype(jnp.float32)
        scale_dot = lax.optimization_barrier(jnp.sum(cot * proj, axis=1, keepdims=True))
        scaled_cot = (scale * cot).astype(jnp.bfloat16)
        g_output = jnp.dot(weighted.T, scaled_cot, preferred_element_type=jnp.float32)
        d_weighted = jnp.dot(scaled_cot, output_proj.T, preferred_element_type=jnp.float32)
        g_gated = lax.optimization_barrier(jnp.sum(d_weighted * mixed, axis=0))
        d_mixed = d_weighted * gain_out - scale_dot * scale ** 3 * mixed / inner_width
        pulled = pullback(d_mixed)
        d_value, d_shared, d_step, d_gate = (pulled[0], pulled[1], pulled[2], pulled[3])
        d_recip = lax.optimization_barrier(jnp.sum(d_gate * q_gate, axis=1, keepdims=True)) + lax.optimization_barrier(jnp.sum(d_value * q_value, axis=1, keepdims=True))
        d_recip = d_recip + lax.optimization_barrier(jnp.sum(d_step * q_step, axis=1, keepdims=True)) + lax.optimization_barrier(jnp.sum(d_shared * q_shared, axis=1, keepdims=True))
        p_gate = (recip * d_gate).astype(jnp.bfloat16)
        p_value = (recip * d_value).astype(jnp.bfloat16)
        p_step = (recip * d_step).astype(jnp.bfloat16)
        p_shared = (recip * d_shared).astype(jnp.bfloat16)
        g_gate = jnp.dot(normed.T, p_gate, preferred_element_type=jnp.float32)
        g_value = jnp.dot(normed.T, p_value, preferred_element_type=jnp.float32)
        g_step = jnp.dot(normed.T, p_step, preferred_element_type=jnp.float32)
        g_state = jnp.dot(normed.T, p_shared, preferred_element_type=jnp.float32)
        d_normed = jnp.dot(p_gate, gate_proj.T, preferred_element_type=jnp.float32)
        d_normed = d_normed + jnp.dot(p_value, value_proj.T, preferred_element_type=jnp.float32)
        d_normed = d_normed + jnp.dot(p_step, step_proj.T, preferred_element_type=jnp.float32)
        d_normed = d_normed + jnp.dot(p_shared, state_proj.T, preferred_element_type=jnp.float32)
        d_hidden = cot + d_normed * input_gain - d_recip * recip ** 3 * hidden32 / width
        g_norm = lax.optimization_barrier(jnp.sum(d_normed * hidden32, axis=0))
        terms = (g_gate, g_value, g_step, g_state, pulled[4], pulled[5], pulled[6], pulled[7], pulled[8], pulled[9], pulled[10], g_norm, g_gated, g_output)
        totals = tuple((total + term for total, term in zip(totals, terms)))
        return (totals, (out_seq, d_hidden))
    shapes = (gate_proj, value_proj, step_proj, state_proj, value_filter, value_shift, shared_kernel, shared_offset, decay_log, step_bias, skip_gain, input_gain, gated_gain, output_proj)
    start = tuple((jnp.zeros(item.shape, jnp.float32) for item in shapes))
    seq_hidden = hidden.reshape(SEQS, LEN, D)
    seq_cots = cotangent.reshape(SEQS, LEN, D)
    totals, (outs, d_hid) = lax.scan(one_sequence, start, (seq_hidden, seq_cots))
    return (outs.reshape(TOKENS, D), d_hid.reshape(TOKENS, D)) + totals
```

```python
import functools

import jax
import jax.numpy as jnp
from jax import lax
from jax.experimental import pallas as pl
from jax.experimental.pallas import tpu as pltpu
from jax.sharding import PartitionSpec as P

LEN = 2048
EPSILON = 1e-05
SUB = 128
STEP = 256
F32 = jnp.float32
BF16 = jnp.bfloat16
SWAP = [(0, 1), (1, 0)]


def dot(a, b):
    return jnp.dot(a, b, preferred_element_type=F32)


def dot_nt(a, b):
    return lax.dot_general(a, b, (((1,), (1,)), ((), ())), preferred_element_type=F32)


def dot_tn(a, b):
    return lax.dot_general(a, b, (((0,), (0,)), ((), ())), preferred_element_type=F32)


def sigmoid(x):
    return 0.5 * jnp.tanh(0.5 * x) + 0.5


def softplus(x):
    return jnp.maximum(x, 0.0) + jnp.log1p(jnp.exp(-jnp.abs(x)))


def fold8(x):
    return jnp.sum(x.reshape(x.shape[0] // 8, 8, x.shape[1]), axis=0)


def row_scan(x, mat):
    hi = x.astype(BF16).astype(F32)
    rest = x - hi
    mid = rest.astype(BF16).astype(F32)
    low = rest - mid
    parts = jnp.concatenate([hi, mid, low, jnp.zeros_like(x)], axis=0).astype(BF16)
    out = dot(parts, mat)
    return out[0:8] + out[8:16] + out[16:24]


def head_sums(sel, z):
    hi = z.astype(BF16)
    low = (z - hi.astype(F32)).astype(BF16)
    return (dot_nt(sel, hi) + dot_nt(sel, low))[0:8]


def iota(shape, dim):
    return lax.broadcasted_iota(jnp.int32, shape, dim)


def spread(cols, first, rows):
    lane = iota((rows, 128), 1)
    return jnp.where(
        lane < 64,
        jnp.broadcast_to(cols[:, first : first + 1], (rows, 128)),
        jnp.broadcast_to(cols[:, first + 1 : first + 2], (rows, 128)),
    )


def pair_stack(x):
    lane = iota(x.shape, 1)
    zero = jnp.zeros_like(x)
    return jnp.concatenate([jnp.where(lane < 64, x, zero), jnp.where(lane < 64, zero, x)], axis=0)


def forward_kernel(
    steps_per_seq,
    width,
    hid_own,
    hid_rec,
    gains,
    w_own,
    w_rec,
    vtap,
    stap,
    head_par,
    mixed_out,
    pre_gate_out,
    pre_value_out,
    conv_value_out,
    pre_shared_out,
    conv_shared_out,
    y_out,
    state_out,
    rows_out,
    state,
    vbuf,
    sbuf,
):
    chan = mixed_out.shape[1]
    pairs = chan // 128

    @pl.when(pl.program_id(0) % steps_per_seq == 0)
    def _():
        state[...] = jnp.zeros_like(state)
        vbuf[0:8, :] = jnp.zeros((8, vbuf.shape[1]), F32)
        sbuf[0:8, :] = jnp.zeros((8, sbuf.shape[1]), F32)

    h0 = hid_own[...].astype(F32)
    h1 = hid_rec[...].astype(F32)
    square = jnp.sum(h0 * h0, axis=1, keepdims=True) + jnp.sum(h1 * h1, axis=1, keepdims=True)
    recip = lax.rsqrt(square / width + EPSILON)
    n0 = (h0 * gains[0:1, :]).astype(BF16)
    n1 = (h1 * gains[1:2, :]).astype(BF16)
    q = dot(n0, w_own[...]) + dot(n1, w_rec[...])
    pre = q * recip
    gate = pre[:, 0:chan]
    pre_gate_out[...] = gate
    pre_value = pre[:, chan : 2 * chan]
    pre_value_out[...] = pre_value
    pre_shared = pre[:, 2 * chan : 2 * chan + 256]
    pre_shared_out[...] = pre_shared
    vbuf[8 : 8 + STEP, :] = pre_value
    sbuf[8 : 8 + STEP, :] = pre_shared
    conv = jnp.broadcast_to(vtap[4:5, :], (STEP, chan))
    conv_s = jnp.broadcast_to(stap[4:5, :], (STEP, 256))
    for k in range(4):
        conv = conv + vbuf[5 + k : 5 + k + STEP, :] * vtap[k : k + 1, :]
        conv_s = conv_s + sbuf[5 + k : 5 + k + STEP, :] * stap[k : k + 1, :]
    vbuf[0:8, :] = vbuf[STEP : STEP + 8, :]
    sbuf[0:8, :] = sbuf[STEP : STEP + 8, :]
    conv_value_out[...] = conv
    conv_shared_out[...] = conv_s
    x = conv * sigmoid(conv)
    act = conv_s * sigmoid(conv_s)

    head_rows = jnp.transpose(pre[:, 2 * chan + 256 : 2 * chan + 384])[0:8]
    v = head_rows + head_par[0:8, 0:1]
    steps = softplus(v)
    logd = head_par[8:16, 0:1] * steps
    rows_out[0:8, :] = v
    rows_out[16:24, :] = jnp.transpose(jnp.broadcast_to(recip, (STEP, 128)))[0:8]

    upper = (iota((SUB, SUB), 0) <= iota((SUB, SUB), 1)).astype(F32).astype(BF16)
    causal = iota((SUB, SUB), 0) >= iota((SUB, SUB), 1)
    sg = gate * sigmoid(gate)
    for sub in range(STEP // SUB):
        lo, hi = sub * SUB, (sub + 1) * SUB
        cum_r = row_scan(logd[:, lo:hi], upper)
        rows_out[8:16, lo:hi] = cum_r
        cols = jnp.transpose(jnp.concatenate([cum_r, steps[:, lo:hi]], axis=0))
        b_in = act[lo:hi, 0:128]
        b_bf = b_in.astype(BF16)
        c_bf = act[lo:hi, 128:256].astype(BF16)
        b_t = jnp.transpose(b_in).astype(BF16)
        scores = dot_nt(c_bf, b_bf)
        for p in range(pairs):
            pl0, pl1 = p * 128, (p + 1) * 128
            c0 = jnp.broadcast_to(cols[:, 2 * p : 2 * p + 1], (SUB, 128))
            c1 = jnp.broadcast_to(cols[:, 2 * p + 1 : 2 * p + 2], (SUB, 128))
            weights = []
            for col, h in ((c0, 2 * p), (c1, 2 * p + 1)):
                gap = jnp.where(causal, col - cum_r[h : h + 1, :], -1e30)
                weights.append((scores * jnp.exp(gap)).astype(BF16))
            lane = iota((SUB, 128), 1)
            cum_e = jnp.where(lane < 64, c0, c1)
            step_e = spread(cols, 8 + 2 * p, SUB)
            xs = x[lo:hi, pl0:pl1]
            xh = step_e * xs
            inside = dot(jnp.concatenate(weights, axis=1), pair_stack(xh.astype(BF16)))
            held = state[:, pl0:pl1]
            held_bf = held.astype(BF16)
            state_out[lo:hi, pl0:pl1] = held_bf
            carried = dot(c_bf, held_bf)
            y = inside + carried * jnp.exp(cum_e)
            y_out[lo:hi, pl0:pl1] = y
            last = cum_e[SUB - 1 : SUB, :]
            tail = (xh * jnp.exp(last - cum_e)).astype(BF16)
            state[:, pl0:pl1] = held * jnp.exp(last) + dot(b_t, tail)
            y = y + vtap[5:6, pl0:pl1] * xs
            mixed_out[lo:hi, pl0:pl1] = (y * sg[lo:hi, pl0:pl1]).astype(BF16)


def backward_kernel(
    steps_per_seq,
    cot_own,
    cot_rec,
    wo_own,
    wo_rec,
    trow,
    rows_in,
    mixed,
    pre_gate,
    pre_value,
    conv_value,
    pre_shared,
    conv_shared,
    y_in,
    state_in,
    w_own,
    w_rec,
    vtap,
    stap,
    head_par,
    sel_ref,
    p_out,
    dn_own,
    dn_rec,
    rsum_out,
    acc_v,
    acc_s,
    acc_h,
    grad,
    vbuf,
    sbuf,
    dxbuf,
    dbbuf,
):
    chan = mixed.shape[1]
    pairs = chan // 128

    @pl.when(pl.program_id(0) == 0)
    def _():
        acc_v[...] = jnp.zeros_like(acc_v)
        acc_s[...] = jnp.zeros_like(acc_s)
        acc_h[...] = jnp.zeros_like(acc_h)

    @pl.when(pl.program_id(0) % steps_per_seq == 0)
    def _():
        grad[...] = jnp.zeros_like(grad)
        vbuf[STEP : STEP + 8, :] = jnp.zeros((8, vbuf.shape[1]), F32)
        sbuf[STEP : STEP + 8, :] = jnp.zeros((8, sbuf.shape[1]), F32)

    tcol = jnp.transpose(jnp.concatenate([trow[...], rows_in[16:24, :]], axis=0))
    scale = tcol[:, 0:1]
    coef = tcol[:, 1:2]
    recip = tcol[:, 8:9]
    s0 = (cot_own[...].astype(F32) * scale).astype(BF16)
    s1 = (cot_rec[...].astype(F32) * scale).astype(BF16)
    d_weighted = dot_nt(s0, wo_own[...]) + dot_nt(s1, wo_rec[...])
    mix = mixed[...].astype(F32)
    acc_v[48:56, :] += fold8(d_weighted * mix)
    d_mixed = d_weighted * vtap[6:7, :] - coef * mix
    gate = pre_gate[...]
    sig = sigmoid(gate)
    silu = gate * sig
    conv = conv_value[...]
    sig_v = sigmoid(conv)
    x = conv * sig_v
    y_scan = y_in[...]
    y = y_scan + vtap[5:6, :] * x
    dy = d_mixed * silu
    d_gate = d_mixed * y * (sig + silu * (1.0 - sig))
    acc_v[40:48, :] += fold8(dy * x)
    conv_s = conv_shared[...]
    sig_s = sigmoid(conv_s)
    act = conv_s * sig_s

    sel = sel_ref[...]
    sel_f = sel.astype(F32)[0:8]
    v = rows_in[0:8, :]
    steps = softplus(v)
    logd = head_par[8:16, 0:1] * steps
    lower = (iota((SUB, SUB), 0) >= iota((SUB, SUB), 1)).astype(F32).astype(BF16)
    strict = (iota((SUB, SUB), 0) < iota((SUB, SUB), 1)).astype(F32).astype(BF16)
    causal_t = iota((SUB, SUB), 0) <= iota((SUB, SUB), 1)
    for sub in reversed(range(STEP // SUB)):
        lo, hi = sub * SUB, (sub + 1) * SUB
        cum_r = rows_in[8:16, lo:hi]
        cols = jnp.transpose(jnp.concatenate([cum_r, steps[:, lo:hi]], axis=0))
        b_bf = act[lo:hi, 0:128].astype(BF16)
        c_in = act[lo:hi, 128:256]
        c_bf = c_in.astype(BF16)
        c_t = jnp.transpose(c_in).astype(BF16)
        scores_t = dot_nt(b_bf, c_bf)
        d_scores = jnp.zeros((SUB, SUB), F32)
        db = jnp.zeros((SUB, 128), F32)
        dc = jnp.zeros((SUB, 128), F32)
        z_sum = jnp.zeros((8, SUB), F32)
        e_sum = jnp.zeros((8, SUB), F32)
        f_sum = jnp.zeros((8, SUB), F32)
        gh = jnp.zeros((8, 1), F32)
        for p in range(pairs):
            pl0, pl1 = p * 128, (p + 1) * 128
            c0 = jnp.broadcast_to(cols[:, 2 * p : 2 * p + 1], (SUB, 128))
            c1 = jnp.broadcast_to(cols[:, 2 * p + 1 : 2 * p + 2], (SUB, 128))
            decays = []
            for col, h in ((c0, 2 * p), (c1, 2 * p + 1)):
                gap = jnp.where(causal_t, cum_r[h : h + 1, :] - col, -1e30)
                decays.append(jnp.exp(gap))
            weights = [(scores_t * d).astype(BF16) for d in decays]
            lane = iota((SUB, 128), 1)
            cum_e = jnp.where(lane < 64, c0, c1)
            step_e = spread(cols, 8 + 2 * p, SUB)
            xs = x[lo:hi, pl0:pl1]
            xh = step_e * xs
            xh_bf = xh.astype(BF16)
            dys = dy[lo:hi, pl0:pl1]
            dys_bf = dys.astype(BF16)
            stack = pair_stack(dys_bf)
            inner = dot(jnp.concatenate(weights, axis=1), stack)
            d_pair = dot_nt(xh_bf, stack)
            d_scores = d_scores + decays[0] * d_pair[:, 0:128] + decays[1] * d_pair[:, 128:256]
            last = cum_e[SUB - 1 : SUB, :]
            tail_e = jnp.exp(last - cum_e)
            g = grad[:, pl0:pl1]
            g_bf = g.astype(BF16)
            outer = dot(b_bf, g_bf) * tail_e
            u = inner + outer
            dxbuf[lo:hi, pl0:pl1] = step_e * u + vtap[5:6, pl0:pl1] * dys
            db = db + dot_nt((xh * tail_e).astype(BF16), g_bf)
            dya = (dys * jnp.exp(cum_e)).astype(BF16)
            held = state_in[lo:hi, pl0:pl1]
            dc = dc + dot_nt(dya, held)
            sel_p = sel[:, pl0:pl1]
            z_sum = z_sum + head_sums(
                sel_p, dys_bf.astype(F32) * y_in[lo:hi, pl0:pl1] - xh_bf.astype(F32) * inner
            )
            e_sum = e_sum + head_sums(sel_p, xh * outer)
            f_sum = f_sum + head_sums(sel_p, xs * u)
            decay_row = jnp.exp(last)
            gh_row = decay_row * jnp.sum(g * held.astype(F32), axis=0, keepdims=True)
            gh = gh + jnp.sum(sel_f[:, pl0:pl1] * gh_row, axis=1, keepdims=True)
            grad[:, pl0:pl1] = g * decay_row + dot(c_t, dya)
        ds_bf = d_scores.astype(BF16)
        dbbuf[lo:hi, 0:128] = db + dot(ds_bf, c_bf)
        dbbuf[lo:hi, 128:256] = dc + dot(jnp.transpose(d_scores).astype(BF16), b_bf)
        d_log = row_scan(z_sum, lower) + row_scan(e_sum, strict) + gh
        d_step = (f_sum + d_log * head_par[8:16, 0:1]) * sigmoid(v[:, lo:hi])
        acc_h[0:8, :] += d_log * logd[:, lo:hi]
        acc_h[8:16, :] += d_step
        pre_step = v[:, lo:hi] - head_par[0:8, 0:1]
        rsum_out[:, lo:hi] = jnp.broadcast_to(
            jnp.sum(d_step * pre_step, axis=0, keepdims=True), (8, SUB)
        )
        d_cols = jnp.transpose(jnp.concatenate([d_step, jnp.zeros((120, SUB), F32)], axis=0))
        p_out[lo:hi, 2 * chan + 256 : 2 * chan + 384] = (recip[lo:hi] * d_cols).astype(BF16)

    d_conv = dxbuf[...] * (sig_v + x * (1.0 - sig_v))
    d_conv_s = dbbuf[...] * (sig_s + act * (1.0 - sig_s))
    vbuf[0:STEP, :] = d_conv
    sbuf[0:STEP, :] = d_conv_s
    acc_v[32:40, :] += fold8(d_conv)
    acc_s[32:40, :] += fold8(d_conv_s)
    pv = pre_value[...]
    ps = pre_shared[...]
    d_value = jnp.zeros((STEP, chan), F32)
    d_shared = jnp.zeros((STEP, 256), F32)
    for k in range(4):
        moved = vbuf[3 - k : 3 - k + STEP, :]
        d_value = d_value + vtap[k : k + 1, :] * moved
        acc_v[8 * k : 8 * k + 8, :] += fold8(pv * moved)
        moved = sbuf[3 - k : 3 - k + STEP, :]
        d_shared = d_shared + stap[k : k + 1, :] * moved
        acc_s[8 * k : 8 * k + 8, :] += fold8(ps * moved)
    vbuf[STEP : STEP + 8, :] = vbuf[0:8, :]
    sbuf[STEP : STEP + 8, :] = sbuf[0:8, :]
    p_out[:, 0:chan] = (recip * d_gate).astype(BF16)
    p_out[:, chan : 2 * chan] = (recip * d_value).astype(BF16)
    p_out[:, 2 * chan : 2 * chan + 256] = (recip * d_shared).astype(BF16)
    ones = jnp.ones((16, chan), BF16)
    rsum_out[...] += head_sums(ones, d_gate * gate + d_value * pv)
    rsum_out[...] += head_sums(ones[:, 0:256], d_shared * ps)
    pb = p_out[...]
    dn_own[...] = dot_nt(pb, w_own[...]).astype(BF16)
    dn_rec[...] = dot_nt(pb, w_rec[...]).astype(BF16)


def swap(x, axis):
    return lax.ppermute(x, axis, SWAP)


def body(
    hidden,
    gate_proj,
    value_proj,
    step_proj,
    state_proj,
    value_filter,
    value_shift,
    shared_kernel,
    shared_offset,
    decay_log,
    step_bias,
    skip_gain,
    input_gain,
    gated_gain,
    output_proj,
    cotangent,
):
    tokens, half = hidden.shape
    width = 2 * half
    chan = gated_gain.shape[0]
    inner_width = 4 * chan
    heads = decay_log.shape[0]
    r = lax.axis_index("row")
    seq_len = min(LEN, tokens)
    steps_per_seq = seq_len // STEP
    grid = tokens // STEP

    def cut(x, start, size, axis):
        return lax.dynamic_slice_in_dim(x, start * size, size, axis)

    def packed(side):
        return jnp.concatenate(
            [
                cut(gate_proj, side, chan, 1),
                cut(value_proj, side, chan, 1),
                state_proj,
                jnp.pad(cut(step_proj, side, heads, 1), ((0, 0), (0, 128 - heads))),
            ],
            axis=1,
        )

    w_own = packed(r)
    w_rec = swap(packed(1 - r), "row")
    hid_rec = swap(hidden, "row")
    cot_rec = swap(cotangent, "row")
    wo_own = cut(output_proj, r, chan, 0)
    wo_part = cut(output_proj, 1 - r, chan, 0)
    wo_rec = swap(wo_part, "row")
    gain_f = gated_gain.astype(F32)
    two = swap(jnp.stack([input_gain, gain_f]), "row")
    gains = jnp.concatenate([input_gain[None], two[0:1], jnp.zeros((6, half), F32)], axis=0)
    gated_rec = two[1]

    skip_lane = jnp.repeat(skip_gain, chan // heads)
    vtap = jnp.concatenate(
        [value_filter, value_shift[None], skip_lane[None], gain_f[None], jnp.zeros((1, chan), F32)], axis=0
    )
    stap = jnp.concatenate([shared_kernel, shared_offset[None], jnp.zeros((3, 256), F32)], axis=0)
    pad_h = (0, 8 - heads)
    head_par = jnp.concatenate([jnp.pad(step_bias, pad_h), jnp.pad(-jnp.exp(decay_log), pad_h)])
    head_par = jnp.broadcast_to(head_par[:, None], (16, 128))

    wide = w_own.shape[1]

    def blk(cols):
        return pl.BlockSpec((STEP, cols), lambda i: (i, 0))

    def whole(shape):
        return pl.BlockSpec(shape, lambda i: (0, 0))

    def arr(cols, dtype=F32):
        return jax.ShapeDtypeStruct((tokens, cols), dtype)

    mixed, pre_gate, pre_value, conv_value, pre_shared, conv_shared, y_scan, states, rows = pl.pallas_call(
        functools.partial(forward_kernel, steps_per_seq, width),
        grid=(grid,),
        in_specs=[
            blk(half),
            blk(half),
            whole((8, half)),
            whole((half, wide)),
            whole((half, wide)),
            whole((8, chan)),
            whole((8, 256)),
            whole((16, 128)),
        ],
        out_specs=[
            blk(chan),
            blk(chan),
            blk(chan),
            blk(chan),
            blk(256),
            blk(256),
            blk(chan),
            blk(chan),
            pl.BlockSpec((24, STEP), lambda i: (0, i)),
        ],
        out_shape=[
            arr(chan, BF16),
            arr(chan),
            arr(chan),
            arr(chan),
            arr(256),
            arr(256),
            arr(chan),
            arr(chan, BF16),
            jax.ShapeDtypeStruct((24, tokens), F32),
        ],
        scratch_shapes=[
            pltpu.VMEM((128, chan), F32),
            pltpu.VMEM((STEP + 8, chan), F32),
            pltpu.VMEM((STEP + 8, 256), F32),
        ],
        name="forward_core",
    )(hidden, hid_rec, gains, w_own, w_rec, vtap, stap, head_par)

    mixed_rec = swap(mixed, "row")
    own32 = mixed.astype(F32)
    rec32 = mixed_rec.astype(F32)
    weighted = (own32 * gain_f).astype(BF16)
    weighted_rec = (rec32 * gated_rec).astype(BF16)
    proj_part = dot(weighted, wo_own) + dot(weighted_rec, wo_part)
    hidden32 = hidden.astype(F32)
    cot32 = cotangent.astype(F32)
    sums = jnp.stack([jnp.sum(own32 * own32, axis=1), jnp.sum(cot32 * proj_part, axis=1)])
    sums = sums + swap(sums, "row")
    sums = sums + swap(sums, "col")
    proj_bf = proj_part.astype(BF16)
    proj = proj_bf.astype(F32) + swap(proj_bf, "col").astype(F32)
    scale = lax.rsqrt(sums[0] / inner_width + EPSILON)
    result = (hidden32 + scale[:, None] * proj).astype(BF16)
    scaled_cot = (scale[:, None] * cot32).astype(BF16)
    g_out_own = dot_tn(weighted, scaled_cot)
    g_out_rec = dot_tn(weighted_rec, scaled_cot)
    trow = jnp.concatenate(
        [scale[None], (sums[1] * scale**3 / inner_width)[None], jnp.zeros((6, tokens), F32)], axis=0
    )

    lane_head = jnp.arange(chan) // (chan // heads)
    sel = (jnp.arange(16)[:, None] == lane_head[None, :]).astype(BF16)
    last = grid - 1

    def rblk(cols):
        return pl.BlockSpec((STEP, cols), lambda i: (last - i, 0))

    def rrow(count):
        return pl.BlockSpec((count, STEP), lambda i: (0, last - i))

    p_all, dn_own, dn_rec, rsum, acc_v, acc_s, acc_h = pl.pallas_call(
        functools.partial(backward_kernel, steps_per_seq),
        grid=(grid,),
        in_specs=[
            rblk(half),
            rblk(half),
            whole((chan, half)),
            whole((chan, half)),
            rrow(8),
            rrow(24),
            rblk(chan),
            rblk(chan),
            rblk(chan),
            rblk(chan),
            rblk(256),
            rblk(256),
            rblk(chan),
            rblk(chan),
            whole((half, wide)),
            whole((half, wide)),
            whole((8, chan)),
            whole((8, 256)),
            whole((16, 128)),
            whole((16, chan)),
        ],
        out_specs=[
            rblk(wide),
            rblk(half),
            rblk(half),
            rrow(8),
            whole((56, chan)),
            whole((40, 256)),
            whole((16, 128)),
        ],
        out_shape=[
            arr(wide, BF16),
            arr(half, BF16),
            arr(half, BF16),
            jax.ShapeDtypeStruct((8, tokens), F32),
            jax.ShapeDtypeStruct((56, chan), F32),
            jax.ShapeDtypeStruct((40, 256), F32),
            jax.ShapeDtypeStruct((16, 128), F32),
        ],
        scratch_shapes=[
            pltpu.VMEM((128, chan), F32),
            pltpu.VMEM((STEP + 8, chan), F32),
            pltpu.VMEM((STEP + 8, 256), F32),
            pltpu.VMEM((STEP, chan), F32),
            pltpu.VMEM((STEP, 256), F32),
        ],
        name="backward_core",
    )(
        cotangent,
        cot_rec,
        wo_own,
        wo_rec,
        trow,
        rows,
        mixed,
        pre_gate,
        pre_value,
        conv_value,
        pre_shared,
        conv_shared,
        y_scan,
        states,
        w_own,
        w_rec,
        vtap,
        stap,
        head_par,
        sel,
    )

    rs = rsum[0]
    rs = rs + swap(rs, "row")
    rs = rs + swap(rs, "col")
    dn_sum = (dn_own.astype(F32) + swap(dn_rec, "row").astype(F32)).astype(BF16)
    d_normed = dn_sum.astype(F32) + swap(dn_sum, "col").astype(F32)
    recip = rows[16]
    hidden_grad = (
        cot32 + d_normed * input_gain - (rs * recip * recip / width)[:, None] * hidden32
    )
    g_norm = jnp.sum(d_normed * hidden32, axis=0)

    normed = (hidden32 * input_gain).astype(BF16)
    normed_rec = (hid_rec.astype(F32) * gains[1]).astype(BF16)
    g_own = dot_tn(normed, p_all)
    g_other = swap(dot_tn(normed_rec, p_all), "row")

    def arrange(mine, theirs, axis):
        first = jnp.where(r == 0, mine, theirs)
        second = jnp.where(r == 0, theirs, mine)
        return jnp.concatenate([first, second], axis=axis)

    g_gate = arrange(g_own[:, 0:chan], g_other[:, 0:chan], 1)
    g_value = arrange(g_own[:, chan : 2 * chan], g_other[:, chan : 2 * chan], 1)
    g_state = g_own[:, 2 * chan : 2 * chan + 256] + g_other[:, 2 * chan : 2 * chan + 256]
    s0 = 2 * chan + 256
    g_step = arrange(g_own[:, s0 : s0 + heads], g_other[:, s0 : s0 + heads], 1)
    g_output = arrange(g_out_own, g_out_rec, 0)

    vsum = jnp.sum(acc_v.reshape(7, 8, chan), axis=1)
    ssum = jnp.sum(acc_s.reshape(5, 8, 256), axis=1)
    hsum = jnp.sum(acc_h.reshape(2, 8, 128), axis=2)[:, 0:heads]
    g_skip = jnp.sum(vsum[5].reshape(heads, chan // heads), axis=1)
    shared_all = jnp.concatenate([g_state, jnp.pad(ssum, ((0, 3), (0, 0)))], axis=0)
    shared_all = shared_all + swap(shared_all, "col")
    g_state = shared_all[0:half]
    s_part = shared_all[half : half + 5]
    s_part = s_part + swap(s_part, "row")
    reduced = lax.psum(
        (
            g_gate,
            g_value,
            g_step,
            g_state,
            vsum[0:4],
            vsum[4],
            s_part[0:4],
            s_part[4],
            hsum[0],
            hsum[1],
            g_skip,
            g_norm,
            vsum[6],
            g_output,
        ),
        "dp",
    )
    return (result, hidden_grad) + tuple(reduced)


def solution(mesh):
    in_specs = (
        P("dp", "row"),
        P("row", "col"),
        P("row", "col"),
        P("row", "col"),
        P("row", None),
        P(None, ("col", "row")),
        P(("col", "row")),
        P(),
        P(),
        P(("col", "row")),
        P(("col", "row")),
        P(("col", "row")),
        P("row"),
        P(("col", "row")),
        P("col", "row"),
        P("dp", "row"),
    )
    out_specs = (
        P("dp", "row"),
        P("dp", "row"),
        P("row", "col"),
        P("row", "col"),
        P("row", "col"),
        P("row", None),
        P(None, ("col", "row")),
        P(("col", "row")),
        P(),
        P(),
        P(("col", "row")),
        P(("col", "row")),
        P(("col", "row")),
        P("row"),
        P(("col", "row")),
        P("col", "row"),
    )
    return jax.shard_map(body, mesh=mesh, in_specs=in_specs, out_specs=out_specs, check_vma=False)
```

```python
import functools

import jax
import jax.numpy as jnp
from jax import lax
from jax.experimental import pallas as pl
from jax.experimental.pallas import tpu as pltpu
from jax.sharding import PartitionSpec as P

LEN = 2048
EPSILON = 1e-05
SUB = 128
STEP = 256
F32 = jnp.float32
BF16 = jnp.bfloat16
SWAP = [(0, 1), (1, 0)]
DN_PARTS = 4


def dot(a, b):
    return jnp.dot(a, b, preferred_element_type=F32)


def dot_nt(a, b):
    return lax.dot_general(a, b, (((1,), (1,)), ((), ())), preferred_element_type=F32)


def dot_tn(a, b):
    return lax.dot_general(a, b, (((0,), (0,)), ((), ())), preferred_element_type=F32)


def sigmoid(x):
    return 0.5 * jnp.tanh(0.5 * x) + 0.5


def softplus(x):
    return jnp.maximum(x, 0.0) + jnp.log1p(jnp.exp(-jnp.abs(x)))


def fold8(x):
    return jnp.sum(x.reshape(x.shape[0] // 8, 8, x.shape[1]), axis=0)


def row_scan(x, mat):
    hi = x.astype(BF16).astype(F32)
    rest = x - hi
    mid = rest.astype(BF16).astype(F32)
    low = rest - mid
    parts = jnp.concatenate([hi, mid, low, jnp.zeros_like(x)], axis=0).astype(BF16)
    out = dot(parts, mat)
    return out[0:8] + out[8:16] + out[16:24]


def head_sums(sel, z):
    hi = z.astype(BF16)
    low = (z - hi.astype(F32)).astype(BF16)
    return (dot_nt(sel, hi) + dot_nt(sel, low))[0:8]


def iota(shape, dim):
    return lax.broadcasted_iota(jnp.int32, shape, dim)


def spread(cols, first, rows):
    lane = iota((rows, 128), 1)
    return jnp.where(
        lane < 64,
        jnp.broadcast_to(cols[:, first : first + 1], (rows, 128)),
        jnp.broadcast_to(cols[:, first + 1 : first + 2], (rows, 128)),
    )


def pair_stack(x):
    lane = iota(x.shape, 1)
    zero = jnp.zeros_like(x)
    return jnp.concatenate([jnp.where(lane < 64, x, zero), jnp.where(lane < 64, zero, x)], axis=0)


def forward_kernel(
    steps_per_seq,
    width,
    hid_own,
    hid_rec,
    gains,
    w_own,
    w_rec,
    vtap,
    stap,
    head_par,
    mixed_out,
    pre_gate_out,
    pre_value_out,
    conv_value_out,
    pre_shared_out,
    conv_shared_out,
    y_out,
    state_out,
    rows_out,
    nt_out,
    state,
    vbuf,
    sbuf,
):
    chan = mixed_out.shape[1]
    pairs = chan // 128

    @pl.when(pl.program_id(0) % steps_per_seq == 0)
    def _():
        state[...] = jnp.zeros_like(state)
        vbuf[0:8, :] = jnp.zeros((8, vbuf.shape[1]), F32)
        sbuf[0:8, :] = jnp.zeros((8, sbuf.shape[1]), F32)

    h0 = hid_own[...].astype(F32)
    h1 = hid_rec[...].astype(F32)
    square = jnp.sum(h0 * h0, axis=1, keepdims=True) + jnp.sum(h1 * h1, axis=1, keepdims=True)
    recip = lax.rsqrt(square / width + EPSILON)
    n0 = (h0 * gains[0:1, :]).astype(BF16)
    n1 = (h1 * gains[1:2, :]).astype(BF16)
    half = n0.shape[1]
    nt_out[0:half, :] = jnp.transpose(n0)
    nt_out[half : 2 * half, :] = jnp.transpose(n1)
    q = dot(n0, w_own[...]) + dot(n1, w_rec[...])
    pre = q * recip
    gate = pre[:, 0:chan]
    pre_gate_out[...] = gate
    pre_value = pre[:, chan : 2 * chan]
    pre_value_out[...] = pre_value
    pre_shared = pre[:, 2 * chan : 2 * chan + 256]
    pre_shared_out[...] = pre_shared
    vbuf[8 : 8 + STEP, :] = pre_value
    sbuf[8 : 8 + STEP, :] = pre_shared
    conv = jnp.broadcast_to(vtap[4:5, :], (STEP, chan))
    conv_s = jnp.broadcast_to(stap[4:5, :], (STEP, 256))
    for k in range(4):
        conv = conv + vbuf[5 + k : 5 + k + STEP, :] * vtap[k : k + 1, :]
        conv_s = conv_s + sbuf[5 + k : 5 + k + STEP, :] * stap[k : k + 1, :]
    vbuf[0:8, :] = vbuf[STEP : STEP + 8, :]
    sbuf[0:8, :] = sbuf[STEP : STEP + 8, :]
    conv_value_out[...] = conv
    conv_shared_out[...] = conv_s
    x = conv * sigmoid(conv)
    act = conv_s * sigmoid(conv_s)

    head_rows = jnp.transpose(pre[:, 2 * chan + 256 : 2 * chan + 384])[0:8]
    v = head_rows + head_par[0:8, 0:1]
    steps = softplus(v)
    logd = head_par[8:16, 0:1] * steps
    rows_out[0:8, :] = v
    rows_out[16:24, :] = jnp.transpose(jnp.broadcast_to(recip, (STEP, 128)))[0:8]

    upper = (iota((SUB, SUB), 0) <= iota((SUB, SUB), 1)).astype(F32).astype(BF16)
    causal = iota((SUB, SUB), 0) >= iota((SUB, SUB), 1)
    sg = gate * sigmoid(gate)
    for sub in range(STEP // SUB):
        lo, hi = sub * SUB, (sub + 1) * SUB
        cum_r = row_scan(logd[:, lo:hi], upper)
        rows_out[8:16, lo:hi] = cum_r
        cols = jnp.transpose(jnp.concatenate([cum_r, steps[:, lo:hi]], axis=0))
        b_in = act[lo:hi, 0:128]
        b_bf = b_in.astype(BF16)
        c_bf = act[lo:hi, 128:256].astype(BF16)
        b_t = jnp.transpose(b_in).astype(BF16)
        scores = dot_nt(c_bf, b_bf)
        for p in range(pairs):
            pl0, pl1 = p * 128, (p + 1) * 128
            c0 = jnp.broadcast_to(cols[:, 2 * p : 2 * p + 1], (SUB, 128))
            c1 = jnp.broadcast_to(cols[:, 2 * p + 1 : 2 * p + 2], (SUB, 128))
            weights = []
            for col, h in ((c0, 2 * p), (c1, 2 * p + 1)):
                gap = jnp.where(causal, col - cum_r[h : h + 1, :], -1e30)
                weights.append((scores * jnp.exp(gap)).astype(BF16))
            lane = iota((SUB, 128), 1)
            cum_e = jnp.where(lane < 64, c0, c1)
            step_e = spread(cols, 8 + 2 * p, SUB)
            xs = x[lo:hi, pl0:pl1]
            xh = step_e * xs
            inside = dot(jnp.concatenate(weights, axis=1), pair_stack(xh.astype(BF16)))
            held = state[:, pl0:pl1]
            held_bf = held.astype(BF16)
            state_out[lo:hi, pl0:pl1] = held_bf
            carried = dot(c_bf, held_bf)
            y = inside + carried * jnp.exp(cum_e)
            y_out[lo:hi, pl0:pl1] = y
            last = cum_e[SUB - 1 : SUB, :]
            tail = (xh * jnp.exp(last - cum_e)).astype(BF16)
            state[:, pl0:pl1] = held * jnp.exp(last) + dot(b_t, tail)
            y = y + vtap[5:6, pl0:pl1] * xs
            mixed_out[lo:hi, pl0:pl1] = (y * sg[lo:hi, pl0:pl1]).astype(BF16)


def backward_kernel(
    steps_per_seq,
    cot_own,
    cot_rec,
    wo_own,
    wo_rec,
    trow,
    rows_in,
    mixed,
    pre_gate,
    pre_value,
    conv_value,
    pre_shared,
    conv_shared,
    y_in,
    state_in,
    w_own,
    w_rec,
    vtap,
    stap,
    head_par,
    sel_ref,
    p_out,
    dn_own,
    dn_rec,
    rsum_out,
    acc_v,
    acc_s,
    acc_h,
    grad,
    vbuf,
    sbuf,
    dxbuf,
    dbbuf,
):
    chan = mixed.shape[1]
    pairs = chan // 128

    @pl.when(pl.program_id(0) == 0)
    def _():
        acc_v[...] = jnp.zeros_like(acc_v)
        acc_s[...] = jnp.zeros_like(acc_s)
        acc_h[...] = jnp.zeros_like(acc_h)

    @pl.when(pl.program_id(0) % steps_per_seq == 0)
    def _():
        grad[...] = jnp.zeros_like(grad)
        vbuf[STEP : STEP + 8, :] = jnp.zeros((8, vbuf.shape[1]), F32)
        sbuf[STEP : STEP + 8, :] = jnp.zeros((8, sbuf.shape[1]), F32)

    tcol = jnp.transpose(jnp.concatenate([trow[...], rows_in[16:24, :]], axis=0))
    scale = tcol[:, 0:1]
    coef = tcol[:, 1:2]
    recip = tcol[:, 8:9]
    s0 = (cot_own[...].astype(F32) * scale).astype(BF16)
    s1 = (cot_rec[...].astype(F32) * scale).astype(BF16)
    d_weighted = dot_nt(s0, wo_own[...]) + dot_nt(s1, wo_rec[...])
    mix = mixed[...].astype(F32)
    acc_v[48:56, :] += fold8(d_weighted * mix)
    d_mixed = d_weighted * vtap[6:7, :] - coef * mix
    gate = pre_gate[...]
    sig = sigmoid(gate)
    silu = gate * sig
    conv = conv_value[...]
    sig_v = sigmoid(conv)
    x = conv * sig_v
    y_scan = y_in[...]
    y = y_scan + vtap[5:6, :] * x
    dy = d_mixed * silu
    d_gate = d_mixed * y * (sig + silu * (1.0 - sig))
    acc_v[40:48, :] += fold8(dy * x)
    conv_s = conv_shared[...]
    sig_s = sigmoid(conv_s)
    act = conv_s * sig_s

    sel = sel_ref[...]
    sel_f = sel.astype(F32)[0:8]
    v = rows_in[0:8, :]
    steps = softplus(v)
    logd = head_par[8:16, 0:1] * steps
    lower = (iota((SUB, SUB), 0) >= iota((SUB, SUB), 1)).astype(F32).astype(BF16)
    strict = (iota((SUB, SUB), 0) < iota((SUB, SUB), 1)).astype(F32).astype(BF16)
    causal_t = iota((SUB, SUB), 0) <= iota((SUB, SUB), 1)
    for sub in reversed(range(STEP // SUB)):
        lo, hi = sub * SUB, (sub + 1) * SUB
        cum_r = rows_in[8:16, lo:hi]
        cols = jnp.transpose(jnp.concatenate([cum_r, steps[:, lo:hi]], axis=0))
        b_bf = act[lo:hi, 0:128].astype(BF16)
        c_in = act[lo:hi, 128:256]
        c_bf = c_in.astype(BF16)
        c_t = jnp.transpose(c_in).astype(BF16)
        scores_t = dot_nt(b_bf, c_bf)
        d_scores = jnp.zeros((SUB, SUB), F32)
        db = jnp.zeros((SUB, 128), F32)
        dc = jnp.zeros((SUB, 128), F32)
        z_sum = jnp.zeros((8, SUB), F32)
        e_sum = jnp.zeros((8, SUB), F32)
        f_sum = jnp.zeros((8, SUB), F32)
        gh = jnp.zeros((8, 1), F32)
        for p in range(pairs):
            pl0, pl1 = p * 128, (p + 1) * 128
            c0 = jnp.broadcast_to(cols[:, 2 * p : 2 * p + 1], (SUB, 128))
            c1 = jnp.broadcast_to(cols[:, 2 * p + 1 : 2 * p + 2], (SUB, 128))
            decays = []
            for col, h in ((c0, 2 * p), (c1, 2 * p + 1)):
                gap = jnp.where(causal_t, cum_r[h : h + 1, :] - col, -1e30)
                decays.append(jnp.exp(gap))
            weights = [(scores_t * d).astype(BF16) for d in decays]
            lane = iota((SUB, 128), 1)
            cum_e = jnp.where(lane < 64, c0, c1)
            step_e = spread(cols, 8 + 2 * p, SUB)
            xs = x[lo:hi, pl0:pl1]
            xh = step_e * xs
            xh_bf = xh.astype(BF16)
            dys = dy[lo:hi, pl0:pl1]
            dys_bf = dys.astype(BF16)
            stack = pair_stack(dys_bf)
            inner = dot(jnp.concatenate(weights, axis=1), stack)
            d_pair = dot_nt(xh_bf, stack)
            d_scores = d_scores + decays[0] * d_pair[:, 0:128] + decays[1] * d_pair[:, 128:256]
            last = cum_e[SUB - 1 : SUB, :]
            tail_e = jnp.exp(last - cum_e)
            g = grad[:, pl0:pl1]
            g_bf = g.astype(BF16)
            outer = dot(b_bf, g_bf) * tail_e
            u = inner + outer
            dxbuf[lo:hi, pl0:pl1] = step_e * u + vtap[5:6, pl0:pl1] * dys
            db = db + dot_nt((xh * tail_e).astype(BF16), g_bf)
            dya = (dys * jnp.exp(cum_e)).astype(BF16)
            held = state_in[lo:hi, pl0:pl1]
            dc = dc + dot_nt(dya, held)
            sel_p = sel[:, pl0:pl1]
            z_sum = z_sum + head_sums(
                sel_p, dys_bf.astype(F32) * y_in[lo:hi, pl0:pl1] - xh_bf.astype(F32) * inner
            )
            e_sum = e_sum + head_sums(sel_p, xh * outer)
            f_sum = f_sum + head_sums(sel_p, xs * u)
            decay_row = jnp.exp(last)
            gh_row = decay_row * jnp.sum(g * held.astype(F32), axis=0, keepdims=True)
            gh = gh + jnp.sum(sel_f[:, pl0:pl1] * gh_row, axis=1, keepdims=True)
            grad[:, pl0:pl1] = g * decay_row + dot(c_t, dya)
        ds_bf = d_scores.astype(BF16)
        dbbuf[lo:hi, 0:128] = db + dot(ds_bf, c_bf)
        dbbuf[lo:hi, 128:256] = dc + dot(jnp.transpose(d_scores).astype(BF16), b_bf)
        d_log = row_scan(z_sum, lower) + row_scan(e_sum, strict) + gh
        d_step = (f_sum + d_log * head_par[8:16, 0:1]) * sigmoid(v[:, lo:hi])
        acc_h[0:8, :] += d_log * logd[:, lo:hi]
        acc_h[8:16, :] += d_step
        pre_step = v[:, lo:hi] - head_par[0:8, 0:1]
        rsum_out[:, lo:hi] = jnp.broadcast_to(
            jnp.sum(d_step * pre_step, axis=0, keepdims=True), (8, SUB)
        )
        d_cols = jnp.transpose(jnp.concatenate([d_step, jnp.zeros((120, SUB), F32)], axis=0))
        p_out[lo:hi, 2 * chan + 256 : 2 * chan + 384] = (recip[lo:hi] * d_cols).astype(BF16)

    d_conv = dxbuf[...] * (sig_v + x * (1.0 - sig_v))
    d_conv_s = dbbuf[...] * (sig_s + act * (1.0 - sig_s))
    vbuf[0:STEP, :] = d_conv
    sbuf[0:STEP, :] = d_conv_s
    acc_v[32:40, :] += fold8(d_conv)
    acc_s[32:40, :] += fold8(d_conv_s)
    pv = pre_value[...]
    ps = pre_shared[...]
    d_value = jnp.zeros((STEP, chan), F32)
    d_shared = jnp.zeros((STEP, 256), F32)
    for k in range(4):
        moved = vbuf[3 - k : 3 - k + STEP, :]
        d_value = d_value + vtap[k : k + 1, :] * moved
        acc_v[8 * k : 8 * k + 8, :] += fold8(pv * moved)
        moved = sbuf[3 - k : 3 - k + STEP, :]
        d_shared = d_shared + stap[k : k + 1, :] * moved
        acc_s[8 * k : 8 * k + 8, :] += fold8(ps * moved)
    vbuf[STEP : STEP + 8, :] = vbuf[0:8, :]
    sbuf[STEP : STEP + 8, :] = sbuf[0:8, :]
    p_out[:, 0:chan] = (recip * d_gate).astype(BF16)
    p_out[:, chan : 2 * chan] = (recip * d_value).astype(BF16)
    p_out[:, 2 * chan : 2 * chan + 256] = (recip * d_shared).astype(BF16)
    ones = jnp.ones((16, chan), BF16)
    rsum_out[...] += head_sums(ones, d_gate * gate + d_value * pv)
    rsum_out[...] += head_sums(ones[:, 0:256], d_shared * ps)
    pb = p_out[...]
    dn_own[...] = dot_nt(pb, w_own[...]).astype(BF16)
    dn_rec[...] = dot_nt(pb, w_rec[...]).astype(BF16)


def unit_rows(dp):
    return 16 * dp


def big_rows(dp, rows):
    return pl.cdiv(rows, unit_rows(dp)) * unit_rows(dp)


def sum_kernel(
    dp,
    g_cat,
    g_out,
    small_row,
    small_own,
    rs_in,
    hid,
    dn_own,
    dn_rec,
    out,
    dn_sum,
    dn_col,
    rs_out,
    acc,
    stage,
    land,
    row_send,
    row_land,
    col_send,
    col_land,
    dn_land,
    rs_land,
    norm,
    send_sem,
    recv_sem,
    pair_send,
    pair_recv,
    dn_send_sem,
    dn_recv_sem,
):
    half = g_cat.shape[0] // 2
    chan = g_out.shape[1]
    wide = g_cat.shape[1]
    size = big_rows(dp, 2 * half)
    tail = out.shape[0] - 3 * size
    bits = dp.bit_length() - 1
    me = lax.axis_index("dp")
    r = lax.axis_index("row")
    c = lax.axis_index("col")

    def bit_of(k):
        return lax.rem(me // (1 << k), 2)

    def partner(k):
        return {"dp": me + (1 - 2 * bit_of(k)) * (1 << k)}

    barrier = pltpu.get_barrier_semaphore()
    for target in [partner(k) for k in range(bits)] + [{"row": 1 - r}, {"col": 1 - c}]:
        pl.semaphore_signal(barrier, inc=1, device_id=target, device_id_type=pl.DeviceIdType.MESH)
    pl.semaphore_wait(barrier, bits + 2)

    other = pl.multiple_of((1 - r) * half, 128)
    mine = pl.multiple_of(r * half, 128)
    to_row, to_col = {"row": 1 - r}, {"col": 1 - c}

    def pair_copy(src, dst, send, recv, target):
        return pltpu.make_async_remote_copy(
            src_ref=src,
            dst_ref=dst,
            send_sem=send,
            recv_sem=recv,
            device_id=target,
            device_id_type=pl.DeviceIdType.MESH,
        )

    tokens = hid.shape[0]
    cut = tokens // DN_PARTS

    def dn_copy(i, side):
        rows = pl.ds(i * cut, cut)
        if side == 0:
            src, dst, target = dn_rec, dn_land, to_row
        else:
            src, dst, target = dn_sum, dn_col, to_col
        return pair_copy(src.at[rows, :], dst.at[rows, :], dn_send_sem.at[side, i], dn_recv_sem.at[side, i], target)

    dn_rows = [dn_copy(i, 0) for i in range(DN_PARTS)]
    dn_cols = [dn_copy(i, 1) for i in range(DN_PARTS)]
    rs_row = pair_copy(rs_in, rs_land.at[0], pair_send.at[2], pair_recv.at[2], to_row)
    rs_col = pair_copy(rs_out, rs_land.at[1], pair_send.at[3], pair_recv.at[3], to_col)
    for copy in dn_rows:
        copy.start()
    rs_row.start()
    row_send[0:half, :] = g_cat[half : 2 * half, :].astype(BF16)
    row_send[half : half + 16, 0:256] = small_row[...].astype(BF16)
    row_send[half : half + 16, 256:wide] = jnp.zeros((16, wide - 256), BF16)
    row_copy = pair_copy(row_send, row_land, pair_send.at[0], pair_recv.at[0], to_row)
    row_copy.start()

    chunks = [
        (0, size, tuple(range(bits))),
        (size, size, tuple(range(1, bits)) + (0,)),
        (2 * size, size, tuple(range(bits))),
        (3 * size, tail, tuple(range(bits))),
    ]
    lows = {}

    def copy_of(i, level, src, rows, dst, dst_rows, k):
        return pltpu.make_async_remote_copy(
            src_ref=src.at[rows, :],
            dst_ref=dst.at[dst_rows, :],
            send_sem=send_sem.at[i, level],
            recv_sem=recv_sem.at[i, level],
            device_id=partner(k),
            device_id_type=pl.DeviceIdType.MESH,
        )

    flying = {}

    def span(start, rows):
        return pl.ds(pl.multiple_of(start, 16), rows)

    def start_level(i, level):
        base, rows, order = chunks[i]
        if level < bits:
            k = order[level]
            low = lows.get(i, base)
            part = rows >> (level + 1)
            keep = low + bit_of(k) * part
            give = low + (1 - bit_of(k)) * part
            stage[span(give, part), :] = acc[span(give, part), :].astype(BF16)
            where = base + rows - (rows >> level)
            copy = copy_of(i, level, stage, span(give, part), land, span(where, part), k)
            lows[i] = keep
            flying[i] = (copy, keep, where, part)
        else:
            back = 2 * bits - 1 - level
            k = order[back]
            part = rows >> (back + 1)
            low = lows[i]
            copy = copy_of(i, level, out, span(low, part), out, span(low, part), k)
            lows[i] = low - bit_of(k) * part
            flying[i] = (copy, low, None, part)
        copy.start()

    def end_level(i, level):
        copy, low, where, part = flying[i]
        copy.wait()
        if level < bits:
            total = acc[span(low, part), :] + land[span(where, part), :].astype(F32)
            acc[span(low, part), :] = total
            if level == bits - 1:
                out[span(low, part), :] = total.astype(BF16)

    acc[span(r * chan, chan), :] = g_out[0:chan, :]
    acc[span((1 - r) * chan, chan), :] = g_out[chan : 2 * chan, :]
    if size > 2 * chan:
        acc[2 * chan : size, :] = jnp.zeros((size - 2 * chan, chan), F32)
    start_level(0, 0)
    norm[...] = jnp.zeros_like(norm)
    for i in range(DN_PARTS):
        rows = slice(i * cut, (i + 1) * cut)
        dn_rows[i].wait()
        part = (dn_own[rows, :].astype(F32) + dn_land[rows, :].astype(F32)).astype(BF16)
        dn_sum[rows, :] = part
        dn_cols[i].start()
        norm[...] += fold8(part.astype(F32) * hid[rows, :].astype(F32))
    row_copy.wait()
    for i in (1, 2):
        lo = (i - 1) * chan
        acc[span(i * size + mine, half), :] = g_cat[0:half, lo : lo + chan]
        acc[span(i * size + other, half), :] = row_land[0:half, lo : lo + chan].astype(F32)
        if size > 2 * half:
            acc[i * size + 2 * half : (i + 1) * size, :] = jnp.zeros((size - 2 * half, chan), F32)
        if i == 1:
            start_level(1, 0)
    misc = 3 * size
    lo = 2 * chan
    state = g_cat[0:half, lo : lo + 256] + row_land[0:half, lo : lo + 256].astype(F32)
    norm_row = jnp.sum(norm[...], axis=0, keepdims=True)
    norm_rows = jnp.concatenate(
        [norm_row[:, 0:256], norm_row[:, 256:half], jnp.zeros((1, 512 - half), F32)], axis=1
    )
    extra = small_row[...] + row_land[half : half + 16, 0:256].astype(F32)
    extra = jnp.concatenate([extra[0:8], norm_rows[:, 0:256], norm_rows[:, 256:512], jnp.zeros((6, 256), F32)])
    acc[misc : misc + half, 0:256] = state
    acc[misc + half : misc + half + 16, 0:256] = extra
    col_send[0:half, :] = state.astype(BF16)
    col_send[half : half + 16, :] = extra.astype(BF16)
    col_copy = pair_copy(col_send, col_land, pair_send.at[1], pair_recv.at[1], to_col)
    col_copy.start()
    start_level(2, 0)
    lo = 2 * chan + 256
    acc[misc : misc + half, 256:384] = jnp.concatenate(
        [g_cat[0:half, lo : lo + 64], row_land[0:half, lo : lo + 64].astype(F32)], axis=1
    )
    acc[misc + half : misc + half + 16, 256:384] = jnp.zeros((16, 128), F32)
    acc[misc + half + 16 : misc + half + 32, :] = small_own[...]
    if tail > half + 32:
        acc[misc + half + 32 : misc + tail, :] = jnp.zeros((tail - half - 32, chan), F32)
    rs_row.wait()
    rs_out[...] = rs_in[...] + rs_land[0]
    rs_col.start()
    for i in (0, 1):
        end_level(i, 0)
        start_level(i, 1)
    col_copy.wait()
    acc[misc : misc + half + 16, 0:256] = (
        col_send[...].astype(F32) + col_land[...].astype(F32)
    )
    start_level(3, 0)
    end_level(2, 0)
    start_level(2, 1)
    for level in range(1, 2 * bits):
        for i in (0, 1):
            end_level(i, level)
            if level + 1 < 2 * bits:
                start_level(i, level + 1)
        end_level(3, level - 1)
        start_level(3, level)
        end_level(2, level)
        if level + 1 < 2 * bits:
            start_level(2, level + 1)
    end_level(3, 2 * bits - 1)
    rs_col.wait()
    for copy in dn_cols:
        copy.wait()
    rs_out[...] = rs_out[...] + rs_land[1]


def sum_over_dp(dp, g_cat, g_out, small_row, small_own, rs, hid, dn_own, dn_rec):
    half = g_cat.shape[0] // 2
    wide = g_cat.shape[1]
    chan = g_out.shape[1]
    rows = 3 * big_rows(dp, 2 * half) + big_rows(dp, half + 32)
    bits = dp.bit_length() - 1
    tokens = hid.shape[0]
    vmem = pl.BlockSpec(memory_space=pltpu.VMEM)
    hbm = pl.BlockSpec(memory_space=pl.ANY)
    act = jax.ShapeDtypeStruct((tokens, half), BF16)
    return pl.pallas_call(
        functools.partial(sum_kernel, dp),
        in_specs=[vmem] * 7 + [hbm],
        out_specs=[vmem, vmem, hbm, vmem],
        out_shape=[jax.ShapeDtypeStruct((rows, chan), BF16), act, act, jax.ShapeDtypeStruct(rs.shape, F32)],
        scratch_shapes=[
            pltpu.VMEM((rows, chan), F32),
            pltpu.VMEM((rows, chan), BF16),
            pltpu.VMEM((rows, chan), BF16),
            pltpu.VMEM((half + 16, wide), BF16),
            pltpu.VMEM((half + 16, wide), BF16),
            pltpu.VMEM((half + 16, 256), BF16),
            pltpu.VMEM((half + 16, 256), BF16),
            pltpu.VMEM((tokens, half), BF16),
            pltpu.VMEM((2,) + rs.shape, F32),
            pltpu.VMEM((8, half), F32),
            pltpu.SemaphoreType.DMA((4, 2 * bits)),
            pltpu.SemaphoreType.DMA((4, 2 * bits)),
            pltpu.SemaphoreType.DMA((4,)),
            pltpu.SemaphoreType.DMA((4,)),
            pltpu.SemaphoreType.DMA((2, DN_PARTS)),
            pltpu.SemaphoreType.DMA((2, DN_PARTS)),
        ],
        compiler_params=pltpu.CompilerParams(collective_id=0, has_side_effects=True),
        cost_estimate=pl.CostEstimate(flops=1_000_000, bytes_accessed=150_000_000, transcendentals=0),
        name="sum_over_dp",
    )(g_cat, g_out, small_row, small_own, rs, hid, dn_own, dn_rec)


def swap(x, axis):
    return lax.ppermute(x, axis, SWAP)


def body(
    hidden,
    gate_proj,
    value_proj,
    step_proj,
    state_proj,
    value_filter,
    value_shift,
    shared_kernel,
    shared_offset,
    decay_log,
    step_bias,
    skip_gain,
    input_gain,
    gated_gain,
    output_proj,
    cotangent,
):
    tokens, half = hidden.shape
    width = 2 * half
    chan = gated_gain.shape[0]
    inner_width = 4 * chan
    heads = decay_log.shape[0]
    r = lax.axis_index("row")
    dp = lax.axis_size("dp")
    seq_len = min(LEN, tokens)
    steps_per_seq = seq_len // STEP
    grid = tokens // STEP

    def cut(x, start, size, axis):
        return lax.dynamic_slice_in_dim(x, start * size, size, axis)

    def packed(side):
        return jnp.concatenate(
            [
                cut(gate_proj, side, chan, 1),
                cut(value_proj, side, chan, 1),
                state_proj,
                jnp.pad(cut(step_proj, side, heads, 1), ((0, 0), (0, 128 - heads))),
            ],
            axis=1,
        )

    w_own = packed(r)
    w_rec = swap(packed(1 - r), "row")
    hid_rec = swap(hidden, "row")
    cot_rec = swap(cotangent, "row")
    wo_own = cut(output_proj, r, chan, 0)
    wo_part = cut(output_proj, 1 - r, chan, 0)
    wo_rec = swap(wo_part, "row")
    gain_f = gated_gain.astype(F32)
    two = swap(jnp.stack([input_gain, gain_f]), "row")
    gains = jnp.concatenate([input_gain[None], two[0:1], jnp.zeros((6, half), F32)], axis=0)
    gated_rec = two[1]

    skip_lane = jnp.repeat(skip_gain, chan // heads)
    vtap = jnp.concatenate(
        [value_filter, value_shift[None], skip_lane[None], gain_f[None], jnp.zeros((1, chan), F32)], axis=0
    )
    stap = jnp.concatenate([shared_kernel, shared_offset[None], jnp.zeros((3, 256), F32)], axis=0)
    pad_h = (0, 8 - heads)
    head_par = jnp.concatenate([jnp.pad(step_bias, pad_h), jnp.pad(-jnp.exp(decay_log), pad_h)])
    head_par = jnp.broadcast_to(head_par[:, None], (16, 128))

    wide = w_own.shape[1]

    def blk(cols):
        return pl.BlockSpec((STEP, cols), lambda i: (i, 0))

    def whole(shape):
        return pl.BlockSpec(shape, lambda i: (0, 0))

    def arr(cols, dtype=F32):
        return jax.ShapeDtypeStruct((tokens, cols), dtype)

    mixed, pre_gate, pre_value, conv_value, pre_shared, conv_shared, y_scan, states, rows, normed_t = pl.pallas_call(
        functools.partial(forward_kernel, steps_per_seq, width),
        grid=(grid,),
        in_specs=[
            blk(half),
            blk(half),
            whole((8, half)),
            whole((half, wide)),
            whole((half, wide)),
            whole((8, chan)),
            whole((8, 256)),
            whole((16, 128)),
        ],
        out_specs=[
            blk(chan),
            blk(chan),
            blk(chan),
            blk(chan),
            blk(256),
            blk(256),
            blk(chan),
            blk(chan),
            pl.BlockSpec((24, STEP), lambda i: (0, i)),
            pl.BlockSpec((width, STEP), lambda i: (0, i)),
        ],
        out_shape=[
            arr(chan, BF16),
            arr(chan),
            arr(chan),
            arr(chan),
            arr(256),
            arr(256),
            arr(chan),
            arr(chan, BF16),
            jax.ShapeDtypeStruct((24, tokens), F32),
            jax.ShapeDtypeStruct((width, tokens), BF16),
        ],
        scratch_shapes=[
            pltpu.VMEM((128, chan), F32),
            pltpu.VMEM((STEP + 8, chan), F32),
            pltpu.VMEM((STEP + 8, 256), F32),
        ],
        cost_estimate=pl.CostEstimate(flops=12_000_000_000, bytes_accessed=40_000_000, transcendentals=8_000_000),
        name="forward_core",
    )(hidden, hid_rec, gains, w_own, w_rec, vtap, stap, head_par)

    mixed_rec = swap(mixed, "row")
    own32 = mixed.astype(F32)
    rec32 = mixed_rec.astype(F32)
    weighted = (own32 * gain_f).astype(BF16)
    weighted_rec = (rec32 * gated_rec).astype(BF16)
    proj_part = dot(weighted, wo_own) + dot(weighted_rec, wo_part)
    hidden32 = hidden.astype(F32)
    cot32 = cotangent.astype(F32)
    sums = jnp.stack([jnp.sum(own32 * own32, axis=1), jnp.sum(cot32 * proj_part, axis=1)])
    sums = sums + swap(sums, "row")
    sums = sums + swap(sums, "col")
    proj_bf = proj_part.astype(BF16)
    proj = proj_bf.astype(F32) + swap(proj_bf, "col").astype(F32)
    scale = lax.rsqrt(sums[0] / inner_width + EPSILON)
    result = (hidden32 + scale[:, None] * proj).astype(BF16)
    scaled_cot = (scale[:, None] * cot32).astype(BF16)
    g_out_own = dot_tn(weighted, scaled_cot)
    g_out_rec = dot_tn(weighted_rec, scaled_cot)
    trow = jnp.concatenate(
        [scale[None], (sums[1] * scale**3 / inner_width)[None], jnp.zeros((6, tokens), F32)], axis=0
    )

    lane_head = jnp.arange(chan) // (chan // heads)
    sel = (jnp.arange(16)[:, None] == lane_head[None, :]).astype(BF16)
    last = grid - 1

    def rblk(cols):
        return pl.BlockSpec((STEP, cols), lambda i: (last - i, 0))

    def rrow(count):
        return pl.BlockSpec((count, STEP), lambda i: (0, last - i))

    p_all, dn_own, dn_rec, rsum, acc_v, acc_s, acc_h = pl.pallas_call(
        functools.partial(backward_kernel, steps_per_seq),
        grid=(grid,),
        in_specs=[
            rblk(half),
            rblk(half),
            whole((chan, half)),
            whole((chan, half)),
            rrow(8),
            rrow(24),
            rblk(chan),
            rblk(chan),
            rblk(chan),
            rblk(chan),
            rblk(256),
            rblk(256),
            rblk(chan),
            rblk(chan),
            whole((half, wide)),
            whole((half, wide)),
            whole((8, chan)),
            whole((8, 256)),
            whole((16, 128)),
            whole((16, chan)),
        ],
        out_specs=[
            rblk(wide),
            rblk(half),
            rblk(half),
            rrow(8),
            whole((56, chan)),
            whole((40, 256)),
            whole((16, 128)),
        ],
        out_shape=[
            arr(wide, BF16),
            arr(half, BF16),
            arr(half, BF16),
            jax.ShapeDtypeStruct((8, tokens), F32),
            jax.ShapeDtypeStruct((56, chan), F32),
            jax.ShapeDtypeStruct((40, 256), F32),
            jax.ShapeDtypeStruct((16, 128), F32),
        ],
        scratch_shapes=[
            pltpu.VMEM((128, chan), F32),
            pltpu.VMEM((STEP + 8, chan), F32),
            pltpu.VMEM((STEP + 8, 256), F32),
            pltpu.VMEM((STEP, chan), F32),
            pltpu.VMEM((STEP, 256), F32),
        ],
        cost_estimate=pl.CostEstimate(flops=24_000_000_000, bytes_accessed=60_000_000, transcendentals=8_000_000),
        name="backward_core",
    )(
        cotangent,
        cot_rec,
        wo_own,
        wo_rec,
        trow,
        rows,
        mixed,
        pre_gate,
        pre_value,
        conv_value,
        pre_shared,
        conv_shared,
        y_scan,
        states,
        w_own,
        w_rec,
        vtap,
        stap,
        head_par,
        sel,
    )

    g_cat = dot(normed_t, p_all)
    vsum = jnp.sum(acc_v.reshape(7, 8, chan), axis=1)
    ssum = jnp.sum(acc_s.reshape(5, 8, 256), axis=1)
    hsum = jnp.sum(acc_h.reshape(2, 8, 128), axis=2)
    small_row = jnp.pad(ssum, ((0, 11), (0, 0)))
    small_own = jnp.concatenate(
        [vsum, jnp.pad(hsum.reshape(1, 16), ((0, 0), (0, chan - 16))), jnp.zeros((8, chan), F32)], axis=0
    )
    g_out = jnp.concatenate([g_out_own, g_out_rec], axis=0)
    out, dn_sum, dn_col, rs = sum_over_dp(
        dp, g_cat, g_out, small_row, small_own, rsum, hidden, dn_own, dn_rec
    )
    size, misc = big_rows(dp, 2 * half), 3 * big_rows(dp, 2 * half)

    def side_by_side(start):
        return jnp.concatenate([out[start : start + half], out[start + half : start + 2 * half]], axis=1).astype(F32)

    g_output = out[0 : 2 * chan].astype(F32)
    g_gate = side_by_side(size)
    g_value = side_by_side(2 * size)
    g_state = out[misc : misc + half, 0:256].astype(F32)
    s_own = out[misc : misc + half, 256 : 256 + heads].astype(F32)
    s_rec = out[misc : misc + half, 320 : 320 + heads].astype(F32)
    g_step = jnp.where(r == 0, jnp.concatenate([s_own, s_rec], axis=1), jnp.concatenate([s_rec, s_own], axis=1))
    small = out[misc + half : misc + half + 32].astype(F32)
    g_norm = small[8:10, 0:256].reshape(512)[0:half]
    d_normed = dn_sum.astype(F32) + dn_col.astype(F32)
    recip = rows[16]
    hidden_grad = (
        cot32 + d_normed * input_gain - (rs[0] * recip * recip / width)[:, None] * hidden32
    )
    return (
        result,
        hidden_grad,
        g_gate,
        g_value,
        g_step,
        g_state,
        small[16:20],
        small[20],
        small[0:4, 0:256],
        small[4, 0:256],
        small[23, 0:heads],
        small[23, 8 : 8 + heads],
        jnp.sum(small[21].reshape(heads, chan // heads), axis=1),
        g_norm,
        small[22],
        g_output,
    )


def solution(mesh):
    in_specs = (
        P("dp", "row"),
        P("row", "col"),
        P("row", "col"),
        P("row", "col"),
        P("row", None),
        P(None, ("col", "row")),
        P(("col", "row")),
        P(),
        P(),
        P(("col", "row")),
        P(("col", "row")),
        P(("col", "row")),
        P("row"),
        P(("col", "row")),
        P("col", "row"),
        P("dp", "row"),
    )
    out_specs = (
        P("dp", "row"),
        P("dp", "row"),
        P("row", "col"),
        P("row", "col"),
        P("row", "col"),
        P("row", None),
        P(None, ("col", "row")),
        P(("col", "row")),
        P(),
        P(),
        P(("col", "row")),
        P(("col", "row")),
        P(("col", "row")),
        P("row"),
        P(("col", "row")),
        P("col", "row"),
    )
    return jax.shard_map(body, mesh=mesh, in_specs=in_specs, out_specs=out_specs, check_vma=False)
```

```python
import functools

import jax
import jax.numpy as jnp
from jax import lax
from jax.experimental import pallas as pl
from jax.experimental.pallas import tpu as pltpu
from jax.sharding import PartitionSpec as P

LEN = 2048
EPSILON = 1e-05
SUB = 128
STEP = 256
F32 = jnp.float32
BF16 = jnp.bfloat16
SWAP = [(0, 1), (1, 0)]
DN_PARTS = 4


def dot(a, b):
    return jnp.dot(a, b, preferred_element_type=F32)


def dot_nt(a, b):
    return lax.dot_general(a, b, (((1,), (1,)), ((), ())), preferred_element_type=F32)


def dot_tn(a, b):
    return lax.dot_general(a, b, (((0,), (0,)), ((), ())), preferred_element_type=F32)


def sigmoid(x):
    return 0.5 * jnp.tanh(0.5 * x) + 0.5


def softplus(x):
    return jnp.maximum(x, 0.0) + jnp.log1p(jnp.exp(-jnp.abs(x)))


def fold8(x):
    return jnp.sum(x.reshape(x.shape[0] // 8, 8, x.shape[1]), axis=0)


def row_scan(x, mat):
    hi = x.astype(BF16).astype(F32)
    rest = x - hi
    mid = rest.astype(BF16).astype(F32)
    low = rest - mid
    parts = jnp.concatenate([hi, mid, low, jnp.zeros_like(x)], axis=0).astype(BF16)
    out = dot(parts, mat)
    return out[0:8] + out[8:16] + out[16:24]


def head_sums(sel, z):
    hi = z.astype(BF16)
    low = (z - hi.astype(F32)).astype(BF16)
    return (dot_nt(sel, hi) + dot_nt(sel, low))[0:8]


def iota(shape, dim):
    return lax.broadcasted_iota(jnp.int32, shape, dim)


def spread(cols, first, rows):
    lane = iota((rows, 128), 1)
    return jnp.where(
        lane < 64,
        jnp.broadcast_to(cols[:, first : first + 1], (rows, 128)),
        jnp.broadcast_to(cols[:, first + 1 : first + 2], (rows, 128)),
    )


def pair_stack(x):
    lane = iota(x.shape, 1)
    zero = jnp.zeros_like(x)
    return jnp.concatenate([jnp.where(lane < 64, x, zero), jnp.where(lane < 64, zero, x)], axis=0)


def forward_kernel(
    steps_per_seq,
    width,
    hid_own,
    hid_rec,
    gains,
    w_own,
    w_rec,
    vtap,
    stap,
    head_par,
    wo_own,
    wo_rec,
    mixed_out,
    po_own,
    po_rec,
    pre_gate_out,
    pre_value_out,
    conv_value_out,
    pre_shared_out,
    conv_shared_out,
    y_out,
    state_out,
    rows_out,
    nt_out,
    state,
    vbuf,
    sbuf,
):
    chan = mixed_out.shape[1]
    pairs = chan // 128

    @pl.when(pl.program_id(0) % steps_per_seq == 0)
    def _():
        state[...] = jnp.zeros_like(state)
        vbuf[0:8, :] = jnp.zeros((8, vbuf.shape[1]), F32)
        sbuf[0:8, :] = jnp.zeros((8, sbuf.shape[1]), F32)

    h0 = hid_own[...].astype(F32)
    h1 = hid_rec[...].astype(F32)
    square = jnp.sum(h0 * h0, axis=1, keepdims=True) + jnp.sum(h1 * h1, axis=1, keepdims=True)
    recip = lax.rsqrt(square / width + EPSILON)
    n0 = (h0 * gains[0:1, :]).astype(BF16)
    n1 = (h1 * gains[1:2, :]).astype(BF16)
    half = n0.shape[1]
    nt_out[0:half, :] = jnp.transpose(n0)
    nt_out[half : 2 * half, :] = jnp.transpose(n1)
    q = dot(n0, w_own[...]) + dot(n1, w_rec[...])
    pre = q * recip
    gate = pre[:, 0:chan]
    pre_gate_out[...] = gate
    pre_value = pre[:, chan : 2 * chan]
    pre_value_out[...] = pre_value
    pre_shared = pre[:, 2 * chan : 2 * chan + 256]
    pre_shared_out[...] = pre_shared
    vbuf[8 : 8 + STEP, :] = pre_value
    sbuf[8 : 8 + STEP, :] = pre_shared
    conv = jnp.broadcast_to(vtap[4:5, :], (STEP, chan))
    conv_s = jnp.broadcast_to(stap[4:5, :], (STEP, 256))
    for k in range(4):
        conv = conv + vbuf[5 + k : 5 + k + STEP, :] * vtap[k : k + 1, :]
        conv_s = conv_s + sbuf[5 + k : 5 + k + STEP, :] * stap[k : k + 1, :]
    vbuf[0:8, :] = vbuf[STEP : STEP + 8, :]
    sbuf[0:8, :] = sbuf[STEP : STEP + 8, :]
    conv_value_out[...] = conv
    conv_shared_out[...] = conv_s
    x = conv * sigmoid(conv)
    act = conv_s * sigmoid(conv_s)

    head_rows = jnp.transpose(pre[:, 2 * chan + 256 : 2 * chan + 384])[0:8]
    v = head_rows + head_par[0:8, 0:1]
    steps = softplus(v)
    logd = head_par[8:16, 0:1] * steps
    rows_out[0:8, :] = v
    rows_out[16:24, :] = jnp.transpose(jnp.broadcast_to(recip, (STEP, 128)))[0:8]

    upper = (iota((SUB, SUB), 0) <= iota((SUB, SUB), 1)).astype(F32).astype(BF16)
    causal = iota((SUB, SUB), 0) >= iota((SUB, SUB), 1)
    sg = gate * sigmoid(gate)
    for sub in range(STEP // SUB):
        lo, hi = sub * SUB, (sub + 1) * SUB
        cum_r = row_scan(logd[:, lo:hi], upper)
        rows_out[8:16, lo:hi] = cum_r
        cols = jnp.transpose(jnp.concatenate([cum_r, steps[:, lo:hi]], axis=0))
        b_in = act[lo:hi, 0:128]
        b_bf = b_in.astype(BF16)
        c_bf = act[lo:hi, 128:256].astype(BF16)
        b_t = jnp.transpose(b_in).astype(BF16)
        scores = dot_nt(c_bf, b_bf)
        for p in range(pairs):
            pl0, pl1 = p * 128, (p + 1) * 128
            c0 = jnp.broadcast_to(cols[:, 2 * p : 2 * p + 1], (SUB, 128))
            c1 = jnp.broadcast_to(cols[:, 2 * p + 1 : 2 * p + 2], (SUB, 128))
            weights = []
            for col, h in ((c0, 2 * p), (c1, 2 * p + 1)):
                gap = jnp.where(causal, col - cum_r[h : h + 1, :], -1e30)
                weights.append((scores * jnp.exp(gap)).astype(BF16))
            lane = iota((SUB, 128), 1)
            cum_e = jnp.where(lane < 64, c0, c1)
            step_e = spread(cols, 8 + 2 * p, SUB)
            xs = x[lo:hi, pl0:pl1]
            xh = step_e * xs
            inside = dot(jnp.concatenate(weights, axis=1), pair_stack(xh.astype(BF16)))
            held = state[:, pl0:pl1]
            held_bf = held.astype(BF16)
            state_out[lo:hi, pl0:pl1] = held_bf
            carried = dot(c_bf, held_bf)
            y = inside + carried * jnp.exp(cum_e)
            y_out[lo:hi, pl0:pl1] = y
            last = cum_e[SUB - 1 : SUB, :]
            tail = (xh * jnp.exp(last - cum_e)).astype(BF16)
            state[:, pl0:pl1] = held * jnp.exp(last) + dot(b_t, tail)
            y = y + vtap[5:6, pl0:pl1] * xs
            mixed_out[lo:hi, pl0:pl1] = (y * sg[lo:hi, pl0:pl1]).astype(BF16)
    mix = mixed_out[...].astype(F32)
    weighted = (mix * vtap[6:7, :]).astype(BF16)
    po_own[...] = dot(weighted, wo_own[...]).astype(BF16)
    po_rec[...] = dot(weighted, wo_rec[...]).astype(BF16)
    rows_out[24:32, :] = head_sums(jnp.ones((16, chan), BF16), mix * mix)


def backward_kernel(
    steps_per_seq,
    cot_own,
    cot_rec,
    wo_own,
    wo_rec,
    trow,
    rows_in,
    mixed,
    pre_gate,
    pre_value,
    conv_value,
    pre_shared,
    conv_shared,
    y_in,
    state_in,
    w_own,
    w_rec,
    vtap,
    stap,
    head_par,
    sel_ref,
    hid_own,
    hid_rec,
    p_out,
    dn_own,
    dn_rec,
    rsum_out,
    acc_v,
    acc_s,
    acc_h,
    acc_n,
    go_own,
    go_rec,
    grad,
    vbuf,
    sbuf,
    dxbuf,
    dbbuf,
):
    chan = mixed.shape[1]
    pairs = chan // 128

    @pl.when(pl.program_id(0) == 0)
    def _():
        acc_v[...] = jnp.zeros_like(acc_v)
        acc_s[...] = jnp.zeros_like(acc_s)
        acc_h[...] = jnp.zeros_like(acc_h)
        acc_n[...] = jnp.zeros_like(acc_n)
        go_own[...] = jnp.zeros_like(go_own)
        go_rec[...] = jnp.zeros_like(go_rec)

    @pl.when(pl.program_id(0) % steps_per_seq == 0)
    def _():
        grad[...] = jnp.zeros_like(grad)
        vbuf[STEP : STEP + 8, :] = jnp.zeros((8, vbuf.shape[1]), F32)
        sbuf[STEP : STEP + 8, :] = jnp.zeros((8, sbuf.shape[1]), F32)

    tcol = jnp.transpose(jnp.concatenate([trow[...], rows_in[16:24, :]], axis=0))
    scale = tcol[:, 0:1]
    coef = tcol[:, 8:9]
    recip = tcol[:, 16:17]
    s0 = (cot_own[...].astype(F32) * scale).astype(BF16)
    s1 = (cot_rec[...].astype(F32) * scale).astype(BF16)
    d_weighted = dot_nt(s0, wo_own[...]) + dot_nt(s1, wo_rec[...])
    mix = mixed[...].astype(F32)
    acc_v[48:56, :] += fold8(d_weighted * mix)
    weighted_t = jnp.transpose((mix * vtap[6:7, :]).astype(BF16))
    go_own[...] += dot(weighted_t, s0)
    go_rec[...] += dot(weighted_t, s1)
    d_mixed = d_weighted * vtap[6:7, :] - coef * mix
    gate = pre_gate[...]
    sig = sigmoid(gate)
    silu = gate * sig
    conv = conv_value[...]
    sig_v = sigmoid(conv)
    x = conv * sig_v
    y_scan = y_in[...]
    y = y_scan + vtap[5:6, :] * x
    dy = d_mixed * silu
    d_gate = d_mixed * y * (sig + silu * (1.0 - sig))
    acc_v[40:48, :] += fold8(dy * x)
    conv_s = conv_shared[...]
    sig_s = sigmoid(conv_s)
    act = conv_s * sig_s

    sel = sel_ref[...]
    sel_f = sel.astype(F32)[0:8]
    v = rows_in[0:8, :]
    steps = softplus(v)
    logd = head_par[8:16, 0:1] * steps
    lower = (iota((SUB, SUB), 0) >= iota((SUB, SUB), 1)).astype(F32).astype(BF16)
    strict = (iota((SUB, SUB), 0) < iota((SUB, SUB), 1)).astype(F32).astype(BF16)
    causal_t = iota((SUB, SUB), 0) <= iota((SUB, SUB), 1)
    for sub in reversed(range(STEP // SUB)):
        lo, hi = sub * SUB, (sub + 1) * SUB
        cum_r = rows_in[8:16, lo:hi]
        cols = jnp.transpose(jnp.concatenate([cum_r, steps[:, lo:hi]], axis=0))
        b_bf = act[lo:hi, 0:128].astype(BF16)
        c_in = act[lo:hi, 128:256]
        c_bf = c_in.astype(BF16)
        c_t = jnp.transpose(c_in).astype(BF16)
        scores_t = dot_nt(b_bf, c_bf)
        d_scores = jnp.zeros((SUB, SUB), F32)
        db = jnp.zeros((SUB, 128), F32)
        dc = jnp.zeros((SUB, 128), F32)
        z_sum = jnp.zeros((8, SUB), F32)
        e_sum = jnp.zeros((8, SUB), F32)
        f_sum = jnp.zeros((8, SUB), F32)
        gh = jnp.zeros((8, 1), F32)
        for p in range(pairs):
            pl0, pl1 = p * 128, (p + 1) * 128
            c0 = jnp.broadcast_to(cols[:, 2 * p : 2 * p + 1], (SUB, 128))
            c1 = jnp.broadcast_to(cols[:, 2 * p + 1 : 2 * p + 2], (SUB, 128))
            decays = []
            for col, h in ((c0, 2 * p), (c1, 2 * p + 1)):
                gap = jnp.where(causal_t, cum_r[h : h + 1, :] - col, -1e30)
                decays.append(jnp.exp(gap))
            weights = [(scores_t * d).astype(BF16) for d in decays]
            lane = iota((SUB, 128), 1)
            cum_e = jnp.where(lane < 64, c0, c1)
            step_e = spread(cols, 8 + 2 * p, SUB)
            xs = x[lo:hi, pl0:pl1]
            xh = step_e * xs
            xh_bf = xh.astype(BF16)
            dys = dy[lo:hi, pl0:pl1]
            dys_bf = dys.astype(BF16)
            stack = pair_stack(dys_bf)
            inner = dot(jnp.concatenate(weights, axis=1), stack)
            d_pair = dot_nt(xh_bf, stack)
            d_scores = d_scores + decays[0] * d_pair[:, 0:128] + decays[1] * d_pair[:, 128:256]
            last = cum_e[SUB - 1 : SUB, :]
            tail_e = jnp.exp(last - cum_e)
            g = grad[:, pl0:pl1]
            g_bf = g.astype(BF16)
            outer = dot(b_bf, g_bf) * tail_e
            u = inner + outer
            dxbuf[lo:hi, pl0:pl1] = step_e * u + vtap[5:6, pl0:pl1] * dys
            db = db + dot_nt((xh * tail_e).astype(BF16), g_bf)
            dya = (dys * jnp.exp(cum_e)).astype(BF16)
            held = state_in[lo:hi, pl0:pl1]
            dc = dc + dot_nt(dya, held)
            sel_p = sel[:, pl0:pl1]
            z_sum = z_sum + head_sums(
                sel_p, dys_bf.astype(F32) * y_in[lo:hi, pl0:pl1] - xh_bf.astype(F32) * inner
            )
            e_sum = e_sum + head_sums(sel_p, xh * outer)
            f_sum = f_sum + head_sums(sel_p, xs * u)
            decay_row = jnp.exp(last)
            gh_row = decay_row * jnp.sum(g * held.astype(F32), axis=0, keepdims=True)
            gh = gh + jnp.sum(sel_f[:, pl0:pl1] * gh_row, axis=1, keepdims=True)
            grad[:, pl0:pl1] = g * decay_row + dot(c_t, dya)
        ds_bf = d_scores.astype(BF16)
        dbbuf[lo:hi, 0:128] = db + dot(ds_bf, c_bf)
        dbbuf[lo:hi, 128:256] = dc + dot(jnp.transpose(d_scores).astype(BF16), b_bf)
        d_log = row_scan(z_sum, lower) + row_scan(e_sum, strict) + gh
        d_step = (f_sum + d_log * head_par[8:16, 0:1]) * sigmoid(v[:, lo:hi])
        acc_h[0:8, :] += d_log * logd[:, lo:hi]
        acc_h[8:16, :] += d_step
        pre_step = v[:, lo:hi] - head_par[0:8, 0:1]
        rsum_out[:, lo:hi] = jnp.broadcast_to(
            jnp.sum(d_step * pre_step, axis=0, keepdims=True), (8, SUB)
        )
        d_cols = jnp.transpose(jnp.concatenate([d_step, jnp.zeros((120, SUB), F32)], axis=0))
        p_out[lo:hi, 2 * chan + 256 : 2 * chan + 384] = (recip[lo:hi] * d_cols).astype(BF16)

    d_conv = dxbuf[...] * (sig_v + x * (1.0 - sig_v))
    d_conv_s = dbbuf[...] * (sig_s + act * (1.0 - sig_s))
    vbuf[0:STEP, :] = d_conv
    sbuf[0:STEP, :] = d_conv_s
    acc_v[32:40, :] += fold8(d_conv)
    acc_s[32:40, :] += fold8(d_conv_s)
    pv = pre_value[...]
    ps = pre_shared[...]
    d_value = jnp.zeros((STEP, chan), F32)
    d_shared = jnp.zeros((STEP, 256), F32)
    for k in range(4):
        moved = vbuf[3 - k : 3 - k + STEP, :]
        d_value = d_value + vtap[k : k + 1, :] * moved
        acc_v[8 * k : 8 * k + 8, :] += fold8(pv * moved)
        moved = sbuf[3 - k : 3 - k + STEP, :]
        d_shared = d_shared + stap[k : k + 1, :] * moved
        acc_s[8 * k : 8 * k + 8, :] += fold8(ps * moved)
    vbuf[STEP : STEP + 8, :] = vbuf[0:8, :]
    sbuf[STEP : STEP + 8, :] = sbuf[0:8, :]
    p_out[:, 0:chan] = (recip * d_gate).astype(BF16)
    p_out[:, chan : 2 * chan] = (recip * d_value).astype(BF16)
    p_out[:, 2 * chan : 2 * chan + 256] = (recip * d_shared).astype(BF16)
    ones = jnp.ones((16, chan), BF16)
    rsum_out[...] += head_sums(ones, d_gate * gate + d_value * pv)
    rsum_out[...] += head_sums(ones[:, 0:256], d_shared * ps)
    pb = p_out[...]
    for n, (hid, weight, dn) in enumerate(((hid_own, w_own, dn_own), (hid_rec, w_rec, dn_rec))):
        part = dot_nt(pb, weight[...])
        dn[...] = part.astype(BF16)
        acc_n[8 * n : 8 * n + 8, :] += fold8(part * hid[...].astype(F32))


def unit_rows(dp):
    return 16 * dp


def big_rows(dp, rows):
    return pl.cdiv(rows, unit_rows(dp)) * unit_rows(dp)


def remote(src, dst, send, recv, target):
    return pltpu.make_async_remote_copy(
        src_ref=src,
        dst_ref=dst,
        send_sem=send,
        recv_sem=recv,
        device_id=target,
        device_id_type=pl.DeviceIdType.MESH,
    )


def greet(targets):
    barrier = pltpu.get_barrier_semaphore()
    for target in targets:
        pl.semaphore_signal(barrier, inc=1, device_id=target, device_id_type=pl.DeviceIdType.MESH)
    pl.semaphore_wait(barrier, len(targets))


def mid_kernel(
    inner_width,
    rows_in,
    cot,
    po_own,
    po_rec,
    proj_out,
    trow,
    po_land,
    sums,
    sums_land,
    po_send_sem,
    po_recv_sem,
    send_sem,
    recv_sem,
):
    r = lax.axis_index("row")
    c = lax.axis_index("col")
    targets = [{"row": 1 - r}, {"col": 1 - c}, {"row": 1 - r, "col": 1 - c}]
    greet(targets)
    tokens, half = cot.shape
    cut = tokens // DN_PARTS
    copies = []
    for i in range(DN_PARTS):
        rows = pl.ds(i * cut, cut)
        copy = remote(po_rec.at[rows, :], po_land.at[rows, :], po_send_sem.at[i], po_recv_sem.at[i], targets[0])
        copy.start()
        copies.append(copy)
    ones = jnp.ones((16, half), BF16)
    sums[0:8, :] = rows_in[24:32, :]
    for i in range(DN_PARTS):
        rows = slice(i * cut, (i + 1) * cut)
        copies[i].wait()
        part = po_own[rows, :].astype(F32) + po_land[rows, :].astype(F32)
        proj_out[rows, :] = part.astype(BF16)
        sums[8:16, rows] = head_sums(ones, part * cot[rows, :].astype(F32))
    ends = []
    for i, target in enumerate(targets):
        copy = remote(sums, sums_land.at[i], send_sem.at[i], recv_sem.at[i], target)
        copy.start()
        ends.append(copy)
    for copy in ends:
        copy.wait()
    total = (sums[...] + sums_land[0]) + (sums_land[1] + sums_land[2])
    scale = lax.rsqrt(total[0:8] / inner_width + EPSILON)
    trow[0:8, :] = scale
    trow[8:16, :] = total[8:16] * (scale * scale * scale) / inner_width


def mid_exchange(inner_width, rows, cot, po_own, po_rec):
    tokens, half = cot.shape
    vmem = pl.BlockSpec(memory_space=pltpu.VMEM)
    return pl.pallas_call(
        functools.partial(mid_kernel, inner_width),
        in_specs=[vmem, vmem, vmem, pl.BlockSpec(memory_space=pl.ANY)],
        out_specs=[vmem, vmem],
        out_shape=[jax.ShapeDtypeStruct((tokens, half), BF16), jax.ShapeDtypeStruct((16, tokens), F32)],
        scratch_shapes=[
            pltpu.VMEM((tokens, half), BF16),
            pltpu.VMEM((16, tokens), F32),
            pltpu.VMEM((3, 16, tokens), F32),
            pltpu.SemaphoreType.DMA((DN_PARTS,)),
            pltpu.SemaphoreType.DMA((DN_PARTS,)),
            pltpu.SemaphoreType.DMA((3,)),
            pltpu.SemaphoreType.DMA((3,)),
        ],
        compiler_params=pltpu.CompilerParams(collective_id=1, has_side_effects=True),
        cost_estimate=pl.CostEstimate(flops=1_000_000, bytes_accessed=20_000_000, transcendentals=0),
        name="mid_exchange",
    )(rows, cot, po_own, po_rec)


def sum_kernel(
    dp,
    g_cat,
    go_own,
    go_rec,
    acc_v,
    acc_s,
    acc_h,
    acc_n,
    rs_in,
    dn_own,
    dn_rec,
    out,
    dn_sum,
    dn_col,
    rs_out,
    acc,
    stage,
    land,
    row_send,
    row_land,
    col_send,
    col_land,
    dn_land,
    rs_land,
    send_sem,
    recv_sem,
    pair_send,
    pair_recv,
    dn_send_sem,
    dn_recv_sem,
):
    half = g_cat.shape[0] // 2
    chan = go_own.shape[0]
    wide = g_cat.shape[1]
    size = big_rows(dp, 2 * half)
    misc = 3 * size
    tail = out.shape[0] - misc
    bits = dp.bit_length() - 1
    me = lax.axis_index("dp")
    r = lax.axis_index("row")
    c = lax.axis_index("col")
    to_row, to_col = {"row": 1 - r}, {"col": 1 - c}

    def bit_of(k):
        return lax.rem(me // (1 << k), 2)

    def partner(k):
        return {"dp": me + (1 - 2 * bit_of(k)) * (1 << k)}

    def sum8(ref, n):
        return jnp.sum(ref[8 * n : 8 * n + 8, :], axis=0, keepdims=True)

    greet([partner(k) for k in range(bits)] + [to_row, to_col])

    row_send[0:half, 0:wide] = g_cat[half : 2 * half, :].astype(BF16)
    row_send[0:half, wide : wide + half] = go_rec[...].astype(BF16)
    small = jnp.concatenate([sum8(acc_s, n) for n in range(5)] + [jnp.zeros((3, 256), F32)], axis=0)
    norm_own, norm_rec = [
        jnp.concatenate([sum8(acc_n, n), jnp.zeros((1, 512 - half), F32)], axis=1) for n in (0, 1)
    ]
    pad6 = jnp.zeros((6, 256), F32)
    row_send[half : half + 16, 0:256] = jnp.concatenate(
        [small, norm_rec[:, 0:256], norm_rec[:, 256:512], pad6], axis=0
    ).astype(BF16)
    row_send[half : half + 16, 256 : wide + half] = jnp.zeros((16, wide + half - 256), BF16)
    row_copy = remote(row_send, row_land, pair_send.at[0], pair_recv.at[0], to_row)
    row_copy.start()

    tokens = dn_own.shape[0]
    cut = tokens // DN_PARTS

    def dn_copy(i, side):
        rows = pl.ds(i * cut, cut)
        if side == 0:
            src, dst, target = dn_rec, dn_land, to_row
        else:
            src, dst, target = dn_sum, dn_col, to_col
        return remote(src.at[rows, :], dst.at[rows, :], dn_send_sem.at[side, i], dn_recv_sem.at[side, i], target)

    dn_rows = [dn_copy(i, 0) for i in range(DN_PARTS)]
    dn_cols = [dn_copy(i, 1) for i in range(DN_PARTS)]
    rs_row = remote(rs_in, rs_land.at[0], pair_send.at[2], pair_recv.at[2], to_row)
    rs_col = remote(rs_out, rs_land.at[1], pair_send.at[3], pair_recv.at[3], to_col)
    rs_row.start()
    for copy in dn_rows:
        copy.start()

    orders = [
        tuple(range(bits)),
        tuple(range(1, bits)) + (0,),
        tuple(range(bits)),
        tuple(range(bits)),
    ]
    bounds = [(0, size), (size, size), (2 * size, size), (misc, tail)]
    lows = {}
    flying = {}

    def span(start, rows):
        return pl.ds(pl.multiple_of(start, 16), rows)

    def copy_of(i, level, src, rows, dst, dst_rows, k):
        return remote(
            src.at[rows, :], dst.at[dst_rows, :], send_sem.at[i, level], recv_sem.at[i, level], partner(k)
        )

    def start_level(i, level):
        base, rows = bounds[i]
        order = orders[i]
        if level < bits:
            k = order[level]
            low = lows.get(i, base)
            part = rows >> (level + 1)
            keep = low + bit_of(k) * part
            give = low + (1 - bit_of(k)) * part
            stage[span(give, part), :] = acc[span(give, part), :].astype(BF16)
            where = base + rows - (rows >> level)
            copy = copy_of(i, level, stage, span(give, part), land, span(where, part), k)
            lows[i] = keep
            flying[i] = (copy, keep, where, part)
        else:
            back = 2 * bits - 1 - level
            k = order[back]
            part = rows >> (back + 1)
            low = lows[i]
            copy = copy_of(i, level, out, span(low, part), out, span(low, part), k)
            lows[i] = low - bit_of(k) * part
            flying[i] = (copy, low, None, part)
        copy.start()

    def end_level(i, level):
        copy, low, where, part = flying[i]
        copy.wait()
        if level < bits:
            total = acc[span(low, part), :] + land[span(where, part), :].astype(F32)
            acc[span(low, part), :] = total
            if level == bits - 1:
                out[span(low, part), :] = total.astype(BF16)
        if level + 1 < 2 * bits:
            start_level(i, level + 1)

    mine = pl.multiple_of(r * half, 128)
    other = pl.multiple_of((1 - r) * half, 128)

    def fill(i, own, lo):
        acc[span(i * size + mine, half), :] = own
        acc[span(i * size + other, half), :] = row_land[0:half, lo : lo + chan].astype(F32)
        if size > 2 * half:
            acc[i * size + 2 * half : (i + 1) * size, :] = jnp.zeros((size - 2 * half, chan), F32)

    for i in range(3):
        acc_own = go_own[...] if i == 0 else g_cat[0:half, (i - 1) * chan : i * chan]
        if i == 0:
            row_copy.wait()
        fill(i, acc_own, wide if i == 0 else (i - 1) * chan)
        start_level(i, 0)
        if i == 0:
            lo = 2 * chan
            state = g_cat[0:half, lo : lo + 256] + row_land[0:half, lo : lo + 256].astype(F32)
            extra = jnp.concatenate([small, norm_own[:, 0:256], norm_own[:, 256:512], pad6], axis=0)
            extra = extra + row_land[half : half + 16, 0:256].astype(F32)
            col_send[0:half, :] = state.astype(BF16)
            col_send[half : half + 16, :] = extra.astype(BF16)
            col_copy = remote(col_send, col_land, pair_send.at[1], pair_recv.at[1], to_col)
            col_copy.start()
            rs_row.wait()
            rs_out[...] = rs_in[...] + rs_land[0]
            rs_col.start()
    for i in range(DN_PARTS):
        rows = slice(i * cut, (i + 1) * cut)
        dn_rows[i].wait()
        dn_sum[rows, :] = (dn_own[rows, :].astype(F32) + dn_land[rows, :].astype(F32)).astype(BF16)
        dn_cols[i].start()

    lo = 2 * chan + 256
    acc[misc : misc + half, 256:384] = jnp.concatenate(
        [g_cat[0:half, lo : lo + 64], row_land[0:half, lo : lo + 64].astype(F32)], axis=1
    )
    acc[misc + half : misc + half + 16, 256:384] = jnp.zeros((16, 128), F32)
    first = misc + half + 16
    acc[first : first + 8, :] = jnp.concatenate(
        [sum8(acc_v, n) for n in range(7)] + [jnp.zeros((1, chan), F32)], axis=0
    )
    acc[first + 8 : first + 24, :] = jnp.broadcast_to(
        jnp.sum(acc_h[...], axis=1, keepdims=True), (16, chan)
    )
    if misc + tail > first + 24:
        acc[first + 24 : misc + tail, :] = jnp.zeros((misc + tail - first - 24, chan), F32)
    end_level(0, 0)
    col_copy.wait()
    acc[misc : misc + half + 16, 0:256] = col_send[...].astype(F32) + col_land[...].astype(F32)
    start_level(3, 0)
    end_level(1, 0)
    end_level(2, 0)
    for level in range(1, 2 * bits):
        for i in (0, 1):
            end_level(i, level)
        end_level(3, level - 1)
        end_level(2, level)
    end_level(3, 2 * bits - 1)
    rs_col.wait()
    for copy in dn_cols:
        copy.wait()
    rs_out[...] = rs_out[...] + rs_land[1]


def sum_over_dp(dp, g_cat, go_own, go_rec, acc_v, acc_s, acc_h, acc_n, rs, dn_own, dn_rec):
    half = g_cat.shape[0] // 2
    wide = g_cat.shape[1]
    chan = go_own.shape[0]
    rows = 3 * big_rows(dp, 2 * half) + big_rows(dp, half + 40)
    bits = dp.bit_length() - 1
    tokens = dn_own.shape[0]
    vmem = pl.BlockSpec(memory_space=pltpu.VMEM)
    hbm = pl.BlockSpec(memory_space=pl.ANY)
    act = jax.ShapeDtypeStruct((tokens, half), BF16)
    return pl.pallas_call(
        functools.partial(sum_kernel, dp),
        in_specs=[vmem] * 9 + [hbm],
        out_specs=[vmem, vmem, hbm, vmem],
        out_shape=[jax.ShapeDtypeStruct((rows, chan), BF16), act, act, jax.ShapeDtypeStruct(rs.shape, F32)],
        scratch_shapes=[
            pltpu.VMEM((rows, chan), F32),
            pltpu.VMEM((rows, chan), BF16),
            pltpu.VMEM((rows, chan), BF16),
            pltpu.VMEM((half + 16, wide + half), BF16),
            pltpu.VMEM((half + 16, wide + half), BF16),
            pltpu.VMEM((half + 16, 256), BF16),
            pltpu.VMEM((half + 16, 256), BF16),
            pltpu.VMEM((tokens, half), BF16),
            pltpu.VMEM((2,) + rs.shape, F32),
            pltpu.SemaphoreType.DMA((4, 2 * bits)),
            pltpu.SemaphoreType.DMA((4, 2 * bits)),
            pltpu.SemaphoreType.DMA((4,)),
            pltpu.SemaphoreType.DMA((4,)),
            pltpu.SemaphoreType.DMA((2, DN_PARTS)),
            pltpu.SemaphoreType.DMA((2, DN_PARTS)),
        ],
        compiler_params=pltpu.CompilerParams(collective_id=0, has_side_effects=True),
        cost_estimate=pl.CostEstimate(flops=1_000_000, bytes_accessed=150_000_000, transcendentals=0),
        name="sum_over_dp",
    )(g_cat, go_own, go_rec, acc_v, acc_s, acc_h, acc_n, rs, dn_own, dn_rec)


def finish_kernel(
    width,
    size,
    out,
    hid,
    cot,
    dn_sum,
    dn_col,
    proj_own,
    proj_col,
    trow,
    rows_in,
    rs,
    gains,
    result,
    hidden_grad,
    g_gate,
    g_value,
    g_step,
    g_state,
    small_a,
    small_b,
    small_h,
    g_output,
):
    half = hid.shape[1]
    step_rows = hid.shape[0]
    hid32 = hid[...].astype(F32)
    recip = rows_in[16:24, :]
    cols = jnp.transpose(jnp.concatenate([trow[0:8, :], rs[...] * recip * recip / width], axis=0))
    proj = proj_own[...].astype(F32) + proj_col[...].astype(F32)
    result[...] = (hid32 + cols[:, 0:1] * proj).astype(BF16)
    d_normed = dn_sum[...].astype(F32) + dn_col[...].astype(F32)
    hidden_grad[...] = cot[...].astype(F32) + d_normed * gains[0:1, :] - cols[:, 8:9] * hid32
    misc = 3 * size

    @pl.when(pl.program_id(0) == 0)
    def _():
        g_output[...] = out[0 : g_output.shape[0], :].astype(F32)
        for n, ref in ((1, g_gate), (2, g_value)):
            ref[:, 0:half] = out[n * size : n * size + half, :].astype(F32)
            ref[:, half : 2 * half] = out[n * size + half : n * size + 2 * half, :].astype(F32)
        g_state[...] = out[misc : misc + half, 0:256].astype(F32)
        step_t = jnp.transpose(out[misc : misc + half, 256:384].astype(F32))
        heads = g_step.shape[0] // 2
        own, rec = step_t[0:heads], step_t[64 : 64 + heads]
        first = lax.axis_index("row") == 0
        g_step[...] = jnp.concatenate([jnp.where(first, own, rec), jnp.where(first, rec, own)], axis=0)
        small = out[misc + half : misc + half + 48, :].astype(F32)
        small_a[...] = small[0:16, 0:256]
        small_b[...] = small[16:24, :]
        small_h[...] = jnp.transpose(small[24:40, 0:128])[0:8]


def finish(size, heads, out, hid, cot, dn_sum, dn_col, proj_own, proj_col, trow, rows, rs, gains):
    tokens, half = hid.shape
    chan = out.shape[1]

    def blk(cols):
        return pl.BlockSpec((STEP, cols), lambda i: (i, 0))

    def row(count):
        return pl.BlockSpec((count, STEP), lambda i: (0, i))

    def whole(shape):
        return pl.BlockSpec(shape, lambda i: (0, 0))

    shapes = [
        (half, 2 * chan),
        (half, 2 * chan),
        (2 * heads, half),
        (half, 256),
        (16, 256),
        (8, chan),
        (8, 16),
        (2 * chan, half),
    ]
    return pl.pallas_call(
        functools.partial(finish_kernel, 2 * half, size),
        grid=(tokens // STEP,),
        in_specs=[
            whole(out.shape),
            blk(half),
            blk(half),
            blk(half),
            blk(half),
            blk(half),
            blk(half),
            row(16),
            row(32),
            row(8),
            whole((8, half)),
        ],
        out_specs=[blk(half), blk(half)] + [whole(shape) for shape in shapes],
        out_shape=[
            jax.ShapeDtypeStruct((tokens, half), BF16),
            jax.ShapeDtypeStruct((tokens, half), F32),
        ]
        + [jax.ShapeDtypeStruct(shape, F32) for shape in shapes],
        cost_estimate=pl.CostEstimate(flops=20_000_000, bytes_accessed=20_000_000, transcendentals=0),
        name="finish",
    )(out, hid, cot, dn_sum, dn_col, proj_own, proj_col, trow, rows, rs, gains)


def swap(x, axis):
    return lax.ppermute(x, axis, SWAP)


def body(
    hidden,
    gate_proj,
    value_proj,
    step_proj,
    state_proj,
    value_filter,
    value_shift,
    shared_kernel,
    shared_offset,
    decay_log,
    step_bias,
    skip_gain,
    input_gain,
    gated_gain,
    output_proj,
    cotangent,
):
    tokens, half = hidden.shape
    width = 2 * half
    chan = gated_gain.shape[0]
    inner_width = 4 * chan
    heads = decay_log.shape[0]
    r = lax.axis_index("row")
    dp = lax.axis_size("dp")
    seq_len = min(LEN, tokens)
    steps_per_seq = seq_len // STEP
    grid = tokens // STEP

    def cut(x, start, size, axis):
        return lax.dynamic_slice_in_dim(x, start * size, size, axis)

    def packed(side):
        return jnp.concatenate(
            [
                cut(gate_proj, side, chan, 1),
                cut(value_proj, side, chan, 1),
                state_proj,
                jnp.pad(cut(step_proj, side, heads, 1), ((0, 0), (0, 128 - heads))),
            ],
            axis=1,
        )

    w_own = packed(r)
    w_rec = swap(packed(1 - r), "row")
    hid_rec = swap(hidden, "row")
    cot_rec = swap(cotangent, "row")
    wo_own = cut(output_proj, r, chan, 0)
    wo_part = cut(output_proj, 1 - r, chan, 0)
    wo_rec = swap(wo_part, "row")
    gain_f = gated_gain.astype(F32)
    gain_rec = swap(input_gain, "row")
    gains = jnp.concatenate([input_gain[None], gain_rec[None], jnp.zeros((6, half), F32)], axis=0)

    skip_lane = jnp.repeat(skip_gain, chan // heads)
    vtap = jnp.concatenate(
        [value_filter, value_shift[None], skip_lane[None], gain_f[None], jnp.zeros((1, chan), F32)], axis=0
    )
    stap = jnp.concatenate([shared_kernel, shared_offset[None], jnp.zeros((3, 256), F32)], axis=0)
    pad_h = (0, 8 - heads)
    head_par = jnp.concatenate([jnp.pad(step_bias, pad_h), jnp.pad(-jnp.exp(decay_log), pad_h)])
    head_par = jnp.broadcast_to(head_par[:, None], (16, 128))

    wide = w_own.shape[1]

    def blk(cols):
        return pl.BlockSpec((STEP, cols), lambda i: (i, 0))

    def whole(shape):
        return pl.BlockSpec(shape, lambda i: (0, 0))

    def arr(cols, dtype=F32):
        return jax.ShapeDtypeStruct((tokens, cols), dtype)

    mixed, po_own, po_rec, pre_gate, pre_value, conv_value, pre_shared, conv_shared, y_scan, states, rows, normed_t = pl.pallas_call(
        functools.partial(forward_kernel, steps_per_seq, width),
        grid=(grid,),
        in_specs=[
            blk(half),
            blk(half),
            whole((8, half)),
            whole((half, wide)),
            whole((half, wide)),
            whole((8, chan)),
            whole((8, 256)),
            whole((16, 128)),
            whole((chan, half)),
            whole((chan, half)),
        ],
        out_specs=[
            blk(chan),
            blk(half),
            blk(half),
            blk(chan),
            blk(chan),
            blk(chan),
            blk(256),
            blk(256),
            blk(chan),
            blk(chan),
            pl.BlockSpec((32, STEP), lambda i: (0, i)),
            pl.BlockSpec((width, STEP), lambda i: (0, i)),
        ],
        out_shape=[
            arr(chan, BF16),
            arr(half, BF16),
            arr(half, BF16),
            arr(chan),
            arr(chan),
            arr(chan),
            arr(256),
            arr(256),
            arr(chan),
            arr(chan, BF16),
            jax.ShapeDtypeStruct((32, tokens), F32),
            jax.ShapeDtypeStruct((width, tokens), BF16),
        ],
        scratch_shapes=[
            pltpu.VMEM((128, chan), F32),
            pltpu.VMEM((STEP + 8, chan), F32),
            pltpu.VMEM((STEP + 8, 256), F32),
        ],
        cost_estimate=pl.CostEstimate(flops=12_000_000_000, bytes_accessed=40_000_000, transcendentals=8_000_000),
        name="forward_core",
    )(hidden, hid_rec, gains, w_own, w_rec, vtap, stap, head_par, wo_own, wo_rec)

    proj_own, trow = mid_exchange(inner_width, rows, cotangent, po_own, po_rec)
    proj_col = swap(proj_own, "col")

    lane_head = jnp.arange(chan) // (chan // heads)
    sel = (jnp.arange(16)[:, None] == lane_head[None, :]).astype(BF16)
    last = grid - 1

    def rblk(cols):
        return pl.BlockSpec((STEP, cols), lambda i: (last - i, 0))

    def rrow(count):
        return pl.BlockSpec((count, STEP), lambda i: (0, last - i))

    p_all, dn_own, dn_rec, rsum, acc_v, acc_s, acc_h, acc_n, go_own, go_rec = pl.pallas_call(
        functools.partial(backward_kernel, steps_per_seq),
        grid=(grid,),
        in_specs=[
            rblk(half),
            rblk(half),
            whole((chan, half)),
            whole((chan, half)),
            rrow(16),
            rrow(32),
            rblk(chan),
            rblk(chan),
            rblk(chan),
            rblk(chan),
            rblk(256),
            rblk(256),
            rblk(chan),
            rblk(chan),
            whole((half, wide)),
            whole((half, wide)),
            whole((8, chan)),
            whole((8, 256)),
            whole((16, 128)),
            whole((16, chan)),
            rblk(half),
            rblk(half),
        ],
        out_specs=[
            rblk(wide),
            rblk(half),
            rblk(half),
            rrow(8),
            whole((56, chan)),
            whole((40, 256)),
            whole((16, 128)),
            whole((16, half)),
            whole((chan, half)),
            whole((chan, half)),
        ],
        out_shape=[
            arr(wide, BF16),
            arr(half, BF16),
            arr(half, BF16),
            jax.ShapeDtypeStruct((8, tokens), F32),
            jax.ShapeDtypeStruct((56, chan), F32),
            jax.ShapeDtypeStruct((40, 256), F32),
            jax.ShapeDtypeStruct((16, 128), F32),
            jax.ShapeDtypeStruct((16, half), F32),
            jax.ShapeDtypeStruct((chan, half), F32),
            jax.ShapeDtypeStruct((chan, half), F32),
        ],
        scratch_shapes=[
            pltpu.VMEM((128, chan), F32),
            pltpu.VMEM((STEP + 8, chan), F32),
            pltpu.VMEM((STEP + 8, 256), F32),
            pltpu.VMEM((STEP, chan), F32),
            pltpu.VMEM((STEP, 256), F32),
        ],
        cost_estimate=pl.CostEstimate(flops=24_000_000_000, bytes_accessed=60_000_000, transcendentals=8_000_000),
        name="backward_core",
    )(
        cotangent,
        cot_rec,
        wo_own,
        wo_rec,
        trow,
        rows,
        mixed,
        pre_gate,
        pre_value,
        conv_value,
        pre_shared,
        conv_shared,
        y_scan,
        states,
        w_own,
        w_rec,
        vtap,
        stap,
        head_par,
        sel,
        hidden,
        hid_rec,
    )

    g_cat = dot(normed_t, p_all)
    out, dn_sum, dn_col, rs = sum_over_dp(
        dp, g_cat, go_own, go_rec, acc_v, acc_s, acc_h, acc_n, rsum, dn_own, dn_rec
    )
    size = big_rows(dp, 2 * half)
    result, hidden_grad, g_gate, g_value, g_step, g_state, sm_a, sm_b, sm_h, g_output = finish(
        size, heads, out, hidden, cotangent, dn_sum, dn_col, proj_own, proj_col, trow, rows, rs, gains
    )
    return (
        result,
        hidden_grad,
        g_gate,
        g_value,
        g_step.T,
        g_state,
        sm_b[0:4],
        sm_b[4],
        sm_a[0:4],
        sm_a[4],
        sm_h[0, 0:heads],
        sm_h[0, 8 : 8 + heads],
        jnp.sum(sm_b[5].reshape(heads, chan // heads), axis=1),
        sm_a[8:10].reshape(512)[0:half],
        sm_b[6],
        g_output,
    )


def solution(mesh):
    in_specs = (
        P("dp", "row"),
        P("row", "col"),
        P("row", "col"),
        P("row", "col"),
        P("row", None),
        P(None, ("col", "row")),
        P(("col", "row")),
        P(),
        P(),
        P(("col", "row")),
        P(("col", "row")),
        P(("col", "row")),
        P("row"),
        P(("col", "row")),
        P("col", "row"),
        P("dp", "row"),
    )
    out_specs = (
        P("dp", "row"),
        P("dp", "row"),
        P("row", "col"),
        P("row", "col"),
        P("row", "col"),
        P("row", None),
        P(None, ("col", "row")),
        P(("col", "row")),
        P(),
        P(),
        P(("col", "row")),
        P(("col", "row")),
        P(("col", "row")),
        P("row"),
        P(("col", "row")),
        P("col", "row"),
    )
    return jax.shard_map(body, mesh=mesh, in_specs=in_specs, out_specs=out_specs, check_vma=False)
```

```python
import functools

import jax
import jax.numpy as jnp
from jax import lax
from jax.experimental import pallas as pl
from jax.experimental.pallas import tpu as pltpu
from jax.sharding import PartitionSpec as P

LEN = 2048
EPSILON = 1e-05
SUB = 128
STEP = 256
F32 = jnp.float32
BF16 = jnp.bfloat16
SWAP = [(0, 1), (1, 0)]
DN_PARTS = 4


def dot(a, b):
    return jnp.dot(a, b, preferred_element_type=F32)


def dot_nt(a, b):
    return lax.dot_general(a, b, (((1,), (1,)), ((), ())), preferred_element_type=F32)


def dot_tn(a, b):
    return lax.dot_general(a, b, (((0,), (0,)), ((), ())), preferred_element_type=F32)


def sigmoid(x):
    return 0.5 * jnp.tanh(0.5 * x) + 0.5


def softplus(x):
    return jnp.maximum(x, 0.0) + jnp.log1p(jnp.exp(-jnp.abs(x)))


def fold8(x):
    return jnp.sum(x.reshape(x.shape[0] // 8, 8, x.shape[1]), axis=0)


def row_scan(x, mat):
    hi = x.astype(BF16).astype(F32)
    rest = x - hi
    mid = rest.astype(BF16).astype(F32)
    low = rest - mid
    parts = jnp.concatenate([hi, mid, low, jnp.zeros_like(x)], axis=0).astype(BF16)
    out = dot(parts, mat)
    return out[0:8] + out[8:16] + out[16:24]


def head_sums(sel, z):
    hi = z.astype(BF16)
    low = (z - hi.astype(F32)).astype(BF16)
    return (dot_nt(sel, hi) + dot_nt(sel, low))[0:8]


def iota(shape, dim):
    return lax.broadcasted_iota(jnp.int32, shape, dim)


def spread(cols, first, rows):
    lane = iota((rows, 128), 1)
    return jnp.where(
        lane < 64,
        jnp.broadcast_to(cols[:, first : first + 1], (rows, 128)),
        jnp.broadcast_to(cols[:, first + 1 : first + 2], (rows, 128)),
    )


def pair_stack(x):
    lane = iota(x.shape, 1)
    zero = jnp.zeros_like(x)
    return jnp.concatenate([jnp.where(lane < 64, x, zero), jnp.where(lane < 64, zero, x)], axis=0)


def forward_kernel(
    steps_per_seq,
    width,
    inner_width,
    col_blocks,
    hid_own,
    hid_rec,
    gains,
    w_own,
    w_rec,
    vtap,
    stap,
    head_par,
    wo_own,
    wo_rec,
    cot,
    mixed_out,
    proj_out,
    proj_col,
    trow,
    pre_gate_out,
    pre_value_out,
    conv_value_out,
    pre_shared_out,
    conv_shared_out,
    y_out,
    state_out,
    rows_out,
    nt_out,
    state,
    vbuf,
    sbuf,
    po_own,
    po_send,
    po_land,
    proj_s,
    sums,
    sums_land,
    row_send_sem,
    row_recv_sem,
    col_send_sem,
    col_recv_sem,
    sum_send_sem,
    sum_recv_sem,
):
    chan = mixed_out.shape[1]
    pairs = chan // 128
    step = pl.program_id(0)
    blocks = pl.num_programs(0) - 1
    r = lax.axis_index("row")
    c = lax.axis_index("col")
    targets = [{"row": 1 - r}, {"col": 1 - c}, {"row": 1 - r, "col": 1 - c}]

    def span(i):
        return pl.ds(pl.multiple_of(i * STEP, STEP), STEP)

    def row_copy(i):
        return remote(
            po_send.at[span(i), :], po_land.at[span(i), :], row_send_sem.at[i], row_recv_sem.at[i], targets[0]
        )

    def col_copy(i):
        return remote(
            proj_s.at[span(i), :], proj_col.at[span(i), :], col_send_sem.at[i], col_recv_sem.at[i], targets[1]
        )

    @pl.when(step == 0)
    def _():
        greet(targets)

    @pl.when(step > 0)
    def _():
        i = step - 1
        row_copy(i).wait()
        part = po_own[span(i), :].astype(F32) + po_land[span(i), :].astype(F32)
        proj_s[span(i), :] = part.astype(BF16)

        @pl.when(i < col_blocks)
        def _():
            col_copy(i).start()

        dots = head_sums(jnp.ones((16, cot.shape[1]), BF16), part * cot[...].astype(F32))
        sums[pl.ds(8 + i, 1), :] = dots[0:1]

    @pl.when(step < blocks)
    def _():
        forward_block(
            steps_per_seq,
            width,
            (hid_own, hid_rec, gains, w_own, w_rec, vtap, stap, head_par, wo_own, wo_rec),
            (mixed_out, pre_gate_out, pre_value_out, conv_value_out, pre_shared_out, conv_shared_out),
            (y_out, state_out, rows_out, nt_out),
            (state, vbuf, sbuf, po_own.at[span(step), :], po_send.at[span(step), :], sums.at[pl.ds(step, 1), :]),
        )
        row_copy(step).start()

    @pl.when(step == blocks)
    def _():
        ends = []
        for i, target in enumerate(targets):
            copy = remote(sums, sums_land.at[i], sum_send_sem.at[i], sum_recv_sem.at[i], target)
            copy.start()
            ends.append(copy)
        proj_out[...] = proj_s[...]
        for copy in ends:
            copy.wait()
        total = (sums[...] + sums_land[0]) + (sums_land[1] + sums_land[2])
        scale = lax.rsqrt(total[0:8] / inner_width + EPSILON)
        coef = total[8:16] * (scale * scale * scale) / inner_width
        for i in range(trow.shape[1] // STEP):
            trow[0:8, i * STEP : (i + 1) * STEP] = jnp.broadcast_to(scale[i : i + 1], (8, STEP))
            trow[8:16, i * STEP : (i + 1) * STEP] = jnp.broadcast_to(coef[i : i + 1], (8, STEP))
        for i in range(col_blocks):
            col_copy(i).wait()


def forward_block(steps_per_seq, width, weights_in, outs_a, outs_b, scratch):
    hid_own, hid_rec, gains, w_own, w_rec, vtap, stap, head_par, wo_own, wo_rec = weights_in
    mixed_out, pre_gate_out, pre_value_out, conv_value_out, pre_shared_out, conv_shared_out = outs_a
    y_out, state_out, rows_out, nt_out = outs_b
    state, vbuf, sbuf, po_own, po_send, square_row = scratch
    chan = mixed_out.shape[1]
    pairs = chan // 128

    @pl.when(pl.program_id(0) % steps_per_seq == 0)
    def _():
        state[...] = jnp.zeros_like(state)
        vbuf[0:8, :] = jnp.zeros((8, vbuf.shape[1]), F32)
        sbuf[0:8, :] = jnp.zeros((8, sbuf.shape[1]), F32)

    h0 = hid_own[...].astype(F32)
    h1 = hid_rec[...].astype(F32)
    square = jnp.sum(h0 * h0, axis=1, keepdims=True) + jnp.sum(h1 * h1, axis=1, keepdims=True)
    recip = lax.rsqrt(square / width + EPSILON)
    n0 = (h0 * gains[0:1, :]).astype(BF16)
    n1 = (h1 * gains[1:2, :]).astype(BF16)
    half = n0.shape[1]
    nt_out[0:half, :] = jnp.transpose(n0)
    nt_out[half : 2 * half, :] = jnp.transpose(n1)
    q = dot(n0, w_own[...]) + dot(n1, w_rec[...])
    pre = q * recip
    gate = pre[:, 0:chan]
    pre_gate_out[...] = gate
    pre_value = pre[:, chan : 2 * chan]
    pre_value_out[...] = pre_value
    pre_shared = pre[:, 2 * chan : 2 * chan + 256]
    pre_shared_out[...] = pre_shared
    vbuf[8 : 8 + STEP, :] = pre_value
    sbuf[8 : 8 + STEP, :] = pre_shared
    conv = jnp.broadcast_to(vtap[4:5, :], (STEP, chan))
    conv_s = jnp.broadcast_to(stap[4:5, :], (STEP, 256))
    for k in range(4):
        conv = conv + vbuf[5 + k : 5 + k + STEP, :] * vtap[k : k + 1, :]
        conv_s = conv_s + sbuf[5 + k : 5 + k + STEP, :] * stap[k : k + 1, :]
    vbuf[0:8, :] = vbuf[STEP : STEP + 8, :]
    sbuf[0:8, :] = sbuf[STEP : STEP + 8, :]
    conv_value_out[...] = conv
    conv_shared_out[...] = conv_s
    x = conv * sigmoid(conv)
    act = conv_s * sigmoid(conv_s)

    head_rows = jnp.transpose(pre[:, 2 * chan + 256 : 2 * chan + 384])[0:8]
    v = head_rows + head_par[0:8, 0:1]
    steps = softplus(v)
    logd = head_par[8:16, 0:1] * steps
    rows_out[0:8, :] = v
    rows_out[16:24, :] = jnp.transpose(jnp.broadcast_to(recip, (STEP, 128)))[0:8]

    upper = (iota((SUB, SUB), 0) <= iota((SUB, SUB), 1)).astype(F32).astype(BF16)
    causal = iota((SUB, SUB), 0) >= iota((SUB, SUB), 1)
    sg = gate * sigmoid(gate)
    for sub in range(STEP // SUB):
        lo, hi = sub * SUB, (sub + 1) * SUB
        cum_r = row_scan(logd[:, lo:hi], upper)
        rows_out[8:16, lo:hi] = cum_r
        cols = jnp.transpose(jnp.concatenate([cum_r, steps[:, lo:hi]], axis=0))
        b_in = act[lo:hi, 0:128]
        b_bf = b_in.astype(BF16)
        c_bf = act[lo:hi, 128:256].astype(BF16)
        b_t = jnp.transpose(b_in).astype(BF16)
        scores = dot_nt(c_bf, b_bf)
        for p in range(pairs):
            pl0, pl1 = p * 128, (p + 1) * 128
            c0 = jnp.broadcast_to(cols[:, 2 * p : 2 * p + 1], (SUB, 128))
            c1 = jnp.broadcast_to(cols[:, 2 * p + 1 : 2 * p + 2], (SUB, 128))
            weights = []
            for col, h in ((c0, 2 * p), (c1, 2 * p + 1)):
                gap = jnp.where(causal, col - cum_r[h : h + 1, :], -1e30)
                weights.append((scores * jnp.exp(gap)).astype(BF16))
            lane = iota((SUB, 128), 1)
            cum_e = jnp.where(lane < 64, c0, c1)
            step_e = spread(cols, 8 + 2 * p, SUB)
            xs = x[lo:hi, pl0:pl1]
            xh = step_e * xs
            inside = dot(jnp.concatenate(weights, axis=1), pair_stack(xh.astype(BF16)))
            held = state[:, pl0:pl1]
            held_bf = held.astype(BF16)
            state_out[lo:hi, pl0:pl1] = held_bf
            carried = dot(c_bf, held_bf)
            y = inside + carried * jnp.exp(cum_e)
            y_out[lo:hi, pl0:pl1] = y
            last = cum_e[SUB - 1 : SUB, :]
            tail = (xh * jnp.exp(last - cum_e)).astype(BF16)
            state[:, pl0:pl1] = held * jnp.exp(last) + dot(b_t, tail)
            y = y + vtap[5:6, pl0:pl1] * xs
            mixed_out[lo:hi, pl0:pl1] = (y * sg[lo:hi, pl0:pl1]).astype(BF16)
    mix = mixed_out[...].astype(F32)
    weighted = (mix * vtap[6:7, :]).astype(BF16)
    po_own[...] = dot(weighted, wo_own[...]).astype(BF16)
    po_send[...] = dot(weighted, wo_rec[...]).astype(BF16)
    square_row[...] = head_sums(jnp.ones((16, chan), BF16), mix * mix)[0:1]


def backward_kernel(
    steps_per_seq,
    cot_own,
    cot_rec,
    wo_own,
    wo_rec,
    trow,
    rows_in,
    mixed,
    pre_gate,
    pre_value,
    conv_value,
    pre_shared,
    conv_shared,
    y_in,
    state_in,
    w_own,
    w_rec,
    vtap,
    stap,
    head_par,
    sel_ref,
    hid_own,
    hid_rec,
    p_out,
    dn_own,
    dn_rec,
    rsum_out,
    acc_v,
    acc_s,
    acc_h,
    acc_n,
    go_own,
    go_rec,
    grad,
    vbuf,
    sbuf,
    dxbuf,
    dbbuf,
):
    chan = mixed.shape[1]
    pairs = chan // 128

    @pl.when(pl.program_id(0) == 0)
    def _():
        acc_v[...] = jnp.zeros_like(acc_v)
        acc_s[...] = jnp.zeros_like(acc_s)
        acc_h[...] = jnp.zeros_like(acc_h)
        acc_n[...] = jnp.zeros_like(acc_n)
        go_own[...] = jnp.zeros_like(go_own)
        go_rec[...] = jnp.zeros_like(go_rec)

    @pl.when(pl.program_id(0) % steps_per_seq == 0)
    def _():
        grad[...] = jnp.zeros_like(grad)
        vbuf[STEP : STEP + 8, :] = jnp.zeros((8, vbuf.shape[1]), F32)
        sbuf[STEP : STEP + 8, :] = jnp.zeros((8, sbuf.shape[1]), F32)

    tcol = jnp.transpose(jnp.concatenate([trow[...], rows_in[16:24, :]], axis=0))
    scale = tcol[:, 0:1]
    coef = tcol[:, 8:9]
    recip = tcol[:, 16:17]
    s0 = (cot_own[...].astype(F32) * scale).astype(BF16)
    s1 = (cot_rec[...].astype(F32) * scale).astype(BF16)
    d_weighted = dot_nt(s0, wo_own[...]) + dot_nt(s1, wo_rec[...])
    mix = mixed[...].astype(F32)
    acc_v[48:56, :] += fold8(d_weighted * mix)
    weighted_t = jnp.transpose((mix * vtap[6:7, :]).astype(BF16))
    go_own[...] += dot(weighted_t, s0)
    go_rec[...] += dot(weighted_t, s1)
    d_mixed = d_weighted * vtap[6:7, :] - coef * mix
    gate = pre_gate[...]
    sig = sigmoid(gate)
    silu = gate * sig
    conv = conv_value[...]
    sig_v = sigmoid(conv)
    x = conv * sig_v
    y_scan = y_in[...]
    y = y_scan + vtap[5:6, :] * x
    dy = d_mixed * silu
    d_gate = d_mixed * y * (sig + silu * (1.0 - sig))
    acc_v[40:48, :] += fold8(dy * x)
    conv_s = conv_shared[...]
    sig_s = sigmoid(conv_s)
    act = conv_s * sig_s

    sel = sel_ref[...]
    sel_f = sel.astype(F32)[0:8]
    v = rows_in[0:8, :]
    steps = softplus(v)
    logd = head_par[8:16, 0:1] * steps
    lower = (iota((SUB, SUB), 0) >= iota((SUB, SUB), 1)).astype(F32).astype(BF16)
    strict = (iota((SUB, SUB), 0) < iota((SUB, SUB), 1)).astype(F32).astype(BF16)
    causal_t = iota((SUB, SUB), 0) <= iota((SUB, SUB), 1)
    for sub in reversed(range(STEP // SUB)):
        lo, hi = sub * SUB, (sub + 1) * SUB
        cum_r = rows_in[8:16, lo:hi]
        cols = jnp.transpose(jnp.concatenate([cum_r, steps[:, lo:hi]], axis=0))
        b_bf = act[lo:hi, 0:128].astype(BF16)
        c_in = act[lo:hi, 128:256]
        c_bf = c_in.astype(BF16)
        c_t = jnp.transpose(c_in).astype(BF16)
        scores_t = dot_nt(b_bf, c_bf)
        d_scores = jnp.zeros((SUB, SUB), F32)
        db = jnp.zeros((SUB, 128), F32)
        dc = jnp.zeros((SUB, 128), F32)
        z_sum = jnp.zeros((8, SUB), F32)
        e_sum = jnp.zeros((8, SUB), F32)
        f_sum = jnp.zeros((8, SUB), F32)
        gh = jnp.zeros((8, 1), F32)
        for p in range(pairs):
            pl0, pl1 = p * 128, (p + 1) * 128
            c0 = jnp.broadcast_to(cols[:, 2 * p : 2 * p + 1], (SUB, 128))
            c1 = jnp.broadcast_to(cols[:, 2 * p + 1 : 2 * p + 2], (SUB, 128))
            decays = []
            for col, h in ((c0, 2 * p), (c1, 2 * p + 1)):
                gap = jnp.where(causal_t, cum_r[h : h + 1, :] - col, -1e30)
                decays.append(jnp.exp(gap))
            weights = [(scores_t * d).astype(BF16) for d in decays]
            lane = iota((SUB, 128), 1)
            cum_e = jnp.where(lane < 64, c0, c1)
            step_e = spread(cols, 8 + 2 * p, SUB)
            xs = x[lo:hi, pl0:pl1]
            xh = step_e * xs
            xh_bf = xh.astype(BF16)
            dys = dy[lo:hi, pl0:pl1]
            dys_bf = dys.astype(BF16)
            stack = pair_stack(dys_bf)
            inner = dot(jnp.concatenate(weights, axis=1), stack)
            d_pair = dot_nt(xh_bf, stack)
            d_scores = d_scores + decays[0] * d_pair[:, 0:128] + decays[1] * d_pair[:, 128:256]
            last = cum_e[SUB - 1 : SUB, :]
            tail_e = jnp.exp(last - cum_e)
            g = grad[:, pl0:pl1]
            g_bf = g.astype(BF16)
            outer = dot(b_bf, g_bf) * tail_e
            u = inner + outer
            dxbuf[lo:hi, pl0:pl1] = step_e * u + vtap[5:6, pl0:pl1] * dys
            db = db + dot_nt((xh * tail_e).astype(BF16), g_bf)
            dya = (dys * jnp.exp(cum_e)).astype(BF16)
            held = state_in[lo:hi, pl0:pl1]
            dc = dc + dot_nt(dya, held)
            sel_p = sel[:, pl0:pl1]
            z_sum = z_sum + head_sums(
                sel_p, dys_bf.astype(F32) * y_in[lo:hi, pl0:pl1] - xh_bf.astype(F32) * inner
            )
            e_sum = e_sum + head_sums(sel_p, xh * outer)
            f_sum = f_sum + head_sums(sel_p, xs * u)
            decay_row = jnp.exp(last)
            gh_row = decay_row * jnp.sum(g * held.astype(F32), axis=0, keepdims=True)
            gh = gh + jnp.sum(sel_f[:, pl0:pl1] * gh_row, axis=1, keepdims=True)
            grad[:, pl0:pl1] = g * decay_row + dot(c_t, dya)
        ds_bf = d_scores.astype(BF16)
        dbbuf[lo:hi, 0:128] = db + dot(ds_bf, c_bf)
        dbbuf[lo:hi, 128:256] = dc + dot(jnp.transpose(d_scores).astype(BF16), b_bf)
        d_log = row_scan(z_sum, lower) + row_scan(e_sum, strict) + gh
        d_step = (f_sum + d_log * head_par[8:16, 0:1]) * sigmoid(v[:, lo:hi])
        acc_h[0:8, :] += d_log * logd[:, lo:hi]
        acc_h[8:16, :] += d_step
        pre_step = v[:, lo:hi] - head_par[0:8, 0:1]
        rsum_out[:, lo:hi] = jnp.broadcast_to(
            jnp.sum(d_step * pre_step, axis=0, keepdims=True), (8, SUB)
        )
        d_cols = jnp.transpose(jnp.concatenate([d_step, jnp.zeros((120, SUB), F32)], axis=0))
        p_out[lo:hi, 2 * chan + 256 : 2 * chan + 384] = (recip[lo:hi] * d_cols).astype(BF16)

    d_conv = dxbuf[...] * (sig_v + x * (1.0 - sig_v))
    d_conv_s = dbbuf[...] * (sig_s + act * (1.0 - sig_s))
    vbuf[0:STEP, :] = d_conv
    sbuf[0:STEP, :] = d_conv_s
    acc_v[32:40, :] += fold8(d_conv)
    acc_s[32:40, :] += fold8(d_conv_s)
    pv = pre_value[...]
    ps = pre_shared[...]
    d_value = jnp.zeros((STEP, chan), F32)
    d_shared = jnp.zeros((STEP, 256), F32)
    for k in range(4):
        moved = vbuf[3 - k : 3 - k + STEP, :]
        d_value = d_value + vtap[k : k + 1, :] * moved
        acc_v[8 * k : 8 * k + 8, :] += fold8(pv * moved)
        moved = sbuf[3 - k : 3 - k + STEP, :]
        d_shared = d_shared + stap[k : k + 1, :] * moved
        acc_s[8 * k : 8 * k + 8, :] += fold8(ps * moved)
    vbuf[STEP : STEP + 8, :] = vbuf[0:8, :]
    sbuf[STEP : STEP + 8, :] = sbuf[0:8, :]
    p_out[:, 0:chan] = (recip * d_gate).astype(BF16)
    p_out[:, chan : 2 * chan] = (recip * d_value).astype(BF16)
    p_out[:, 2 * chan : 2 * chan + 256] = (recip * d_shared).astype(BF16)
    ones = jnp.ones((16, chan), BF16)
    rsum_out[...] += head_sums(ones, d_gate * gate + d_value * pv)
    rsum_out[...] += head_sums(ones[:, 0:256], d_shared * ps)
    pb = p_out[...]
    for n, (hid, weight, dn) in enumerate(((hid_own, w_own, dn_own), (hid_rec, w_rec, dn_rec))):
        part = dot_nt(pb, weight[...])
        dn[...] = part.astype(BF16)
        acc_n[8 * n : 8 * n + 8, :] += fold8(part * hid[...].astype(F32))


def unit_rows(dp):
    return 16 * dp


def big_rows(dp, rows):
    return pl.cdiv(rows, unit_rows(dp)) * unit_rows(dp)


def remote(src, dst, send, recv, target):
    return pltpu.make_async_remote_copy(
        src_ref=src,
        dst_ref=dst,
        send_sem=send,
        recv_sem=recv,
        device_id=target,
        device_id_type=pl.DeviceIdType.MESH,
    )


def greet(targets):
    barrier = pltpu.get_barrier_semaphore()
    for target in targets:
        pl.semaphore_signal(barrier, inc=1, device_id=target, device_id_type=pl.DeviceIdType.MESH)
    pl.semaphore_wait(barrier, len(targets))


def sum_kernel(
    dp,
    normed_t_hbm,
    p_hbm,
    go_own,
    go_rec,
    acc_v,
    acc_s,
    acc_h,
    acc_n,
    rs_in,
    dn_own,
    dn_rec,
    out,
    dn_sum,
    dn_col,
    rs_out,
    acc,
    stage,
    land,
    row_send,
    row_land,
    col_send,
    col_land,
    dn_land,
    rs_land,
    normed_t,
    p_all,
    go_send,
    go_land,
    load_sem,
    send_sem,
    recv_sem,
    pair_send,
    pair_recv,
    dn_send_sem,
    dn_recv_sem,
):
    chan, half = go_own.shape
    wide = p_all.shape[1]
    size = big_rows(dp, 2 * half)
    misc = 3 * size
    tail = out.shape[0] - misc
    bits = dp.bit_length() - 1
    me = lax.axis_index("dp")
    r = lax.axis_index("row")
    c = lax.axis_index("col")
    to_row, to_col = {"row": 1 - r}, {"col": 1 - c}

    def bit_of(k):
        return lax.rem(me // (1 << k), 2)

    def partner(k):
        return {"dp": me + (1 - 2 * bit_of(k)) * (1 << k)}

    def sum8(ref, n):
        return jnp.sum(ref[8 * n : 8 * n + 8, :], axis=0, keepdims=True)

    loads = [
        pltpu.make_async_copy(normed_t_hbm, normed_t, load_sem.at[0]),
        pltpu.make_async_copy(p_hbm, p_all, load_sem.at[1]),
    ]
    for load in loads:
        load.start()
    greet([partner(k) for k in range(bits)] + [to_row, to_col])
    go_send[...] = go_rec[...].astype(BF16)
    go_copy = remote(go_send, go_land, pair_send.at[4], pair_recv.at[4], to_row)
    go_copy.start()

    small = jnp.concatenate([sum8(acc_s, n) for n in range(5)] + [jnp.zeros((3, 256), F32)], axis=0)
    norm_own, norm_rec = [
        jnp.concatenate([sum8(acc_n, n), jnp.zeros((1, 512 - half), F32)], axis=1) for n in (0, 1)
    ]
    pad6 = jnp.zeros((6, 256), F32)
    row_send[half : half + 16, 0:256] = jnp.concatenate(
        [small, norm_rec[:, 0:256], norm_rec[:, 256:512], pad6], axis=0
    ).astype(BF16)
    row_send[half : half + 16, 256:wide] = jnp.zeros((16, wide - 256), BF16)
    row_copy = remote(row_send, row_land, pair_send.at[0], pair_recv.at[0], to_row)

    tokens = dn_own.shape[0]
    cut = tokens // DN_PARTS

    def dn_copy(i, side):
        rows = pl.ds(i * cut, cut)
        if side == 0:
            src, dst, target = dn_rec, dn_land, to_row
        else:
            src, dst, target = dn_sum, dn_col, to_col
        return remote(src.at[rows, :], dst.at[rows, :], dn_send_sem.at[side, i], dn_recv_sem.at[side, i], target)

    dn_rows = [dn_copy(i, 0) for i in range(DN_PARTS)]
    dn_cols = [dn_copy(i, 1) for i in range(DN_PARTS)]
    rs_row = remote(rs_in, rs_land.at[0], pair_send.at[2], pair_recv.at[2], to_row)
    rs_col = remote(rs_out, rs_land.at[1], pair_send.at[3], pair_recv.at[3], to_col)
    rs_row.start()
    for copy in dn_rows:
        copy.start()

    orders = [
        tuple(range(bits)),
        tuple(range(1, bits)) + (0,),
        tuple(range(bits)),
        tuple(range(bits)),
    ]
    bounds = [(0, size), (size, size), (2 * size, size), (misc, tail)]
    lows = {}
    flying = {}

    def span(start, rows):
        return pl.ds(pl.multiple_of(start, 16), rows)

    def copy_of(i, level, src, rows, dst, dst_rows, k):
        return remote(
            src.at[rows, :], dst.at[dst_rows, :], send_sem.at[i, level], recv_sem.at[i, level], partner(k)
        )

    def start_level(i, level):
        base, rows = bounds[i]
        order = orders[i]
        if level < bits:
            k = order[level]
            low = lows.get(i, base)
            part = rows >> (level + 1)
            keep = low + bit_of(k) * part
            give = low + (1 - bit_of(k)) * part
            stage[span(give, part), :] = acc[span(give, part), :].astype(BF16)
            where = base + rows - (rows >> level)
            copy = copy_of(i, level, stage, span(give, part), land, span(where, part), k)
            lows[i] = keep
            flying[i] = (copy, keep, where, part)
        else:
            back = 2 * bits - 1 - level
            k = order[back]
            part = rows >> (back + 1)
            low = lows[i]
            copy = copy_of(i, level, out, span(low, part), out, span(low, part), k)
            lows[i] = low - bit_of(k) * part
            flying[i] = (copy, low, None, part)
        copy.start()

    def end_level(i, level):
        copy, low, where, part = flying[i]
        copy.wait()
        if level < bits:
            total = acc[span(low, part), :] + land[span(where, part), :].astype(F32)
            acc[span(low, part), :] = total
            if level == bits - 1:
                out[span(low, part), :] = total.astype(BF16)
        if level + 1 < 2 * bits:
            start_level(i, level + 1)

    mine = pl.multiple_of(r * half, 128)
    other = pl.multiple_of((1 - r) * half, 128)

    def fill(i, theirs):
        acc[span(i * size + other, half), :] = theirs.astype(F32)
        if size > 2 * half:
            acc[i * size + 2 * half : (i + 1) * size, :] = jnp.zeros((size - 2 * half, chan), F32)
        start_level(i, 0)

    acc[span(mine, half), :] = go_own[...]
    go_copy.wait()
    fill(0, go_land[...])
    for load in loads:
        load.wait()
    for lo in range(0, wide, 384):
        row_send[0:half, lo : lo + 384] = dot(normed_t[half : 2 * half, :], p_all[:, lo : lo + 384]).astype(BF16)
    row_copy.start()
    rs_row.wait()
    rs_out[...] = rs_in[...] + rs_land[0]
    rs_col.start()
    lo = 2 * chan
    acc[misc : misc + half, :] = dot(normed_t[0:half, :], p_all[:, lo:wide])
    acc[span(size + mine, half), :] = dot(normed_t[0:half, :], p_all[:, 0:chan])
    row_copy.wait()
    fill(1, row_land[0:half, 0:chan])
    state = acc[misc : misc + half, 0:256] + row_land[0:half, lo : lo + 256].astype(F32)
    extra = jnp.concatenate([small, norm_own[:, 0:256], norm_own[:, 256:512], pad6], axis=0)
    extra = extra + row_land[half : half + 16, 0:256].astype(F32)
    col_send[0:half, :] = state.astype(BF16)
    col_send[half : half + 16, :] = extra.astype(BF16)
    col_copy = remote(col_send, col_land, pair_send.at[1], pair_recv.at[1], to_col)
    col_copy.start()
    acc[span(2 * size + mine, half), :] = dot(normed_t[0:half, :], p_all[:, chan : 2 * chan])
    fill(2, row_land[0:half, chan : 2 * chan])
    for i in range(DN_PARTS):
        rows = slice(i * cut, (i + 1) * cut)
        dn_rows[i].wait()
        dn_sum[rows, :] = (dn_own[rows, :].astype(F32) + dn_land[rows, :].astype(F32)).astype(BF16)
        dn_cols[i].start()

    lo = 2 * chan + 256
    acc[misc : misc + half, 256:384] = jnp.concatenate(
        [acc[misc : misc + half, 256:320], row_land[0:half, lo : lo + 64].astype(F32)], axis=1
    )
    acc[misc + half : misc + half + 16, 256:384] = jnp.zeros((16, 128), F32)
    first = misc + half + 16
    acc[first : first + 8, :] = jnp.concatenate(
        [sum8(acc_v, n) for n in range(7)] + [jnp.zeros((1, chan), F32)], axis=0
    )
    acc[first + 8 : first + 24, :] = jnp.broadcast_to(
        jnp.sum(acc_h[...], axis=1, keepdims=True), (16, chan)
    )
    if misc + tail > first + 24:
        acc[first + 24 : misc + tail, :] = jnp.zeros((misc + tail - first - 24, chan), F32)
    end_level(0, 0)
    col_copy.wait()
    acc[misc : misc + half + 16, 0:256] = col_send[...].astype(F32) + col_land[...].astype(F32)
    start_level(3, 0)
    end_level(1, 0)
    end_level(2, 0)
    for level in range(1, 2 * bits):
        for i in (0, 1):
            end_level(i, level)
        end_level(3, level - 1)
        end_level(2, level)
    end_level(3, 2 * bits - 1)
    rs_col.wait()
    for copy in dn_cols:
        copy.wait()
    rs_out[...] = rs_out[...] + rs_land[1]


def sum_over_dp(dp, normed_t, p_all, go_own, go_rec, acc_v, acc_s, acc_h, acc_n, rs, dn_own, dn_rec):
    chan, half = go_own.shape
    wide = p_all.shape[1]
    rows = 3 * big_rows(dp, 2 * half) + big_rows(dp, half + 40)
    bits = dp.bit_length() - 1
    tokens = dn_own.shape[0]
    vmem = pl.BlockSpec(memory_space=pltpu.VMEM)
    hbm = pl.BlockSpec(memory_space=pl.ANY)
    act = jax.ShapeDtypeStruct((tokens, half), BF16)
    return pl.pallas_call(
        functools.partial(sum_kernel, dp),
        in_specs=[hbm] * 2 + [vmem] * 8 + [hbm],
        out_specs=[vmem, vmem, hbm, vmem],
        out_shape=[jax.ShapeDtypeStruct((rows, chan), BF16), act, act, jax.ShapeDtypeStruct(rs.shape, F32)],
        scratch_shapes=[
            pltpu.VMEM((rows, chan), F32),
            pltpu.VMEM((rows, chan), BF16),
            pltpu.VMEM((rows, chan), BF16),
            pltpu.VMEM((half + 16, wide), BF16),
            pltpu.VMEM((half + 16, wide), BF16),
            pltpu.VMEM((half + 16, 256), BF16),
            pltpu.VMEM((half + 16, 256), BF16),
            pltpu.VMEM((tokens, half), BF16),
            pltpu.VMEM((2,) + rs.shape, F32),
            pltpu.VMEM(normed_t.shape, BF16),
            pltpu.VMEM(p_all.shape, BF16),
            pltpu.VMEM((chan, half), BF16),
            pltpu.VMEM((chan, half), BF16),
            pltpu.SemaphoreType.DMA((2,)),
            pltpu.SemaphoreType.DMA((4, 2 * bits)),
            pltpu.SemaphoreType.DMA((4, 2 * bits)),
            pltpu.SemaphoreType.DMA((5,)),
            pltpu.SemaphoreType.DMA((5,)),
            pltpu.SemaphoreType.DMA((2, DN_PARTS)),
            pltpu.SemaphoreType.DMA((2, DN_PARTS)),
        ],
        compiler_params=pltpu.CompilerParams(collective_id=0, has_side_effects=True),
        cost_estimate=pl.CostEstimate(flops=1_000_000, bytes_accessed=150_000_000, transcendentals=0),
        name="sum_over_dp",
    )(normed_t, p_all, go_own, go_rec, acc_v, acc_s, acc_h, acc_n, rs, dn_own, dn_rec)


def finish_kernel(
    width,
    size,
    out,
    hid,
    cot,
    dn_sum,
    dn_col,
    proj_own,
    proj_first,
    proj_rest,
    sel,
    trow,
    rows_in,
    rs,
    gains,
    result,
    hidden_grad,
    g_gate,
    g_value,
    g_step,
    g_state,
    g_filter,
    g_shift,
    g_kernel,
    g_offset,
    g_decay,
    g_bias,
    g_skip,
    g_norm,
    g_gated,
    g_output,
):
    half = hid.shape[1]
    hid32 = hid[...].astype(F32)
    recip = rows_in[16:24, :]
    cols = jnp.transpose(jnp.concatenate([trow[0:8, :], rs[...] * recip * recip / width], axis=0))
    early = pl.program_id(0) < pl.num_programs(0) // 2
    proj_col = jnp.where(early, proj_first[...].astype(F32), proj_rest[...].astype(F32))
    proj = proj_own[...].astype(F32) + proj_col
    result[...] = (hid32 + cols[:, 0:1] * proj).astype(BF16)
    d_normed = dn_sum[...].astype(F32) + dn_col[...].astype(F32)
    hidden_grad[...] = cot[...].astype(F32) + d_normed * gains[0:1, :] - cols[:, 8:9] * hid32
    misc = 3 * size

    @pl.when(pl.program_id(0) == 0)
    def _():
        g_output[...] = out[0 : g_output.shape[0], :].astype(F32)
        for n, ref in ((1, g_gate), (2, g_value)):
            ref[:, 0:half] = out[n * size : n * size + half, :].astype(F32)
            ref[:, half : 2 * half] = out[n * size + half : n * size + 2 * half, :].astype(F32)
        g_state[...] = out[misc : misc + half, 0:256].astype(F32)
        step_t = jnp.transpose(out[misc : misc + half, 256:384].astype(F32))
        heads = g_step.shape[0] // 2
        own, rec = step_t[0:heads], step_t[64 : 64 + heads]
        first = lax.axis_index("row") == 0
        g_step[...] = jnp.concatenate([jnp.where(first, own, rec), jnp.where(first, rec, own)], axis=0)
        small = out[misc + half : misc + half + 48, :].astype(F32)
        g_kernel[...] = small[0:4, 0:256]
        g_offset[...] = small[4, 0:256]
        g_norm[0:256] = small[8, 0:256]
        g_norm[256:half] = small[9, 0 : half - 256]
        g_filter[...] = small[16:20]
        g_shift[...] = small[20]
        g_gated[...] = small[22]
        head = jnp.transpose(small[24:40, 0:128])[0:8]
        g_decay[...] = head[0, 0:heads]
        g_bias[...] = head[0, 8 : 8 + heads]
        skip = dot_nt(small[16:32].astype(BF16), sel[...])
        g_skip[...] = skip[5, 0:heads]


def finish(size, heads, out, hid, cot, dn_sum, dn_col, proj_own, proj_first, proj_rest, sel, trow, rows, rs, gains):
    tokens, half = hid.shape
    chan = out.shape[1]
    grid = tokens // STEP
    split = grid // 2

    def blk(cols):
        return pl.BlockSpec((STEP, cols), lambda i: (i, 0))

    def row(count):
        return pl.BlockSpec((count, STEP), lambda i: (0, i))

    def whole(shape):
        return pl.BlockSpec(shape, lambda i: (0,) * len(shape))

    shapes = [
        (half, 2 * chan),
        (half, 2 * chan),
        (2 * heads, half),
        (half, 256),
        (4, chan),
        (chan,),
        (4, 256),
        (256,),
        (heads,),
        (heads,),
        (heads,),
        (half,),
        (chan,),
        (2 * chan, half),
    ]
    return pl.pallas_call(
        functools.partial(finish_kernel, 2 * half, size),
        grid=(grid,),
        in_specs=[
            whole(out.shape),
            blk(half),
            blk(half),
            blk(half),
            blk(half),
            blk(half),
            pl.BlockSpec((STEP, half), lambda i: (jnp.minimum(i, split - 1), 0)),
            pl.BlockSpec((STEP, half), lambda i: (jnp.maximum(i - split, 0), 0)),
            whole(sel.shape),
            row(16),
            row(24),
            row(8),
            whole((8, half)),
        ],
        out_specs=[blk(half), blk(half)] + [whole(shape) for shape in shapes],
        out_shape=[
            jax.ShapeDtypeStruct((tokens, half), BF16),
            jax.ShapeDtypeStruct((tokens, half), F32),
        ]
        + [jax.ShapeDtypeStruct(shape, F32) for shape in shapes],
        cost_estimate=pl.CostEstimate(flops=20_000_000, bytes_accessed=20_000_000, transcendentals=0),
        name="finish",
    )(out, hid, cot, dn_sum, dn_col, proj_own, proj_first, proj_rest, sel, trow, rows, rs, gains)


def swap(x, axis):
    return lax.ppermute(x, axis, SWAP)


def body(
    hidden,
    gate_proj,
    value_proj,
    step_proj,
    state_proj,
    value_filter,
    value_shift,
    shared_kernel,
    shared_offset,
    decay_log,
    step_bias,
    skip_gain,
    input_gain,
    gated_gain,
    output_proj,
    cotangent,
):
    tokens, half = hidden.shape
    width = 2 * half
    chan = gated_gain.shape[0]
    inner_width = 4 * chan
    heads = decay_log.shape[0]
    r = lax.axis_index("row")
    dp = lax.axis_size("dp")
    seq_len = min(LEN, tokens)
    steps_per_seq = seq_len // STEP
    grid = tokens // STEP

    def cut(x, start, size, axis):
        return lax.dynamic_slice_in_dim(x, start * size, size, axis)

    def packed(side):
        return jnp.concatenate(
            [
                cut(gate_proj, side, chan, 1),
                cut(value_proj, side, chan, 1),
                state_proj,
                jnp.pad(cut(step_proj, side, heads, 1), ((0, 0), (0, 128 - heads))),
            ],
            axis=1,
        )

    w_own = packed(r)
    w_rec = swap(packed(1 - r), "row")
    hid_rec = swap(hidden, "row")
    cot_rec = swap(cotangent, "row")
    wo_own = cut(output_proj, r, chan, 0)
    wo_part = cut(output_proj, 1 - r, chan, 0)
    wo_rec = swap(wo_part, "row")
    gain_f = gated_gain.astype(F32)
    gain_rec = swap(input_gain, "row")
    gains = jnp.concatenate([input_gain[None], gain_rec[None], jnp.zeros((6, half), F32)], axis=0)

    skip_lane = jnp.repeat(skip_gain, chan // heads)
    vtap = jnp.concatenate(
        [value_filter, value_shift[None], skip_lane[None], gain_f[None], jnp.zeros((1, chan), F32)], axis=0
    )
    stap = jnp.concatenate([shared_kernel, shared_offset[None], jnp.zeros((3, 256), F32)], axis=0)
    pad_h = (0, 8 - heads)
    head_par = jnp.concatenate([jnp.pad(step_bias, pad_h), jnp.pad(-jnp.exp(decay_log), pad_h)])
    head_par = jnp.broadcast_to(head_par[:, None], (16, 128))

    wide = w_own.shape[1]

    last = grid - 1
    col_blocks = grid // 2

    def blk(cols):
        return pl.BlockSpec((STEP, cols), lambda i: (jnp.minimum(i, last), 0))

    def row_blk(count):
        return pl.BlockSpec((count, STEP), lambda i: (0, jnp.minimum(i, last)))

    def whole(shape):
        return pl.BlockSpec(shape, lambda i: (0, 0))

    def arr(cols, dtype=F32):
        return jax.ShapeDtypeStruct((tokens, cols), dtype)

    (
        mixed,
        proj_own,
        proj_first,
        trow,
        pre_gate,
        pre_value,
        conv_value,
        pre_shared,
        conv_shared,
        y_scan,
        states,
        rows,
        normed_t,
    ) = pl.pallas_call(
        functools.partial(forward_kernel, steps_per_seq, width, inner_width, col_blocks),
        grid=(grid + 1,),
        in_specs=[
            blk(half),
            blk(half),
            whole((8, half)),
            whole((half, wide)),
            whole((half, wide)),
            whole((8, chan)),
            whole((8, 256)),
            whole((16, 128)),
            whole((chan, half)),
            whole((chan, half)),
            pl.BlockSpec((STEP, half), lambda i: (jnp.maximum(i - 1, 0), 0)),
        ],
        out_specs=[
            blk(chan),
            whole((tokens, half)),
            pl.BlockSpec(memory_space=pl.ANY),
            whole((16, tokens)),
            blk(chan),
            blk(chan),
            blk(chan),
            blk(256),
            blk(256),
            blk(chan),
            blk(chan),
            row_blk(24),
            row_blk(width),
        ],
        out_shape=[
            arr(chan, BF16),
            arr(half, BF16),
            jax.ShapeDtypeStruct((col_blocks * STEP, half), BF16),
            jax.ShapeDtypeStruct((16, tokens), F32),
            arr(chan),
            arr(chan),
            arr(chan),
            arr(256),
            arr(256),
            arr(chan),
            arr(chan, BF16),
            jax.ShapeDtypeStruct((24, tokens), F32),
            jax.ShapeDtypeStruct((width, tokens), BF16),
        ],
        scratch_shapes=[
            pltpu.VMEM((128, chan), F32),
            pltpu.VMEM((STEP + 8, chan), F32),
            pltpu.VMEM((STEP + 8, 256), F32),
            pltpu.VMEM((tokens, half), BF16),
            pltpu.VMEM((tokens, half), BF16),
            pltpu.VMEM((tokens, half), BF16),
            pltpu.VMEM((tokens, half), BF16),
            pltpu.VMEM((16, STEP), F32),
            pltpu.VMEM((3, 16, STEP), F32),
            pltpu.SemaphoreType.DMA((grid,)),
            pltpu.SemaphoreType.DMA((grid,)),
            pltpu.SemaphoreType.DMA((col_blocks,)),
            pltpu.SemaphoreType.DMA((col_blocks,)),
            pltpu.SemaphoreType.DMA((3,)),
            pltpu.SemaphoreType.DMA((3,)),
        ],
        compiler_params=pltpu.CompilerParams(collective_id=1, has_side_effects=True),
        cost_estimate=pl.CostEstimate(flops=12_000_000_000, bytes_accessed=40_000_000, transcendentals=8_000_000),
        name="forward_core",
    )(hidden, hid_rec, gains, w_own, w_rec, vtap, stap, head_par, wo_own, wo_rec, cotangent)
    proj_rest = swap(proj_own[col_blocks * STEP :], "col")

    lane_head = jnp.arange(chan) // (chan // heads)
    sel = (jnp.arange(16)[:, None] == lane_head[None, :]).astype(BF16)
    def rblk(cols):
        return pl.BlockSpec((STEP, cols), lambda i: (last - i, 0))

    def rrow(count):
        return pl.BlockSpec((count, STEP), lambda i: (0, last - i))

    p_all, dn_own, dn_rec, rsum, acc_v, acc_s, acc_h, acc_n, go_own, go_rec = pl.pallas_call(
        functools.partial(backward_kernel, steps_per_seq),
        grid=(grid,),
        in_specs=[
            rblk(half),
            rblk(half),
            whole((chan, half)),
            whole((chan, half)),
            rrow(16),
            rrow(24),
            rblk(chan),
            rblk(chan),
            rblk(chan),
            rblk(chan),
            rblk(256),
            rblk(256),
            rblk(chan),
            rblk(chan),
            whole((half, wide)),
            whole((half, wide)),
            whole((8, chan)),
            whole((8, 256)),
            whole((16, 128)),
            whole((16, chan)),
            rblk(half),
            rblk(half),
        ],
        out_specs=[
            rblk(wide),
            rblk(half),
            rblk(half),
            rrow(8),
            whole((56, chan)),
            whole((40, 256)),
            whole((16, 128)),
            whole((16, half)),
            whole((chan, half)),
            whole((chan, half)),
        ],
        out_shape=[
            arr(wide, BF16),
            arr(half, BF16),
            arr(half, BF16),
            jax.ShapeDtypeStruct((8, tokens), F32),
            jax.ShapeDtypeStruct((56, chan), F32),
            jax.ShapeDtypeStruct((40, 256), F32),
            jax.ShapeDtypeStruct((16, 128), F32),
            jax.ShapeDtypeStruct((16, half), F32),
            jax.ShapeDtypeStruct((chan, half), F32),
            jax.ShapeDtypeStruct((chan, half), F32),
        ],
        scratch_shapes=[
            pltpu.VMEM((128, chan), F32),
            pltpu.VMEM((STEP + 8, chan), F32),
            pltpu.VMEM((STEP + 8, 256), F32),
            pltpu.VMEM((STEP, chan), F32),
            pltpu.VMEM((STEP, 256), F32),
        ],
        cost_estimate=pl.CostEstimate(flops=24_000_000_000, bytes_accessed=60_000_000, transcendentals=8_000_000),
        name="backward_core",
    )(
        cotangent,
        cot_rec,
        wo_own,
        wo_rec,
        trow,
        rows,
        mixed,
        pre_gate,
        pre_value,
        conv_value,
        pre_shared,
        conv_shared,
        y_scan,
        states,
        w_own,
        w_rec,
        vtap,
        stap,
        head_par,
        sel,
        hidden,
        hid_rec,
    )

    out, dn_sum, dn_col, rs = sum_over_dp(
        dp, normed_t, p_all, go_own, go_rec, acc_v, acc_s, acc_h, acc_n, rsum, dn_own, dn_rec
    )
    size = big_rows(dp, 2 * half)
    outs = finish(
        size,
        heads,
        out,
        hidden,
        cotangent,
        dn_sum,
        dn_col,
        proj_own,
        proj_first,
        proj_rest,
        sel,
        trow,
        rows,
        rs,
        gains,
    )
    return tuple(outs[0:4]) + (outs[4].T,) + tuple(outs[5:])


def solution(mesh):
    in_specs = (
        P("dp", "row"),
        P("row", "col"),
        P("row", "col"),
        P("row", "col"),
        P("row", None),
        P(None, ("col", "row")),
        P(("col", "row")),
        P(),
        P(),
        P(("col", "row")),
        P(("col", "row")),
        P(("col", "row")),
        P("row"),
        P(("col", "row")),
        P("col", "row"),
        P("dp", "row"),
    )
    out_specs = (
        P("dp", "row"),
        P("dp", "row"),
        P("row", "col"),
        P("row", "col"),
        P("row", "col"),
        P("row", None),
        P(None, ("col", "row")),
        P(("col", "row")),
        P(),
        P(),
        P(("col", "row")),
        P(("col", "row")),
        P(("col", "row")),
        P("row"),
        P(("col", "row")),
        P("col", "row"),
    )
    return jax.shard_map(body, mesh=mesh, in_specs=in_specs, out_specs=out_specs, check_vma=False)
```

```python
import functools

import jax
import jax.numpy as jnp
from jax import lax
from jax.experimental import pallas as pl
from jax.experimental.pallas import tpu as pltpu
from jax.sharding import PartitionSpec as P

LEN = 2048
EPSILON = 1e-05
SUB = 128
STEP = 256
F32 = jnp.float32
BF16 = jnp.bfloat16
SWAP = [(0, 1), (1, 0)]
DN_PARTS = 4
AR_SPLIT = 2
AR_FAR = (1, 3)
AR_MISC = 3


def dot(a, b):
    return jnp.dot(a, b, preferred_element_type=F32)


def dot_nt(a, b):
    return lax.dot_general(a, b, (((1,), (1,)), ((), ())), preferred_element_type=F32)


def dot_tn(a, b):
    return lax.dot_general(a, b, (((0,), (0,)), ((), ())), preferred_element_type=F32)


def sigmoid(x):
    return 0.5 * jnp.tanh(0.5 * x) + 0.5


def softplus(x):
    return jnp.maximum(x, 0.0) + jnp.log1p(jnp.exp(-jnp.abs(x)))


def fold8(x):
    return jnp.sum(x.reshape(x.shape[0] // 8, 8, x.shape[1]), axis=0)


def row_scan(x, mat):
    hi = x.astype(BF16).astype(F32)
    rest = x - hi
    mid = rest.astype(BF16).astype(F32)
    low = rest - mid
    parts = jnp.concatenate([hi, mid, low, jnp.zeros_like(x)], axis=0).astype(BF16)
    out = dot(parts, mat)
    return out[0:8] + out[8:16] + out[16:24]


def plain_sums(sel, z):
    return dot_nt(sel, z.astype(BF16))[0:8]


def head_sums(sel, z):
    hi = z.astype(BF16)
    low = (z - hi.astype(F32)).astype(BF16)
    return (dot_nt(sel, hi) + dot_nt(sel, low))[0:8]


def iota(shape, dim):
    return lax.broadcasted_iota(jnp.int32, shape, dim)


def spread(cols, first, rows):
    lane = iota((rows, 128), 1)
    return jnp.where(
        lane < 64,
        jnp.broadcast_to(cols[:, first : first + 1], (rows, 128)),
        jnp.broadcast_to(cols[:, first + 1 : first + 2], (rows, 128)),
    )


def pair_stack(x):
    lane = iota(x.shape, 1)
    zero = jnp.zeros_like(x)
    return jnp.concatenate([jnp.where(lane < 64, x, zero), jnp.where(lane < 64, zero, x)], axis=0)


def forward_kernel(
    steps_per_seq,
    width,
    inner_width,
    col_blocks,
    hid_own,
    hid_rec,
    gains,
    w_own,
    w_rec,
    vtap,
    stap,
    head_par,
    wo_own,
    wo_rec,
    cot,
    mixed_out,
    proj_out,
    proj_col,
    trow,
    pre_gate_out,
    pre_value_out,
    conv_value_out,
    pre_shared_out,
    conv_shared_out,
    y_out,
    state_out,
    rows_out,
    nt_out,
    state,
    vbuf,
    sbuf,
    po_own,
    po_send,
    po_land,
    proj_s,
    sums,
    sums_land,
    row_send_sem,
    row_recv_sem,
    col_send_sem,
    col_recv_sem,
    sum_send_sem,
    sum_recv_sem,
):
    chan = mixed_out.shape[1]
    pairs = chan // 128
    step = pl.program_id(0)
    blocks = pl.num_programs(0) - 1
    r = lax.axis_index("row")
    c = lax.axis_index("col")
    targets = [{"row": 1 - r}, {"col": 1 - c}, {"row": 1 - r, "col": 1 - c}]

    def span(i):
        return pl.ds(pl.multiple_of(i * STEP, STEP), STEP)

    def row_copy(i):
        return remote(
            po_send.at[span(i), :], po_land.at[span(i), :], row_send_sem.at[i], row_recv_sem.at[i], targets[0]
        )

    def col_copy(i):
        return remote(
            proj_s.at[span(i), :], proj_col.at[span(i), :], col_send_sem.at[i], col_recv_sem.at[i], targets[1]
        )

    @pl.when(step == 0)
    def _():
        greet(targets)

    @pl.when(step < blocks)
    def _():
        forward_block(
            steps_per_seq,
            width,
            (hid_own, hid_rec, gains, w_own, w_rec, vtap, stap, head_par, wo_own, wo_rec),
            (mixed_out, pre_gate_out, pre_value_out, conv_value_out, pre_shared_out, conv_shared_out),
            (y_out, state_out, rows_out, nt_out),
            (state, vbuf, sbuf, po_own.at[span(step), :], po_send.at[span(step), :], sums.at[pl.ds(step, 1), :]),
        )

    @pl.when(step > 0)
    def _():
        i = step - 1
        row_copy(i).wait()
        part = po_own[span(i), :].astype(F32) + po_land[span(i), :].astype(F32)
        proj_s[span(i), :] = part.astype(BF16)

        @pl.when(i < col_blocks)
        def _():
            col_copy(i).start()

        dots = plain_sums(jnp.ones((16, cot.shape[1]), BF16), part * cot[...].astype(F32))
        sums[pl.ds(8 + i, 1), :] = dots[0:1]

    @pl.when(step < blocks)
    def _():
        row_copy(step).start()

    @pl.when(step == blocks)
    def _():
        ends = []
        for i, target in enumerate(targets):
            copy = remote(sums, sums_land.at[i], sum_send_sem.at[i], sum_recv_sem.at[i], target)
            copy.start()
            ends.append(copy)
        proj_out[...] = proj_s[...]
        for copy in ends:
            copy.wait()
        total = (sums[...] + sums_land[0]) + (sums_land[1] + sums_land[2])
        scale = lax.rsqrt(total[0:8] / inner_width + EPSILON)
        coef = total[8:16] * (scale * scale * scale) / inner_width
        for i in range(trow.shape[1] // STEP):
            trow[0:8, i * STEP : (i + 1) * STEP] = jnp.broadcast_to(scale[i : i + 1], (8, STEP))
            trow[8:16, i * STEP : (i + 1) * STEP] = jnp.broadcast_to(coef[i : i + 1], (8, STEP))
        for i in range(col_blocks):
            col_copy(i).wait()


def forward_block(steps_per_seq, width, weights_in, outs_a, outs_b, scratch):
    hid_own, hid_rec, gains, w_own, w_rec, vtap, stap, head_par, wo_own, wo_rec = weights_in
    mixed_out, pre_gate_out, pre_value_out, conv_value_out, pre_shared_out, conv_shared_out = outs_a
    y_out, state_out, rows_out, nt_out = outs_b
    state, vbuf, sbuf, po_own, po_send, square_row = scratch
    chan = mixed_out.shape[1]
    pairs = chan // 128

    @pl.when(pl.program_id(0) % steps_per_seq == 0)
    def _():
        state[...] = jnp.zeros_like(state)
        vbuf[0:8, :] = jnp.zeros((8, vbuf.shape[1]), F32)
        sbuf[0:8, :] = jnp.zeros((8, sbuf.shape[1]), F32)

    h0 = hid_own[...].astype(F32)
    h1 = hid_rec[...].astype(F32)
    square = jnp.sum(h0 * h0, axis=1, keepdims=True) + jnp.sum(h1 * h1, axis=1, keepdims=True)
    recip = lax.rsqrt(square / width + EPSILON)
    n0 = (h0 * gains[0:1, :]).astype(BF16)
    n1 = (h1 * gains[1:2, :]).astype(BF16)
    half = n0.shape[1]
    nt_out[0:half, :] = jnp.transpose(n0)
    nt_out[half : 2 * half, :] = jnp.transpose(n1)
    q = dot(n0, w_own[...]) + dot(n1, w_rec[...])
    pre = q * recip
    gate = pre[:, 0:chan]
    pre_gate_out[...] = gate
    pre_value = pre[:, chan : 2 * chan]
    pre_value_out[...] = pre_value
    pre_shared = pre[:, 2 * chan : 2 * chan + 256]
    pre_shared_out[...] = pre_shared
    vbuf[8 : 8 + STEP, :] = pre_value
    sbuf[8 : 8 + STEP, :] = pre_shared
    conv = jnp.broadcast_to(vtap[4:5, :], (STEP, chan))
    conv_s = jnp.broadcast_to(stap[4:5, :], (STEP, 256))
    for k in range(4):
        conv = conv + vbuf[5 + k : 5 + k + STEP, :] * vtap[k : k + 1, :]
        conv_s = conv_s + sbuf[5 + k : 5 + k + STEP, :] * stap[k : k + 1, :]
    vbuf[0:8, :] = vbuf[STEP : STEP + 8, :]
    sbuf[0:8, :] = sbuf[STEP : STEP + 8, :]
    conv_value_out[...] = conv
    conv_shared_out[...] = conv_s
    x = conv * sigmoid(conv)
    act = conv_s * sigmoid(conv_s)

    head_rows = jnp.transpose(pre[:, 2 * chan + 256 : 2 * chan + 384])[0:8]
    v = head_rows + head_par[0:8, 0:1]
    steps = softplus(v)
    logd = head_par[8:16, 0:1] * steps
    rows_out[0:8, :] = v
    rows_out[16:24, :] = jnp.transpose(jnp.broadcast_to(recip, (STEP, 128)))[0:8]

    upper = (iota((SUB, SUB), 0) <= iota((SUB, SUB), 1)).astype(F32).astype(BF16)
    causal = iota((SUB, SUB), 0) >= iota((SUB, SUB), 1)
    sg = gate * sigmoid(gate)
    for sub in range(STEP // SUB):
        lo, hi = sub * SUB, (sub + 1) * SUB
        cum_r = row_scan(logd[:, lo:hi], upper)
        rows_out[8:16, lo:hi] = cum_r
        cols = jnp.transpose(jnp.concatenate([cum_r, steps[:, lo:hi]], axis=0))
        b_in = act[lo:hi, 0:128]
        b_bf = b_in.astype(BF16)
        c_bf = act[lo:hi, 128:256].astype(BF16)
        b_t = jnp.transpose(b_in).astype(BF16)
        scores = dot_nt(c_bf, b_bf)
        for p in range(pairs):
            pl0, pl1 = p * 128, (p + 1) * 128
            c0 = jnp.broadcast_to(cols[:, 2 * p : 2 * p + 1], (SUB, 128))
            c1 = jnp.broadcast_to(cols[:, 2 * p + 1 : 2 * p + 2], (SUB, 128))
            weights = []
            for col, h in ((c0, 2 * p), (c1, 2 * p + 1)):
                gap = jnp.where(causal, col - cum_r[h : h + 1, :], -1e30)
                weights.append((scores * jnp.exp(gap)).astype(BF16))
            lane = iota((SUB, 128), 1)
            cum_e = jnp.where(lane < 64, c0, c1)
            step_e = spread(cols, 8 + 2 * p, SUB)
            xs = x[lo:hi, pl0:pl1]
            xh = step_e * xs
            inside = dot(jnp.concatenate(weights, axis=1), pair_stack(xh.astype(BF16)))
            held = state[:, pl0:pl1]
            held_bf = held.astype(BF16)
            state_out[lo:hi, pl0:pl1] = held_bf
            carried = dot(c_bf, held_bf)
            y = inside + carried * jnp.exp(cum_e)
            y_out[lo:hi, pl0:pl1] = y
            last = cum_e[SUB - 1 : SUB, :]
            tail = (xh * jnp.exp(last - cum_e)).astype(BF16)
            state[:, pl0:pl1] = held * jnp.exp(last) + dot(b_t, tail)
            y = y + vtap[5:6, pl0:pl1] * xs
            mixed_out[lo:hi, pl0:pl1] = (y * sg[lo:hi, pl0:pl1]).astype(BF16)
    mix = mixed_out[...].astype(F32)
    weighted = (mix * vtap[6:7, :]).astype(BF16)
    po_own[...] = dot(weighted, wo_own[...]).astype(BF16)
    po_send[...] = dot(weighted, wo_rec[...]).astype(BF16)
    square_row[...] = plain_sums(jnp.ones((16, chan), BF16), mix * mix)[0:1]


def backward_kernel(
    steps_per_seq,
    cot_own,
    cot_rec,
    wo_own,
    wo_rec,
    trow,
    rows_in,
    mixed,
    pre_gate,
    pre_value,
    conv_value,
    pre_shared,
    conv_shared,
    y_in,
    state_in,
    w_own,
    w_rec,
    vtap,
    stap,
    head_par,
    sel_ref,
    hid_own,
    hid_rec,
    p_out,
    dn_own,
    dn_rec,
    rsum_out,
    acc_v,
    acc_s,
    acc_h,
    acc_n,
    go_own,
    go_rec,
    grad,
    vbuf,
    sbuf,
    dxbuf,
    dbbuf,
):
    chan = mixed.shape[1]
    pairs = chan // 128

    @pl.when(pl.program_id(0) == 0)
    def _():
        acc_v[...] = jnp.zeros_like(acc_v)
        acc_s[...] = jnp.zeros_like(acc_s)
        acc_h[...] = jnp.zeros_like(acc_h)
        acc_n[...] = jnp.zeros_like(acc_n)
        go_own[...] = jnp.zeros_like(go_own)
        go_rec[...] = jnp.zeros_like(go_rec)

    @pl.when(pl.program_id(0) % steps_per_seq == 0)
    def _():
        grad[...] = jnp.zeros_like(grad)
        vbuf[STEP : STEP + 8, :] = jnp.zeros((8, vbuf.shape[1]), F32)
        sbuf[STEP : STEP + 8, :] = jnp.zeros((8, sbuf.shape[1]), F32)

    tcol = jnp.transpose(jnp.concatenate([trow[...], rows_in[16:24, :]], axis=0))
    scale = tcol[:, 0:1]
    coef = tcol[:, 8:9]
    recip = tcol[:, 16:17]
    s0 = (cot_own[...].astype(F32) * scale).astype(BF16)
    s1 = (cot_rec[...].astype(F32) * scale).astype(BF16)
    d_weighted = dot_nt(s0, wo_own[...]) + dot_nt(s1, wo_rec[...])
    mix = mixed[...].astype(F32)
    acc_v[48:56, :] += fold8(d_weighted * mix)
    weighted_t = jnp.transpose((mix * vtap[6:7, :]).astype(BF16))
    go_own[...] += dot(weighted_t, s0)
    go_rec[...] += dot(weighted_t, s1)
    d_mixed = d_weighted * vtap[6:7, :] - coef * mix
    gate = pre_gate[...]
    sig = sigmoid(gate)
    silu = gate * sig
    conv = conv_value[...]
    sig_v = sigmoid(conv)
    x = conv * sig_v
    y_scan = y_in[...]
    y = y_scan + vtap[5:6, :] * x
    dy = d_mixed * silu
    d_gate = d_mixed * y * (sig + silu * (1.0 - sig))
    acc_v[40:48, :] += fold8(dy * x)
    conv_s = conv_shared[...]
    sig_s = sigmoid(conv_s)
    act = conv_s * sig_s

    sel = sel_ref[...]
    sel_f = sel.astype(F32)[0:8]
    v = rows_in[0:8, :]
    steps = softplus(v)
    logd = head_par[8:16, 0:1] * steps
    lower = (iota((SUB, SUB), 0) >= iota((SUB, SUB), 1)).astype(F32).astype(BF16)
    strict = (iota((SUB, SUB), 0) < iota((SUB, SUB), 1)).astype(F32).astype(BF16)
    causal_t = iota((SUB, SUB), 0) <= iota((SUB, SUB), 1)
    for sub in reversed(range(STEP // SUB)):
        lo, hi = sub * SUB, (sub + 1) * SUB
        cum_r = rows_in[8:16, lo:hi]
        cols = jnp.transpose(jnp.concatenate([cum_r, steps[:, lo:hi]], axis=0))
        b_bf = act[lo:hi, 0:128].astype(BF16)
        c_in = act[lo:hi, 128:256]
        c_bf = c_in.astype(BF16)
        c_t = jnp.transpose(c_in).astype(BF16)
        scores_t = dot_nt(b_bf, c_bf)
        d_scores = jnp.zeros((SUB, SUB), F32)
        db = jnp.zeros((SUB, 128), F32)
        dc = jnp.zeros((SUB, 128), F32)
        z_sum = jnp.zeros((8, SUB), F32)
        e_sum = jnp.zeros((8, SUB), F32)
        f_sum = jnp.zeros((8, SUB), F32)
        gh = jnp.zeros((8, 1), F32)
        for p in range(pairs):
            pl0, pl1 = p * 128, (p + 1) * 128
            c0 = jnp.broadcast_to(cols[:, 2 * p : 2 * p + 1], (SUB, 128))
            c1 = jnp.broadcast_to(cols[:, 2 * p + 1 : 2 * p + 2], (SUB, 128))
            decays = []
            for col, h in ((c0, 2 * p), (c1, 2 * p + 1)):
                gap = jnp.where(causal_t, cum_r[h : h + 1, :] - col, -1e30)
                decays.append(jnp.exp(gap))
            weights = [(scores_t * d).astype(BF16) for d in decays]
            lane = iota((SUB, 128), 1)
            cum_e = jnp.where(lane < 64, c0, c1)
            step_e = spread(cols, 8 + 2 * p, SUB)
            xs = x[lo:hi, pl0:pl1]
            xh = step_e * xs
            xh_bf = xh.astype(BF16)
            dys = dy[lo:hi, pl0:pl1]
            dys_bf = dys.astype(BF16)
            stack = pair_stack(dys_bf)
            inner = dot(jnp.concatenate(weights, axis=1), stack)
            d_pair = dot_nt(xh_bf, stack)
            d_scores = d_scores + decays[0] * d_pair[:, 0:128] + decays[1] * d_pair[:, 128:256]
            last = cum_e[SUB - 1 : SUB, :]
            tail_e = jnp.exp(last - cum_e)
            g = grad[:, pl0:pl1]
            g_bf = g.astype(BF16)
            outer = dot(b_bf, g_bf) * tail_e
            u = inner + outer
            dxbuf[lo:hi, pl0:pl1] = step_e * u + vtap[5:6, pl0:pl1] * dys
            db = db + dot_nt((xh * tail_e).astype(BF16), g_bf)
            dya = (dys * jnp.exp(cum_e)).astype(BF16)
            held = state_in[lo:hi, pl0:pl1]
            dc = dc + dot_nt(dya, held)
            sel_p = sel[:, pl0:pl1]
            z_sum = z_sum + head_sums(
                sel_p, dys_bf.astype(F32) * y_in[lo:hi, pl0:pl1] - xh_bf.astype(F32) * inner
            )
            e_sum = e_sum + plain_sums(sel_p, xh * outer)
            f_sum = f_sum + plain_sums(sel_p, xs * u)
            decay_row = jnp.exp(last)
            gh_row = decay_row * jnp.sum(g * held.astype(F32), axis=0, keepdims=True)
            gh = gh + jnp.sum(sel_f[:, pl0:pl1] * gh_row, axis=1, keepdims=True)
            grad[:, pl0:pl1] = g * decay_row + dot(c_t, dya)
        ds_bf = d_scores.astype(BF16)
        dbbuf[lo:hi, 0:128] = db + dot(ds_bf, c_bf)
        dbbuf[lo:hi, 128:256] = dc + dot(jnp.transpose(d_scores).astype(BF16), b_bf)
        d_log = row_scan(z_sum, lower) + row_scan(e_sum, strict) + gh
        d_step = (f_sum + d_log * head_par[8:16, 0:1]) * sigmoid(v[:, lo:hi])
        acc_h[0:8, :] += d_log * logd[:, lo:hi]
        acc_h[8:16, :] += d_step
        pre_step = v[:, lo:hi] - head_par[0:8, 0:1]
        rsum_out[:, lo:hi] = jnp.broadcast_to(
            jnp.sum(d_step * pre_step, axis=0, keepdims=True), (8, SUB)
        )
        d_cols = jnp.transpose(jnp.concatenate([d_step, jnp.zeros((120, SUB), F32)], axis=0))
        p_out[lo:hi, 2 * chan + 256 : 2 * chan + 384] = (recip[lo:hi] * d_cols).astype(BF16)

    d_conv = dxbuf[...] * (sig_v + x * (1.0 - sig_v))
    d_conv_s = dbbuf[...] * (sig_s + act * (1.0 - sig_s))
    vbuf[0:STEP, :] = d_conv
    sbuf[0:STEP, :] = d_conv_s
    acc_v[32:40, :] += fold8(d_conv)
    acc_s[32:40, :] += fold8(d_conv_s)
    pv = pre_value[...]
    ps = pre_shared[...]
    d_value = jnp.zeros((STEP, chan), F32)
    d_shared = jnp.zeros((STEP, 256), F32)
    for k in range(4):
        moved = vbuf[3 - k : 3 - k + STEP, :]
        d_value = d_value + vtap[k : k + 1, :] * moved
        acc_v[8 * k : 8 * k + 8, :] += fold8(pv * moved)
        moved = sbuf[3 - k : 3 - k + STEP, :]
        d_shared = d_shared + stap[k : k + 1, :] * moved
        acc_s[8 * k : 8 * k + 8, :] += fold8(ps * moved)
    vbuf[STEP : STEP + 8, :] = vbuf[0:8, :]
    sbuf[STEP : STEP + 8, :] = sbuf[0:8, :]
    p_out[:, 0:chan] = (recip * d_gate).astype(BF16)
    p_out[:, chan : 2 * chan] = (recip * d_value).astype(BF16)
    p_out[:, 2 * chan : 2 * chan + 256] = (recip * d_shared).astype(BF16)
    ones = jnp.ones((16, chan), BF16)
    rsum_out[...] += plain_sums(ones, d_gate * gate + d_value * pv)
    rsum_out[...] += plain_sums(ones[:, 0:256], d_shared * ps)
    pb = p_out[...]
    for n, (hid, weight, dn) in enumerate(((hid_own, w_own, dn_own), (hid_rec, w_rec, dn_rec))):
        part = dot_nt(pb, weight[...])
        dn[...] = part.astype(BF16)
        acc_n[8 * n : 8 * n + 8, :] += fold8(part * hid[...].astype(F32))


def unit_rows(dp):
    return 16 * dp


def misc_rows(dp, rows):
    unit = max(unit_rows(dp), 256)
    return pl.cdiv(rows, unit) * unit


def big_rows(dp, rows):
    return pl.cdiv(rows, unit_rows(dp)) * unit_rows(dp)


def remote(src, dst, send, recv, target):
    return pltpu.make_async_remote_copy(
        src_ref=src,
        dst_ref=dst,
        send_sem=send,
        recv_sem=recv,
        device_id=target,
        device_id_type=pl.DeviceIdType.MESH,
    )


def greet(targets):
    barrier = pltpu.get_barrier_semaphore()
    for target in targets:
        pl.semaphore_signal(barrier, inc=1, device_id=target, device_id_type=pl.DeviceIdType.MESH)
    pl.semaphore_wait(barrier, len(targets))


def sum_kernel(
    dp,
    normed_t_hbm,
    p_hbm,
    go_own,
    go_rec,
    acc_v,
    acc_s,
    acc_h,
    acc_n,
    rs_in,
    dn_own,
    dn_rec,
    out,
    dn_sum,
    dn_col,
    rs_out,
    acc,
    stage,
    land,
    row_send,
    row_land,
    col_send,
    col_land,
    dn_land,
    rs_land,
    normed_t,
    p_all,
    go_send,
    go_land,
    load_sem,
    send_sem,
    recv_sem,
    pair_send,
    pair_recv,
    dn_send_sem,
    dn_recv_sem,
):
    chan, half = go_own.shape
    wide = p_all.shape[1]
    size = big_rows(dp, 2 * half)
    tail = out.shape[0] - 3 * size
    misc = 0
    bits = dp.bit_length() - 1
    me = lax.axis_index("dp")
    r = lax.axis_index("row")
    c = lax.axis_index("col")
    to_row, to_col = {"row": 1 - r}, {"col": 1 - c}

    def bit_of(k):
        return lax.rem(me // (1 << k), 2)

    def partner(k):
        return {"dp": me + (1 - 2 * bit_of(k)) * (1 << k)}

    def sum8(ref, n):
        return jnp.sum(ref[8 * n : 8 * n + 8, :], axis=0, keepdims=True)

    loads = [
        pltpu.make_async_copy(normed_t_hbm, normed_t, load_sem.at[0]),
        pltpu.make_async_copy(p_hbm, p_all, load_sem.at[1]),
    ]
    for load in loads:
        load.start()
    greet([partner(k) for k in range(bits)] + [to_row, to_col])
    go_send[...] = go_rec[...].astype(BF16)
    go_copy = remote(go_send, go_land, pair_send.at[4], pair_recv.at[4], to_row)
    go_copy.start()

    small = jnp.concatenate([sum8(acc_s, n) for n in range(5)] + [jnp.zeros((3, 256), F32)], axis=0)
    norm_own, norm_rec = [
        jnp.concatenate([sum8(acc_n, n), jnp.zeros((1, 512 - half), F32)], axis=1) for n in (0, 1)
    ]
    pad6 = jnp.zeros((6, 256), F32)
    row_send[half : half + 16, 0:256] = jnp.concatenate(
        [small, norm_rec[:, 0:256], norm_rec[:, 256:512], pad6], axis=0
    ).astype(BF16)
    row_send[half : half + 16, 256:wide] = jnp.zeros((16, wide - 256), BF16)
    row_copy = remote(row_send, row_land, pair_send.at[0], pair_recv.at[0], to_row)

    tokens = dn_own.shape[0]
    cut = tokens // DN_PARTS

    def dn_copy(i, side):
        rows = pl.ds(i * cut, cut)
        if side == 0:
            src, dst, target = dn_rec, dn_land, to_row
        else:
            src, dst, target = dn_sum, dn_col, to_col
        return remote(src.at[rows, :], dst.at[rows, :], dn_send_sem.at[side, i], dn_recv_sem.at[side, i], target)

    dn_rows = [dn_copy(i, 0) for i in range(DN_PARTS)]
    dn_cols = [dn_copy(i, 1) for i in range(DN_PARTS)]
    rs_row = remote(rs_in, rs_land.at[0], pair_send.at[2], pair_recv.at[2], to_row)
    rs_col = remote(rs_out, rs_land.at[1], pair_send.at[3], pair_recv.at[3], to_col)
    rs_row.start()
    for copy in dn_rows:
        copy.start()

    near = tuple(range(bits))
    far = tuple(range(1, bits)) + (0,)
    part_rows = size // AR_SPLIT
    bounds = [(tail + n * part_rows, part_rows) for n in range(3 * AR_SPLIT)] + [(misc, tail)]
    orders = [far if n in AR_FAR else near for n in range(3 * AR_SPLIT + 1)]
    misc_chunk = 3 * AR_SPLIT
    lows = {}
    flying = {}

    def span(start, rows):
        return pl.ds(pl.multiple_of(start, 16), rows)

    def copy_of(i, level, src, rows, dst, dst_rows, k):
        return remote(
            src.at[rows, :], dst.at[dst_rows, :], send_sem.at[i, level], recv_sem.at[i, level], partner(k)
        )

    def start_level(i, level):
        base, rows = bounds[i]
        order = orders[i]
        if level < bits:
            k = order[level]
            low = lows.get(i, base)
            part = rows >> (level + 1)
            keep = low + bit_of(k) * part
            give = low + (1 - bit_of(k)) * part
            stage[span(give, part), :] = acc[span(give, part), :].astype(BF16)
            where = base + rows - (rows >> level)
            copy = copy_of(i, level, stage, span(give, part), land, span(where, part), k)
            lows[i] = keep
            flying[i] = (copy, keep, where, part)
        else:
            back = 2 * bits - 1 - level
            k = order[back]
            part = rows >> (back + 1)
            low = lows[i]
            copy = copy_of(i, level, out, span(low, part), out, span(low, part), k)
            lows[i] = low - bit_of(k) * part
            flying[i] = (copy, low, None, part)
        copy.start()

    def end_level(i, level):
        copy, low, where, part = flying[i]
        copy.wait()
        if level < bits:
            total = acc[span(low, part), :] + land[span(where, part), :].astype(F32)
            acc[span(low, part), :] = total
            if level == bits - 1:
                out[span(low, part), :] = total.astype(BF16)
        if level + 1 < 2 * bits:
            start_level(i, level + 1)

    mine = pl.multiple_of(r * half, 128)
    other = pl.multiple_of((1 - r) * half, 128)

    def fill(i, theirs):
        acc[span(tail + i * size + other, half), :] = theirs.astype(F32)
        if size > 2 * half:
            acc[tail + i * size + 2 * half : tail + (i + 1) * size, :] = jnp.zeros((size - 2 * half, chan), F32)
        for n in range(AR_SPLIT):
            start_level(i * AR_SPLIT + n, 0)

    acc[span(tail + mine, half), :] = go_own[...]
    go_copy.wait()
    fill(0, go_land[...])
    for load in loads:
        load.wait()
    for lo in range(0, wide, 384):
        row_send[0:half, lo : lo + 384] = dot(normed_t[half : 2 * half, :], p_all[:, lo : lo + 384]).astype(BF16)
    row_copy.start()
    rs_row.wait()
    rs_out[...] = rs_in[...] + rs_land[0]
    rs_col.start()
    lo = 2 * chan
    acc[misc : misc + half, :] = dot(normed_t[0:half, :], p_all[:, lo:wide])
    acc[span(tail + size + mine, half), :] = dot(normed_t[0:half, :], p_all[:, 0:chan])
    row_copy.wait()
    fill(1, row_land[0:half, 0:chan])
    state = acc[misc : misc + half, 0:256] + row_land[0:half, lo : lo + 256].astype(F32)
    extra = jnp.concatenate([small, norm_own[:, 0:256], norm_own[:, 256:512], pad6], axis=0)
    extra = extra + row_land[half : half + 16, 0:256].astype(F32)
    col_send[0:half, :] = state.astype(BF16)
    col_send[half : half + 16, :] = extra.astype(BF16)
    col_copy = remote(col_send, col_land, pair_send.at[1], pair_recv.at[1], to_col)
    col_copy.start()
    acc[span(tail + 2 * size + mine, half), :] = dot(normed_t[0:half, :], p_all[:, chan : 2 * chan])
    fill(2, row_land[0:half, chan : 2 * chan])
    for i in range(DN_PARTS):
        rows = slice(i * cut, (i + 1) * cut)
        dn_rows[i].wait()
        dn_sum[rows, :] = (dn_own[rows, :].astype(F32) + dn_land[rows, :].astype(F32)).astype(BF16)
        dn_cols[i].start()

    lo = 2 * chan + 256
    acc[misc : misc + half, 256:384] = jnp.concatenate(
        [acc[misc : misc + half, 256:320], row_land[0:half, lo : lo + 64].astype(F32)], axis=1
    )
    acc[misc + half : misc + half + 16, 256:384] = jnp.zeros((16, 128), F32)
    first = misc + half + 16
    acc[first : first + 8, :] = jnp.concatenate(
        [sum8(acc_v, n) for n in range(7)] + [jnp.zeros((1, chan), F32)], axis=0
    )
    acc[first + 8 : first + 24, :] = jnp.broadcast_to(
        jnp.sum(acc_h[...], axis=1, keepdims=True), (16, chan)
    )
    if misc + tail > first + 24:
        acc[first + 24 : misc + tail, :] = jnp.zeros((misc + tail - first - 24, chan), F32)
    for n in range(AR_SPLIT):
        end_level(n, 0)
    col_copy.wait()
    acc[misc : misc + half + 16, 0:256] = col_send[...].astype(F32) + col_land[...].astype(F32)
    start_level(misc_chunk, 0)
    for n in range(AR_SPLIT, misc_chunk):
        end_level(n, 0)
    for level in range(1, 2 * bits):
        for n in range(misc_chunk):
            end_level(n, level)
            if n == AR_MISC:
                end_level(misc_chunk, level - 1)
    end_level(misc_chunk, 2 * bits - 1)
    rs_col.wait()
    for copy in dn_cols:
        copy.wait()
    rs_out[...] = rs_out[...] + rs_land[1]


def sum_over_dp(dp, normed_t, p_all, go_own, go_rec, acc_v, acc_s, acc_h, acc_n, rs, dn_own, dn_rec):
    chan, half = go_own.shape
    wide = p_all.shape[1]
    rows = 3 * big_rows(dp, 2 * half) + misc_rows(dp, half + 48)
    bits = dp.bit_length() - 1
    tokens = dn_own.shape[0]
    vmem = pl.BlockSpec(memory_space=pltpu.VMEM)
    hbm = pl.BlockSpec(memory_space=pl.ANY)
    act = jax.ShapeDtypeStruct((tokens, half), BF16)
    return pl.pallas_call(
        functools.partial(sum_kernel, dp),
        in_specs=[hbm] * 2 + [vmem] * 8 + [hbm],
        out_specs=[vmem, vmem, hbm, vmem],
        out_shape=[jax.ShapeDtypeStruct((rows, chan), BF16), act, act, jax.ShapeDtypeStruct(rs.shape, F32)],
        scratch_shapes=[
            pltpu.VMEM((rows, chan), F32),
            pltpu.VMEM((rows, chan), BF16),
            pltpu.VMEM((rows, chan), BF16),
            pltpu.VMEM((half + 16, wide), BF16),
            pltpu.VMEM((half + 16, wide), BF16),
            pltpu.VMEM((half + 16, 256), BF16),
            pltpu.VMEM((half + 16, 256), BF16),
            pltpu.VMEM((tokens, half), BF16),
            pltpu.VMEM((2,) + rs.shape, F32),
            pltpu.VMEM(normed_t.shape, BF16),
            pltpu.VMEM(p_all.shape, BF16),
            pltpu.VMEM((chan, half), BF16),
            pltpu.VMEM((chan, half), BF16),
            pltpu.SemaphoreType.DMA((2,)),
            pltpu.SemaphoreType.DMA((3 * AR_SPLIT + 1, 2 * bits)),
            pltpu.SemaphoreType.DMA((3 * AR_SPLIT + 1, 2 * bits)),
            pltpu.SemaphoreType.DMA((5,)),
            pltpu.SemaphoreType.DMA((5,)),
            pltpu.SemaphoreType.DMA((2, DN_PARTS)),
            pltpu.SemaphoreType.DMA((2, DN_PARTS)),
        ],
        compiler_params=pltpu.CompilerParams(collective_id=0, has_side_effects=True),
        cost_estimate=pl.CostEstimate(flops=1_000_000, bytes_accessed=150_000_000, transcendentals=0),
        name="sum_over_dp",
    )(normed_t, p_all, go_own, go_rec, acc_v, acc_s, acc_h, acc_n, rs, dn_own, dn_rec)


def finish_kernel(
    width,
    out_rows,
    gate_a,
    gate_b,
    value_a,
    value_b,
    misc,
    hid,
    cot,
    dn_sum,
    dn_col,
    proj_own,
    proj_first,
    proj_rest,
    sel,
    trow,
    rows_in,
    rs,
    gains,
    result,
    hidden_grad,
    g_gate,
    g_value,
    g_step,
    g_state,
    g_filter,
    g_shift,
    g_kernel,
    g_offset,
    g_decay,
    g_bias,
    g_skip,
    g_norm,
    g_gated,
    g_output,
):
    half = hid.shape[1]
    hid32 = hid[...].astype(F32)
    recip = rows_in[16:24, :]
    cols = jnp.transpose(jnp.concatenate([trow[0:8, :], rs[...] * recip * recip / width], axis=0))
    early = pl.program_id(0) < pl.num_programs(0) // 2
    proj_col = jnp.where(early, proj_first[...].astype(F32), proj_rest[...].astype(F32))
    proj = proj_own[...].astype(F32) + proj_col
    result[...] = (hid32 + cols[:, 0:1] * proj).astype(BF16)
    d_normed = dn_sum[...].astype(F32) + dn_col[...].astype(F32)
    hidden_grad[...] = cot[...].astype(F32) + d_normed * gains[0:1, :] - cols[:, 8:9] * hid32
    @pl.when(pl.program_id(0) < half // 128)
    def _():
        g_output[...] = out_rows[...].astype(F32)
        g_gate[:, 0:half] = gate_a[...].astype(F32)
        g_gate[:, half : 2 * half] = gate_b[...].astype(F32)
        g_value[:, 0:half] = value_a[...].astype(F32)
        g_value[:, half : 2 * half] = value_b[...].astype(F32)

    @pl.when(pl.program_id(0) == 0)
    def _():
        g_state[...] = misc[0:half, 0:256].astype(F32)
        step_t = jnp.transpose(misc[0:half, 256:384].astype(F32))
        heads = g_step.shape[0] // 2
        own, rec = step_t[0:heads], step_t[64 : 64 + heads]
        first = lax.axis_index("row") == 0
        g_step[...] = jnp.concatenate([jnp.where(first, own, rec), jnp.where(first, rec, own)], axis=0)
        small = misc[half : half + 48, :].astype(F32)
        g_kernel[...] = small[0:4, 0:256]
        g_offset[...] = small[4, 0:256]
        g_norm[0:256] = small[8, 0:256]
        g_norm[256:half] = small[9, 0 : half - 256]
        g_filter[...] = small[16:20]
        g_shift[...] = small[20]
        g_gated[...] = small[22]
        head = jnp.transpose(small[24:40, 0:128])[0:8]
        g_decay[...] = head[0, 0:heads]
        g_bias[...] = head[0, 8 : 8 + heads]
        skip = dot_nt(small[16:32].astype(BF16), sel[...])
        g_skip[...] = skip[5, 0:heads]


def finish(size, heads, out, hid, cot, dn_sum, dn_col, proj_own, proj_first, proj_rest, sel, trow, rows, rs, gains):
    tokens, half = hid.shape
    chan = out.shape[1]
    size_f = tokens // 4
    grid = 4
    split = 2

    def blk(cols):
        return pl.BlockSpec((size_f, cols), lambda i: (i, 0))

    def row(count):
        return pl.BlockSpec((count, size_f), lambda i: (0, i))

    def whole(shape):
        return pl.BlockSpec(shape, lambda i: (0,) * len(shape))

    parts = half // 128
    tail = out.shape[0] - 3 * size

    def part(start):
        return pl.BlockSpec((128, chan), lambda i: (start // 128 + jnp.minimum(i, parts - 1), 0))

    def streamed(rows, cols):
        return pl.BlockSpec((rows // parts, cols), lambda i: (jnp.minimum(i, parts - 1), 0))

    small = [
        (2 * heads, half),
        (half, 256),
        (4, chan),
        (chan,),
        (4, 256),
        (256,),
        (heads,),
        (heads,),
        (heads,),
        (half,),
        (chan,),
    ]
    big = (half, 2 * chan)
    shapes = [big, big] + small + [(2 * chan, half)]
    return pl.pallas_call(
        functools.partial(finish_kernel, 2 * half),
        grid=(grid,),
        in_specs=[
            pl.BlockSpec((256, half), lambda i: (tail // 256 + jnp.minimum(i, parts - 1), 0)),
            part(tail + size),
            part(tail + size + half),
            part(tail + 2 * size),
            part(tail + 2 * size + half),
            whole((tail, chan)),
            blk(half),
            blk(half),
            blk(half),
            blk(half),
            blk(half),
            pl.BlockSpec((size_f, half), lambda i: (jnp.minimum(i, split - 1), 0)),
            pl.BlockSpec((size_f, half), lambda i: (jnp.maximum(i - split, 0), 0)),
            whole(sel.shape),
            row(16),
            row(24),
            row(8),
            whole((8, half)),
        ],
        out_specs=[blk(half), blk(half), streamed(*big), streamed(*big)]
        + [whole(shape) for shape in small]
        + [streamed(2 * chan, half)],
        out_shape=[
            jax.ShapeDtypeStruct((tokens, half), BF16),
            jax.ShapeDtypeStruct((tokens, half), F32),
        ]
        + [jax.ShapeDtypeStruct(shape, F32) for shape in shapes],
        cost_estimate=pl.CostEstimate(flops=20_000_000, bytes_accessed=20_000_000, transcendentals=0),
        name="finish",
    )(
        out,
        out,
        out,
        out,
        out,
        out,
        hid,
        cot,
        dn_sum,
        dn_col,
        proj_own,
        proj_first,
        proj_rest,
        sel,
        trow,
        rows,
        rs,
        gains,
    )


def swap(x, axis):
    return lax.ppermute(x, axis, SWAP)


def body(
    hidden,
    gate_proj,
    value_proj,
    step_proj,
    state_proj,
    value_filter,
    value_shift,
    shared_kernel,
    shared_offset,
    decay_log,
    step_bias,
    skip_gain,
    input_gain,
    gated_gain,
    output_proj,
    cotangent,
):
    tokens, half = hidden.shape
    width = 2 * half
    chan = gated_gain.shape[0]
    inner_width = 4 * chan
    heads = decay_log.shape[0]
    r = lax.axis_index("row")
    dp = lax.axis_size("dp")
    seq_len = min(LEN, tokens)
    steps_per_seq = seq_len // STEP
    grid = tokens // STEP

    def cut(x, start, size, axis):
        return lax.dynamic_slice_in_dim(x, start * size, size, axis)

    def packed(side):
        return jnp.concatenate(
            [
                cut(gate_proj, side, chan, 1),
                cut(value_proj, side, chan, 1),
                state_proj,
                jnp.pad(cut(step_proj, side, heads, 1), ((0, 0), (0, 128 - heads))),
            ],
            axis=1,
        )

    w_own = packed(r)
    w_rec = swap(packed(1 - r), "row")
    hid_rec = swap(hidden, "row")
    cot_rec = swap(cotangent, "row")
    wo_own = cut(output_proj, r, chan, 0)
    wo_part = cut(output_proj, 1 - r, chan, 0)
    wo_rec = swap(wo_part, "row")
    gain_f = gated_gain.astype(F32)
    gain_rec = swap(input_gain, "row")
    gains = jnp.concatenate([input_gain[None], gain_rec[None], jnp.zeros((6, half), F32)], axis=0)

    skip_lane = jnp.repeat(skip_gain, chan // heads)
    vtap = jnp.concatenate(
        [value_filter, value_shift[None], skip_lane[None], gain_f[None], jnp.zeros((1, chan), F32)], axis=0
    )
    stap = jnp.concatenate([shared_kernel, shared_offset[None], jnp.zeros((3, 256), F32)], axis=0)
    pad_h = (0, 8 - heads)
    head_par = jnp.concatenate([jnp.pad(step_bias, pad_h), jnp.pad(-jnp.exp(decay_log), pad_h)])
    head_par = jnp.broadcast_to(head_par[:, None], (16, 128))

    wide = w_own.shape[1]

    last = grid - 1
    col_blocks = grid // 2

    def blk(cols):
        return pl.BlockSpec((STEP, cols), lambda i: (jnp.minimum(i, last), 0))

    def row_blk(count):
        return pl.BlockSpec((count, STEP), lambda i: (0, jnp.minimum(i, last)))

    def whole(shape):
        return pl.BlockSpec(shape, lambda i: (0, 0))

    def arr(cols, dtype=F32):
        return jax.ShapeDtypeStruct((tokens, cols), dtype)

    (
        mixed,
        proj_own,
        proj_first,
        trow,
        pre_gate,
        pre_value,
        conv_value,
        pre_shared,
        conv_shared,
        y_scan,
        states,
        rows,
        normed_t,
    ) = pl.pallas_call(
        functools.partial(forward_kernel, steps_per_seq, width, inner_width, col_blocks),
        grid=(grid + 1,),
        in_specs=[
            blk(half),
            blk(half),
            whole((8, half)),
            whole((half, wide)),
            whole((half, wide)),
            whole((8, chan)),
            whole((8, 256)),
            whole((16, 128)),
            whole((chan, half)),
            whole((chan, half)),
            pl.BlockSpec((STEP, half), lambda i: (jnp.maximum(i - 1, 0), 0)),
        ],
        out_specs=[
            blk(chan),
            whole((tokens, half)),
            pl.BlockSpec(memory_space=pl.ANY),
            whole((16, tokens)),
            blk(chan),
            blk(chan),
            blk(chan),
            blk(256),
            blk(256),
            blk(chan),
            blk(chan),
            row_blk(24),
            row_blk(width),
        ],
        out_shape=[
            arr(chan, BF16),
            arr(half, BF16),
            jax.ShapeDtypeStruct((col_blocks * STEP, half), BF16),
            jax.ShapeDtypeStruct((16, tokens), F32),
            arr(chan),
            arr(chan),
            arr(chan),
            arr(256),
            arr(256),
            arr(chan),
            arr(chan, BF16),
            jax.ShapeDtypeStruct((24, tokens), F32),
            jax.ShapeDtypeStruct((width, tokens), BF16),
        ],
        scratch_shapes=[
            pltpu.VMEM((128, chan), F32),
            pltpu.VMEM((STEP + 8, chan), F32),
            pltpu.VMEM((STEP + 8, 256), F32),
            pltpu.VMEM((tokens, half), BF16),
            pltpu.VMEM((tokens, half), BF16),
            pltpu.VMEM((tokens, half), BF16),
            pltpu.VMEM((tokens, half), BF16),
            pltpu.VMEM((16, STEP), F32),
            pltpu.VMEM((3, 16, STEP), F32),
            pltpu.SemaphoreType.DMA((grid,)),
            pltpu.SemaphoreType.DMA((grid,)),
            pltpu.SemaphoreType.DMA((col_blocks,)),
            pltpu.SemaphoreType.DMA((col_blocks,)),
            pltpu.SemaphoreType.DMA((3,)),
            pltpu.SemaphoreType.DMA((3,)),
        ],
        compiler_params=pltpu.CompilerParams(collective_id=1, has_side_effects=True),
        cost_estimate=pl.CostEstimate(flops=12_000_000_000, bytes_accessed=40_000_000, transcendentals=8_000_000),
        name="forward_core",
    )(hidden, hid_rec, gains, w_own, w_rec, vtap, stap, head_par, wo_own, wo_rec, cotangent)
    proj_rest = swap(proj_own[col_blocks * STEP :], "col")

    lane_head = jnp.arange(chan) // (chan // heads)
    sel = (jnp.arange(16)[:, None] == lane_head[None, :]).astype(BF16)
    def rblk(cols):
        return pl.BlockSpec((STEP, cols), lambda i: (last - i, 0))

    def rrow(count):
        return pl.BlockSpec((count, STEP), lambda i: (0, last - i))

    p_all, dn_own, dn_rec, rsum, acc_v, acc_s, acc_h, acc_n, go_own, go_rec = pl.pallas_call(
        functools.partial(backward_kernel, steps_per_seq),
        grid=(grid,),
        in_specs=[
            rblk(half),
            rblk(half),
            whole((chan, half)),
            whole((chan, half)),
            rrow(16),
            rrow(24),
            rblk(chan),
            rblk(chan),
            rblk(chan),
            rblk(chan),
            rblk(256),
            rblk(256),
            rblk(chan),
            rblk(chan),
            whole((half, wide)),
            whole((half, wide)),
            whole((8, chan)),
            whole((8, 256)),
            whole((16, 128)),
            whole((16, chan)),
            rblk(half),
            rblk(half),
        ],
        out_specs=[
            rblk(wide),
            rblk(half),
            rblk(half),
            rrow(8),
            whole((56, chan)),
            whole((40, 256)),
            whole((16, 128)),
            whole((16, half)),
            whole((chan, half)),
            whole((chan, half)),
        ],
        out_shape=[
            arr(wide, BF16),
            arr(half, BF16),
            arr(half, BF16),
            jax.ShapeDtypeStruct((8, tokens), F32),
            jax.ShapeDtypeStruct((56, chan), F32),
            jax.ShapeDtypeStruct((40, 256), F32),
            jax.ShapeDtypeStruct((16, 128), F32),
            jax.ShapeDtypeStruct((16, half), F32),
            jax.ShapeDtypeStruct((chan, half), F32),
            jax.ShapeDtypeStruct((chan, half), F32),
        ],
        scratch_shapes=[
            pltpu.VMEM((128, chan), F32),
            pltpu.VMEM((STEP + 8, chan), F32),
            pltpu.VMEM((STEP + 8, 256), F32),
            pltpu.VMEM((STEP, chan), F32),
            pltpu.VMEM((STEP, 256), F32),
        ],
        cost_estimate=pl.CostEstimate(flops=24_000_000_000, bytes_accessed=60_000_000, transcendentals=8_000_000),
        name="backward_core",
    )(
        cotangent,
        cot_rec,
        wo_own,
        wo_rec,
        trow,
        rows,
        mixed,
        pre_gate,
        pre_value,
        conv_value,
        pre_shared,
        conv_shared,
        y_scan,
        states,
        w_own,
        w_rec,
        vtap,
        stap,
        head_par,
        sel,
        hidden,
        hid_rec,
    )

    out, dn_sum, dn_col, rs = sum_over_dp(
        dp, normed_t, p_all, go_own, go_rec, acc_v, acc_s, acc_h, acc_n, rsum, dn_own, dn_rec
    )
    size = big_rows(dp, 2 * half)
    outs = finish(
        size,
        heads,
        out,
        hidden,
        cotangent,
        dn_sum,
        dn_col,
        proj_own,
        proj_first,
        proj_rest,
        sel,
        trow,
        rows,
        rs,
        gains,
    )
    return tuple(outs[0:4]) + (outs[4].T,) + tuple(outs[5:])


def solution(mesh):
    in_specs = (
        P("dp", "row"),
        P("row", "col"),
        P("row", "col"),
        P("row", "col"),
        P("row", None),
        P(None, ("col", "row")),
        P(("col", "row")),
        P(),
        P(),
        P(("col", "row")),
        P(("col", "row")),
        P(("col", "row")),
        P("row"),
        P(("col", "row")),
        P("col", "row"),
        P("dp", "row"),
    )
    out_specs = (
        P("dp", "row"),
        P("dp", "row"),
        P("row", "col"),
        P("row", "col"),
        P("row", "col"),
        P("row", None),
        P(None, ("col", "row")),
        P(("col", "row")),
        P(),
        P(),
        P(("col", "row")),
        P(("col", "row")),
        P(("col", "row")),
        P("row"),
        P(("col", "row")),
        P("col", "row"),
    )
    return jax.shard_map(body, mesh=mesh, in_specs=in_specs, out_specs=out_specs, check_vma=False)
```

```python
import functools

import jax
import jax.numpy as jnp
from jax import lax
from jax.experimental import pallas as pl
from jax.experimental.pallas import tpu as pltpu
from jax.sharding import PartitionSpec as P

LEN = 2048
EPSILON = 1e-05
SUB = 128
STEP = 256
F32 = jnp.float32
BF16 = jnp.bfloat16
SWAP = [(0, 1), (1, 0)]
AR_SPLIT = 2
PROJ_EARLY = 5
DN_LATE = 2
EARLY_STEPS = [3, 5, 6, 7]


def dot(a, b):
    return jnp.dot(a, b, preferred_element_type=F32)


def dot_nt(a, b):
    return lax.dot_general(a, b, (((1,), (1,)), ((), ())), preferred_element_type=F32)


def dot_tn(a, b):
    return lax.dot_general(a, b, (((0,), (0,)), ((), ())), preferred_element_type=F32)


def sigmoid(x):
    return 0.5 * jnp.tanh(0.5 * x) + 0.5


def softplus(x):
    return jnp.maximum(x, 0.0) + jnp.log1p(jnp.exp(-jnp.abs(x)))


def fold8(x):
    return jnp.sum(x.reshape(x.shape[0] // 8, 8, x.shape[1]), axis=0)


def row_scan(x, mat):
    hi = x.astype(BF16).astype(F32)
    rest = x - hi
    mid = rest.astype(BF16).astype(F32)
    low = rest - mid
    parts = jnp.concatenate([hi, mid, low, jnp.zeros_like(x)], axis=0).astype(BF16)
    out = dot(parts, mat)
    return out[0:8] + out[8:16] + out[16:24]


def plain_sums(sel, z):
    return dot_nt(sel, z.astype(BF16))[0:8]


def head_sums(sel, z):
    hi = z.astype(BF16)
    low = (z - hi.astype(F32)).astype(BF16)
    return (dot_nt(sel, hi) + dot_nt(sel, low))[0:8]


def iota(shape, dim):
    return lax.broadcasted_iota(jnp.int32, shape, dim)


def spread(cols, first, rows):
    lane = iota((rows, 128), 1)
    return jnp.where(
        lane < 64,
        jnp.broadcast_to(cols[:, first : first + 1], (rows, 128)),
        jnp.broadcast_to(cols[:, first + 1 : first + 2], (rows, 128)),
    )


def pair_stack(x):
    lane = iota(x.shape, 1)
    zero = jnp.zeros_like(x)
    return jnp.concatenate([jnp.where(lane < 64, x, zero), jnp.where(lane < 64, zero, x)], axis=0)


def forward_block(fresh, width, weights_in, outs_a, outs_b, scratch):
    hid_own, hid_rec, gains, w_own, w_rec, vtap, stap, head_par, wo_own, wo_rec = weights_in
    mixed_out, pre_gate_out, pre_value_out, conv_value_out, pre_shared_out, conv_shared_out = outs_a
    y_out, state_out, rows_out, nt_out = outs_b
    state, vbuf, sbuf, po_own, po_send, square_row = scratch
    chan = mixed_out.shape[1]
    pairs = chan // 128

    @pl.when(fresh)
    def _():
        state[...] = jnp.zeros_like(state)
        vbuf[0:8, :] = jnp.zeros((8, vbuf.shape[1]), F32)
        sbuf[0:8, :] = jnp.zeros((8, sbuf.shape[1]), F32)

    h0 = hid_own[...].astype(F32)
    h1 = hid_rec[...].astype(F32)
    square = jnp.sum(h0 * h0, axis=1, keepdims=True) + jnp.sum(h1 * h1, axis=1, keepdims=True)
    recip = lax.rsqrt(square / width + EPSILON)
    n0 = (h0 * gains[0:1, :]).astype(BF16)
    n1 = (h1 * gains[1:2, :]).astype(BF16)
    half = n0.shape[1]
    nt_out[0:half, :] = jnp.transpose(n0)
    nt_out[half : 2 * half, :] = jnp.transpose(n1)
    q = dot(n0, w_own[...]) + dot(n1, w_rec[...])
    pre = q * recip
    gate = pre[:, 0:chan]
    pre_gate_out[...] = gate
    pre_value = pre[:, chan : 2 * chan]
    pre_value_out[...] = pre_value.astype(BF16)
    pre_shared = pre[:, 2 * chan : 2 * chan + 256]
    pre_shared_out[...] = pre_shared.astype(BF16)
    vbuf[8 : 8 + STEP, :] = pre_value
    sbuf[8 : 8 + STEP, :] = pre_shared
    conv = jnp.broadcast_to(vtap[4:5, :], (STEP, chan))
    conv_s = jnp.broadcast_to(stap[4:5, :], (STEP, 256))
    for k in range(4):
        conv = conv + vbuf[5 + k : 5 + k + STEP, :] * vtap[k : k + 1, :]
        conv_s = conv_s + sbuf[5 + k : 5 + k + STEP, :] * stap[k : k + 1, :]
    vbuf[0:8, :] = vbuf[STEP : STEP + 8, :]
    sbuf[0:8, :] = sbuf[STEP : STEP + 8, :]
    conv_value_out[...] = conv
    conv_shared_out[...] = conv_s
    x = conv * sigmoid(conv)
    act = conv_s * sigmoid(conv_s)

    head_rows = jnp.transpose(pre[:, 2 * chan + 256 : 2 * chan + 384])[0:8]
    v = head_rows + head_par[0:8, 0:1]
    steps = softplus(v)
    logd = head_par[8:16, 0:1] * steps
    rows_out[0:8, :] = v
    rows_out[16:24, :] = jnp.transpose(jnp.broadcast_to(recip, (STEP, 128)))[0:8]

    upper = (iota((SUB, SUB), 0) <= iota((SUB, SUB), 1)).astype(F32).astype(BF16)
    causal = iota((SUB, SUB), 0) >= iota((SUB, SUB), 1)
    sg = gate * sigmoid(gate)
    for sub in range(STEP // SUB):
        lo, hi = sub * SUB, (sub + 1) * SUB
        cum_r = row_scan(logd[:, lo:hi], upper)
        rows_out[8:16, lo:hi] = cum_r
        cols = jnp.transpose(jnp.concatenate([cum_r, steps[:, lo:hi]], axis=0))
        b_in = act[lo:hi, 0:128]
        b_bf = b_in.astype(BF16)
        c_bf = act[lo:hi, 128:256].astype(BF16)
        b_t = jnp.transpose(b_in).astype(BF16)
        scores = dot_nt(c_bf, b_bf)
        for p in range(pairs):
            pl0, pl1 = p * 128, (p + 1) * 128
            c0 = jnp.broadcast_to(cols[:, 2 * p : 2 * p + 1], (SUB, 128))
            c1 = jnp.broadcast_to(cols[:, 2 * p + 1 : 2 * p + 2], (SUB, 128))
            weights = []
            for col, h in ((c0, 2 * p), (c1, 2 * p + 1)):
                gap = jnp.where(causal, col - cum_r[h : h + 1, :], -1e30)
                weights.append((scores * jnp.exp(gap)).astype(BF16))
            lane = iota((SUB, 128), 1)
            cum_e = jnp.where(lane < 64, c0, c1)
            step_e = spread(cols, 8 + 2 * p, SUB)
            xs = x[lo:hi, pl0:pl1]
            xh = step_e * xs
            inside = dot(jnp.concatenate(weights, axis=1), pair_stack(xh.astype(BF16)))
            held = state[:, pl0:pl1]
            held_bf = held.astype(BF16)
            state_out[lo:hi, pl0:pl1] = held_bf
            carried = dot(c_bf, held_bf)
            y = inside + carried * jnp.exp(cum_e)
            y_out[lo:hi, pl0:pl1] = y
            last = cum_e[SUB - 1 : SUB, :]
            tail = (xh * jnp.exp(last - cum_e)).astype(BF16)
            state[:, pl0:pl1] = held * jnp.exp(last) + dot(b_t, tail)
            y = y + vtap[5:6, pl0:pl1] * xs
            mixed_out[lo:hi, pl0:pl1] = (y * sg[lo:hi, pl0:pl1]).astype(BF16)
    mix = mixed_out[...].astype(F32)
    weighted = (mix * vtap[6:7, :]).astype(BF16)
    po_own[...] = dot(weighted, wo_own[...]).astype(BF16)
    po_send[...] = dot(weighted, wo_rec[...]).astype(BF16)
    square_row[...] = plain_sums(jnp.ones((16, chan), BF16), mix * mix)[0:1]


def early_levels(dp):
    return dp.bit_length()


def early_steps(dp, blocks):
    count = early_levels(dp)
    if count == 4 and blocks == 8:
        return EARLY_STEPS
    return [max(2, blocks - count + n) if blocks > count else blocks - 1 for n in range(count)]


def early_orders(dp):
    bits = dp.bit_length() - 1
    near = tuple(range(bits))
    far = tuple(range(1, bits)) + (0,)
    return [far if n % 2 else near for n in range(2 * AR_SPLIT)]


def partner_of(me, k):
    return {"dp": me + (1 - 2 * lax.rem(me // (1 << k), 2)) * (1 << k)}


def levels(dp, me, bounds, orders, acc, stage, land, out, send_sem, recv_sem):
    bits = dp.bit_length() - 1

    def span(start, rows):
        return pl.ds(pl.multiple_of(start, 16), rows)

    def bit_of(k):
        return lax.rem(me // (1 << k), 2)

    def low_at(i, count):
        low, rows = bounds[i]
        for n in range(count):
            low = low + bit_of(orders[i][n]) * (rows >> (n + 1))
        return low

    def places(i, level):
        base, rows = bounds[i]
        if level < bits:
            k = orders[i][level]
            part = rows >> (level + 1)
            give = span(low_at(i, level) + (1 - bit_of(k)) * part, part)
            where = span(base + rows - (rows >> level), part)
            return k, give, where, span(low_at(i, level + 1), part)
        back = 2 * bits - 1 - level
        own = span(low_at(i, back + 1), rows >> (back + 1))
        return orders[i][back], own, own, None

    def copy_of(i, level):
        k, give, where, _ = places(i, level)
        src, dst = (stage, land) if level < bits else (out, out)
        return remote(
            src.at[give, :], dst.at[where, :], send_sem.at[i, level], recv_sem.at[i, level], partner_of(me, k)
        )

    def start_level(i, level):
        if level < bits:
            give = places(i, level)[1]
            stage[give, :] = acc[give, :].astype(BF16)
        copy_of(i, level).start()

    def end_level(i, level, go_on=True):
        copy_of(i, level).wait()
        if level < bits:
            _, _, where, keep = places(i, level)
            total = acc[keep, :] + land[where, :].astype(F32)
            acc[keep, :] = total
            if level == bits - 1:
                out[keep, :] = total.astype(BF16)
        if go_on and level + 1 < 2 * bits:
            start_level(i, level + 1)

    return start_level, end_level


def gate_block(ins, outs):
    cot_own, cot_rec, wo_own, wo_rec, trow, rows_in, mixed, pre_gate, conv_value, y_in, vtap = ins
    acc_v, go_own, go_rec, dy_out, p_gate, rs_gate = outs
    chan = mixed.shape[1]
    tcol = jnp.transpose(jnp.concatenate([trow[...], rows_in[16:24, :]], axis=0))
    scale = tcol[:, 0:1]
    coef = tcol[:, 8:9]
    recip = tcol[:, 16:17]
    s0 = (cot_own[...].astype(F32) * scale).astype(BF16)
    s1 = (cot_rec[...].astype(F32) * scale).astype(BF16)
    d_weighted = dot_nt(s0, wo_own[...]) + dot_nt(s1, wo_rec[...])
    mix = mixed[...].astype(F32)
    acc_v[48:56, :] += fold8(d_weighted * mix)
    weighted_t = jnp.transpose((mix * vtap[6:7, :]).astype(BF16))
    go_own[...] += dot(weighted_t, s0)
    go_rec[...] += dot(weighted_t, s1)
    d_mixed = d_weighted * vtap[6:7, :] - coef * mix
    gate = pre_gate[...]
    sig = sigmoid(gate)
    silu = gate * sig
    conv = conv_value[...]
    sig_v = sigmoid(conv)
    x = conv * sig_v
    y_scan = y_in[...]
    y = y_scan + vtap[5:6, :] * x
    dy = d_mixed * silu
    d_gate = d_mixed * y * (sig + silu * (1.0 - sig))
    acc_v[40:48, :] += fold8(dy * x)
    dy_out[...] = dy.astype(BF16)
    p_gate[...] = (recip * d_gate).astype(BF16)
    rs_gate[...] = plain_sums(jnp.ones((16, chan), BF16), d_gate * gate)


def scan_block(fresh, ins, weights_in, outs, scratch):
    rows_in, pre_value, conv_value, pre_shared, conv_shared, y_in, state_in, hid_own, hid_rec = ins
    w_own, w_rec, vtap, stap, head_par, sel_ref, dy_in, p_gate, rs_gate = weights_in
    p_out, rsum_out, acc_v, acc_s, acc_h, acc_n, dn_own, dn_rec = outs
    grad, vbuf, sbuf, dxbuf, dbbuf = scratch
    chan = conv_value.shape[1]
    pairs = chan // 128

    @pl.when(fresh)
    def _():
        grad[...] = jnp.zeros_like(grad)
        vbuf[STEP : STEP + 8, :] = jnp.zeros((8, vbuf.shape[1]), F32)
        sbuf[STEP : STEP + 8, :] = jnp.zeros((8, sbuf.shape[1]), F32)

    recip = jnp.transpose(rows_in[16:24, :])[:, 0:1]
    conv = conv_value[...]
    sig_v = sigmoid(conv)
    x = conv * sig_v
    dy_bf = dy_in[...]
    conv_s = conv_shared[...]
    sig_s = sigmoid(conv_s)
    act = conv_s * sig_s

    sel = sel_ref[...]
    sel_f = sel.astype(F32)[0:8]
    v = rows_in[0:8, :]
    steps = softplus(v)
    logd = head_par[8:16, 0:1] * steps
    lower = (iota((SUB, SUB), 0) >= iota((SUB, SUB), 1)).astype(F32).astype(BF16)
    strict = (iota((SUB, SUB), 0) < iota((SUB, SUB), 1)).astype(F32).astype(BF16)
    causal_t = iota((SUB, SUB), 0) <= iota((SUB, SUB), 1)
    for sub in reversed(range(STEP // SUB)):
        lo, hi = sub * SUB, (sub + 1) * SUB
        cum_r = rows_in[8:16, lo:hi]
        cols = jnp.transpose(jnp.concatenate([cum_r, steps[:, lo:hi]], axis=0))
        b_bf = act[lo:hi, 0:128].astype(BF16)
        c_in = act[lo:hi, 128:256]
        c_bf = c_in.astype(BF16)
        c_t = jnp.transpose(c_in).astype(BF16)
        scores_t = dot_nt(b_bf, c_bf)
        d_scores = jnp.zeros((SUB, SUB), F32)
        db = jnp.zeros((SUB, 128), F32)
        dc = jnp.zeros((SUB, 128), F32)
        z_sum = jnp.zeros((8, SUB), F32)
        e_sum = jnp.zeros((8, SUB), F32)
        f_sum = jnp.zeros((8, SUB), F32)
        gh = jnp.zeros((8, 1), F32)
        for p in range(pairs):
            pl0, pl1 = p * 128, (p + 1) * 128
            c0 = jnp.broadcast_to(cols[:, 2 * p : 2 * p + 1], (SUB, 128))
            c1 = jnp.broadcast_to(cols[:, 2 * p + 1 : 2 * p + 2], (SUB, 128))
            decays = []
            for col, h in ((c0, 2 * p), (c1, 2 * p + 1)):
                gap = jnp.where(causal_t, cum_r[h : h + 1, :] - col, -1e30)
                decays.append(jnp.exp(gap))
            weights = [(scores_t * d).astype(BF16) for d in decays]
            lane = iota((SUB, 128), 1)
            cum_e = jnp.where(lane < 64, c0, c1)
            step_e = spread(cols, 8 + 2 * p, SUB)
            xs = x[lo:hi, pl0:pl1]
            xh = step_e * xs
            xh_bf = xh.astype(BF16)
            dys_bf = dy_bf[lo:hi, pl0:pl1]
            dys = dys_bf.astype(F32)
            stack = pair_stack(dys_bf)
            inner = dot(jnp.concatenate(weights, axis=1), stack)
            d_pair = dot_nt(xh_bf, stack)
            d_scores = d_scores + decays[0] * d_pair[:, 0:128] + decays[1] * d_pair[:, 128:256]
            last = cum_e[SUB - 1 : SUB, :]
            tail_e = jnp.exp(last - cum_e)
            g = grad[:, pl0:pl1]
            g_bf = g.astype(BF16)
            outer = dot(b_bf, g_bf) * tail_e
            u = inner + outer
            dxbuf[lo:hi, pl0:pl1] = step_e * u + vtap[5:6, pl0:pl1] * dys
            db = db + dot_nt((xh * tail_e).astype(BF16), g_bf)
            dya = (dys * jnp.exp(cum_e)).astype(BF16)
            held = state_in[lo:hi, pl0:pl1]
            dc = dc + dot_nt(dya, held)
            sel_p = sel[:, pl0:pl1]
            z_sum = z_sum + head_sums(
                sel_p, dys * y_in[lo:hi, pl0:pl1] - xh_bf.astype(F32) * inner
            )
            e_sum = e_sum + plain_sums(sel_p, xh * outer)
            f_sum = f_sum + plain_sums(sel_p, xs * u)
            decay_row = jnp.exp(last)
            gh_row = decay_row * jnp.sum(g * held.astype(F32), axis=0, keepdims=True)
            gh = gh + jnp.sum(sel_f[:, pl0:pl1] * gh_row, axis=1, keepdims=True)
            grad[:, pl0:pl1] = g * decay_row + dot(c_t, dya)
        ds_bf = d_scores.astype(BF16)
        dbbuf[lo:hi, 0:128] = db + dot(ds_bf, c_bf)
        dbbuf[lo:hi, 128:256] = dc + dot(jnp.transpose(d_scores).astype(BF16), b_bf)
        d_log = row_scan(z_sum, lower) + row_scan(e_sum, strict) + gh
        d_step = (f_sum + d_log * head_par[8:16, 0:1]) * sigmoid(v[:, lo:hi])
        acc_h[0:8, :] += d_log * logd[:, lo:hi]
        acc_h[8:16, :] += d_step
        pre_step = v[:, lo:hi] - head_par[0:8, 0:1]
        rsum_out[:, lo:hi] += jnp.broadcast_to(
            jnp.sum(d_step * pre_step, axis=0, keepdims=True), (8, SUB)
        )
        d_cols = jnp.transpose(jnp.concatenate([d_step, jnp.zeros((120, SUB), F32)], axis=0))
        p_out[lo:hi, chan + 256 : chan + 384] = (recip[lo:hi] * d_cols).astype(BF16)

    d_conv = dxbuf[...] * (sig_v + x * (1.0 - sig_v))
    d_conv_s = dbbuf[...] * (sig_s + act * (1.0 - sig_s))
    vbuf[0:STEP, :] = d_conv
    sbuf[0:STEP, :] = d_conv_s
    acc_v[32:40, :] += fold8(d_conv)
    acc_s[32:40, :] += fold8(d_conv_s)
    pv = pre_value[...].astype(F32)
    ps = pre_shared[...].astype(F32)
    d_value = jnp.zeros((STEP, chan), F32)
    d_shared = jnp.zeros((STEP, 256), F32)
    for k in range(4):
        moved = vbuf[3 - k : 3 - k + STEP, :]
        d_value = d_value + vtap[k : k + 1, :] * moved
        acc_v[8 * k : 8 * k + 8, :] += fold8(pv * moved)
        moved = sbuf[3 - k : 3 - k + STEP, :]
        d_shared = d_shared + stap[k : k + 1, :] * moved
        acc_s[8 * k : 8 * k + 8, :] += fold8(ps * moved)
    vbuf[STEP : STEP + 8, :] = vbuf[0:8, :]
    sbuf[STEP : STEP + 8, :] = sbuf[0:8, :]
    p_out[:, 0:chan] = (recip * d_value).astype(BF16)
    p_out[:, chan : chan + 256] = (recip * d_shared).astype(BF16)
    ones = jnp.ones((16, chan), BF16)
    rsum_out[...] += plain_sums(ones, d_value * pv)
    rsum_out[...] += plain_sums(ones[:, 0:256], d_shared * ps)
    pg = p_gate[...]
    pb = p_out[...]
    for n, (hid, weight, dn) in enumerate(((hid_own, w_own, dn_own), (hid_rec, w_rec, dn_rec))):
        part = dot_nt(pg, weight[:, 0:chan]) + dot_nt(pb, weight[:, chan:])
        dn[...] = part.astype(BF16)
        acc_n[8 * n : 8 * n + 8, :] += fold8(part * hid[...].astype(F32))


def unit_rows(dp):
    return 16 * dp


def misc_rows(dp, rows):
    unit = max(unit_rows(dp), 256)
    return pl.cdiv(rows, unit) * unit


def big_rows(dp, rows):
    return pl.cdiv(rows, unit_rows(dp)) * unit_rows(dp)


def remote(src, dst, send, recv, target):
    return pltpu.make_async_remote_copy(
        src_ref=src,
        dst_ref=dst,
        send_sem=send,
        recv_sem=recv,
        device_id=target,
        device_id_type=pl.DeviceIdType.MESH,
    )


def greet(targets):
    barrier = pltpu.get_barrier_semaphore()
    for target in targets:
        pl.semaphore_signal(barrier, inc=1, device_id=target, device_id_type=pl.DeviceIdType.MESH)
    pl.semaphore_wait(barrier, len(targets))


def layer_kernel(
    seq_len,
    dp,
    inner_width,
    hid_own_hbm,
    hid_rec_hbm,
    cot_own_hbm,
    cot_rec_hbm,
    gains,
    w_own,
    w_rec,
    vtap,
    stap,
    head_par,
    wo_own,
    wo_rec,
    sel,
    sums_out,
    proj_out,
    proj_col,
    dn_out,
    dn_col,
    trow,
    rs_out,
    recip_out,
    hid_own,
    hid_rec,
    cot_own,
    cot_rec,
    pre_gate,
    pre_value,
    conv_value,
    pre_shared,
    conv_shared,
    y_scan,
    states,
    mixed,
    rows,
    normed_t,
    p_gate,
    p_all,
    dy_s,
    rs_in,
    state,
    vbuf,
    sbuf,
    dxbuf,
    dbbuf,
    pair_own,
    pair_send,
    pair_land,
    proj_s,
    dn_sum,
    sums,
    sums_land,
    go_own,
    go_rec,
    swap_send,
    swap_land,
    row_send,
    row_land,
    col_send,
    col_land,
    rs_land,
    acc_v,
    acc_s,
    acc_h,
    acc_n,
    acc,
    stage,
    land,
    out,
    load_sem,
    save_sem,
    po_sem,
    dn_sem,
    col_sem,
    sum_sem,
    swap_sem,
    ar_send_sem,
    ar_recv_sem,
    out_sem,
):
    tokens, half = hid_own.shape
    chan = mixed.shape[1]
    width = 2 * half
    wide = p_all.shape[1]
    blocks = tokens // STEP
    steps_per_seq = seq_len // STEP
    size = big_rows(dp, width)
    tail = out.shape[0] - 3 * size
    bits = dp.bit_length() - 1
    me = lax.axis_index("dp")
    r = lax.axis_index("row")
    c = lax.axis_index("col")
    to_row, to_col, to_both = {"row": 1 - r}, {"col": 1 - c}, {"row": 1 - r, "col": 1 - c}
    part_rows = size // AR_SPLIT
    near = tuple(range(bits))
    far = tuple(range(1, bits)) + (0,)
    bounds = [(tail + n * part_rows, part_rows) for n in range(3 * AR_SPLIT)] + [(0, tail)]
    orders = [far if n % 2 else near for n in range(3 * AR_SPLIT)] + [near]
    firsts, values, misc = range(2 * AR_SPLIT), range(2 * AR_SPLIT, 3 * AR_SPLIT), 3 * AR_SPLIT
    start_level, end_level = levels(dp, me, bounds, orders, acc, stage, land, out, ar_send_sem, ar_recv_sem)

    def span(i):
        return pl.ds(pl.multiple_of(i * STEP, STEP), STEP)

    def load(n, i):
        src, dst = ((hid_own_hbm, hid_own), (hid_rec_hbm, hid_rec), (cot_own_hbm, cot_own), (cot_rec_hbm, cot_rec))[n]
        return pltpu.make_async_copy(src.at[span(i), :], dst.at[span(i), :], load_sem.at[n, i])

    def save(n, i):
        src, dst = ((proj_s, proj_out), (dn_sum, dn_out))[n]
        return pltpu.make_async_copy(src.at[span(i), :], dst.at[span(i), :], save_sem.at[n, i])

    def pair_copy(sem, i):
        return remote(pair_send.at[span(i), :], pair_land.at[span(i), :], sem.at[0, i], sem.at[1, i], to_row)

    def col_copy(n, i):
        src, dst = ((proj_s, proj_col), (dn_sum, dn_col))[n]
        return remote(src.at[span(i), :], dst.at[span(i), :], col_sem.at[n, 0, i], col_sem.at[n, 1, i], to_col)

    def small_copy(src, dst, n, target):
        return remote(src, dst, swap_sem.at[0, n], swap_sem.at[1, n], target)

    for n in range(4):
        for i in range(blocks):
            load(n, i).start()
    greet([partner_of(me, k) for k in range(bits)] + [to_row, to_col, to_both])
    for ref in (acc_v, acc_s, acc_h, acc_n, go_own, go_rec):
        ref[...] = jnp.zeros_like(ref)

    def take_proj(i):
        pair_copy(po_sem, i).wait()
        part = pair_own[span(i), :].astype(F32) + pair_land[span(i), :].astype(F32)
        proj_s[span(i), :] = part.astype(BF16)
        save(0, i).start()

        @pl.when(i < PROJ_EARLY)
        def _():
            col_copy(0, i).start()

        load(2, i).wait()
        dots = plain_sums(jnp.ones((16, half), BF16), part * cot_own[span(i), :].astype(F32))
        sums[pl.ds(8 + i, 1), :] = dots[0:1]

    @pl.loop(0, blocks)
    def _(i):
        here = span(i)
        load(0, i).wait()
        load(1, i).wait()
        forward_block(
            i % steps_per_seq == 0,
            width,
            (
                hid_own.at[here, :],
                hid_rec.at[here, :],
                gains,
                w_own,
                w_rec,
                vtap,
                stap,
                head_par,
                wo_own,
                wo_rec,
            ),
            (
                mixed.at[here, :],
                pre_gate.at[here, :],
                pre_value.at[here, :],
                conv_value.at[here, :],
                pre_shared.at[here, :],
                conv_shared.at[here, :],
            ),
            (y_scan.at[here, :], states.at[here, :], rows.at[:, here], normed_t.at[:, here]),
            (state, vbuf, sbuf, pair_own.at[here, :], pair_send.at[here, :], sums.at[pl.ds(i, 1), :]),
        )

        @pl.when(i > 0)
        def _():
            take_proj(i - 1)

        pair_copy(po_sem, i).start()

    take_proj(blocks - 1)
    ends = []
    for n, target in enumerate((to_row, to_col, to_both)):
        copy = remote(sums, sums_land.at[n], sum_sem.at[0, n], sum_sem.at[1, n], target)
        copy.start()
        ends.append(copy)
    for i in range(PROJ_EARLY, blocks):
        col_copy(0, i).start()
    recip_out[...] = rows[16:24, :]
    for i in range(blocks):
        load(3, i).wait()
    for copy in ends:
        copy.wait()
    total = (sums[...] + sums_land[0]) + (sums_land[1] + sums_land[2])
    scale = lax.rsqrt(total[0:8] / inner_width + EPSILON)
    coef = total[8:16] * (scale * scale * scale) / inner_width
    for i in range(blocks):
        trow[0:8, i * STEP : (i + 1) * STEP] = jnp.broadcast_to(scale[i : i + 1], (8, STEP))
        trow[8:16, i * STEP : (i + 1) * STEP] = jnp.broadcast_to(coef[i : i + 1], (8, STEP))

    @pl.loop(0, blocks)
    def _(i):
        here = span(i)
        gate_block(
            (
                cot_own.at[here, :],
                cot_rec.at[here, :],
                wo_own,
                wo_rec,
                trow.at[:, here],
                rows.at[:, here],
                mixed.at[here, :],
                pre_gate.at[here, :],
                conv_value.at[here, :],
                y_scan.at[here, :],
                vtap,
            ),
            (acc_v, go_own, go_rec, dy_s.at[here, :], p_gate.at[here, :], rs_in.at[:, here]),
        )

    def chunk_rows(n, side):
        return pl.ds(pl.multiple_of(tail + n * size + side * half, 128), half)

    swaps = [small_copy(swap_send.at[n], swap_land.at[n], n, to_row) for n in range(2)]
    swap_send[0] = go_rec[...].astype(BF16)
    swaps[0].start()
    swap_send[1] = dot(normed_t[half:width, :], p_gate[...]).astype(BF16)
    swaps[1].start()
    acc[chunk_rows(0, r), :] = go_own[...]
    acc[chunk_rows(1, r), :] = dot(normed_t[0:half, :], p_gate[...])
    if size > width:
        for n in range(3):
            acc[tail + n * size + width : tail + (n + 1) * size, :] = jnp.zeros((size - width, chan), F32)
    for n in range(2):
        swaps[n].wait()
        acc[chunk_rows(n, 1 - r), :] = swap_land[n].astype(F32)
        for i in range(AR_SPLIT):
            start_level(n * AR_SPLIT + i, 0)

    def take_dn(i):
        pair_copy(dn_sem, i).wait()
        part = pair_own[span(i), :].astype(F32) + pair_land[span(i), :].astype(F32)
        dn_sum[span(i), :] = part.astype(BF16)
        save(1, i).start()

    @pl.loop(0, blocks)
    def _(later):
        i = blocks - 1 - later
        here = span(i)
        scan_block(
            later % steps_per_seq == 0,
            (
                rows.at[:, here],
                pre_value.at[here, :],
                conv_value.at[here, :],
                pre_shared.at[here, :],
                conv_shared.at[here, :],
                y_scan.at[here, :],
                states.at[here, :],
                hid_own.at[here, :],
                hid_rec.at[here, :],
            ),
            (
                w_own,
                w_rec,
                vtap,
                stap,
                head_par,
                sel,
                dy_s.at[here, :],
                p_gate.at[here, :],
                rs_in.at[:, here],
            ),
            (
                p_all.at[here, :],
                rs_in.at[:, here],
                acc_v,
                acc_s,
                acc_h,
                acc_n,
                pair_own.at[here, :],
                pair_send.at[here, :],
            ),
            (state, vbuf, sbuf, dxbuf, dbbuf),
        )

        @pl.when(later > 0)
        def _():
            take_dn(i + 1)

            @pl.when(i + 1 >= DN_LATE)
            def _():
                col_copy(1, i + 1).start()

        pair_copy(dn_sem, i).start()
        for level, when in enumerate(early_steps(dp, blocks)):

            @pl.when(later == when)
            def _(level=level):
                for n in firsts:
                    end_level(n, level)

    def sum8(ref, n):
        return jnp.sum(ref[8 * n : 8 * n + 8, :], axis=0, keepdims=True)

    small = jnp.concatenate([sum8(acc_s, n) for n in range(5)] + [jnp.zeros((3, 256), F32)], axis=0)
    norm_own, norm_rec = [
        jnp.concatenate([sum8(acc_n, n), jnp.zeros((1, 512 - half), F32)], axis=1) for n in (0, 1)
    ]
    pad6 = jnp.zeros((6, 256), F32)
    row_send[half : half + 16, 0:256] = jnp.concatenate(
        [small, norm_rec[:, 0:256], norm_rec[:, 256:512], pad6], axis=0
    ).astype(BF16)
    row_send[half : half + 16, 256:wide] = jnp.zeros((16, wide - 256), BF16)
    for lo in range(0, wide, 384):
        row_send[0:half, lo : lo + 384] = dot(normed_t[half:width, :], p_all[:, lo : lo + 384]).astype(BF16)
    row_copy = small_copy(row_send, row_land, 2, to_row)
    row_copy.start()
    rs_row = small_copy(rs_in, rs_land.at[0], 3, to_row)
    rs_row.start()
    acc[0:half, :] = dot(normed_t[0:half, :], p_all[:, chan:wide])
    acc[chunk_rows(2, r), :] = dot(normed_t[0:half, :], p_all[:, 0:chan])
    row_copy.wait()
    acc[chunk_rows(2, 1 - r), :] = row_land[0:half, 0:chan].astype(F32)
    for n in values:
        start_level(n, 0)
    gate_sums = acc[0:half, 0:256] + row_land[0:half, chan : chan + 256].astype(F32)
    extra = jnp.concatenate([small, norm_own[:, 0:256], norm_own[:, 256:512], pad6], axis=0)
    extra = extra + row_land[half : half + 16, 0:256].astype(F32)
    col_send[0:half, :] = gate_sums.astype(BF16)
    col_send[half : half + 16, :] = extra.astype(BF16)
    mid_copy = small_copy(col_send, col_land, 4, to_col)
    mid_copy.start()
    rs_row.wait()
    rs_out[...] = rs_in[...] + rs_land[0]
    rs_col = small_copy(rs_out, rs_land.at[1], 5, to_col)
    rs_col.start()
    take_dn(0)
    for i in reversed(range(DN_LATE)):
        col_copy(1, i).start()

    acc[0:half, 256:384] = jnp.concatenate(
        [acc[0:half, 256:320], row_land[0:half, chan + 256 : chan + 320].astype(F32)], axis=1
    )
    acc[half : half + 16, 256:384] = jnp.zeros((16, 128), F32)
    first = half + 16
    acc[first : first + 8, :] = jnp.concatenate(
        [sum8(acc_v, n) for n in range(7)] + [jnp.zeros((1, chan), F32)], axis=0
    )
    acc[first + 8 : first + 24, :] = jnp.broadcast_to(
        jnp.sum(acc_h[...], axis=1, keepdims=True), (16, chan)
    )
    if tail > first + 24:
        acc[first + 24 : tail, :] = jnp.zeros((tail - first - 24, chan), F32)
    mid_copy.wait()
    acc[0 : half + 16, 0:256] = col_send[...].astype(F32) + col_land[...].astype(F32)
    start_level(misc, 0)
    early = early_levels(dp)
    done = []

    def save_chunk(n):
        rows_n = pl.ds(*bounds[n])
        copy = pltpu.make_async_copy(out.at[rows_n, :], sums_out.at[rows_n, :], out_sem.at[n])
        copy.start()
        done.append(copy)

    def end(n, level):
        end_level(n, level)
        if level == 2 * bits - 1:
            save_chunk(n)

    if early >= 2 * bits:
        for n in firsts:
            save_chunk(n)

    for level in range(2 * bits):
        if early + level < 2 * bits:
            for n in firsts:
                end(n, early + level)
        for n in values:
            end(n, level)
        end(misc, level)
    for copy in done:
        copy.wait()
    rs_col.wait()
    rs_out[...] = rs_out[...] + rs_land[1]
    for i in range(blocks):
        for n in range(2):
            save(n, i).wait()
            col_copy(n, i).wait()


def layer(seq_len, dp, hidden, hid_rec, cot, cot_rec, gains, w_own, w_rec, vtap, stap, head_par, wo_own, wo_rec, sel):
    tokens, half = hidden.shape
    chan = vtap.shape[1]
    wide = w_own.shape[1] - chan
    bits = dp.bit_length() - 1
    size = big_rows(dp, 2 * half)
    tail = misc_rows(dp, half + 48)
    total = tail + 3 * size
    blocks = tokens // STEP
    vmem = pl.BlockSpec(memory_space=pltpu.VMEM)
    hbm = pl.BlockSpec(memory_space=pl.ANY)

    def act(cols=half, dtype=BF16):
        return jax.ShapeDtypeStruct((tokens, cols), dtype)

    def room(*shape, dtype=BF16):
        return pltpu.VMEM(shape, dtype)

    def flags(*shape):
        return pltpu.SemaphoreType.DMA(shape)

    return pl.pallas_call(
        functools.partial(layer_kernel, seq_len, dp, 4 * chan),
        in_specs=[hbm] * 4 + [vmem] * 9,
        out_specs=[hbm, hbm, hbm, hbm, hbm, vmem, vmem, vmem],
        out_shape=[
            jax.ShapeDtypeStruct((total, chan), BF16),
            act(),
            act(),
            act(),
            act(),
            jax.ShapeDtypeStruct((16, tokens), F32),
            jax.ShapeDtypeStruct((8, tokens), F32),
            jax.ShapeDtypeStruct((8, tokens), F32),
        ],
        scratch_shapes=[
            room(tokens, half),
            room(tokens, half),
            room(tokens, half),
            room(tokens, half),
            room(tokens, chan, dtype=F32),
            room(tokens, chan),
            room(tokens, chan, dtype=F32),
            room(tokens, 256),
            room(tokens, 256, dtype=F32),
            room(tokens, chan, dtype=F32),
            room(tokens, chan),
            room(tokens, chan),
            room(24, tokens, dtype=F32),
            room(2 * half, tokens),
            room(tokens, chan),
            room(tokens, wide),
            room(tokens, chan),
            room(8, tokens, dtype=F32),
            room(128, chan, dtype=F32),
            room(STEP + 8, chan, dtype=F32),
            room(STEP + 8, 256, dtype=F32),
            room(STEP, chan, dtype=F32),
            room(STEP, 256, dtype=F32),
            room(tokens, half),
            room(tokens, half),
            room(tokens, half),
            room(tokens, half),
            room(tokens, half),
            room(16, STEP, dtype=F32),
            room(3, 16, STEP, dtype=F32),
            room(chan, half, dtype=F32),
            room(chan, half, dtype=F32),
            room(2, half, chan),
            room(2, half, chan),
            room(half + 16, wide),
            room(half + 16, wide),
            room(half + 16, 256),
            room(half + 16, 256),
            room(2, 8, tokens, dtype=F32),
            room(56, chan, dtype=F32),
            room(40, 256, dtype=F32),
            room(16, 128, dtype=F32),
            room(16, half, dtype=F32),
            room(total, chan, dtype=F32),
            room(total, chan),
            room(total, chan),
            room(total, chan),
            flags(4, blocks),
            flags(2, blocks),
            flags(2, blocks),
            flags(2, blocks),
            flags(2, 2, blocks),
            flags(2, 3),
            flags(2, 6),
            flags(3 * AR_SPLIT + 1, 2 * bits),
            flags(3 * AR_SPLIT + 1, 2 * bits),
            flags(3 * AR_SPLIT + 1),
        ],
        compiler_params=pltpu.CompilerParams(
            collective_id=0, has_side_effects=True, vmem_limit_bytes=67_000_000
        ),
        name="layer",
    )(hidden, hid_rec, cot, cot_rec, gains, w_own, w_rec, vtap, stap, head_par, wo_own, wo_rec, sel)


def finish_kernel(
    width,
    out_rows,
    gate_a,
    gate_b,
    value_a,
    value_b,
    misc,
    hid,
    cot,
    dn_sum,
    dn_col,
    proj_own,
    proj_col,
    sel,
    trow,
    recip_in,
    rs,
    gains,
    result,
    hidden_grad,
    g_gate,
    g_value,
    g_step,
    g_state,
    g_filter,
    g_shift,
    g_kernel,
    g_offset,
    g_decay,
    g_bias,
    g_skip,
    g_norm,
    g_gated,
    g_output,
):
    half = hid.shape[1]
    hid32 = hid[...].astype(F32)
    recip = recip_in[...]
    cols = jnp.transpose(jnp.concatenate([trow[0:8, :], rs[...] * recip * recip / width], axis=0))
    proj = proj_own[...].astype(F32) + proj_col[...].astype(F32)
    result[...] = (hid32 + cols[:, 0:1] * proj).astype(BF16)
    d_normed = dn_sum[...].astype(F32) + dn_col[...].astype(F32)
    hidden_grad[...] = cot[...].astype(F32) + d_normed * gains[0:1, :] - cols[:, 8:9] * hid32
    @pl.when(pl.program_id(0) < half // 128)
    def _():
        g_output[...] = out_rows[...].astype(F32)
        g_gate[:, 0:half] = gate_a[...].astype(F32)
        g_gate[:, half : 2 * half] = gate_b[...].astype(F32)
        g_value[:, 0:half] = value_a[...].astype(F32)
        g_value[:, half : 2 * half] = value_b[...].astype(F32)

    @pl.when(pl.program_id(0) == 0)
    def _():
        g_state[...] = misc[0:half, 0:256].astype(F32)
        step_t = jnp.transpose(misc[0:half, 256:384].astype(F32))
        heads = g_step.shape[0] // 2
        own, rec = step_t[0:heads], step_t[64 : 64 + heads]
        first = lax.axis_index("row") == 0
        g_step[...] = jnp.concatenate([jnp.where(first, own, rec), jnp.where(first, rec, own)], axis=0)
        small = misc[half : half + 48, :].astype(F32)
        g_kernel[...] = small[0:4, 0:256]
        g_offset[...] = small[4, 0:256]
        g_norm[0:256] = small[8, 0:256]
        g_norm[256:half] = small[9, 0 : half - 256]
        g_filter[...] = small[16:20]
        g_shift[...] = small[20]
        g_gated[...] = small[22]
        head = jnp.transpose(small[24:40, 0:128])[0:8]
        g_decay[...] = head[0, 0:heads]
        g_bias[...] = head[0, 8 : 8 + heads]
        skip = dot_nt(small[16:32].astype(BF16), sel[...])
        g_skip[...] = skip[5, 0:heads]


def finish(size, heads, out, hid, cot, dn_sum, dn_col, proj_own, proj_col, sel, trow, recip, rs, gains):
    tokens, half = hid.shape
    chan = out.shape[1]
    size_f = tokens // 4
    grid = 4

    def blk(cols):
        return pl.BlockSpec((size_f, cols), lambda i: (i, 0))

    def row(count):
        return pl.BlockSpec((count, size_f), lambda i: (0, i))

    def whole(shape):
        return pl.BlockSpec(shape, lambda i: (0,) * len(shape))

    parts = half // 128
    tail = out.shape[0] - 3 * size

    def part(start):
        return pl.BlockSpec((128, chan), lambda i: (start // 128 + jnp.minimum(i, parts - 1), 0))

    def streamed(rows, cols):
        return pl.BlockSpec((rows // parts, cols), lambda i: (jnp.minimum(i, parts - 1), 0))

    small = [
        (2 * heads, half),
        (half, 256),
        (4, chan),
        (chan,),
        (4, 256),
        (256,),
        (heads,),
        (heads,),
        (heads,),
        (half,),
        (chan,),
    ]
    big = (half, 2 * chan)
    shapes = [big, big] + small + [(2 * chan, half)]
    return pl.pallas_call(
        functools.partial(finish_kernel, 2 * half),
        grid=(grid,),
        in_specs=[
            pl.BlockSpec((256, half), lambda i: (tail // 256 + jnp.minimum(i, parts - 1), 0)),
            part(tail + size),
            part(tail + size + half),
            part(tail + 2 * size),
            part(tail + 2 * size + half),
            whole((tail, chan)),
            blk(half),
            blk(half),
            blk(half),
            blk(half),
            blk(half),
            blk(half),
            whole(sel.shape),
            row(16),
            row(8),
            row(8),
            whole((8, half)),
        ],
        out_specs=[blk(half), blk(half), streamed(*big), streamed(*big)]
        + [whole(shape) for shape in small]
        + [streamed(2 * chan, half)],
        out_shape=[
            jax.ShapeDtypeStruct((tokens, half), BF16),
            jax.ShapeDtypeStruct((tokens, half), F32),
        ]
        + [jax.ShapeDtypeStruct(shape, F32) for shape in shapes],
        cost_estimate=pl.CostEstimate(flops=20_000_000, bytes_accessed=20_000_000, transcendentals=0),
        name="finish",
    )(
        out,
        out,
        out,
        out,
        out,
        out,
        hid,
        cot,
        dn_sum,
        dn_col,
        proj_own,
        proj_col,
        sel,
        trow,
        recip,
        rs,
        gains,
    )


def swap(x, axis):
    return lax.ppermute(x, axis, SWAP)


def body(
    hidden,
    gate_proj,
    value_proj,
    step_proj,
    state_proj,
    value_filter,
    value_shift,
    shared_kernel,
    shared_offset,
    decay_log,
    step_bias,
    skip_gain,
    input_gain,
    gated_gain,
    output_proj,
    cotangent,
):
    tokens, half = hidden.shape
    width = 2 * half
    chan = gated_gain.shape[0]
    inner_width = 4 * chan
    heads = decay_log.shape[0]
    r = lax.axis_index("row")
    dp = lax.axis_size("dp")
    seq_len = min(LEN, tokens)

    def cut(x, start, size, axis):
        return lax.dynamic_slice_in_dim(x, start * size, size, axis)

    def packed(side):
        return jnp.concatenate(
            [
                cut(gate_proj, side, chan, 1),
                cut(value_proj, side, chan, 1),
                state_proj,
                jnp.pad(cut(step_proj, side, heads, 1), ((0, 0), (0, 128 - heads))),
            ],
            axis=1,
        )

    w_own = packed(r)
    w_rec = swap(packed(1 - r), "row")
    hid_rec = swap(hidden, "row")
    cot_rec = swap(cotangent, "row")
    wo_own = cut(output_proj, r, chan, 0)
    wo_part = cut(output_proj, 1 - r, chan, 0)
    wo_rec = swap(wo_part, "row")
    gain_f = gated_gain.astype(F32)
    gain_rec = swap(input_gain, "row")
    gains = jnp.concatenate([input_gain[None], gain_rec[None], jnp.zeros((6, half), F32)], axis=0)

    skip_lane = jnp.repeat(skip_gain, chan // heads)
    vtap = jnp.concatenate(
        [value_filter, value_shift[None], skip_lane[None], gain_f[None], jnp.zeros((1, chan), F32)], axis=0
    )
    stap = jnp.concatenate([shared_kernel, shared_offset[None], jnp.zeros((3, 256), F32)], axis=0)
    pad_h = (0, 8 - heads)
    head_par = jnp.concatenate([jnp.pad(step_bias, pad_h), jnp.pad(-jnp.exp(decay_log), pad_h)])
    head_par = jnp.broadcast_to(head_par[:, None], (16, 128))

    lane_head = jnp.arange(chan) // (chan // heads)
    sel = (jnp.arange(16)[:, None] == lane_head[None, :]).astype(BF16)
    out, proj_own, proj_col, dn_sum, dn_col, trow, rs, recip = layer(
        seq_len,
        dp,
        hidden,
        hid_rec,
        cotangent,
        cot_rec,
        gains,
        w_own,
        w_rec,
        vtap,
        stap,
        head_par,
        wo_own,
        wo_rec,
        sel,
    )
    outs = finish(
        big_rows(dp, width),
        heads,
        out,
        hidden,
        cotangent,
        dn_sum,
        dn_col,
        proj_own,
        proj_col,
        sel,
        trow,
        recip,
        rs,
        gains,
    )
    return tuple(outs[0:4]) + (outs[4].T,) + tuple(outs[5:])


def solution(mesh):
    in_specs = (
        P("dp", "row"),
        P("row", "col"),
        P("row", "col"),
        P("row", "col"),
        P("row", None),
        P(None, ("col", "row")),
        P(("col", "row")),
        P(),
        P(),
        P(("col", "row")),
        P(("col", "row")),
        P(("col", "row")),
        P("row"),
        P(("col", "row")),
        P("col", "row"),
        P("dp", "row"),
    )
    out_specs = (
        P("dp", "row"),
        P("dp", "row"),
        P("row", "col"),
        P("row", "col"),
        P("row", "col"),
        P("row", None),
        P(None, ("col", "row")),
        P(("col", "row")),
        P(),
        P(),
        P(("col", "row")),
        P(("col", "row")),
        P(("col", "row")),
        P("row"),
        P(("col", "row")),
        P("col", "row"),
    )
    return jax.shard_map(body, mesh=mesh, in_specs=in_specs, out_specs=out_specs, check_vma=False)
```

```python
import functools

import jax
import jax.numpy as jnp
from jax import lax
from jax.experimental import pallas as pl
from jax.experimental.pallas import tpu as pltpu
from jax.sharding import PartitionSpec as P

LEN = 2048
EPSILON = 1e-05
SUB = 128
STEP = 256
F32 = jnp.float32
BF16 = jnp.bfloat16
AR_SPLIT = 2
EARLY_NEAR = [1, 2, 3, 4, 5, 7]
EARLY_FAR = [1, 3, 4, 5, 7]


def dot(a, b):
    return jnp.dot(a, b, preferred_element_type=F32)


def dot_nt(a, b):
    return lax.dot_general(a, b, (((1,), (1,)), ((), ())), preferred_element_type=F32)


def dot_tn(a, b):
    return lax.dot_general(a, b, (((0,), (0,)), ((), ())), preferred_element_type=F32)


def sigmoid(x):
    return 0.5 * jnp.tanh(0.5 * x) + 0.5


def softplus(x):
    return jnp.maximum(x, 0.0) + jnp.log1p(jnp.exp(-jnp.abs(x)))


def fold8(x):
    return jnp.sum(x.reshape(x.shape[0] // 8, 8, x.shape[1]), axis=0)


def row_scan(x, mat):
    hi = x.astype(BF16).astype(F32)
    rest = x - hi
    mid = rest.astype(BF16).astype(F32)
    low = rest - mid
    parts = jnp.concatenate([hi, mid, low, jnp.zeros_like(x)], axis=0).astype(BF16)
    out = dot(parts, mat)
    return out[0:8] + out[8:16] + out[16:24]


def plain_sums(sel, z):
    return dot_nt(sel, z.astype(BF16))[0:8]


def head_sums(sel, z):
    hi = z.astype(BF16)
    low = (z - hi.astype(F32)).astype(BF16)
    return (dot_nt(sel, hi) + dot_nt(sel, low))[0:8]


def iota(shape, dim):
    return lax.broadcasted_iota(jnp.int32, shape, dim)


def spread(cols, first, rows):
    lane = iota((rows, 128), 1)
    return jnp.where(
        lane < 64,
        jnp.broadcast_to(cols[:, first : first + 1], (rows, 128)),
        jnp.broadcast_to(cols[:, first + 1 : first + 2], (rows, 128)),
    )


def pair_stack(x):
    lane = iota(x.shape, 1)
    zero = jnp.zeros_like(x)
    return jnp.concatenate([jnp.where(lane < 64, x, zero), jnp.where(lane < 64, zero, x)], axis=0)


def forward_block(width, weights_in, outs_a, outs_b, scratch):
    hid_own, hid_rec, gains, w_own, w_rec, vtap, stap, head_par, wo_own, wo_rec = weights_in
    mixed_out, pre_gate_out, pre_value_out, conv_value_out, pre_shared_out, conv_shared_out = outs_a
    y_out, state_out, rows_out, nt_out = outs_b
    state, vbuf, sbuf, po_own, po_send, square_rows = scratch
    chan = mixed_out.shape[1]
    pairs = chan // 128

    h0 = hid_own[...].astype(F32)
    h1 = hid_rec[...].astype(F32)
    square = jnp.sum(h0 * h0, axis=1, keepdims=True) + jnp.sum(h1 * h1, axis=1, keepdims=True)
    recip = lax.rsqrt(square / width + EPSILON)
    n0 = (h0 * gains[0:1, :]).astype(BF16)
    n1 = (h1 * gains[1:2, :]).astype(BF16)
    half = n0.shape[1]
    nt_out[0:half, :] = jnp.transpose(n0)
    nt_out[half : 2 * half, :] = jnp.transpose(n1)
    q = dot(n0, w_own[...]) + dot(n1, w_rec[...])
    pre = q * recip
    gate = pre[:, 0:chan]
    pre_gate_out[...] = gate
    pre_value = pre[:, chan : 2 * chan]
    pre_value_out[...] = pre_value.astype(BF16)
    pre_shared = pre[:, 2 * chan : 2 * chan + 256]
    pre_shared_out[...] = pre_shared.astype(BF16)
    vbuf[8 : 8 + STEP, :] = pre_value
    sbuf[8 : 8 + STEP, :] = pre_shared
    conv = jnp.broadcast_to(vtap[4:5, :], (STEP, chan))
    conv_s = jnp.broadcast_to(stap[4:5, :], (STEP, 256))
    for k in range(4):
        conv = conv + vbuf[5 + k : 5 + k + STEP, :] * vtap[k : k + 1, :]
        conv_s = conv_s + sbuf[5 + k : 5 + k + STEP, :] * stap[k : k + 1, :]
    vbuf[0:8, :] = vbuf[STEP : STEP + 8, :]
    sbuf[0:8, :] = sbuf[STEP : STEP + 8, :]
    conv_value_out[...] = conv
    conv_shared_out[...] = conv_s
    x = conv * sigmoid(conv)
    act = conv_s * sigmoid(conv_s)

    head_rows = jnp.transpose(pre[:, 2 * chan + 256 : 2 * chan + 384])
    first = lax.axis_index("row") == 0
    v = jnp.where(first, head_rows[0:8], head_rows[6:14]) + head_par[0:8, 0:1]
    steps = softplus(v)
    logd = head_par[8:16, 0:1] * steps
    rows_out[0:8, :] = v
    rows_out[16:24, :] = jnp.transpose(jnp.broadcast_to(recip, (STEP, 128)))[0:8]

    upper = (iota((SUB, SUB), 0) <= iota((SUB, SUB), 1)).astype(F32).astype(BF16)
    causal = iota((SUB, SUB), 0) >= iota((SUB, SUB), 1)
    sg = gate * sigmoid(gate)
    for sub in range(STEP // SUB):
        lo, hi = sub * SUB, (sub + 1) * SUB
        cum_r = row_scan(logd[:, lo:hi], upper)
        rows_out[8:16, lo:hi] = cum_r
        cols = jnp.transpose(jnp.concatenate([cum_r, steps[:, lo:hi]], axis=0))
        b_in = act[lo:hi, 0:128]
        b_bf = b_in.astype(BF16)
        c_bf = act[lo:hi, 128:256].astype(BF16)
        b_t = jnp.transpose(b_in).astype(BF16)
        scores = dot_nt(c_bf, b_bf)
        for p in range(pairs):
            pl0, pl1 = p * 128, (p + 1) * 128
            c0 = jnp.broadcast_to(cols[:, 2 * p : 2 * p + 1], (SUB, 128))
            c1 = jnp.broadcast_to(cols[:, 2 * p + 1 : 2 * p + 2], (SUB, 128))
            weights = []
            for col, h in ((c0, 2 * p), (c1, 2 * p + 1)):
                gap = jnp.where(causal, col - cum_r[h : h + 1, :], -1e30)
                weights.append((scores * jnp.exp(gap)).astype(BF16))
            lane = iota((SUB, 128), 1)
            cum_e = jnp.where(lane < 64, c0, c1)
            step_e = spread(cols, 8 + 2 * p, SUB)
            xs = x[lo:hi, pl0:pl1]
            xh = step_e * xs
            inside = dot(jnp.concatenate(weights, axis=1), pair_stack(xh.astype(BF16)))
            held = state[:, pl0:pl1]
            held_bf = held.astype(BF16)
            state_out[lo:hi, pl0:pl1] = held_bf
            carried = dot(c_bf, held_bf)
            y = inside + carried * jnp.exp(cum_e)
            y_out[lo:hi, pl0:pl1] = y
            last = cum_e[SUB - 1 : SUB, :]
            tail = (xh * jnp.exp(last - cum_e)).astype(BF16)
            state[:, pl0:pl1] = held * jnp.exp(last) + dot(b_t, tail)
            y = y + vtap[5:6, pl0:pl1] * xs
            mixed_out[lo:hi, pl0:pl1] = (y * sg[lo:hi, pl0:pl1]).astype(BF16)
    mix = mixed_out[...].astype(F32)
    weighted = (mix * vtap[6:7, :]).astype(BF16)
    po_own[...] = dot(weighted, wo_own[...]).astype(BF16)
    po_send[...] = dot(weighted, wo_rec[...]).astype(BF16)
    square_rows[0:4, :] = plain_sums(jnp.ones((16, chan), BF16), mix * mix)[0:4]


def early_steps(dp, blocks):
    count = 2 * (dp.bit_length() - 1)
    if count == 6 and blocks == 8:
        return EARLY_NEAR, EARLY_FAR
    steps = [min(blocks - 1, 1 + n * (blocks - 1) // count) for n in range(count)]
    return steps, steps[:-1]


def partner_of(me, k):
    return {"dp": me + (1 - 2 * lax.rem(me // (1 << k), 2)) * (1 << k)}


def levels(dp, me, bounds, orders, acc, stage, land, out, send_sem, recv_sem):
    bits = dp.bit_length() - 1

    def span(start, rows):
        return pl.ds(pl.multiple_of(start, 16), rows)

    def bit_of(k):
        return lax.rem(me // (1 << k), 2)

    def low_at(i, count):
        low, rows = bounds[i]
        for n in range(count):
            low = low + bit_of(orders[i][n]) * (rows >> (n + 1))
        return low

    def places(i, level):
        base, rows = bounds[i]
        if level < bits:
            k = orders[i][level]
            part = rows >> (level + 1)
            give = span(low_at(i, level) + (1 - bit_of(k)) * part, part)
            where = span(base + rows - (rows >> level), part)
            return k, give, where, span(low_at(i, level + 1), part)
        back = 2 * bits - 1 - level
        own = span(low_at(i, back + 1), rows >> (back + 1))
        return orders[i][back], own, own, None

    def copy_of(i, level):
        k, give, where, _ = places(i, level)
        src, dst = (stage, land) if level < bits else (out, out)
        return remote(
            src.at[give, :], dst.at[where, :], send_sem.at[i, level], recv_sem.at[i, level], partner_of(me, k)
        )

    def start_level(i, level):
        if level < bits:
            give = places(i, level)[1]
            stage[give, :] = acc[give, :].astype(BF16)
        copy_of(i, level).start()

    def end_level(i, level, go_on=True):
        copy_of(i, level).wait()
        if level < bits:
            _, _, where, keep = places(i, level)
            total = acc[keep, :] + land[where, :].astype(F32)
            acc[keep, :] = total
            if level == bits - 1:
                out[keep, :] = total.astype(BF16)
        if go_on and level + 1 < 2 * bits:
            start_level(i, level + 1)

    return start_level, end_level


def gate_block(ins, outs):
    cot_own, cot_rec, wo_own, wo_rec, trow, rows_in, mixed, pre_gate, conv_value, y_in, vtap = ins
    acc_v, go_own, go_rec, dy_out, p_gate, rs_gate = outs
    chan = mixed.shape[1]
    tcol = jnp.transpose(jnp.concatenate([trow[...], rows_in[16:24, :]], axis=0))
    scale = tcol[:, 0:1]
    coef = tcol[:, 8:9]
    recip = tcol[:, 16:17]
    s0 = (cot_own[...].astype(F32) * scale).astype(BF16)
    s1 = (cot_rec[...].astype(F32) * scale).astype(BF16)
    d_weighted = dot_nt(s0, wo_own[...]) + dot_nt(s1, wo_rec[...])
    mix = mixed[...].astype(F32)
    acc_v[48:56, :] += fold8(d_weighted * mix)
    weighted_t = jnp.transpose((mix * vtap[6:7, :]).astype(BF16))
    go_own[...] += dot(weighted_t, s0)
    go_rec[...] += dot(weighted_t, s1)
    d_mixed = d_weighted * vtap[6:7, :] - coef * mix
    gate = pre_gate[...]
    sig = sigmoid(gate)
    silu = gate * sig
    conv = conv_value[...]
    sig_v = sigmoid(conv)
    x = conv * sig_v
    y_scan = y_in[...]
    y = y_scan + vtap[5:6, :] * x
    dy = d_mixed * silu
    d_gate = d_mixed * y * (sig + silu * (1.0 - sig))
    acc_v[40:48, :] += fold8(dy * x)
    dy_out[...] = dy.astype(BF16)
    p_gate[...] = (recip * d_gate).astype(BF16)
    rs_gate[...] = plain_sums(jnp.ones((16, chan), BF16), d_gate * gate)


def scan_block(ins, weights_in, outs, scratch):
    rows_in, pre_value, conv_value, pre_shared, conv_shared, y_in, state_in = ins
    vtap, stap, head_par, sel_ref, dy_in = weights_in
    p_out, rsum_out, acc_v, acc_s, acc_h = outs
    grad, vbuf, sbuf, dxbuf, dbbuf = scratch
    chan = conv_value.shape[1]
    pairs = chan // 128

    recip = jnp.transpose(rows_in[16:24, :])[:, 0:1]
    conv = conv_value[...]
    sig_v = sigmoid(conv)
    x = conv * sig_v
    dy_bf = dy_in[...]
    conv_s = conv_shared[...]
    sig_s = sigmoid(conv_s)
    act = conv_s * sig_s

    sel = sel_ref[...]
    sel_f = sel.astype(F32)[0:8]
    v = rows_in[0:8, :]
    steps = softplus(v)
    logd = head_par[8:16, 0:1] * steps
    lower = (iota((SUB, SUB), 0) >= iota((SUB, SUB), 1)).astype(F32).astype(BF16)
    strict = (iota((SUB, SUB), 0) < iota((SUB, SUB), 1)).astype(F32).astype(BF16)
    causal_t = iota((SUB, SUB), 0) <= iota((SUB, SUB), 1)
    for sub in reversed(range(STEP // SUB)):
        lo, hi = sub * SUB, (sub + 1) * SUB
        cum_r = rows_in[8:16, lo:hi]
        cols = jnp.transpose(jnp.concatenate([cum_r, steps[:, lo:hi]], axis=0))
        b_bf = act[lo:hi, 0:128].astype(BF16)
        c_in = act[lo:hi, 128:256]
        c_bf = c_in.astype(BF16)
        c_t = jnp.transpose(c_in).astype(BF16)
        scores_t = dot_nt(b_bf, c_bf)
        d_scores = jnp.zeros((SUB, SUB), F32)
        db = jnp.zeros((SUB, 128), F32)
        dc = jnp.zeros((SUB, 128), F32)
        z_sum = jnp.zeros((8, SUB), F32)
        e_sum = jnp.zeros((8, SUB), F32)
        f_sum = jnp.zeros((8, SUB), F32)
        gh = jnp.zeros((8, 1), F32)
        for p in range(pairs):
            pl0, pl1 = p * 128, (p + 1) * 128
            c0 = jnp.broadcast_to(cols[:, 2 * p : 2 * p + 1], (SUB, 128))
            c1 = jnp.broadcast_to(cols[:, 2 * p + 1 : 2 * p + 2], (SUB, 128))
            decays = []
            for col, h in ((c0, 2 * p), (c1, 2 * p + 1)):
                gap = jnp.where(causal_t, cum_r[h : h + 1, :] - col, -1e30)
                decays.append(jnp.exp(gap))
            weights = [(scores_t * d).astype(BF16) for d in decays]
            lane = iota((SUB, 128), 1)
            cum_e = jnp.where(lane < 64, c0, c1)
            step_e = spread(cols, 8 + 2 * p, SUB)
            xs = x[lo:hi, pl0:pl1]
            xh = step_e * xs
            xh_bf = xh.astype(BF16)
            dys_bf = dy_bf[lo:hi, pl0:pl1]
            dys = dys_bf.astype(F32)
            stack = pair_stack(dys_bf)
            inner = dot(jnp.concatenate(weights, axis=1), stack)
            d_pair = dot_nt(xh_bf, stack)
            d_scores = d_scores + decays[0] * d_pair[:, 0:128] + decays[1] * d_pair[:, 128:256]
            last = cum_e[SUB - 1 : SUB, :]
            tail_e = jnp.exp(last - cum_e)
            g = grad[:, pl0:pl1]
            g_bf = g.astype(BF16)
            outer = dot(b_bf, g_bf) * tail_e
            u = inner + outer
            dxbuf[lo:hi, pl0:pl1] = step_e * u + vtap[5:6, pl0:pl1] * dys
            db = db + dot_nt((xh * tail_e).astype(BF16), g_bf)
            dya = (dys * jnp.exp(cum_e)).astype(BF16)
            held = state_in[lo:hi, pl0:pl1]
            dc = dc + dot_nt(dya, held)
            sel_p = sel[:, pl0:pl1]
            z_sum = z_sum + head_sums(
                sel_p, dys * y_in[lo:hi, pl0:pl1] - xh_bf.astype(F32) * inner
            )
            e_sum = e_sum + plain_sums(sel_p, xh * outer)
            f_sum = f_sum + plain_sums(sel_p, xs * u)
            decay_row = jnp.exp(last)
            gh_row = decay_row * jnp.sum(g * held.astype(F32), axis=0, keepdims=True)
            gh = gh + jnp.sum(sel_f[:, pl0:pl1] * gh_row, axis=1, keepdims=True)
            grad[:, pl0:pl1] = g * decay_row + dot(c_t, dya)
        ds_bf = d_scores.astype(BF16)
        dbbuf[lo:hi, 0:128] = db + dot(ds_bf, c_bf)
        dbbuf[lo:hi, 128:256] = dc + dot(jnp.transpose(d_scores).astype(BF16), b_bf)
        d_log = row_scan(z_sum, lower) + row_scan(e_sum, strict) + gh
        d_step = (f_sum + d_log * head_par[8:16, 0:1]) * sigmoid(v[:, lo:hi])
        acc_h[0:8, :] += d_log * logd[:, lo:hi]
        acc_h[8:16, :] += d_step
        pre_step = v[:, lo:hi] - head_par[0:8, 0:1]
        rsum_out[:, lo:hi] += jnp.broadcast_to(
            jnp.sum(d_step * pre_step, axis=0, keepdims=True), (8, SUB)
        )
        zeros = jnp.zeros((6, SUB), F32)
        both = jnp.where(
            lax.axis_index("row") == 0,
            jnp.concatenate([d_step[0:6], zeros, zeros[0:4]], axis=0),
            jnp.concatenate([zeros, d_step[0:6], zeros[0:4]], axis=0),
        )
        d_cols = jnp.transpose(jnp.concatenate([both, jnp.zeros((112, SUB), F32)], axis=0))
        p_out[lo:hi, chan + 256 : chan + 384] = (recip[lo:hi] * d_cols).astype(BF16)

    d_conv = dxbuf[...] * (sig_v + x * (1.0 - sig_v))
    d_conv_s = dbbuf[...] * (sig_s + act * (1.0 - sig_s))
    vbuf[0:STEP, :] = d_conv
    sbuf[0:STEP, :] = d_conv_s
    acc_v[32:40, :] += fold8(d_conv)
    acc_s[32:40, :] += fold8(d_conv_s)
    pv = pre_value[...].astype(F32)
    ps = pre_shared[...].astype(F32)
    d_value = jnp.zeros((STEP, chan), F32)
    d_shared = jnp.zeros((STEP, 256), F32)
    for k in range(4):
        moved = vbuf[3 - k : 3 - k + STEP, :]
        d_value = d_value + vtap[k : k + 1, :] * moved
        acc_v[8 * k : 8 * k + 8, :] += fold8(pv * moved)
        moved = sbuf[3 - k : 3 - k + STEP, :]
        d_shared = d_shared + stap[k : k + 1, :] * moved
        acc_s[8 * k : 8 * k + 8, :] += fold8(ps * moved)
    vbuf[STEP : STEP + 8, :] = vbuf[0:8, :]
    sbuf[STEP : STEP + 8, :] = sbuf[0:8, :]
    p_out[:, 0:chan] = (recip * d_value).astype(BF16)
    p_out[:, chan : chan + 256] = (recip * d_shared).astype(BF16)
    ones = jnp.ones((16, chan), BF16)
    rsum_out[...] += plain_sums(ones, d_value * pv)
    rsum_out[...] += plain_sums(ones[:, 0:256], d_shared * ps)


def width_block(valid, ins, outs):
    p_gate, p_all, hid_own, hid_rec, w_own, w_rec = ins
    dn_own, dn_rec, acc_n = outs
    chan = p_gate.shape[1]
    pg = p_gate[...]
    pb = p_all[...]
    for n, (hid, weight, dn) in enumerate(((hid_own, w_own, dn_own), (hid_rec, w_rec, dn_rec))):
        part = dot_nt(pg, weight[:, 0:chan]) + dot_nt(pb, weight[:, chan:])
        dn[...] = part.astype(BF16)
        acc_n[8 * n : 8 * n + 8, :] += jnp.where(valid, fold8(part * hid[...].astype(F32)), 0.0)


def unit_rows(dp):
    return 16 * dp


def misc_rows(dp, rows):
    unit = max(unit_rows(dp), 256)
    return pl.cdiv(rows, unit) * unit


def big_rows(dp, rows):
    return pl.cdiv(rows, unit_rows(dp)) * unit_rows(dp)


def remote(src, dst, send, recv, target):
    return pltpu.make_async_remote_copy(
        src_ref=src,
        dst_ref=dst,
        send_sem=send,
        recv_sem=recv,
        device_id=target,
        device_id_type=pl.DeviceIdType.MESH,
    )


def greet(targets):
    barrier = pltpu.get_barrier_semaphore()
    for target in targets:
        pl.semaphore_signal(barrier, inc=1, device_id=target, device_id_type=pl.DeviceIdType.MESH)
    pl.semaphore_wait(barrier, len(targets))


def layer_kernel(
    seq_len,
    dp,
    inner_width,
    hid_hbm,
    cot_hbm,
    gate_w,
    value_w,
    state_w,
    out_w,
    step_t,
    value_filter,
    value_shift,
    shared_kernel,
    shared_offset,
    decay_log,
    step_bias,
    skip_gain,
    input_gain,
    gated_gain,
    sums_out,
    proj_out,
    proj_col,
    dn_out,
    dn_col,
    trow,
    rs_out,
    recip_out,
    state_out,
    w_own,
    w_rec,
    wo_own,
    wo_rec,
    vtap,
    stap,
    head_par,
    head_rows,
    gains,
    gains_land,
    sel,
    hid_own,
    hid_rec,
    cot_own,
    cot_rec,
    pre_gate,
    pre_value,
    conv_value,
    pre_shared,
    conv_shared,
    y_scan,
    states,
    mixed,
    rows,
    normed_t,
    p_gate,
    p_all,
    dy_s,
    rs_in,
    state,
    vbuf,
    sbuf,
    dxbuf,
    dbbuf,
    pair_own,
    pair_send,
    pair_land,
    proj_s,
    dn_sum,
    sums,
    sums_land,
    go_rec,
    swap_send,
    swap_land,
    extra_send,
    extra_land,
    extra_sum,
    shared_sum,
    col_land,
    rs_land,
    acc_v,
    acc_s,
    acc_h,
    acc_n,
    acc,
    stage,
    land,
    out,
    load_sem,
    feed_sem,
    weight_sem,
    save_sem,
    po_sem,
    dn_sem,
    col_sem,
    sum_sem,
    swap_sem,
    ar_send_sem,
    ar_recv_sem,
    out_sem,
):
    tokens, half = hid_own.shape
    chan = mixed.shape[1]
    width = 2 * half
    wide = p_all.shape[1]
    blocks = tokens // STEP
    steps_per_seq = seq_len // STEP
    size = big_rows(dp, width)
    tail = out.shape[0] - 3 * size
    bits = dp.bit_length() - 1
    me = lax.axis_index("dp")
    r = lax.axis_index("row")
    c = lax.axis_index("col")
    to_row, to_col, to_both = {"row": 1 - r}, {"col": 1 - c}, {"row": 1 - r, "col": 1 - c}
    part_rows = size // AR_SPLIT
    near = tuple(range(bits))
    far = tuple(range(1, bits)) + (0,)
    bounds = [(tail + n * part_rows, part_rows) for n in range(3 * AR_SPLIT)] + [(0, tail)]
    orders = [far if n % 2 else near for n in range(3 * AR_SPLIT)] + [near]
    firsts, values, misc = range(2 * AR_SPLIT), range(2 * AR_SPLIT, 3 * AR_SPLIT), 3 * AR_SPLIT
    start_level, end_level = levels(dp, me, bounds, orders, acc, stage, land, out, ar_send_sem, ar_recv_sem)

    def span(i):
        return pl.ds(pl.multiple_of(i * STEP, STEP), STEP)

    def load(n, i):
        src, dst = ((hid_hbm, hid_own), (cot_hbm, cot_own))[n]
        return pltpu.make_async_copy(src.at[span(i), :], dst.at[span(i), :], load_sem.at[n, i])

    def feed(n, i):
        src, dst = ((hid_hbm, hid_rec), (cot_hbm, cot_rec))[n]
        return remote(src.at[span(i), :], dst.at[span(i), :], feed_sem.at[0, n, i], feed_sem.at[1, n, i], to_row)

    def weight_parts(side, to_w, to_wo):
        cols = pl.ds(pl.multiple_of(side * chan, 128), chan)
        return (
            (gate_w.at[:, cols], to_w.at[:, 0:chan]),
            (value_w.at[:, cols], to_w.at[:, chan : 2 * chan]),
            (state_w, to_w.at[:, 2 * chan : 2 * chan + 256]),
            (out_w.at[cols, :], to_wo),
        )

    own_weights = [
        pltpu.make_async_copy(src, dst, weight_sem.at[0, n])
        for n, (src, dst) in enumerate(weight_parts(r, w_own, wo_own))
    ]
    rec_weights = [
        remote(src, dst, weight_sem.at[1, n], weight_sem.at[2, n], to_row)
        for n, (src, dst) in enumerate(weight_parts(1 - r, w_rec, wo_rec))
    ]
    step_cols = pl.ds(2 * chan + 256, 128)
    rec_weights.append(
        remote(w_own.at[:, step_cols], w_rec.at[:, step_cols], weight_sem.at[1, 4], weight_sem.at[2, 4], to_row)
    )
    rec_weights.append(remote(gains, gains_land, weight_sem.at[1, 5], weight_sem.at[2, 5], to_row))

    def save(n, i):
        src, dst = ((proj_s, proj_out), (dn_sum, dn_out))[n]
        return pltpu.make_async_copy(src.at[span(i), :], dst.at[span(i), :], save_sem.at[n, i])

    def pair_copy(sem, i):
        return remote(pair_send.at[span(i), :], pair_land.at[span(i), :], sem.at[0, i], sem.at[1, i], to_row)

    def small_copy(src, dst, n, target):
        return remote(src, dst, swap_sem.at[0, n], swap_sem.at[1, n], target)

    for copy in own_weights:
        copy.start()
    for n in range(2):
        for i in range(blocks):
            load(n, i).start()
    heads = decay_log.shape[0]
    sel[...] = (iota(sel.shape, 0) == iota(sel.shape, 1) // 64).astype(F32).astype(BF16)
    head_rows[...] = jnp.zeros_like(head_rows)
    for n, ref in enumerate((step_bias, decay_log, skip_gain)):
        head_rows[n, 0:heads] = ref[...]
    head_cols = jnp.transpose(head_rows[...])[0:8]
    real = iota((8, 128), 0) < heads
    head_par[0:8, :] = jnp.broadcast_to(head_cols[:, 0:1], (8, 128))
    head_par[8:16, :] = jnp.where(real, -jnp.exp(jnp.broadcast_to(head_cols[:, 1:2], (8, 128))), 0.0)
    vtap[0:4, :] = value_filter[...]
    vtap[4, :] = value_shift[...]
    vtap[5:6, :] = jnp.sum(sel[0:8, :].astype(F32) * head_cols[:, 2:3], axis=0, keepdims=True)
    vtap[6, :] = gated_gain[...].astype(F32)
    stap[0:4, :] = shared_kernel[...]
    stap[4, :] = shared_offset[...]
    gains[...] = jnp.zeros_like(gains)
    gains[0, :] = input_gain[...]
    dxbuf[0:128, :] = jnp.zeros((128, half), F32)
    dxbuf[0 : step_t.shape[0], :] = step_t[...].astype(F32)
    w_own[:, 2 * chan + 256 : 2 * chan + 384] = jnp.transpose(dxbuf[0:128, :]).astype(BF16)
    greet([partner_of(me, k) for k in range(bits)] + [to_row, to_col, to_both])
    for copy in rec_weights:
        copy.start()
    for n in range(2):
        for i in range(blocks):
            feed(n, i).start()

    def chunk_rows(n, side):
        return pl.ds(pl.multiple_of(tail + n * size + side * half, 128), half)

    go_own = acc.at[chunk_rows(0, r), :]
    for ref in (acc_v, acc_s, acc_h, acc_n, go_rec):
        ref[...] = jnp.zeros_like(ref)
    go_own[...] = jnp.zeros((chan, half), F32)

    for copy in own_weights + rec_weights:
        copy.wait()
    gains[1:2, :] = gains_land[0:1, :]

    def sums_copy(n, i):
        target = (to_row, to_col, to_both)[n]
        return remote(sums.at[i], sums_land.at[n, i], sum_sem.at[0, n, i], sum_sem.at[1, n, i], target)

    def take_proj(i):
        pair_copy(po_sem, i).wait()
        part = pair_own[span(i), :].astype(F32) + pair_land[span(i), :].astype(F32)
        proj_s[span(i), :] = part.astype(BF16)
        dots = plain_sums(jnp.ones((16, half), BF16), part * cot_own[span(i), :].astype(F32))
        sums[i, 4:8, :] = dots[4:8]
        for n in range(3):
            sums_copy(n, i).start()
        save(0, i).start()

    def take_sums(i):
        for n in range(3):
            sums_copy(n, i).wait()
        total = (sums[i] + sums_land[0, i]) + (sums_land[1, i] + sums_land[2, i])
        scale = lax.rsqrt(total[0:1] / inner_width + EPSILON)
        coef = total[4:5] * (scale * scale * scale) / inner_width
        trow[0:8, span(i)] = jnp.broadcast_to(scale, (8, STEP))
        trow[8:16, span(i)] = jnp.broadcast_to(coef, (8, STEP))

    def forward(i):
        here = span(i)
        forward_block(
            width,
            (
                hid_own.at[here, :],
                hid_rec.at[here, :],
                gains,
                w_own,
                w_rec,
                vtap,
                stap,
                head_par,
                wo_own,
                wo_rec,
            ),
            (
                mixed.at[here, :],
                pre_gate.at[here, :],
                pre_value.at[here, :],
                conv_value.at[here, :],
                pre_shared.at[here, :],
                conv_shared.at[here, :],
            ),
            (y_scan.at[here, :], states.at[here, :], rows.at[:, here], normed_t.at[:, here]),
            (state, vbuf, sbuf, pair_own.at[here, :], pair_send.at[here, :], sums.at[i]),
        )

    def gate(i):
        here = span(i)
        gate_block(
            (
                cot_own.at[here, :],
                cot_rec.at[here, :],
                wo_own,
                wo_rec,
                trow.at[:, here],
                rows.at[:, here],
                mixed.at[here, :],
                pre_gate.at[here, :],
                conv_value.at[here, :],
                y_scan.at[here, :],
                vtap,
            ),
            (acc_v, go_own, go_rec, dy_s.at[here, :], p_gate.at[here, :], rs_in.at[:, here]),
        )

    first_part = max(1, blocks // 4)
    proj_parts = [(0, first_part), (first_part, blocks)]
    half_way = blocks // 2
    dn_parts = [(half_way, blocks), (0, half_way)] if half_way else [(0, blocks)]

    def wide_copy(n, part, index):
        src, dst = ((proj_s, proj_col), (dn_sum, dn_col))[n]
        rows_n = pl.ds(part[0] * STEP, (part[1] - part[0]) * STEP)
        return remote(src.at[rows_n, :], dst.at[rows_n, :], col_sem.at[n, 0, index], col_sem.at[n, 1, index], to_col)

    @pl.loop(0, blocks)
    def _(i):
        load(0, i).wait()
        feed(0, i).wait()

        @pl.when(i % steps_per_seq == 0)
        def _():
            state[...] = jnp.zeros_like(state)
            vbuf[0:8, :] = jnp.zeros((8, chan), F32)
            sbuf[0:8, :] = jnp.zeros((8, 256), F32)

        forward(i)
        load(1, i).wait()
        feed(1, i).wait()

        @pl.when(i > 0)
        def _():
            take_proj(i - 1)

        pair_copy(po_sem, i).start()
        if first_part < blocks:

            @pl.when(i == first_part)
            def _():
                wide_copy(0, proj_parts[0], 0).start()

    take_proj(blocks - 1)
    if first_part < blocks:
        wide_copy(0, proj_parts[1], 1).start()
    else:
        wide_copy(0, proj_parts[0], 0).start()
    recip_out[...] = rows[16:24, :]

    @pl.loop(0, blocks)
    def _(i):
        take_sums(i)
        gate(i)

    swaps = [small_copy(swap_send.at[n], swap_land.at[n], n, to_row) for n in range(2)]
    swap_send[0] = go_rec[...].astype(BF16)
    swaps[0].start()
    swap_send[1] = dot(normed_t[half:width, :], p_gate[...]).astype(BF16)
    swaps[1].start()
    acc[chunk_rows(1, r), :] = dot(normed_t[0:half, :], p_gate[...])
    if size > width:
        for n in range(3):
            acc[tail + n * size + width : tail + (n + 1) * size, :] = jnp.zeros((size - width, chan), F32)
    for n in range(2):
        swaps[n].wait()
        acc[chunk_rows(n, 1 - r), :] = swap_land[n].astype(F32)
        for i in range(AR_SPLIT):
            start_level(n * AR_SPLIT + i, 0)

    def take_dn(i):
        pair_copy(dn_sem, i).wait()
        part = pair_own[span(i), :].astype(F32) + pair_land[span(i), :].astype(F32)
        dn_sum[span(i), :] = part.astype(BF16)
        save(1, i).start()

    def over_width(valid, i):
        here = span(i)
        width_block(
            valid,
            (p_gate.at[here, :], p_all.at[here, :], hid_own.at[here, :], hid_rec.at[here, :], w_own, w_rec),
            (pair_own.at[here, :], pair_send.at[here, :], acc_n),
        )

    p_all[span(blocks - 1), :] = jnp.zeros((STEP, wide), BF16)

    @pl.loop(0, blocks)
    def _(later):
        i = blocks - 1 - later
        here = span(i)

        @pl.when(later % steps_per_seq == 0)
        def _():
            state[...] = jnp.zeros_like(state)
            vbuf[STEP : STEP + 8, :] = jnp.zeros((8, chan), F32)
            sbuf[STEP : STEP + 8, :] = jnp.zeros((8, 256), F32)

        over_width(later > 0, jnp.minimum(i + 1, blocks - 1))
        scan_block(
            (
                rows.at[:, here],
                pre_value.at[here, :],
                conv_value.at[here, :],
                pre_shared.at[here, :],
                conv_shared.at[here, :],
                y_scan.at[here, :],
                states.at[here, :],
            ),
            (vtap, stap, head_par, sel, dy_s.at[here, :]),
            (p_all.at[here, :], rs_in.at[:, here], acc_v, acc_s, acc_h),
            (state, vbuf, sbuf, dxbuf, dbbuf),
        )

        @pl.when(later > 1)
        def _():
            take_dn(i + 2)
            for index, part in enumerate(dn_parts[:-1]):

                @pl.when(i + 2 == part[0])
                def _(index=index, part=part):
                    wide_copy(1, part, index).start()

        @pl.when(later > 0)
        def _():
            pair_copy(dn_sem, i + 1).start()

        for kind, steps in enumerate(early_steps(dp, blocks)):
            for level, when in enumerate(steps):

                @pl.when(later == when)
                def _(kind=kind, level=level):
                    for n in firsts[kind::2]:
                        end_level(n, level)

    over_width(True, 0)
    pair_copy(dn_sem, 0).start()
    if blocks > 1:
        take_dn(1)

    def sum8(ref, n):
        return jnp.sum(ref[8 * n : 8 * n + 8, :], axis=0, keepdims=True)

    small = jnp.concatenate([sum8(acc_s, n) for n in range(5)] + [jnp.zeros((3, 256), F32)], axis=0)
    norm_own, norm_rec = [
        jnp.concatenate([sum8(acc_n, n), jnp.zeros((1, 512 - half), F32)], axis=1) for n in (0, 1)
    ]
    pad6 = jnp.zeros((6, 256), F32)
    misc_row = small_copy(swap_send.at[0], swap_land.at[0], 4, to_row)
    value_row = small_copy(swap_send.at[1], swap_land.at[1], 5, to_row)
    swap_send[1] = dot(normed_t[half:width, :], p_all[:, 0:chan]).astype(BF16)
    value_row.start()
    extra_send[...] = jnp.concatenate([small, norm_rec[:, 0:256], norm_rec[:, 256:512], pad6], axis=0)
    extra_row = small_copy(extra_send, extra_land.at[0], 2, to_row)
    extra_row.start()
    rs_row = small_copy(rs_in, rs_land.at[0], 3, to_row)
    rs_row.start()
    acc[chunk_rows(2, r), :] = dot(normed_t[0:half, :], p_all[:, 0:chan])
    value_row.wait()
    acc[chunk_rows(2, 1 - r), :] = swap_land[1].astype(F32)
    for n in values:
        start_level(n, 0)
    swap_send[0] = dot(normed_t[half:width, :], p_all[:, chan:wide]).astype(BF16)
    misc_row.start()
    extra_row.wait()
    extra = jnp.concatenate([small, norm_own[:, 0:256], norm_own[:, 256:512], pad6], axis=0)
    extra_sum[...] = extra + extra_land[0]
    extra_col = small_copy(extra_sum, extra_land.at[1], 6, to_col)
    extra_col.start()
    shared = dot(normed_t[0:half, :], p_all[:, chan:wide])
    split = half // 2
    misc_row.wait()
    shared_sum[...] = (shared[:, 0:256] + swap_land[0, :, 0:256].astype(F32)).astype(BF16)
    theirs = pl.ds(pl.multiple_of((1 - c) * split, 16), split)
    state_col = small_copy(shared_sum.at[theirs, :], col_land, 7, to_col)
    state_col.start()
    step_t = jnp.transpose(shared[:, 256:384] + swap_land[0, :, 256:384].astype(F32))[0:16]
    rs_row.wait()
    rs_out[...] = rs_in[...] + rs_land[0]
    rs_col = small_copy(rs_out, rs_land.at[1], 8, to_col)
    rs_col.start()
    take_dn(0)
    wide_copy(1, dn_parts[-1], len(dn_parts) - 1).start()

    acc[0:split, 256:384] = jnp.zeros((split, 128), F32)
    first = split
    acc[first : first + 16, 256:384] = jnp.zeros((16, 128), F32)
    acc[first + 16 : first + 24, :] = jnp.concatenate(
        [sum8(acc_v, n) for n in range(7)] + [jnp.zeros((1, chan), F32)], axis=0
    )
    acc[first + 24 : first + 40, :] = jnp.broadcast_to(
        jnp.sum(acc_h[...], axis=1, keepdims=True), (16, chan)
    )
    acc[first + 40 : first + 56, :] = step_t
    if tail > first + 56:
        acc[first + 56 : tail, :] = jnp.zeros((tail - first - 56, chan), F32)
    extra_col.wait()
    acc[first : first + 16, 0:256] = extra_sum[...] + extra_land[1]
    state_col.wait()
    acc[0:split, 0:256] = (
        shared_sum[pl.ds(pl.multiple_of(c * split, 16), split), :].astype(F32)
        + col_land[...].astype(F32)
    )
    start_level(misc, 0)
    mine = pl.ds(pl.multiple_of(c * split, 16), split)
    last_col = small_copy(out.at[pl.ds(0, split), pl.ds(0, 256)], state_out.at[mine, :], 9, to_col)
    done = []

    def save_chunk(n):
        rows_n = pl.ds(*bounds[n])
        copy = pltpu.make_async_copy(out.at[rows_n, :], sums_out.at[rows_n, :], out_sem.at[n])
        copy.start()
        done.append(copy)

    for n in firsts[0::2]:
        save_chunk(n)
    for level in range(2 * bits):
        if level == 0:
            for n in firsts[1::2]:
                end_level(n, 2 * bits - 1)
                save_chunk(n)
        if level == 2 * bits - 1:
            end_level(misc, level)
            last_col.start()
            save_chunk(misc)
            state_out[mine, :] = out[0:split, 0:256]
        for n in values:
            end_level(n, level)
            if level == 2 * bits - 1:
                save_chunk(n)
        if level < 2 * bits - 1:
            end_level(misc, level)
    for copy in done:
        copy.wait()
    last_col.wait()
    rs_col.wait()
    rs_out[...] = rs_out[...] + rs_land[1]
    for i in range(blocks):
        for n in range(2):
            save(n, i).wait()
    for n, parts in enumerate((proj_parts if first_part < blocks else proj_parts[:1], dn_parts)):
        for index, part in enumerate(parts):
            wide_copy(n, part, index).wait()


def layer(seq_len, dp, hidden, cot, gate_w, value_w, state_w, out_w, *params):
    tokens, half = hidden.shape
    chan = params[1].shape[1]
    wide = chan + 384
    bits = dp.bit_length() - 1
    size = big_rows(dp, 2 * half)
    tail = misc_rows(dp, half // 2 + 64)
    total = tail + 3 * size
    blocks = tokens // STEP
    vmem = pl.BlockSpec(memory_space=pltpu.VMEM)
    hbm = pl.BlockSpec(memory_space=pl.ANY)

    def act(cols=half, dtype=BF16):
        return jax.ShapeDtypeStruct((tokens, cols), dtype)

    def room(*shape, dtype=BF16):
        return pltpu.VMEM(shape, dtype)

    def flags(*shape):
        return pltpu.SemaphoreType.DMA(shape)

    return pl.pallas_call(
        functools.partial(layer_kernel, seq_len, dp, 4 * chan),
        in_specs=[hbm] * 6 + [vmem] * len(params),
        out_specs=[hbm, hbm, hbm, hbm, hbm, vmem, vmem, vmem, vmem],
        out_shape=[
            jax.ShapeDtypeStruct((total, chan), BF16),
            act(),
            act(),
            act(),
            act(),
            jax.ShapeDtypeStruct((16, tokens), F32),
            jax.ShapeDtypeStruct((8, tokens), F32),
            jax.ShapeDtypeStruct((8, tokens), F32),
            jax.ShapeDtypeStruct((half, 256), BF16),
        ],
        scratch_shapes=[
            room(half, chan + wide),
            room(half, chan + wide),
            room(chan, half),
            room(chan, half),
            room(8, chan, dtype=F32),
            room(8, 256, dtype=F32),
            room(16, 128, dtype=F32),
            room(8, 128, dtype=F32),
            room(8, half, dtype=F32),
            room(8, half, dtype=F32),
            room(16, chan),
            room(tokens, half),
            room(tokens, half),
            room(tokens, half),
            room(tokens, half),
            room(tokens, chan, dtype=F32),
            room(tokens, chan),
            room(tokens, chan, dtype=F32),
            room(tokens, 256),
            room(tokens, 256, dtype=F32),
            room(tokens, chan, dtype=F32),
            room(tokens, chan),
            room(tokens, chan),
            room(24, tokens, dtype=F32),
            room(2 * half, tokens),
            room(tokens, chan),
            room(tokens, wide),
            room(tokens, chan),
            room(8, tokens, dtype=F32),
            room(128, chan, dtype=F32),
            room(STEP + 8, chan, dtype=F32),
            room(STEP + 8, 256, dtype=F32),
            room(STEP, chan, dtype=F32),
            room(STEP, 256, dtype=F32),
            room(tokens, half),
            room(tokens, half),
            room(tokens, half),
            room(tokens, half),
            room(tokens, half),
            room(blocks, 8, STEP, dtype=F32),
            room(3, blocks, 8, STEP, dtype=F32),
            room(chan, half, dtype=F32),
            room(2, half, chan),
            room(2, half, chan),
            room(16, 256, dtype=F32),
            room(2, 16, 256, dtype=F32),
            room(16, 256, dtype=F32),
            room(half, 256),
            room(half // 2, 256),
            room(2, 8, tokens, dtype=F32),
            room(56, chan, dtype=F32),
            room(40, 256, dtype=F32),
            room(16, 128, dtype=F32),
            room(16, half, dtype=F32),
            room(total, chan, dtype=F32),
            room(total, chan),
            room(total, chan),
            room(total, chan),
            flags(2, blocks),
            flags(2, 2, blocks),
            flags(3, 6),
            flags(2, blocks),
            flags(2, blocks),
            flags(2, blocks),
            flags(2, 2, 3),
            flags(2, 3, blocks),
            flags(2, 10),
            flags(3 * AR_SPLIT + 1, 2 * bits),
            flags(3 * AR_SPLIT + 1, 2 * bits),
            flags(3 * AR_SPLIT + 1),
        ],
        compiler_params=pltpu.CompilerParams(
            collective_id=0, has_side_effects=True, vmem_limit_bytes=67_000_000
        ),
        name="layer",
    )(hidden, cot, gate_w, value_w, state_w, out_w, *params)


def finish_kernel(
    width,
    out_rows,
    gate_a,
    gate_b,
    value_a,
    value_b,
    misc,
    state,
    hid,
    cot,
    dn_sum,
    dn_col,
    proj_own,
    proj_col,
    trow,
    recip_in,
    rs,
    gains,
    result,
    hidden_grad,
    g_gate,
    g_value,
    g_step,
    g_state,
    g_filter,
    g_shift,
    g_kernel,
    g_offset,
    g_decay,
    g_bias,
    g_skip,
    g_norm,
    g_gated,
    g_output,
):
    half = hid.shape[1]
    hid32 = hid[...].astype(F32)
    recip = recip_in[...]
    cols = jnp.transpose(jnp.concatenate([trow[0:8, :], rs[...] * recip * recip / width], axis=0))
    proj = proj_own[...].astype(F32) + proj_col[...].astype(F32)
    result[...] = (hid32 + cols[:, 0:1] * proj).astype(BF16)
    d_normed = dn_sum[...].astype(F32) + dn_col[...].astype(F32)
    hidden_grad[...] = cot[...].astype(F32) + d_normed * gains[...].reshape(1, half) - cols[:, 8:9] * hid32
    @pl.when(pl.program_id(0) < half // 128)
    def _():
        g_output[...] = out_rows[...].astype(F32)
        g_gate[:, 0:half] = gate_a[...].astype(F32)
        g_gate[:, half : 2 * half] = gate_b[...].astype(F32)
        g_value[:, 0:half] = value_a[...].astype(F32)
        g_value[:, half : 2 * half] = value_b[...].astype(F32)

    @pl.when(pl.program_id(0) == 0)
    def _():
        g_state[...] = state[...].astype(F32)
        small = misc[half // 2 : half // 2 + 64, :].astype(F32)
        heads = g_step.shape[0] // 2
        g_step[...] = small[40 : 40 + 2 * heads]
        g_kernel[...] = small[0:4, 0:256]
        g_offset[...] = small[4, 0:256]
        g_norm[0:256] = small[8, 0:256]
        g_norm[256:half] = small[9, 0 : half - 256]
        g_filter[...] = small[16:20]
        g_shift[...] = small[20]
        g_gated[...] = small[22]
        head = jnp.transpose(small[24:40, 0:128])[0:8]
        g_decay[...] = head[0, 0:heads]
        g_bias[...] = head[0, 8 : 8 + heads]
        sel = (iota((16, half), 0) == iota((16, half), 1) // (half // heads)).astype(F32).astype(BF16)
        skip = dot_nt(small[16:32].astype(BF16), sel)
        g_skip[...] = skip[5, 0:heads]


def finish(size, heads, out, state, hid, cot, dn_sum, dn_col, proj_own, proj_col, trow, recip, rs, params):
    tokens, half = hid.shape
    chan = out.shape[1]
    size_f = tokens // 4
    grid = 4

    def blk(cols):
        return pl.BlockSpec((size_f, cols), lambda i: (i, 0))

    def row(count):
        return pl.BlockSpec((count, size_f), lambda i: (0, i))

    def whole(shape):
        return pl.BlockSpec(shape, lambda i: (0,) * len(shape))

    parts = half // 128
    tail = out.shape[0] - 3 * size

    def part(start):
        return pl.BlockSpec((128, chan), lambda i: (start // 128 + jnp.minimum(i, parts - 1), 0))

    def streamed(rows, cols):
        return pl.BlockSpec((rows // parts, cols), lambda i: (jnp.minimum(i, parts - 1), 0))

    small = [
        (2 * heads, half),
        (half, 256),
        (4, chan),
        (chan,),
        (4, 256),
        (256,),
        (heads,),
        (heads,),
        (heads,),
        (half,),
        (chan,),
    ]
    big = (half, 2 * chan)
    shapes = [big, big] + small + [(2 * chan, half)]
    return pl.pallas_call(
        functools.partial(finish_kernel, 2 * half),
        grid=(grid,),
        in_specs=[
            pl.BlockSpec((256, half), lambda i: (tail // 256 + jnp.minimum(i, parts - 1), 0)),
            part(tail + size),
            part(tail + size + half),
            part(tail + 2 * size),
            part(tail + 2 * size + half),
            whole((tail, chan)),
            whole(state.shape),
            blk(half),
            blk(half),
            blk(half),
            blk(half),
            blk(half),
            blk(half),
            row(16),
            row(8),
            row(8),
            whole((half,)),
        ],
        out_specs=[blk(half), blk(half), streamed(*big), streamed(*big)]
        + [whole(shape) for shape in small]
        + [streamed(2 * chan, half)],
        out_shape=[
            jax.ShapeDtypeStruct((tokens, half), BF16),
            jax.ShapeDtypeStruct((tokens, half), F32),
        ]
        + [jax.ShapeDtypeStruct(shape, F32) for shape in shapes],
        cost_estimate=pl.CostEstimate(flops=20_000_000, bytes_accessed=20_000_000, transcendentals=0),
        name="finish",
    )(
        out,
        out,
        out,
        out,
        out,
        out,
        state,
        hid,
        cot,
        dn_sum,
        dn_col,
        proj_own,
        proj_col,
        trow,
        recip,
        rs,
        params,
    )


def body(
    hidden,
    gate_proj,
    value_proj,
    step_proj,
    state_proj,
    value_filter,
    value_shift,
    shared_kernel,
    shared_offset,
    decay_log,
    step_bias,
    skip_gain,
    input_gain,
    gated_gain,
    output_proj,
    cotangent,
):
    tokens, half = hidden.shape
    width = 2 * half
    chan = gated_gain.shape[0]
    heads = decay_log.shape[0]
    dp = lax.axis_size("dp")
    seq_len = min(LEN, tokens)

    out, proj_own, proj_col, dn_sum, dn_col, trow, rs, recip, g_state = layer(
        seq_len,
        dp,
        hidden,
        cotangent,
        gate_proj,
        value_proj,
        state_proj,
        output_proj,
        step_proj.T,
        value_filter,
        value_shift,
        shared_kernel,
        shared_offset,
        decay_log,
        step_bias,
        skip_gain,
        input_gain,
        gated_gain,
    )
    outs = finish(
        big_rows(dp, width),
        heads,
        out,
        g_state,
        hidden,
        cotangent,
        dn_sum,
        dn_col,
        proj_own,
        proj_col,
        trow,
        recip,
        rs,
        input_gain,
    )
    return tuple(outs[0:4]) + (outs[4].T,) + tuple(outs[5:])


def solution(mesh):
    in_specs = (
        P("dp", "row"),
        P("row", "col"),
        P("row", "col"),
        P("row", "col"),
        P("row", None),
        P(None, ("col", "row")),
        P(("col", "row")),
        P(),
        P(),
        P(("col", "row")),
        P(("col", "row")),
        P(("col", "row")),
        P("row"),
        P(("col", "row")),
        P("col", "row"),
        P("dp", "row"),
    )
    out_specs = (
        P("dp", "row"),
        P("dp", "row"),
        P("row", "col"),
        P("row", "col"),
        P("row", "col"),
        P("row", None),
        P(None, ("col", "row")),
        P(("col", "row")),
        P(),
        P(),
        P(("col", "row")),
        P(("col", "row")),
        P(("col", "row")),
        P("row"),
        P(("col", "row")),
        P("col", "row"),
    )
    return jax.shard_map(body, mesh=mesh, in_specs=in_specs, out_specs=out_specs, check_vma=False)
```

```python
import functools

import jax
import jax.numpy as jnp
from jax import lax
from jax.experimental import pallas as pl
from jax.experimental.pallas import tpu as pltpu
from jax.sharding import PartitionSpec as P

LEN = 2048
EPSILON = 1e-05
LOG2E = 1.4426950408889634
SUB = 128
STEP = 256
F32 = jnp.float32
BF16 = jnp.bfloat16
AR_SPLIT = 2
EARLY_NEAR = [1, 2, 3, 4, 5, 7]
EARLY_FAR = [1, 3, 4, 5, 7]


def dot(a, b):
    return jnp.dot(a, b, preferred_element_type=F32)


def dot_nt(a, b):
    return lax.dot_general(a, b, (((1,), (1,)), ((), ())), preferred_element_type=F32)


def dot_tn(a, b):
    return lax.dot_general(a, b, (((0,), (0,)), ((), ())), preferred_element_type=F32)


def sigmoid(x):
    return 0.5 * jnp.tanh(0.5 * x) + 0.5


def softplus(x):
    return jnp.maximum(x, 0.0) + jnp.log1p(jnp.exp(-jnp.abs(x)))


def fold8(x):
    return jnp.sum(x.reshape(x.shape[0] // 8, 8, x.shape[1]), axis=0)


def row_scan(x, mat):
    hi = x.astype(BF16).astype(F32)
    rest = x - hi
    mid = rest.astype(BF16).astype(F32)
    low = rest - mid
    parts = jnp.concatenate([hi, mid, low, jnp.zeros_like(x)], axis=0).astype(BF16)
    out = dot(parts, mat)
    return out[0:8] + out[8:16] + out[16:24]


def plain_sums(sel, z):
    return dot_nt(sel, z.astype(BF16))[0:8]


def head_sums(sel, z):
    hi = z.astype(BF16)
    low = (z - hi.astype(F32)).astype(BF16)
    return (dot_nt(sel, hi) + dot_nt(sel, low))[0:8]


def iota(shape, dim):
    return lax.broadcasted_iota(jnp.int32, shape, dim)


def spread(cols, first, rows):
    lane = iota((rows, 128), 1)
    return jnp.where(
        lane < 64,
        jnp.broadcast_to(cols[:, first : first + 1], (rows, 128)),
        jnp.broadcast_to(cols[:, first + 1 : first + 2], (rows, 128)),
    )


def pair_stack(x):
    lane = iota(x.shape, 1)
    zero = jnp.zeros_like(x)
    return jnp.concatenate([jnp.where(lane < 64, x, zero), jnp.where(lane < 64, zero, x)], axis=0)


def forward_block(width, weights_in, outs_a, outs_b, scratch):
    hid_own, hid_rec, gains, w_own, w_rec, vtap, stap, head_par, wo_own, wo_rec = weights_in
    mixed_out, pre_gate_out, pre_value_out, conv_value_out, pre_shared_out, conv_shared_out = outs_a
    y_out, state_out, rows_out, nt_out = outs_b
    state, vbuf, sbuf, po_own, po_send, square_rows = scratch
    chan = mixed_out.shape[1]
    pairs = chan // 128

    h0 = hid_own[...].astype(F32)
    h1 = hid_rec[...].astype(F32)
    square = jnp.sum(h0 * h0, axis=1, keepdims=True) + jnp.sum(h1 * h1, axis=1, keepdims=True)
    recip = lax.rsqrt(square / width + EPSILON)
    n0 = (h0 * gains[0:1, :]).astype(BF16)
    n1 = (h1 * gains[1:2, :]).astype(BF16)
    half = n0.shape[1]
    nt_out[0:half, :] = jnp.transpose(n0)
    nt_out[half : 2 * half, :] = jnp.transpose(n1)
    q = dot(n0, w_own[...]) + dot(n1, w_rec[...])
    pre = q * recip
    gate = pre[:, 0:chan]
    pre_gate_out[...] = gate
    pre_value = pre[:, chan : 2 * chan]
    pre_value_out[...] = pre_value.astype(BF16)
    pre_shared = pre[:, 2 * chan : 2 * chan + 256]
    pre_shared_out[...] = pre_shared.astype(BF16)
    vbuf[8 : 8 + STEP, :] = pre_value
    sbuf[8 : 8 + STEP, :] = pre_shared
    conv = jnp.broadcast_to(vtap[4:5, :], (STEP, chan))
    conv_s = jnp.broadcast_to(stap[4:5, :], (STEP, 256))
    for k in range(4):
        conv = conv + vbuf[5 + k : 5 + k + STEP, :] * vtap[k : k + 1, :]
        conv_s = conv_s + sbuf[5 + k : 5 + k + STEP, :] * stap[k : k + 1, :]
    vbuf[0:8, :] = vbuf[STEP : STEP + 8, :]
    sbuf[0:8, :] = sbuf[STEP : STEP + 8, :]
    conv_value_out[...] = conv
    conv_shared_out[...] = conv_s
    x = conv * sigmoid(conv)
    act = conv_s * sigmoid(conv_s)

    head_rows = jnp.transpose(pre[:, 2 * chan + 256 : 2 * chan + 384])
    first = lax.axis_index("row") == 0
    v = jnp.where(first, head_rows[0:8], head_rows[6:14]) + head_par[0:8, 0:1]
    steps = softplus(v)
    logd = head_par[8:16, 0:1] * steps
    rows_out[0:8, :] = v
    rows_out[16:24, :] = jnp.transpose(jnp.broadcast_to(recip, (STEP, 128)))[0:8]

    upper = (iota((SUB, SUB), 0) <= iota((SUB, SUB), 1)).astype(F32).astype(BF16)
    causal = iota((SUB, SUB), 0) >= iota((SUB, SUB), 1)
    sg = gate * sigmoid(gate)
    for sub in range(STEP // SUB):
        lo, hi = sub * SUB, (sub + 1) * SUB
        cum_r = row_scan(logd[:, lo:hi] * LOG2E, upper)
        rows_out[8:16, lo:hi] = cum_r
        cols = jnp.transpose(jnp.concatenate([cum_r, steps[:, lo:hi]], axis=0))
        b_in = act[lo:hi, 0:128]
        b_bf = b_in.astype(BF16)
        c_bf = act[lo:hi, 128:256].astype(BF16)
        b_t = jnp.transpose(b_in).astype(BF16)
        scores = dot_nt(c_bf, b_bf)
        for p in range(pairs):
            pl0, pl1 = p * 128, (p + 1) * 128
            c0 = jnp.broadcast_to(cols[:, 2 * p : 2 * p + 1], (SUB, 128))
            c1 = jnp.broadcast_to(cols[:, 2 * p + 1 : 2 * p + 2], (SUB, 128))
            weights = []
            for col, h in ((c0, 2 * p), (c1, 2 * p + 1)):
                gap = jnp.where(causal, col - cum_r[h : h + 1, :], -1e30)
                weights.append((scores * jnp.exp2(gap)).astype(BF16))
            lane = iota((SUB, 128), 1)
            cum_e = jnp.where(lane < 64, c0, c1)
            step_e = spread(cols, 8 + 2 * p, SUB)
            xs = x[lo:hi, pl0:pl1]
            xh = step_e * xs
            inside = dot(jnp.concatenate(weights, axis=1), pair_stack(xh.astype(BF16)))
            held = state[:, pl0:pl1]
            held_bf = held.astype(BF16)
            state_out[lo:hi, pl0:pl1] = held_bf
            carried = dot(c_bf, held_bf)
            y = inside + carried * jnp.exp2(cum_e)
            y_out[lo:hi, pl0:pl1] = y
            last = cum_e[SUB - 1 : SUB, :]
            tail = (xh * jnp.exp2(last - cum_e)).astype(BF16)
            state[:, pl0:pl1] = held * jnp.exp2(last) + dot(b_t, tail)
            y = y + vtap[5:6, pl0:pl1] * xs
            mixed_out[lo:hi, pl0:pl1] = (y * sg[lo:hi, pl0:pl1]).astype(BF16)
    mix = mixed_out[...].astype(F32)
    weighted = (mix * vtap[6:7, :]).astype(BF16)
    po_own[...] = dot(weighted, wo_own[...]).astype(BF16)
    po_send[...] = dot(weighted, wo_rec[...]).astype(BF16)
    square_rows[0:4, :] = plain_sums(jnp.ones((16, chan), BF16), mix * mix)[0:4]


def early_steps(dp, blocks):
    count = 2 * (dp.bit_length() - 1)
    if count == 6 and blocks == 8:
        return EARLY_NEAR, EARLY_FAR
    steps = [min(blocks - 1, 1 + n * (blocks - 1) // count) for n in range(count)]
    return steps, steps[:-1]


def partner_of(me, k):
    return {"dp": me + (1 - 2 * lax.rem(me // (1 << k), 2)) * (1 << k)}


def levels(dp, me, bounds, orders, acc, stage, land, out, send_sem, recv_sem):
    bits = dp.bit_length() - 1

    def span(start, rows):
        return pl.ds(pl.multiple_of(start, 16), rows)

    def bit_of(k):
        return lax.rem(me // (1 << k), 2)

    def low_at(i, count):
        low, rows = bounds[i]
        for n in range(count):
            low = low + bit_of(orders[i][n]) * (rows >> (n + 1))
        return low

    def places(i, level):
        base, rows = bounds[i]
        if level < bits:
            k = orders[i][level]
            part = rows >> (level + 1)
            give = span(low_at(i, level) + (1 - bit_of(k)) * part, part)
            where = span(base + rows - (rows >> level), part)
            return k, give, where, span(low_at(i, level + 1), part)
        back = 2 * bits - 1 - level
        own = span(low_at(i, back + 1), rows >> (back + 1))
        return orders[i][back], own, own, None

    def copy_of(i, level):
        k, give, where, _ = places(i, level)
        src, dst = (stage, land) if level < bits else (out, out)
        return remote(
            src.at[give, :], dst.at[where, :], send_sem.at[i, level], recv_sem.at[i, level], partner_of(me, k)
        )

    def start_level(i, level):
        if level < bits:
            give = places(i, level)[1]
            stage[give, :] = acc[give, :].astype(BF16)
        copy_of(i, level).start()

    def end_level(i, level, go_on=True):
        copy_of(i, level).wait()
        if level < bits:
            _, _, where, keep = places(i, level)
            total = acc[keep, :] + land[where, :].astype(F32)
            acc[keep, :] = total
            if level == bits - 1:
                out[keep, :] = total.astype(BF16)
        if go_on and level + 1 < 2 * bits:
            start_level(i, level + 1)

    return start_level, end_level


def gate_block(ins, outs):
    cot_own, cot_rec, wo_own, wo_rec, trow, rows_in, mixed, pre_gate, conv_value, y_in, vtap = ins
    acc_v, go_own, go_rec, dy_out, p_gate, rs_gate = outs
    chan = mixed.shape[1]
    tcol = jnp.transpose(jnp.concatenate([trow[...], rows_in[16:24, :]], axis=0))
    scale = tcol[:, 0:1]
    coef = tcol[:, 8:9]
    recip = tcol[:, 16:17]
    s0 = (cot_own[...].astype(F32) * scale).astype(BF16)
    s1 = (cot_rec[...].astype(F32) * scale).astype(BF16)
    d_weighted = dot_nt(s0, wo_own[...]) + dot_nt(s1, wo_rec[...])
    mix = mixed[...].astype(F32)
    acc_v[48:56, :] += fold8(d_weighted * mix)
    weighted_t = jnp.transpose((mix * vtap[6:7, :]).astype(BF16))
    go_own[...] += dot(weighted_t, s0)
    go_rec[...] += dot(weighted_t, s1)
    d_mixed = d_weighted * vtap[6:7, :] - coef * mix
    gate = pre_gate[...]
    sig = sigmoid(gate)
    silu = gate * sig
    conv = conv_value[...]
    sig_v = sigmoid(conv)
    x = conv * sig_v
    y_scan = y_in[...]
    y = y_scan + vtap[5:6, :] * x
    dy = d_mixed * silu
    d_gate = d_mixed * y * (sig + silu * (1.0 - sig))
    acc_v[40:48, :] += fold8(dy * x)
    dy_out[...] = dy.astype(BF16)
    p_gate[...] = (recip * d_gate).astype(BF16)
    rs_gate[...] = plain_sums(jnp.ones((16, chan), BF16), d_gate * gate)


def scan_block(ins, weights_in, outs, scratch):
    rows_in, pre_value, conv_value, pre_shared, conv_shared, y_in, state_in = ins
    vtap, stap, head_par, sel_ref, dy_in = weights_in
    p_out, rsum_out, acc_v, acc_s, acc_h = outs
    grad, vbuf, sbuf, dxbuf, dbbuf = scratch
    chan = conv_value.shape[1]
    pairs = chan // 128

    recip = jnp.transpose(rows_in[16:24, :])[:, 0:1]
    conv = conv_value[...]
    sig_v = sigmoid(conv)
    x = conv * sig_v
    dy_bf = dy_in[...]
    conv_s = conv_shared[...]
    sig_s = sigmoid(conv_s)
    act = conv_s * sig_s

    sel = sel_ref[...]
    sel_f = sel.astype(F32)[0:8]
    v = rows_in[0:8, :]
    steps = softplus(v)
    logd = head_par[8:16, 0:1] * steps
    lower = (iota((SUB, SUB), 0) >= iota((SUB, SUB), 1)).astype(F32).astype(BF16)
    strict = (iota((SUB, SUB), 0) < iota((SUB, SUB), 1)).astype(F32).astype(BF16)
    causal_t = iota((SUB, SUB), 0) <= iota((SUB, SUB), 1)
    for sub in reversed(range(STEP // SUB)):
        lo, hi = sub * SUB, (sub + 1) * SUB
        cum_r = rows_in[8:16, lo:hi]
        cols = jnp.transpose(jnp.concatenate([cum_r, steps[:, lo:hi]], axis=0))
        b_bf = act[lo:hi, 0:128].astype(BF16)
        c_in = act[lo:hi, 128:256]
        c_bf = c_in.astype(BF16)
        c_t = jnp.transpose(c_in).astype(BF16)
        scores_t = dot_nt(b_bf, c_bf)
        d_scores = jnp.zeros((SUB, SUB), F32)
        db = jnp.zeros((SUB, 128), F32)
        dc = jnp.zeros((SUB, 128), F32)
        z_sum = jnp.zeros((8, SUB), F32)
        e_sum = jnp.zeros((8, SUB), F32)
        f_sum = jnp.zeros((8, SUB), F32)
        gh = jnp.zeros((8, 1), F32)
        for p in range(pairs):
            pl0, pl1 = p * 128, (p + 1) * 128
            c0 = jnp.broadcast_to(cols[:, 2 * p : 2 * p + 1], (SUB, 128))
            c1 = jnp.broadcast_to(cols[:, 2 * p + 1 : 2 * p + 2], (SUB, 128))
            decays = []
            for col, h in ((c0, 2 * p), (c1, 2 * p + 1)):
                gap = jnp.where(causal_t, cum_r[h : h + 1, :] - col, -1e30)
                decays.append(jnp.exp2(gap))
            weights = [(scores_t * d).astype(BF16) for d in decays]
            lane = iota((SUB, 128), 1)
            cum_e = jnp.where(lane < 64, c0, c1)
            step_e = spread(cols, 8 + 2 * p, SUB)
            xs = x[lo:hi, pl0:pl1]
            xh = step_e * xs
            xh_bf = xh.astype(BF16)
            dys_bf = dy_bf[lo:hi, pl0:pl1]
            dys = dys_bf.astype(F32)
            stack = pair_stack(dys_bf)
            inner = dot(jnp.concatenate(weights, axis=1), stack)
            d_pair = dot_nt(xh_bf, stack)
            d_scores = d_scores + decays[0] * d_pair[:, 0:128] + decays[1] * d_pair[:, 128:256]
            last = cum_e[SUB - 1 : SUB, :]
            tail_e = jnp.exp2(last - cum_e)
            g = grad[:, pl0:pl1]
            g_bf = g.astype(BF16)
            outer = dot(b_bf, g_bf) * tail_e
            u = inner + outer
            dxbuf[lo:hi, pl0:pl1] = step_e * u + vtap[5:6, pl0:pl1] * dys
            db = db + dot_nt((xh * tail_e).astype(BF16), g_bf)
            dya = (dys * jnp.exp2(cum_e)).astype(BF16)
            held = state_in[lo:hi, pl0:pl1]
            dc = dc + dot_nt(dya, held)
            sel_p = sel[:, pl0:pl1]
            z_sum = z_sum + head_sums(
                sel_p, dys * y_in[lo:hi, pl0:pl1] - xh_bf.astype(F32) * inner
            )
            e_sum = e_sum + plain_sums(sel_p, xh * outer)
            f_sum = f_sum + plain_sums(sel_p, xs * u)
            decay_row = jnp.exp2(last)
            gh_row = decay_row * jnp.sum(g * held.astype(F32), axis=0, keepdims=True)
            gh = gh + jnp.sum(sel_f[:, pl0:pl1] * gh_row, axis=1, keepdims=True)
            grad[:, pl0:pl1] = g * decay_row + dot(c_t, dya)
        ds_bf = d_scores.astype(BF16)
        dbbuf[lo:hi, 0:128] = db + dot(ds_bf, c_bf)
        dbbuf[lo:hi, 128:256] = dc + dot(jnp.transpose(d_scores).astype(BF16), b_bf)
        d_log = row_scan(z_sum, lower) + row_scan(e_sum, strict) + gh
        d_step = (f_sum + d_log * head_par[8:16, 0:1]) * sigmoid(v[:, lo:hi])
        acc_h[0:8, :] += d_log * logd[:, lo:hi]
        acc_h[8:16, :] += d_step
        pre_step = v[:, lo:hi] - head_par[0:8, 0:1]
        rsum_out[:, lo:hi] += jnp.broadcast_to(
            jnp.sum(d_step * pre_step, axis=0, keepdims=True), (8, SUB)
        )
        zeros = jnp.zeros((6, SUB), F32)
        both = jnp.where(
            lax.axis_index("row") == 0,
            jnp.concatenate([d_step[0:6], zeros, zeros[0:4]], axis=0),
            jnp.concatenate([zeros, d_step[0:6], zeros[0:4]], axis=0),
        )
        d_cols = jnp.transpose(jnp.concatenate([both, jnp.zeros((112, SUB), F32)], axis=0))
        p_out[lo:hi, chan + 256 : chan + 384] = (recip[lo:hi] * d_cols).astype(BF16)

    d_conv = dxbuf[...] * (sig_v + x * (1.0 - sig_v))
    d_conv_s = dbbuf[...] * (sig_s + act * (1.0 - sig_s))
    vbuf[0:STEP, :] = d_conv
    sbuf[0:STEP, :] = d_conv_s
    acc_v[32:40, :] += fold8(d_conv)
    acc_s[32:40, :] += fold8(d_conv_s)
    pv = pre_value[...].astype(F32)
    ps = pre_shared[...].astype(F32)
    d_value = jnp.zeros((STEP, chan), F32)
    d_shared = jnp.zeros((STEP, 256), F32)
    for k in range(4):
        moved = vbuf[3 - k : 3 - k + STEP, :]
        d_value = d_value + vtap[k : k + 1, :] * moved
        acc_v[8 * k : 8 * k + 8, :] += fold8(pv * moved)
        moved = sbuf[3 - k : 3 - k + STEP, :]
        d_shared = d_shared + stap[k : k + 1, :] * moved
        acc_s[8 * k : 8 * k + 8, :] += fold8(ps * moved)
    vbuf[STEP : STEP + 8, :] = vbuf[0:8, :]
    sbuf[STEP : STEP + 8, :] = sbuf[0:8, :]
    p_out[:, 0:chan] = (recip * d_value).astype(BF16)
    p_out[:, chan : chan + 256] = (recip * d_shared).astype(BF16)
    ones = jnp.ones((16, chan), BF16)
    rsum_out[...] += plain_sums(ones, d_value * pv)
    rsum_out[...] += plain_sums(ones[:, 0:256], d_shared * ps)


def width_block(valid, ins, outs):
    p_gate, p_all, hid_own, hid_rec, w_own, w_rec = ins
    dn_own, dn_rec, acc_n = outs
    chan = p_gate.shape[1]
    pg = p_gate[...]
    pb = p_all[...]
    for n, (hid, weight, dn) in enumerate(((hid_own, w_own, dn_own), (hid_rec, w_rec, dn_rec))):
        part = dot_nt(pg, weight[:, 0:chan]) + dot_nt(pb, weight[:, chan:])
        dn[...] = part.astype(BF16)
        acc_n[8 * n : 8 * n + 8, :] += jnp.where(valid, fold8(part * hid[...].astype(F32)), 0.0)


def unit_rows(dp):
    return 16 * dp


def misc_rows(dp, rows):
    unit = max(unit_rows(dp), 256)
    return pl.cdiv(rows, unit) * unit


def big_rows(dp, rows):
    return pl.cdiv(rows, unit_rows(dp)) * unit_rows(dp)


def remote(src, dst, send, recv, target):
    return pltpu.make_async_remote_copy(
        src_ref=src,
        dst_ref=dst,
        send_sem=send,
        recv_sem=recv,
        device_id=target,
        device_id_type=pl.DeviceIdType.MESH,
    )


def greet(targets):
    barrier = pltpu.get_barrier_semaphore()
    for target in targets:
        pl.semaphore_signal(barrier, inc=1, device_id=target, device_id_type=pl.DeviceIdType.MESH)
    pl.semaphore_wait(barrier, len(targets))


def layer_kernel(
    seq_len,
    dp,
    inner_width,
    hid_hbm,
    cot_hbm,
    gate_w,
    value_w,
    state_w,
    out_w,
    step_t,
    value_filter,
    value_shift,
    shared_kernel,
    shared_offset,
    decay_log,
    step_bias,
    skip_gain,
    input_gain,
    gated_gain,
    sums_out,
    result_out,
    hidden_out,
    proj_col,
    dn_col,
    state_out,
    trow,
    rs_out,
    w_own,
    w_rec,
    wo_own,
    wo_rec,
    vtap,
    stap,
    head_par,
    head_rows,
    gains,
    gains_land,
    sel,
    hid_own,
    hid_rec,
    cot_own,
    cot_rec,
    pre_gate,
    pre_value,
    conv_value,
    pre_shared,
    conv_shared,
    y_scan,
    states,
    mixed,
    rows,
    normed_t,
    p_gate,
    p_all,
    dy_s,
    rs_in,
    state,
    vbuf,
    sbuf,
    dxbuf,
    dbbuf,
    pair_own,
    pair_send,
    pair_land,
    proj_s,
    dn_sum,
    sums,
    sums_land,
    go_rec,
    swap_send,
    swap_land,
    extra_send,
    extra_land,
    extra_sum,
    shared_sum,
    col_land,
    rs_land,
    acc_v,
    acc_s,
    acc_h,
    acc_n,
    acc,
    stage,
    land,
    out,
    load_sem,
    feed_sem,
    weight_sem,
    fetch_sem,
    save_sem,
    po_sem,
    dn_sem,
    col_sem,
    sum_sem,
    swap_sem,
    ar_send_sem,
    ar_recv_sem,
    out_sem,
):
    tokens, half = hid_own.shape
    chan = mixed.shape[1]
    width = 2 * half
    wide = p_all.shape[1]
    blocks = tokens // STEP
    steps_per_seq = seq_len // STEP
    size = big_rows(dp, width)
    tail = out.shape[0] - 3 * size
    bits = dp.bit_length() - 1
    me = lax.axis_index("dp")
    r = lax.axis_index("row")
    c = lax.axis_index("col")
    to_row, to_col, to_both = {"row": 1 - r}, {"col": 1 - c}, {"row": 1 - r, "col": 1 - c}
    part_rows = size // AR_SPLIT
    near = tuple(range(bits))
    far = tuple(range(1, bits)) + (0,)
    bounds = [(tail + n * part_rows, part_rows) for n in range(3 * AR_SPLIT)] + [(0, tail)]
    orders = [far if n % 2 else near for n in range(3 * AR_SPLIT)] + [near]
    firsts, values, misc = range(2 * AR_SPLIT), range(2 * AR_SPLIT, 3 * AR_SPLIT), 3 * AR_SPLIT
    start_level, end_level = levels(dp, me, bounds, orders, acc, stage, land, out, ar_send_sem, ar_recv_sem)

    def span(i):
        return pl.ds(pl.multiple_of(i * STEP, STEP), STEP)

    def load(n, i):
        src, dst = ((hid_hbm, hid_own), (cot_hbm, cot_own))[n]
        return pltpu.make_async_copy(src.at[span(i), :], dst.at[span(i), :], load_sem.at[n, i])

    def feed(n, i):
        src, dst = ((hid_hbm, hid_rec), (cot_hbm, cot_rec))[n]
        return remote(src.at[span(i), :], dst.at[span(i), :], feed_sem.at[0, n, i], feed_sem.at[1, n, i], to_row)

    def weight_parts(side, to_w, to_wo):
        cols = pl.ds(pl.multiple_of(side * chan, 128), chan)
        return (
            (gate_w.at[:, cols], to_w.at[:, 0:chan]),
            (value_w.at[:, cols], to_w.at[:, chan : 2 * chan]),
            (state_w, to_w.at[:, 2 * chan : 2 * chan + 256]),
            (out_w.at[cols, :], to_wo),
        )

    own_weights = [
        pltpu.make_async_copy(src, dst, weight_sem.at[0, n])
        for n, (src, dst) in enumerate(weight_parts(r, w_own, wo_own))
    ]
    rec_weights = [
        remote(src, dst, weight_sem.at[1, n], weight_sem.at[2, n], to_row)
        for n, (src, dst) in enumerate(weight_parts(1 - r, w_rec, wo_rec))
    ]
    step_cols = pl.ds(2 * chan + 256, 128)
    rec_weights.append(
        remote(w_own.at[:, step_cols], w_rec.at[:, step_cols], weight_sem.at[1, 4], weight_sem.at[2, 4], to_row)
    )
    rec_weights.append(remote(gains, gains_land, weight_sem.at[1, 5], weight_sem.at[2, 5], to_row))

    def save(n, i):
        src, dst = ((pre_value, result_out), (p_gate, hidden_out))[n]
        return pltpu.make_async_copy(src.at[span(i), :], dst.at[span(i), :], save_sem.at[n, i])

    def fetch(n, i):
        src, dst = ((proj_col, mixed), (dn_col, dy_s))[n]
        return pltpu.make_async_copy(src.at[span(i), :], dst.at[span(i), :], fetch_sem.at[n, i])

    def pair_copy(sem, i):
        return remote(pair_send.at[span(i), :], pair_land.at[span(i), :], sem.at[0, i], sem.at[1, i], to_row)

    def small_copy(src, dst, n, target):
        return remote(src, dst, swap_sem.at[0, n], swap_sem.at[1, n], target)

    for copy in own_weights:
        copy.start()
    for n in range(2):
        for i in range(blocks):
            load(n, i).start()
    heads = decay_log.shape[0]
    sel[...] = (iota(sel.shape, 0) == iota(sel.shape, 1) // 64).astype(F32).astype(BF16)
    head_rows[...] = jnp.zeros_like(head_rows)
    for n, ref in enumerate((step_bias, decay_log, skip_gain)):
        head_rows[n, 0:heads] = ref[...]
    head_cols = jnp.transpose(head_rows[...])[0:8]
    real = iota((8, 128), 0) < heads
    head_par[0:8, :] = jnp.broadcast_to(head_cols[:, 0:1], (8, 128))
    head_par[8:16, :] = jnp.where(real, -jnp.exp(jnp.broadcast_to(head_cols[:, 1:2], (8, 128))), 0.0)
    vtap[0:4, :] = value_filter[...]
    vtap[4, :] = value_shift[...]
    vtap[5:6, :] = jnp.sum(sel[0:8, :].astype(F32) * head_cols[:, 2:3], axis=0, keepdims=True)
    vtap[6, :] = gated_gain[...].astype(F32)
    stap[0:4, :] = shared_kernel[...]
    stap[4, :] = shared_offset[...]
    gains[...] = jnp.zeros_like(gains)
    gains[0, :] = input_gain[...]
    dxbuf[0:128, :] = jnp.zeros((128, half), F32)
    dxbuf[0 : step_t.shape[0], :] = step_t[...].astype(F32)
    w_own[:, 2 * chan + 256 : 2 * chan + 384] = jnp.transpose(dxbuf[0:128, :]).astype(BF16)
    greet([partner_of(me, k) for k in range(bits)] + [to_row, to_col, to_both])
    for copy in rec_weights:
        copy.start()
    for n in range(2):
        for i in range(blocks):
            feed(n, i).start()

    def chunk_rows(n, side):
        return pl.ds(pl.multiple_of(tail + n * size + side * half, 128), half)

    go_own = acc.at[chunk_rows(0, r), :]
    for ref in (acc_v, acc_s, acc_h, acc_n, go_rec):
        ref[...] = jnp.zeros_like(ref)
    go_own[...] = jnp.zeros((chan, half), F32)

    for copy in own_weights + rec_weights:
        copy.wait()
    gains[1:2, :] = gains_land[0:1, :]

    def sums_copy(n, i):
        target = (to_row, to_col, to_both)[n]
        return remote(sums.at[i], sums_land.at[n, i], sum_sem.at[0, n, i], sum_sem.at[1, n, i], target)

    def take_proj(i):
        pair_copy(po_sem, i).wait()
        part = pair_own[span(i), :].astype(F32) + pair_land[span(i), :].astype(F32)
        proj_s[span(i), :] = part.astype(BF16)
        dots = plain_sums(jnp.ones((16, half), BF16), part * cot_own[span(i), :].astype(F32))
        sums[i, 4:8, :] = dots[4:8]
        for n in range(3):
            sums_copy(n, i).start()

    def take_sums(i):
        for n in range(3):
            sums_copy(n, i).wait()
        total = (sums[i] + sums_land[0, i]) + (sums_land[1, i] + sums_land[2, i])
        scale = lax.rsqrt(total[0:1] / inner_width + EPSILON)
        coef = total[4:5] * (scale * scale * scale) / inner_width
        trow[0:8, span(i)] = jnp.broadcast_to(scale, (8, STEP))
        trow[8:16, span(i)] = jnp.broadcast_to(coef, (8, STEP))

    def forward(i):
        here = span(i)
        forward_block(
            width,
            (
                hid_own.at[here, :],
                hid_rec.at[here, :],
                gains,
                w_own,
                w_rec,
                vtap,
                stap,
                head_par,
                wo_own,
                wo_rec,
            ),
            (
                mixed.at[here, :],
                pre_gate.at[here, :],
                pre_value.at[here, :],
                conv_value.at[here, :],
                pre_shared.at[here, :],
                conv_shared.at[here, :],
            ),
            (y_scan.at[here, :], states.at[here, :], rows.at[:, here], normed_t.at[:, here]),
            (state, vbuf, sbuf, pair_own.at[here, :], pair_send.at[here, :], sums.at[i]),
        )

    def gate(i):
        here = span(i)
        gate_block(
            (
                cot_own.at[here, :],
                cot_rec.at[here, :],
                wo_own,
                wo_rec,
                trow.at[:, here],
                rows.at[:, here],
                mixed.at[here, :],
                pre_gate.at[here, :],
                conv_value.at[here, :],
                y_scan.at[here, :],
                vtap,
            ),
            (acc_v, go_own, go_rec, dy_s.at[here, :], p_gate.at[here, :], rs_in.at[:, here]),
        )

    first_part = max(1, blocks // 4)
    proj_parts = [(0, first_part), (first_part, blocks)]
    half_way = blocks // 2
    dn_parts = [(half_way, blocks), (0, half_way)] if half_way else [(0, blocks)]

    def wide_copy(n, part, index):
        src, dst = ((proj_s, proj_col), (dn_sum, dn_col))[n]
        rows_n = pl.ds(part[0] * STEP, (part[1] - part[0]) * STEP)
        return remote(src.at[rows_n, :], dst.at[rows_n, :], col_sem.at[n, 0, index], col_sem.at[n, 1, index], to_col)

    @pl.loop(0, blocks)
    def _(i):
        load(0, i).wait()
        feed(0, i).wait()

        @pl.when(i % steps_per_seq == 0)
        def _():
            state[...] = jnp.zeros_like(state)
            vbuf[0:8, :] = jnp.zeros((8, chan), F32)
            sbuf[0:8, :] = jnp.zeros((8, 256), F32)

        forward(i)
        load(1, i).wait()
        feed(1, i).wait()

        @pl.when(i > 0)
        def _():
            take_proj(i - 1)

        pair_copy(po_sem, i).start()
        if first_part < blocks:

            @pl.when(i == first_part)
            def _():
                wide_copy(0, proj_parts[0], 0).start()

    take_proj(blocks - 1)
    if first_part < blocks:
        wide_copy(0, proj_parts[1], 1).start()
    else:
        wide_copy(0, proj_parts[0], 0).start()

    @pl.loop(0, blocks)
    def _(i):
        take_sums(i)
        gate(i)

    swaps = [small_copy(swap_send.at[n], swap_land.at[n], n, to_row) for n in range(2)]
    swap_send[0] = go_rec[...].astype(BF16)
    swaps[0].start()
    swap_send[1] = dot(normed_t[half:width, :], p_gate[...]).astype(BF16)
    swaps[1].start()
    acc[chunk_rows(1, r), :] = dot(normed_t[0:half, :], p_gate[...])
    if size > width:
        for n in range(3):
            acc[tail + n * size + width : tail + (n + 1) * size, :] = jnp.zeros((size - width, chan), F32)
    for n in range(2):
        swaps[n].wait()
        acc[chunk_rows(n, 1 - r), :] = swap_land[n].astype(F32)
        for i in range(AR_SPLIT):
            start_level(n * AR_SPLIT + i, 0)

    def take_dn(i):
        pair_copy(dn_sem, i).wait()
        part = pair_own[span(i), :].astype(F32) + pair_land[span(i), :].astype(F32)
        dn_sum[span(i), :] = part.astype(BF16)

    def over_width(valid, i):
        here = span(i)
        width_block(
            valid,
            (p_gate.at[here, :], p_all.at[here, :], hid_own.at[here, :], hid_rec.at[here, :], w_own, w_rec),
            (pair_own.at[here, :], pair_send.at[here, :], acc_n),
        )

    p_all[span(blocks - 1), :] = jnp.zeros((STEP, wide), BF16)

    @pl.loop(0, blocks)
    def _(later):
        i = blocks - 1 - later
        here = span(i)

        @pl.when(later % steps_per_seq == 0)
        def _():
            state[...] = jnp.zeros_like(state)
            vbuf[STEP : STEP + 8, :] = jnp.zeros((8, chan), F32)
            sbuf[STEP : STEP + 8, :] = jnp.zeros((8, 256), F32)

        over_width(later > 0, jnp.minimum(i + 1, blocks - 1))
        scan_block(
            (
                rows.at[:, here],
                pre_value.at[here, :],
                conv_value.at[here, :],
                pre_shared.at[here, :],
                conv_shared.at[here, :],
                y_scan.at[here, :],
                states.at[here, :],
            ),
            (vtap, stap, head_par, sel, dy_s.at[here, :]),
            (p_all.at[here, :], rs_in.at[:, here], acc_v, acc_s, acc_h),
            (state, vbuf, sbuf, dxbuf, dbbuf),
        )

        @pl.when(later > 1)
        def _():
            take_dn(i + 2)
            for index, part in enumerate(dn_parts[:-1]):

                @pl.when(i + 2 == part[0])
                def _(index=index, part=part):
                    wide_copy(1, part, index).start()

        @pl.when(later > 0)
        def _():
            pair_copy(dn_sem, i + 1).start()

        for kind, steps in enumerate(early_steps(dp, blocks)):
            for level, when in enumerate(steps):

                @pl.when(later == when)
                def _(kind=kind, level=level):
                    for n in firsts[kind::2]:
                        end_level(n, level)

    def sum8(ref, n):
        return jnp.sum(ref[8 * n : 8 * n + 8, :], axis=0, keepdims=True)

    misc_row = small_copy(swap_send.at[0], swap_land.at[0], 4, to_row)
    value_row = small_copy(swap_send.at[1], swap_land.at[1], 5, to_row)
    swap_send[1] = dot(normed_t[half:width, :], p_all[:, 0:chan]).astype(BF16)
    value_row.start()
    over_width(True, 0)
    pair_copy(dn_sem, 0).start()
    if blocks > 1:
        take_dn(1)
    small = jnp.concatenate([sum8(acc_s, n) for n in range(5)] + [jnp.zeros((3, 256), F32)], axis=0)
    norm_own, norm_rec = [
        jnp.concatenate([sum8(acc_n, n), jnp.zeros((1, 512 - half), F32)], axis=1) for n in (0, 1)
    ]
    pad6 = jnp.zeros((6, 256), F32)
    extra_send[...] = jnp.concatenate([small, norm_rec[:, 0:256], norm_rec[:, 256:512], pad6], axis=0)
    extra_row = small_copy(extra_send, extra_land.at[0], 2, to_row)
    extra_row.start()
    rs_row = small_copy(rs_in, rs_land.at[0], 3, to_row)
    rs_row.start()
    acc[chunk_rows(2, r), :] = dot(normed_t[0:half, :], p_all[:, 0:chan])
    value_row.wait()
    acc[chunk_rows(2, 1 - r), :] = swap_land[1].astype(F32)
    for n in values:
        start_level(n, 0)
    swap_send[0] = dot(normed_t[half:width, :], p_all[:, chan:wide]).astype(BF16)
    misc_row.start()
    extra_row.wait()
    extra = jnp.concatenate([small, norm_own[:, 0:256], norm_own[:, 256:512], pad6], axis=0)
    extra_sum[...] = extra + extra_land[0]
    extra_col = small_copy(extra_sum, extra_land.at[1], 6, to_col)
    extra_col.start()
    shared = dot(normed_t[0:half, :], p_all[:, chan:wide])
    split = half // 2
    misc_row.wait()
    shared_sum[...] = (shared[:, 0:256] + swap_land[0, :, 0:256].astype(F32)).astype(BF16)
    theirs = pl.ds(pl.multiple_of((1 - c) * split, 16), split)
    state_col = small_copy(shared_sum.at[theirs, :], col_land, 7, to_col)
    state_col.start()
    step_t = jnp.transpose(shared[:, 256:384] + swap_land[0, :, 256:384].astype(F32))[0:16]
    rs_row.wait()
    rs_out[...] = rs_in[...] + rs_land[0]
    rs_col = small_copy(rs_out, rs_land.at[1], 8, to_col)
    rs_col.start()
    take_dn(0)
    wide_copy(1, dn_parts[-1], len(dn_parts) - 1).start()

    acc[0:split, 256:384] = jnp.zeros((split, 128), F32)
    first = split
    acc[first : first + 16, 256:384] = jnp.zeros((16, 128), F32)
    acc[first + 16 : first + 24, :] = jnp.concatenate(
        [sum8(acc_v, n) for n in range(7)] + [jnp.zeros((1, chan), F32)], axis=0
    )
    acc[first + 24 : first + 40, :] = jnp.broadcast_to(
        jnp.sum(acc_h[...], axis=1, keepdims=True), (16, chan)
    )
    acc[first + 40 : first + 56, :] = step_t
    if tail > first + 56:
        acc[first + 56 : tail, :] = jnp.zeros((tail - first - 56, chan), F32)
    extra_col.wait()
    acc[first : first + 16, 0:256] = extra_sum[...] + extra_land[1]
    state_col.wait()
    acc[0:split, 0:256] = (
        shared_sum[pl.ds(pl.multiple_of(c * split, 16), split), :].astype(F32)
        + col_land[...].astype(F32)
    )
    start_level(misc, 0)

    parts_of = (proj_parts if first_part < blocks else proj_parts[:1], dn_parts)

    def arrive(n, index):
        part = parts_of[n][index]
        wide_copy(n, part, index).wait()

        @pl.loop(part[0], part[1])
        def _(i):
            fetch(n, i).start()

    def write_result(part):
        @pl.loop(part[0], part[1])
        def _(i):
            here = span(i)
            fetch(0, i).wait()
            scale = jnp.transpose(trow[0:8, here])[:, 0:1]
            proj = proj_s[here, :].astype(F32) + mixed[here, :].astype(F32)
            pre_value[here, :] = (hid_own[here, :].astype(F32) + scale * proj).astype(BF16)
            save(0, i).start()

    def write_hidden(part):
        @pl.loop(part[0], part[1])
        def _(i):
            here = span(i)
            fetch(1, i).wait()
            recip = rows[16:24, here]
            pull = jnp.transpose(rs_out[:, here] * recip * recip / width)[:, 0:1]
            d_normed = dn_sum[here, :].astype(F32) + dy_s[here, :].astype(F32)
            grad_in = cot_own[here, :].astype(F32) + d_normed * gains[0:1, :]
            p_gate[here, :] = (grad_in - pull * hid_own[here, :].astype(F32)).astype(BF16)
            save(1, i).start()

    mine = pl.ds(pl.multiple_of(c * split, 16), split)
    last_col = small_copy(out.at[pl.ds(0, split), pl.ds(0, 256)], state_out.at[mine, :], 9, to_col)
    done = []

    def save_chunk(n):
        rows_n = pl.ds(*bounds[n])
        copy = pltpu.make_async_copy(out.at[rows_n, :], sums_out.at[rows_n, :], out_sem.at[n])
        copy.start()
        done.append(copy)

    for n in firsts[0::2]:
        save_chunk(n)
    for level in range(2 * bits):
        if level == min(3, 2 * bits - 1):
            for index in range(len(parts_of[0])):
                arrive(0, index)
            write_result((0, blocks))
            rs_col.wait()
            rs_out[...] = rs_out[...] + rs_land[1]
        if level == min(5, 2 * bits - 1):
            for index in range(len(dn_parts) - 1):
                arrive(1, index)
                write_hidden(dn_parts[index])
        if level == 0:
            for n in firsts[1::2]:
                end_level(n, 2 * bits - 1)
                save_chunk(n)
        if level == 2 * bits - 1:
            end_level(misc, level)
            last_col.start()
            save_chunk(misc)
            state_out[mine, :] = out[0:split, 0:256]
        for n in values:
            end_level(n, level)
            if level == 2 * bits - 1:
                save_chunk(n)
        if level < 2 * bits - 1:
            end_level(misc, level)
    arrive(1, len(dn_parts) - 1)
    write_hidden(dn_parts[-1])
    for copy in done:
        copy.wait()
    last_col.wait()
    for i in range(blocks):
        for n in range(2):
            save(n, i).wait()


def layer(seq_len, dp, hidden, cot, gate_w, value_w, state_w, out_w, *params):
    tokens, half = hidden.shape
    chan = params[1].shape[1]
    wide = chan + 384
    bits = dp.bit_length() - 1
    size = big_rows(dp, 2 * half)
    tail = misc_rows(dp, half // 2 + 64)
    total = tail + 3 * size
    blocks = tokens // STEP
    vmem = pl.BlockSpec(memory_space=pltpu.VMEM)
    hbm = pl.BlockSpec(memory_space=pl.ANY)

    def act(cols=half, dtype=BF16):
        return jax.ShapeDtypeStruct((tokens, cols), dtype)

    def room(*shape, dtype=BF16):
        return pltpu.VMEM(shape, dtype)

    def flags(*shape):
        return pltpu.SemaphoreType.DMA(shape)

    return pl.pallas_call(
        functools.partial(layer_kernel, seq_len, dp, 4 * chan),
        in_specs=[hbm] * 6 + [vmem] * len(params),
        out_specs=[hbm] * 5 + [vmem],
        out_shape=[
            jax.ShapeDtypeStruct((total, chan), BF16),
            act(),
            act(),
            act(),
            act(),
            jax.ShapeDtypeStruct((half, 256), BF16),
        ],
        scratch_shapes=[
            room(16, tokens, dtype=F32),
            room(8, tokens, dtype=F32),
            room(half, chan + wide),
            room(half, chan + wide),
            room(chan, half),
            room(chan, half),
            room(8, chan, dtype=F32),
            room(8, 256, dtype=F32),
            room(16, 128, dtype=F32),
            room(8, 128, dtype=F32),
            room(8, half, dtype=F32),
            room(8, half, dtype=F32),
            room(16, chan),
            room(tokens, half),
            room(tokens, half),
            room(tokens, half),
            room(tokens, half),
            room(tokens, chan, dtype=F32),
            room(tokens, chan),
            room(tokens, chan, dtype=F32),
            room(tokens, 256),
            room(tokens, 256, dtype=F32),
            room(tokens, chan, dtype=F32),
            room(tokens, chan),
            room(tokens, chan),
            room(24, tokens, dtype=F32),
            room(2 * half, tokens),
            room(tokens, chan),
            room(tokens, wide),
            room(tokens, chan),
            room(8, tokens, dtype=F32),
            room(128, chan, dtype=F32),
            room(STEP + 8, chan, dtype=F32),
            room(STEP + 8, 256, dtype=F32),
            room(STEP, chan, dtype=F32),
            room(STEP, 256, dtype=F32),
            room(tokens, half),
            room(tokens, half),
            room(tokens, half),
            room(tokens, half),
            room(tokens, half),
            room(blocks, 8, STEP, dtype=F32),
            room(3, blocks, 8, STEP, dtype=F32),
            room(chan, half, dtype=F32),
            room(2, half, chan),
            room(2, half, chan),
            room(16, 256, dtype=F32),
            room(2, 16, 256, dtype=F32),
            room(16, 256, dtype=F32),
            room(half, 256),
            room(half // 2, 256),
            room(2, 8, tokens, dtype=F32),
            room(56, chan, dtype=F32),
            room(40, 256, dtype=F32),
            room(16, 128, dtype=F32),
            room(16, half, dtype=F32),
            room(total, chan, dtype=F32),
            room(total, chan),
            room(total, chan),
            room(total, chan),
            flags(2, blocks),
            flags(2, 2, blocks),
            flags(3, 6),
            flags(2, blocks),
            flags(2, blocks),
            flags(2, blocks),
            flags(2, blocks),
            flags(2, 2, 3),
            flags(2, 3, blocks),
            flags(2, 10),
            flags(3 * AR_SPLIT + 1, 2 * bits),
            flags(3 * AR_SPLIT + 1, 2 * bits),
            flags(3 * AR_SPLIT + 1),
        ],
        compiler_params=pltpu.CompilerParams(
            collective_id=0, has_side_effects=True, vmem_limit_bytes=67_000_000
        ),
        name="layer",
    )(hidden, cot, gate_w, value_w, state_w, out_w, *params)


def finish_kernel(
    out_rows,
    gate_a,
    gate_b,
    value_a,
    value_b,
    misc,
    state,
    result_in,
    hidden_in,
    result,
    hidden_grad,
    g_gate,
    g_value,
    g_step,
    g_state,
    g_filter,
    g_shift,
    g_kernel,
    g_offset,
    g_decay,
    g_bias,
    g_skip,
    g_norm,
    g_gated,
    g_output,
):
    half = result.shape[1]
    result[...] = result_in[...]
    hidden_grad[...] = hidden_in[...].astype(F32)

    @pl.when(pl.program_id(0) < half // 128)
    def _():
        g_output[...] = out_rows[...].astype(F32)
        g_gate[:, 0:half] = gate_a[...].astype(F32)
        g_gate[:, half : 2 * half] = gate_b[...].astype(F32)
        g_value[:, 0:half] = value_a[...].astype(F32)
        g_value[:, half : 2 * half] = value_b[...].astype(F32)

    @pl.when(pl.program_id(0) == 0)
    def _():
        g_state[...] = state[...].astype(F32)
        small = misc[half // 2 : half // 2 + 64, :].astype(F32)
        heads = g_step.shape[0] // 2
        g_step[...] = small[40 : 40 + 2 * heads]
        g_kernel[...] = small[0:4, 0:256]
        g_offset[...] = small[4, 0:256]
        g_norm[0:256] = small[8, 0:256]
        g_norm[256:half] = small[9, 0 : half - 256]
        g_filter[...] = small[16:20]
        g_shift[...] = small[20]
        g_gated[...] = small[22]
        head = jnp.transpose(small[24:40, 0:128])[0:8]
        g_decay[...] = head[0, 0:heads]
        g_bias[...] = head[0, 8 : 8 + heads]
        sel = (iota((16, half), 0) == iota((16, half), 1) // (half // heads)).astype(F32).astype(BF16)
        skip = dot_nt(small[16:32].astype(BF16), sel)
        g_skip[...] = skip[5, 0:heads]


def finish(size, heads, out, state, result, hidden_grad):
    tokens, half = result.shape
    chan = out.shape[1]
    size_f = tokens // 4
    grid = 4

    def blk(cols):
        return pl.BlockSpec((size_f, cols), lambda i: (i, 0))

    def whole(shape):
        return pl.BlockSpec(shape, lambda i: (0,) * len(shape))

    parts = half // 128
    tail = out.shape[0] - 3 * size

    def part(start):
        return pl.BlockSpec((128, chan), lambda i: (start // 128 + jnp.minimum(i, parts - 1), 0))

    def streamed(rows, cols):
        return pl.BlockSpec((rows // parts, cols), lambda i: (jnp.minimum(i, parts - 1), 0))

    small = [
        (2 * heads, half),
        (half, 256),
        (4, chan),
        (chan,),
        (4, 256),
        (256,),
        (heads,),
        (heads,),
        (heads,),
        (half,),
        (chan,),
    ]
    big = (half, 2 * chan)
    shapes = [big, big] + small + [(2 * chan, half)]
    return pl.pallas_call(
        finish_kernel,
        grid=(grid,),
        in_specs=[
            pl.BlockSpec((256, half), lambda i: (tail // 256 + jnp.minimum(i, parts - 1), 0)),
            part(tail + size),
            part(tail + size + half),
            part(tail + 2 * size),
            part(tail + 2 * size + half),
            whole((tail, chan)),
            whole(state.shape),
            blk(half),
            blk(half),
        ],
        out_specs=[blk(half), blk(half), streamed(*big), streamed(*big)]
        + [whole(shape) for shape in small]
        + [streamed(2 * chan, half)],
        out_shape=[
            jax.ShapeDtypeStruct((tokens, half), BF16),
            jax.ShapeDtypeStruct((tokens, half), F32),
        ]
        + [jax.ShapeDtypeStruct(shape, F32) for shape in shapes],
        cost_estimate=pl.CostEstimate(flops=20_000_000, bytes_accessed=20_000_000, transcendentals=0),
        name="finish",
    )(
        out,
        out,
        out,
        out,
        out,
        out,
        state,
        result,
        hidden_grad,
    )


def body(
    hidden,
    gate_proj,
    value_proj,
    step_proj,
    state_proj,
    value_filter,
    value_shift,
    shared_kernel,
    shared_offset,
    decay_log,
    step_bias,
    skip_gain,
    input_gain,
    gated_gain,
    output_proj,
    cotangent,
):
    tokens, half = hidden.shape
    width = 2 * half
    chan = gated_gain.shape[0]
    heads = decay_log.shape[0]
    dp = lax.axis_size("dp")
    seq_len = min(LEN, tokens)

    out, result, hidden_grad, _, _, g_state = layer(
        seq_len,
        dp,
        hidden,
        cotangent,
        gate_proj,
        value_proj,
        state_proj,
        output_proj,
        step_proj.T,
        value_filter,
        value_shift,
        shared_kernel,
        shared_offset,
        decay_log,
        step_bias,
        skip_gain,
        input_gain,
        gated_gain,
    )
    outs = finish(big_rows(dp, width), heads, out, g_state, result, hidden_grad)
    return tuple(outs[0:4]) + (outs[4].T,) + tuple(outs[5:])


def solution(mesh):
    in_specs = (
        P("dp", "row"),
        P("row", "col"),
        P("row", "col"),
        P("row", "col"),
        P("row", None),
        P(None, ("col", "row")),
        P(("col", "row")),
        P(),
        P(),
        P(("col", "row")),
        P(("col", "row")),
        P(("col", "row")),
        P("row"),
        P(("col", "row")),
        P("col", "row"),
        P("dp", "row"),
    )
    out_specs = (
        P("dp", "row"),
        P("dp", "row"),
        P("row", "col"),
        P("row", "col"),
        P("row", "col"),
        P("row", None),
        P(None, ("col", "row")),
        P(("col", "row")),
        P(),
        P(),
        P(("col", "row")),
        P(("col", "row")),
        P(("col", "row")),
        P("row"),
        P(("col", "row")),
        P("col", "row"),
    )
    return jax.shard_map(body, mesh=mesh, in_specs=in_specs, out_specs=out_specs, check_vma=False)
```

```python
import functools

import jax
import jax.numpy as jnp
from jax import lax
from jax.experimental import pallas as pl
from jax.experimental.pallas import tpu as pltpu
from jax.sharding import PartitionSpec as P

LEN = 2048
EPSILON = 1e-05
LOG2E = 1.4426950408889634
SUB = 128
STEP = 256
F32 = jnp.float32
BF16 = jnp.bfloat16
AR_SPLIT = 2
EARLY_NEAR = [1, 2, 3, 4, 5, 7]
EARLY_FAR = [1, 3, 4, 5, 7]


def dot(a, b):
    return jnp.dot(a, b, preferred_element_type=F32)


def dot_nt(a, b):
    return lax.dot_general(a, b, (((1,), (1,)), ((), ())), preferred_element_type=F32)


def dot_tn(a, b):
    return lax.dot_general(a, b, (((0,), (0,)), ((), ())), preferred_element_type=F32)


def sigmoid(x):
    return 0.5 * jnp.tanh(0.5 * x) + 0.5


def softplus(x):
    return jnp.maximum(x, 0.0) + jnp.log1p(jnp.exp(-jnp.abs(x)))


def fold8(x):
    return jnp.sum(x.reshape(x.shape[0] // 8, 8, x.shape[1]), axis=0)


def row_scan(x, mat):
    hi = x.astype(BF16).astype(F32)
    rest = x - hi
    mid = rest.astype(BF16).astype(F32)
    low = rest - mid
    parts = jnp.concatenate([hi, mid, low, jnp.zeros_like(x)], axis=0).astype(BF16)
    out = dot(parts, mat)
    return out[0:8] + out[8:16] + out[16:24]


def plain_sums(sel, z):
    return dot_nt(sel, z.astype(BF16))[0:8]


def head_sums(sel, z):
    hi = z.astype(BF16)
    low = (z - hi.astype(F32)).astype(BF16)
    return (dot_nt(sel, hi) + dot_nt(sel, low))[0:8]


def iota(shape, dim):
    return lax.broadcasted_iota(jnp.int32, shape, dim)


def spread(cols, first, rows):
    lane = iota((rows, 128), 1)
    return jnp.where(
        lane < 64,
        jnp.broadcast_to(cols[:, first : first + 1], (rows, 128)),
        jnp.broadcast_to(cols[:, first + 1 : first + 2], (rows, 128)),
    )


def pair_stack(x):
    lane = iota(x.shape, 1)
    zero = jnp.zeros_like(x)
    return jnp.concatenate([jnp.where(lane < 64, x, zero), jnp.where(lane < 64, zero, x)], axis=0)


def forward_block(width, weights_in, outs_a, outs_b, scratch):
    hid_own, hid_rec, gains, w_own, w_rec, vtap, stap, head_par, wo_own, wo_rec = weights_in
    mixed_out, pre_gate_out, pre_value_out, conv_value_out, pre_shared_out, conv_shared_out = outs_a
    y_out, state_out, rows_out, nt_out = outs_b
    state, vbuf, sbuf, po_own, po_send, square_rows = scratch
    chan = mixed_out.shape[1]
    pairs = chan // 128

    h0 = hid_own[...].astype(F32)
    h1 = hid_rec[...].astype(F32)
    square = jnp.sum(h0 * h0, axis=1, keepdims=True) + jnp.sum(h1 * h1, axis=1, keepdims=True)
    recip = lax.rsqrt(square / width + EPSILON)
    n0 = (h0 * gains[0:1, :]).astype(BF16)
    n1 = (h1 * gains[1:2, :]).astype(BF16)
    half = n0.shape[1]
    nt_out[0:half, :] = jnp.transpose(n0)
    nt_out[half : 2 * half, :] = jnp.transpose(n1)
    q = dot(n0, w_own[...]) + dot(n1, w_rec[...])
    pre = q * recip
    gate = pre[:, 0:chan]
    pre_gate_out[...] = gate
    pre_value = pre[:, chan : 2 * chan]
    pre_value_out[...] = pre_value.astype(BF16)
    pre_shared = pre[:, 2 * chan : 2 * chan + 256]
    pre_shared_out[...] = pre_shared.astype(BF16)
    vbuf[8 : 8 + STEP, :] = pre_value
    sbuf[8 : 8 + STEP, :] = pre_shared
    conv = jnp.broadcast_to(vtap[4:5, :], (STEP, chan))
    conv_s = jnp.broadcast_to(stap[4:5, :], (STEP, 256))
    for k in range(4):
        conv = conv + vbuf[5 + k : 5 + k + STEP, :] * vtap[k : k + 1, :]
        conv_s = conv_s + sbuf[5 + k : 5 + k + STEP, :] * stap[k : k + 1, :]
    vbuf[0:8, :] = vbuf[STEP : STEP + 8, :]
    sbuf[0:8, :] = sbuf[STEP : STEP + 8, :]
    conv_value_out[...] = conv
    conv_shared_out[...] = conv_s
    x = conv * sigmoid(conv)
    act = conv_s * sigmoid(conv_s)

    head_rows = jnp.transpose(pre[:, 2 * chan + 256 : 2 * chan + 384])
    first = lax.axis_index("row") == 0
    v = jnp.where(first, head_rows[0:8], head_rows[6:14]) + head_par[0:8, 0:1]
    steps = softplus(v)
    logd = head_par[8:16, 0:1] * steps
    rows_out[0:8, :] = v
    rows_out[16:24, :] = jnp.transpose(jnp.broadcast_to(recip, (STEP, 128)))[0:8]

    upper = (iota((SUB, SUB), 0) <= iota((SUB, SUB), 1)).astype(F32).astype(BF16)
    causal = iota((SUB, SUB), 0) >= iota((SUB, SUB), 1)
    sg = gate * sigmoid(gate)
    for sub in range(STEP // SUB):
        lo, hi = sub * SUB, (sub + 1) * SUB
        cum_r = row_scan(logd[:, lo:hi] * LOG2E, upper)
        rows_out[8:16, lo:hi] = cum_r
        cols = jnp.transpose(jnp.concatenate([cum_r, steps[:, lo:hi]], axis=0))
        b_in = act[lo:hi, 0:128]
        b_bf = b_in.astype(BF16)
        c_bf = act[lo:hi, 128:256].astype(BF16)
        b_t = jnp.transpose(b_in).astype(BF16)
        scores = dot_nt(c_bf, b_bf)
        for p in range(pairs):
            pl0, pl1 = p * 128, (p + 1) * 128
            c0 = jnp.broadcast_to(cols[:, 2 * p : 2 * p + 1], (SUB, 128))
            c1 = jnp.broadcast_to(cols[:, 2 * p + 1 : 2 * p + 2], (SUB, 128))
            weights = []
            for col, h in ((c0, 2 * p), (c1, 2 * p + 1)):
                gap = jnp.where(causal, col - cum_r[h : h + 1, :], -1e30)
                weights.append((scores * jnp.exp2(gap)).astype(BF16))
            lane = iota((SUB, 128), 1)
            cum_e = jnp.where(lane < 64, c0, c1)
            step_e = spread(cols, 8 + 2 * p, SUB)
            xs = x[lo:hi, pl0:pl1]
            xh = step_e * xs
            inside = dot(jnp.concatenate(weights, axis=1), pair_stack(xh.astype(BF16)))
            held = state[:, pl0:pl1]
            held_bf = held.astype(BF16)
            state_out[lo:hi, pl0:pl1] = held_bf
            carried = dot(c_bf, held_bf)
            y = inside + carried * jnp.exp2(cum_e)
            y_out[lo:hi, pl0:pl1] = y
            last = cum_e[SUB - 1 : SUB, :]
            tail = (xh * jnp.exp2(last - cum_e)).astype(BF16)
            state[:, pl0:pl1] = held * jnp.exp2(last) + dot(b_t, tail)
            y = y + vtap[5:6, pl0:pl1] * xs
            mixed_out[lo:hi, pl0:pl1] = (y * sg[lo:hi, pl0:pl1]).astype(BF16)
    mix = mixed_out[...].astype(F32)
    weighted = (mix * vtap[6:7, :]).astype(BF16)
    po_own[...] = dot(weighted, wo_own[...]).astype(BF16)
    po_send[...] = dot(weighted, wo_rec[...]).astype(BF16)
    square_rows[0:4, :] = plain_sums(jnp.ones((16, chan), BF16), mix * mix)[0:4]


def early_steps(dp, blocks):
    count = 2 * (dp.bit_length() - 1)
    if count == 6 and blocks == 8:
        return EARLY_NEAR, EARLY_FAR
    steps = [min(blocks - 1, 1 + n * (blocks - 1) // count) for n in range(count)]
    return steps, steps[:-1]


def partner_of(me, k):
    return {"dp": me + (1 - 2 * lax.rem(me // (1 << k), 2)) * (1 << k)}


def levels(dp, me, bounds, orders, acc, stage, land, out, send_sem, recv_sem):
    bits = dp.bit_length() - 1

    def span(start, rows):
        return pl.ds(pl.multiple_of(start, 16), rows)

    def bit_of(k):
        return lax.rem(me // (1 << k), 2)

    def low_at(i, count):
        low, rows = bounds[i]
        for n in range(count):
            low = low + bit_of(orders[i][n]) * (rows >> (n + 1))
        return low

    def places(i, level):
        base, rows = bounds[i]
        if level < bits:
            k = orders[i][level]
            part = rows >> (level + 1)
            give = span(low_at(i, level) + (1 - bit_of(k)) * part, part)
            where = span(base + rows - (rows >> level), part)
            return k, give, where, span(low_at(i, level + 1), part)
        back = 2 * bits - 1 - level
        own = span(low_at(i, back + 1), rows >> (back + 1))
        return orders[i][back], own, own, None

    def copy_of(i, level):
        k, give, where, _ = places(i, level)
        src, dst = (stage, land) if level < bits else (out, out)
        return remote(
            src.at[give, :], dst.at[where, :], send_sem.at[i, level], recv_sem.at[i, level], partner_of(me, k)
        )

    def start_level(i, level):
        if level < bits:
            give = places(i, level)[1]
            stage[give, :] = acc[give, :].astype(BF16)
        copy_of(i, level).start()

    def end_level(i, level, go_on=True):
        copy_of(i, level).wait()
        if level < bits:
            _, _, where, keep = places(i, level)
            total = acc[keep, :] + land[where, :].astype(F32)
            acc[keep, :] = total
            if level == bits - 1:
                out[keep, :] = total.astype(BF16)
        if go_on and level + 1 < 2 * bits:
            start_level(i, level + 1)

    return start_level, end_level


def gate_block(ins, outs):
    cot_own, cot_rec, wo_own, wo_rec, trow, rows_in, mixed, pre_gate, conv_value, y_in, vtap = ins
    acc_v, go_own, go_rec, dy_out, p_gate, rs_gate = outs
    chan = mixed.shape[1]
    tcol = jnp.transpose(jnp.concatenate([trow[...], rows_in[16:24, :]], axis=0))
    scale = tcol[:, 0:1]
    coef = tcol[:, 8:9]
    recip = tcol[:, 16:17]
    s0 = (cot_own[...].astype(F32) * scale).astype(BF16)
    s1 = (cot_rec[...].astype(F32) * scale).astype(BF16)
    d_weighted = dot_nt(s0, wo_own[...]) + dot_nt(s1, wo_rec[...])
    mix = mixed[...].astype(F32)
    acc_v[48:56, :] += fold8(d_weighted * mix)
    weighted_t = jnp.transpose((mix * vtap[6:7, :]).astype(BF16))
    go_own[...] += dot(weighted_t, s0)
    go_rec[...] += dot(weighted_t, s1)
    d_mixed = d_weighted * vtap[6:7, :] - coef * mix
    gate = pre_gate[...]
    sig = sigmoid(gate)
    silu = gate * sig
    conv = conv_value[...]
    sig_v = sigmoid(conv)
    x = conv * sig_v
    y_scan = y_in[...]
    y = y_scan + vtap[5:6, :] * x
    dy = d_mixed * silu
    d_gate = d_mixed * y * (sig + silu * (1.0 - sig))
    acc_v[40:48, :] += fold8(dy * x)
    dy_out[...] = dy.astype(BF16)
    p_gate[...] = (recip * d_gate).astype(BF16)
    rs_gate[...] = plain_sums(jnp.ones((16, chan), BF16), d_gate * gate)


def scan_block(ins, weights_in, outs, scratch):
    rows_in, pre_value, conv_value, pre_shared, conv_shared, y_in, state_in = ins
    vtap, stap, head_par, sel_ref, dy_in = weights_in
    p_out, rsum_out, acc_v, acc_s, acc_h = outs
    grad, vbuf, sbuf, dxbuf, dbbuf = scratch
    chan = conv_value.shape[1]
    pairs = chan // 128

    recip = jnp.transpose(rows_in[16:24, :])[:, 0:1]
    conv = conv_value[...]
    sig_v = sigmoid(conv)
    x = conv * sig_v
    dy_bf = dy_in[...]
    conv_s = conv_shared[...]
    sig_s = sigmoid(conv_s)
    act = conv_s * sig_s

    sel = sel_ref[...]
    sel_f = sel.astype(F32)[0:8]
    v = rows_in[0:8, :]
    steps = softplus(v)
    logd = head_par[8:16, 0:1] * steps
    lower = (iota((SUB, SUB), 0) >= iota((SUB, SUB), 1)).astype(F32).astype(BF16)
    strict = (iota((SUB, SUB), 0) < iota((SUB, SUB), 1)).astype(F32).astype(BF16)
    causal_t = iota((SUB, SUB), 0) <= iota((SUB, SUB), 1)
    for sub in reversed(range(STEP // SUB)):
        lo, hi = sub * SUB, (sub + 1) * SUB
        cum_r = rows_in[8:16, lo:hi]
        cols = jnp.transpose(jnp.concatenate([cum_r, steps[:, lo:hi]], axis=0))
        b_bf = act[lo:hi, 0:128].astype(BF16)
        c_in = act[lo:hi, 128:256]
        c_bf = c_in.astype(BF16)
        c_t = jnp.transpose(c_in).astype(BF16)
        scores_t = dot_nt(b_bf, c_bf)
        d_scores = jnp.zeros((SUB, SUB), F32)
        db = jnp.zeros((SUB, 128), F32)
        dc = jnp.zeros((SUB, 128), F32)
        z_sum = jnp.zeros((8, SUB), F32)
        e_sum = jnp.zeros((8, SUB), F32)
        f_sum = jnp.zeros((8, SUB), F32)
        gh = jnp.zeros((8, 1), F32)
        for p in range(pairs):
            pl0, pl1 = p * 128, (p + 1) * 128
            c0 = jnp.broadcast_to(cols[:, 2 * p : 2 * p + 1], (SUB, 128))
            c1 = jnp.broadcast_to(cols[:, 2 * p + 1 : 2 * p + 2], (SUB, 128))
            decays = []
            for col, h in ((c0, 2 * p), (c1, 2 * p + 1)):
                gap = jnp.where(causal_t, cum_r[h : h + 1, :] - col, -1e30)
                decays.append(jnp.exp2(gap))
            weights = [(scores_t * d).astype(BF16) for d in decays]
            lane = iota((SUB, 128), 1)
            cum_e = jnp.where(lane < 64, c0, c1)
            step_e = spread(cols, 8 + 2 * p, SUB)
            xs = x[lo:hi, pl0:pl1]
            xh = step_e * xs
            xh_bf = xh.astype(BF16)
            dys_bf = dy_bf[lo:hi, pl0:pl1]
            dys = dys_bf.astype(F32)
            stack = pair_stack(dys_bf)
            inner = dot(jnp.concatenate(weights, axis=1), stack)
            d_pair = dot_nt(xh_bf, stack)
            d_scores = d_scores + decays[0] * d_pair[:, 0:128] + decays[1] * d_pair[:, 128:256]
            last = cum_e[SUB - 1 : SUB, :]
            tail_e = jnp.exp2(last - cum_e)
            g = grad[:, pl0:pl1]
            g_bf = g.astype(BF16)
            outer = dot(b_bf, g_bf) * tail_e
            u = inner + outer
            dxbuf[lo:hi, pl0:pl1] = step_e * u + vtap[5:6, pl0:pl1] * dys
            db = db + dot_nt((xh * tail_e).astype(BF16), g_bf)
            dya = (dys * jnp.exp2(cum_e)).astype(BF16)
            held = state_in[lo:hi, pl0:pl1]
            dc = dc + dot_nt(dya, held)
            sel_p = sel[:, pl0:pl1]
            z_sum = z_sum + head_sums(
                sel_p, dys * y_in[lo:hi, pl0:pl1] - xh_bf.astype(F32) * inner
            )
            e_sum = e_sum + plain_sums(sel_p, xh * outer)
            f_sum = f_sum + plain_sums(sel_p, xs * u)
            decay_row = jnp.exp2(last)
            gh_row = decay_row * jnp.sum(g * held.astype(F32), axis=0, keepdims=True)
            gh = gh + jnp.sum(sel_f[:, pl0:pl1] * gh_row, axis=1, keepdims=True)
            grad[:, pl0:pl1] = g * decay_row + dot(c_t, dya)
        ds_bf = d_scores.astype(BF16)
        dbbuf[lo:hi, 0:128] = db + dot(ds_bf, c_bf)
        dbbuf[lo:hi, 128:256] = dc + dot(jnp.transpose(d_scores).astype(BF16), b_bf)
        d_log = row_scan(z_sum, lower) + row_scan(e_sum, strict) + gh
        d_step = (f_sum + d_log * head_par[8:16, 0:1]) * sigmoid(v[:, lo:hi])
        acc_h[0:8, :] += d_log * logd[:, lo:hi]
        acc_h[8:16, :] += d_step
        pre_step = v[:, lo:hi] - head_par[0:8, 0:1]
        rsum_out[:, lo:hi] += jnp.broadcast_to(
            jnp.sum(d_step * pre_step, axis=0, keepdims=True), (8, SUB)
        )
        zeros = jnp.zeros((6, SUB), F32)
        both = jnp.where(
            lax.axis_index("row") == 0,
            jnp.concatenate([d_step[0:6], zeros, zeros[0:4]], axis=0),
            jnp.concatenate([zeros, d_step[0:6], zeros[0:4]], axis=0),
        )
        d_cols = jnp.transpose(jnp.concatenate([both, jnp.zeros((112, SUB), F32)], axis=0))
        p_out[lo:hi, chan + 256 : chan + 384] = (recip[lo:hi] * d_cols).astype(BF16)

    d_conv = dxbuf[...] * (sig_v + x * (1.0 - sig_v))
    d_conv_s = dbbuf[...] * (sig_s + act * (1.0 - sig_s))
    vbuf[0:STEP, :] = d_conv
    sbuf[0:STEP, :] = d_conv_s
    acc_v[32:40, :] += fold8(d_conv)
    acc_s[32:40, :] += fold8(d_conv_s)
    pv = pre_value[...].astype(F32)
    ps = pre_shared[...].astype(F32)
    d_value = jnp.zeros((STEP, chan), F32)
    d_shared = jnp.zeros((STEP, 256), F32)
    for k in range(4):
        moved = vbuf[3 - k : 3 - k + STEP, :]
        d_value = d_value + vtap[k : k + 1, :] * moved
        acc_v[8 * k : 8 * k + 8, :] += fold8(pv * moved)
        moved = sbuf[3 - k : 3 - k + STEP, :]
        d_shared = d_shared + stap[k : k + 1, :] * moved
        acc_s[8 * k : 8 * k + 8, :] += fold8(ps * moved)
    vbuf[STEP : STEP + 8, :] = vbuf[0:8, :]
    sbuf[STEP : STEP + 8, :] = sbuf[0:8, :]
    p_out[:, 0:chan] = (recip * d_value).astype(BF16)
    p_out[:, chan : chan + 256] = (recip * d_shared).astype(BF16)
    ones = jnp.ones((16, chan), BF16)
    rsum_out[...] += plain_sums(ones, d_value * pv)
    rsum_out[...] += plain_sums(ones[:, 0:256], d_shared * ps)


def width_block(valid, ins, outs):
    p_gate, p_all, hid_own, hid_rec, w_own, w_rec = ins
    dn_own, dn_rec, acc_n = outs
    chan = p_gate.shape[1]
    pg = p_gate[...]
    pb = p_all[...]
    for n, (hid, weight, dn) in enumerate(((hid_own, w_own, dn_own), (hid_rec, w_rec, dn_rec))):
        part = dot_nt(pg, weight[:, 0:chan]) + dot_nt(pb, weight[:, chan:])
        dn[...] = part.astype(BF16)
        acc_n[8 * n : 8 * n + 8, :] += jnp.where(valid, fold8(part * hid[...].astype(F32)), 0.0)


def unit_rows(dp):
    return 16 * dp


def misc_rows(dp, rows):
    unit = max(unit_rows(dp), 256)
    return pl.cdiv(rows, unit) * unit


def big_rows(dp, rows):
    return pl.cdiv(rows, unit_rows(dp)) * unit_rows(dp)


def remote(src, dst, send, recv, target):
    return pltpu.make_async_remote_copy(
        src_ref=src,
        dst_ref=dst,
        send_sem=send,
        recv_sem=recv,
        device_id=target,
        device_id_type=pl.DeviceIdType.MESH,
    )


def greet(targets):
    barrier = pltpu.get_barrier_semaphore()
    for target in targets:
        pl.semaphore_signal(barrier, inc=1, device_id=target, device_id_type=pl.DeviceIdType.MESH)
    pl.semaphore_wait(barrier, len(targets))


def layer_kernel(
    seq_len,
    dp,
    inner_width,
    hid_hbm,
    cot_hbm,
    gate_w,
    value_w,
    state_w,
    out_w,
    step_t,
    value_filter,
    value_shift,
    shared_kernel,
    shared_offset,
    decay_log,
    step_bias,
    skip_gain,
    input_gain,
    gated_gain,
    sums_out,
    result_out,
    hidden_out,
    proj_col,
    dn_col,
    state_out,
    trow,
    rs_out,
    w_own,
    w_rec,
    wo_own,
    wo_rec,
    vtap,
    stap,
    head_par,
    head_rows,
    gains,
    gains_land,
    sel,
    hid_own,
    hid_rec,
    cot_own,
    cot_rec,
    pre_gate,
    pre_value,
    conv_value,
    pre_shared,
    conv_shared,
    y_scan,
    states,
    mixed,
    rows,
    normed_t,
    p_gate,
    p_all,
    dy_s,
    rs_in,
    state,
    vbuf,
    sbuf,
    dxbuf,
    dbbuf,
    pair_own,
    pair_send,
    pair_land,
    proj_s,
    dn_sum,
    sums,
    sums_land,
    go_rec,
    swap_send,
    swap_land,
    extra_send,
    extra_land,
    extra_sum,
    shared_sum,
    col_land,
    rs_land,
    acc_v,
    acc_s,
    acc_h,
    acc_n,
    acc,
    stage,
    land,
    out,
    load_sem,
    feed_sem,
    weight_sem,
    fetch_sem,
    save_sem,
    po_sem,
    dn_sem,
    col_sem,
    sum_sem,
    swap_sem,
    ar_send_sem,
    ar_recv_sem,
    out_sem,
):
    tokens, half = hid_own.shape
    chan = mixed.shape[1]
    width = 2 * half
    wide = p_all.shape[1]
    blocks = tokens // STEP
    steps_per_seq = seq_len // STEP
    size = big_rows(dp, width)
    tail = out.shape[0] - 3 * size
    bits = dp.bit_length() - 1
    me = lax.axis_index("dp")
    r = lax.axis_index("row")
    c = lax.axis_index("col")
    to_row, to_col, to_both = {"row": 1 - r}, {"col": 1 - c}, {"row": 1 - r, "col": 1 - c}
    part_rows = size // AR_SPLIT
    near = tuple(range(bits))
    far = tuple(range(1, bits)) + (0,)
    bounds = [(tail + n * part_rows, part_rows) for n in range(3 * AR_SPLIT)] + [(0, tail)]
    orders = [far if n % 2 else near for n in range(3 * AR_SPLIT)] + [near]
    firsts, values, misc = range(2 * AR_SPLIT), range(2 * AR_SPLIT, 3 * AR_SPLIT), 3 * AR_SPLIT
    start_level, end_level = levels(dp, me, bounds, orders, acc, stage, land, out, ar_send_sem, ar_recv_sem)

    def span(i):
        return pl.ds(pl.multiple_of(i * STEP, STEP), STEP)

    def load(n, i):
        src, dst = ((hid_hbm, hid_own), (cot_hbm, cot_own))[n]
        return pltpu.make_async_copy(src.at[span(i), :], dst.at[span(i), :], load_sem.at[n, i])

    def feed(n, i):
        src, dst = ((hid_hbm, hid_rec), (cot_hbm, cot_rec))[n]
        return remote(src.at[span(i), :], dst.at[span(i), :], feed_sem.at[0, n, i], feed_sem.at[1, n, i], to_row)

    def weight_parts(side, to_w, to_wo):
        cols = pl.ds(pl.multiple_of(side * chan, 128), chan)
        return (
            (gate_w.at[:, cols], to_w.at[:, 0:chan]),
            (value_w.at[:, cols], to_w.at[:, chan : 2 * chan]),
            (state_w, to_w.at[:, 2 * chan : 2 * chan + 256]),
            (out_w.at[cols, :], to_wo),
        )

    own_weights = [
        pltpu.make_async_copy(src, dst, weight_sem.at[0, n])
        for n, (src, dst) in enumerate(weight_parts(r, w_own, wo_own))
    ]
    rec_weights = [
        remote(src, dst, weight_sem.at[1, n], weight_sem.at[2, n], to_row)
        for n, (src, dst) in enumerate(weight_parts(1 - r, w_rec, wo_rec))
    ]
    step_cols = pl.ds(2 * chan + 256, 128)
    rec_weights.append(
        remote(w_own.at[:, step_cols], w_rec.at[:, step_cols], weight_sem.at[1, 4], weight_sem.at[2, 4], to_row)
    )
    rec_weights.append(remote(gains, gains_land, weight_sem.at[1, 5], weight_sem.at[2, 5], to_row))

    def save(n, i):
        src, dst = ((pre_value, result_out), (p_gate, hidden_out))[n]
        return pltpu.make_async_copy(src.at[span(i), :], dst.at[span(i), :], save_sem.at[n, i])

    def fetch(n, i):
        src, dst = ((proj_col, mixed), (dn_col, dy_s))[n]
        return pltpu.make_async_copy(src.at[span(i), :], dst.at[span(i), :], fetch_sem.at[n, i])

    def pair_copy(sem, i):
        return remote(pair_send.at[span(i), :], pair_land.at[span(i), :], sem.at[0, i], sem.at[1, i], to_row)

    def small_copy(src, dst, n, target):
        return remote(src, dst, swap_sem.at[0, n], swap_sem.at[1, n], target)

    for copy in own_weights:
        copy.start()
    for n in range(2):
        for i in range(blocks):
            load(n, i).start()
    heads = decay_log.shape[0]
    sel[...] = (iota(sel.shape, 0) == iota(sel.shape, 1) // 64).astype(F32).astype(BF16)
    head_rows[...] = jnp.zeros_like(head_rows)
    for n, ref in enumerate((step_bias, decay_log, skip_gain)):
        head_rows[n, 0:heads] = ref[...]
    head_cols = jnp.transpose(head_rows[...])[0:8]
    real = iota((8, 128), 0) < heads
    head_par[0:8, :] = jnp.broadcast_to(head_cols[:, 0:1], (8, 128))
    head_par[8:16, :] = jnp.where(real, -jnp.exp(jnp.broadcast_to(head_cols[:, 1:2], (8, 128))), 0.0)
    vtap[0:4, :] = value_filter[...]
    vtap[4, :] = value_shift[...]
    vtap[5:6, :] = jnp.sum(sel[0:8, :].astype(F32) * head_cols[:, 2:3], axis=0, keepdims=True)
    vtap[6, :] = gated_gain[...].astype(F32)
    stap[0:4, :] = shared_kernel[...]
    stap[4, :] = shared_offset[...]
    gains[...] = jnp.zeros_like(gains)
    gains[0, :] = input_gain[...]
    dxbuf[0:128, :] = jnp.zeros((128, half), F32)
    dxbuf[0 : step_t.shape[0], :] = step_t[...].astype(F32)
    w_own[:, 2 * chan + 256 : 2 * chan + 384] = jnp.transpose(dxbuf[0:128, :]).astype(BF16)
    greet([partner_of(me, k) for k in range(bits)] + [to_row, to_col, to_both])
    for copy in rec_weights:
        copy.start()
    for n in range(2):
        for i in range(blocks):
            feed(n, i).start()

    def chunk_rows(n, side):
        return pl.ds(pl.multiple_of(tail + n * size + side * half, 128), half)

    go_own = acc.at[chunk_rows(0, r), :]
    for ref in (acc_v, acc_s, acc_h, acc_n, go_rec):
        ref[...] = jnp.zeros_like(ref)
    go_own[...] = jnp.zeros((chan, half), F32)

    for copy in own_weights + rec_weights:
        copy.wait()
    gains[1:2, :] = gains_land[0:1, :]

    def sums_copy(n, i):
        target = (to_row, to_col, to_both)[n]
        return remote(sums.at[i], sums_land.at[n, i], sum_sem.at[0, n, i], sum_sem.at[1, n, i], target)

    def take_proj(i):
        pair_copy(po_sem, i).wait()
        part = pair_own[span(i), :].astype(F32) + pair_land[span(i), :].astype(F32)
        proj_s[span(i), :] = part.astype(BF16)
        dots = plain_sums(jnp.ones((16, half), BF16), part * cot_own[span(i), :].astype(F32))
        sums[i, 4:8, :] = dots[4:8]
        for n in range(3):
            sums_copy(n, i).start()

    def take_sums(i):
        for n in range(3):
            sums_copy(n, i).wait()
        total = (sums[i] + sums_land[0, i]) + (sums_land[1, i] + sums_land[2, i])
        scale = lax.rsqrt(total[0:1] / inner_width + EPSILON)
        coef = total[4:5] * (scale * scale * scale) / inner_width
        trow[0:8, span(i)] = jnp.broadcast_to(scale, (8, STEP))
        trow[8:16, span(i)] = jnp.broadcast_to(coef, (8, STEP))

    def forward(i):
        here = span(i)
        forward_block(
            width,
            (
                hid_own.at[here, :],
                hid_rec.at[here, :],
                gains,
                w_own,
                w_rec,
                vtap,
                stap,
                head_par,
                wo_own,
                wo_rec,
            ),
            (
                mixed.at[here, :],
                pre_gate.at[here, :],
                pre_value.at[here, :],
                conv_value.at[here, :],
                pre_shared.at[here, :],
                conv_shared.at[here, :],
            ),
            (y_scan.at[here, :], states.at[here, :], rows.at[:, here], normed_t.at[:, here]),
            (state, vbuf, sbuf, pair_own.at[here, :], pair_send.at[here, :], sums.at[i]),
        )

    def gate(i):
        here = span(i)
        gate_block(
            (
                cot_own.at[here, :],
                cot_rec.at[here, :],
                wo_own,
                wo_rec,
                trow.at[:, here],
                rows.at[:, here],
                mixed.at[here, :],
                pre_gate.at[here, :],
                conv_value.at[here, :],
                y_scan.at[here, :],
                vtap,
            ),
            (acc_v, go_own, go_rec, dy_s.at[here, :], p_gate.at[here, :], rs_in.at[:, here]),
        )

    first_part = max(1, blocks // 4)
    proj_parts = [(0, first_part), (first_part, blocks)]
    half_way = max(2, 5 * blocks // 8) if blocks > 2 else 0
    dn_parts = [(half_way, blocks), (0, half_way)] if half_way else [(0, blocks)]

    def wide_copy(n, part, index):
        src, dst = ((proj_s, proj_col), (dn_sum, dn_col))[n]
        rows_n = pl.ds(part[0] * STEP, (part[1] - part[0]) * STEP)
        return remote(src.at[rows_n, :], dst.at[rows_n, :], col_sem.at[n, 0, index], col_sem.at[n, 1, index], to_col)

    @pl.loop(0, blocks)
    def _(i):
        load(0, i).wait()
        feed(0, i).wait()

        @pl.when(i % steps_per_seq == 0)
        def _():
            state[...] = jnp.zeros_like(state)
            vbuf[0:8, :] = jnp.zeros((8, chan), F32)
            sbuf[0:8, :] = jnp.zeros((8, 256), F32)

        forward(i)
        load(1, i).wait()
        feed(1, i).wait()

        @pl.when(i > 0)
        def _():
            take_proj(i - 1)

        pair_copy(po_sem, i).start()
        if first_part < blocks:

            @pl.when(i == first_part)
            def _():
                wide_copy(0, proj_parts[0], 0).start()

    take_proj(blocks - 1)
    if first_part < blocks:
        wide_copy(0, proj_parts[1], 1).start()
    else:
        wide_copy(0, proj_parts[0], 0).start()

    @pl.loop(0, blocks)
    def _(i):
        take_sums(i)
        gate(i)

    swaps = [small_copy(swap_send.at[n], swap_land.at[n], n, to_row) for n in range(2)]
    swap_send[0] = go_rec[...].astype(BF16)
    swaps[0].start()
    swap_send[1] = dot(normed_t[half:width, :], p_gate[...]).astype(BF16)
    swaps[1].start()
    acc[chunk_rows(1, r), :] = dot(normed_t[0:half, :], p_gate[...])
    if size > width:
        for n in range(3):
            acc[tail + n * size + width : tail + (n + 1) * size, :] = jnp.zeros((size - width, chan), F32)
    for n in range(2):
        swaps[n].wait()
        acc[chunk_rows(n, 1 - r), :] = swap_land[n].astype(F32)
        for i in range(AR_SPLIT):
            start_level(n * AR_SPLIT + i, 0)

    def take_dn(i):
        pair_copy(dn_sem, i).wait()
        part = pair_own[span(i), :].astype(F32) + pair_land[span(i), :].astype(F32)
        dn_sum[span(i), :] = part.astype(BF16)

    def over_width(valid, i):
        here = span(i)
        width_block(
            valid,
            (p_gate.at[here, :], p_all.at[here, :], hid_own.at[here, :], hid_rec.at[here, :], w_own, w_rec),
            (pair_own.at[here, :], pair_send.at[here, :], acc_n),
        )

    p_all[span(blocks - 1), :] = jnp.zeros((STEP, wide), BF16)

    @pl.loop(0, blocks)
    def _(later):
        i = blocks - 1 - later
        here = span(i)

        @pl.when(later % steps_per_seq == 0)
        def _():
            state[...] = jnp.zeros_like(state)
            vbuf[STEP : STEP + 8, :] = jnp.zeros((8, chan), F32)
            sbuf[STEP : STEP + 8, :] = jnp.zeros((8, 256), F32)

        over_width(later > 0, jnp.minimum(i + 1, blocks - 1))
        scan_block(
            (
                rows.at[:, here],
                pre_value.at[here, :],
                conv_value.at[here, :],
                pre_shared.at[here, :],
                conv_shared.at[here, :],
                y_scan.at[here, :],
                states.at[here, :],
            ),
            (vtap, stap, head_par, sel, dy_s.at[here, :]),
            (p_all.at[here, :], rs_in.at[:, here], acc_v, acc_s, acc_h),
            (state, vbuf, sbuf, dxbuf, dbbuf),
        )

        @pl.when(later > 1)
        def _():
            take_dn(i + 2)
            for index, part in enumerate(dn_parts[:-1]):

                @pl.when(i + 2 == part[0])
                def _(index=index, part=part):
                    wide_copy(1, part, index).start()

        @pl.when(later > 0)
        def _():
            pair_copy(dn_sem, i + 1).start()

        for kind, steps in enumerate(early_steps(dp, blocks)):
            for level, when in enumerate(steps):

                @pl.when(later == when)
                def _(kind=kind, level=level):
                    for n in firsts[kind::2]:
                        end_level(n, level)

    def sum8(ref, n):
        return jnp.sum(ref[8 * n : 8 * n + 8, :], axis=0, keepdims=True)

    misc_row = small_copy(swap_send.at[0], swap_land.at[0], 4, to_row)
    value_row = small_copy(swap_send.at[1], swap_land.at[1], 5, to_row)
    swap_send[1] = dot(normed_t[half:width, :], p_all[:, 0:chan]).astype(BF16)
    value_row.start()
    over_width(True, 0)
    pair_copy(dn_sem, 0).start()
    if blocks > 1:
        take_dn(1)
    small = jnp.concatenate([sum8(acc_s, n) for n in range(5)] + [jnp.zeros((3, 256), F32)], axis=0)
    norm_own, norm_rec = [
        jnp.concatenate([sum8(acc_n, n), jnp.zeros((1, 512 - half), F32)], axis=1) for n in (0, 1)
    ]
    pad6 = jnp.zeros((6, 256), F32)
    extra_send[...] = jnp.concatenate([small, norm_rec[:, 0:256], norm_rec[:, 256:512], pad6], axis=0)
    extra_row = small_copy(extra_send, extra_land.at[0], 2, to_row)
    extra_row.start()
    rs_row = small_copy(rs_in, rs_land.at[0], 3, to_row)
    rs_row.start()
    acc[chunk_rows(2, r), :] = dot(normed_t[0:half, :], p_all[:, 0:chan])
    value_row.wait()
    acc[chunk_rows(2, 1 - r), :] = swap_land[1].astype(F32)
    for n in values:
        start_level(n, 0)
    swap_send[0] = dot(normed_t[half:width, :], p_all[:, chan:wide]).astype(BF16)
    misc_row.start()
    extra_row.wait()
    extra = jnp.concatenate([small, norm_own[:, 0:256], norm_own[:, 256:512], pad6], axis=0)
    extra_sum[...] = extra + extra_land[0]
    extra_col = small_copy(extra_sum, extra_land.at[1], 6, to_col)
    extra_col.start()
    shared = dot(normed_t[0:half, :], p_all[:, chan:wide])
    split = half // 2
    misc_row.wait()
    shared_sum[...] = (shared[:, 0:256] + swap_land[0, :, 0:256].astype(F32)).astype(BF16)
    theirs = pl.ds(pl.multiple_of((1 - c) * split, 16), split)
    state_col = small_copy(shared_sum.at[theirs, :], col_land, 7, to_col)
    state_col.start()
    step_t = jnp.transpose(shared[:, 256:384] + swap_land[0, :, 256:384].astype(F32))[0:16]
    rs_row.wait()
    rs_out[...] = rs_in[...] + rs_land[0]
    rs_col = small_copy(rs_out, rs_land.at[1], 8, to_col)
    rs_col.start()
    take_dn(0)
    wide_copy(1, dn_parts[-1], len(dn_parts) - 1).start()

    acc[0:split, 256:384] = jnp.zeros((split, 128), F32)
    first = split
    acc[first : first + 16, 256:384] = jnp.zeros((16, 128), F32)
    acc[first + 16 : first + 24, :] = jnp.concatenate(
        [sum8(acc_v, n) for n in range(7)] + [jnp.zeros((1, chan), F32)], axis=0
    )
    acc[first + 24 : first + 40, :] = jnp.broadcast_to(
        jnp.sum(acc_h[...], axis=1, keepdims=True), (16, chan)
    )
    acc[first + 40 : first + 56, :] = step_t
    if tail > first + 56:
        acc[first + 56 : tail, :] = jnp.zeros((tail - first - 56, chan), F32)
    extra_col.wait()
    acc[first : first + 16, 0:256] = extra_sum[...] + extra_land[1]
    state_col.wait()
    acc[0:split, 0:256] = (
        shared_sum[pl.ds(pl.multiple_of(c * split, 16), split), :].astype(F32)
        + col_land[...].astype(F32)
    )
    start_level(misc, 0)

    parts_of = (proj_parts if first_part < blocks else proj_parts[:1], dn_parts)

    def arrive(n, index):
        part = parts_of[n][index]
        wide_copy(n, part, index).wait()

        @pl.loop(part[0], part[1])
        def _(i):
            fetch(n, i).start()

    def write_result(part):
        @pl.loop(part[0], part[1])
        def _(i):
            here = span(i)
            fetch(0, i).wait()
            scale = jnp.transpose(trow[0:8, here])[:, 0:1]
            proj = proj_s[here, :].astype(F32) + mixed[here, :].astype(F32)
            pre_value[here, :] = (hid_own[here, :].astype(F32) + scale * proj).astype(BF16)
            save(0, i).start()

    def write_hidden(part):
        @pl.loop(part[0], part[1])
        def _(i):
            here = span(i)
            fetch(1, i).wait()
            recip = rows[16:24, here]
            pull = jnp.transpose(rs_out[:, here] * recip * recip / width)[:, 0:1]
            d_normed = dn_sum[here, :].astype(F32) + dy_s[here, :].astype(F32)
            grad_in = cot_own[here, :].astype(F32) + d_normed * gains[0:1, :]
            p_gate[here, :] = (grad_in - pull * hid_own[here, :].astype(F32)).astype(BF16)
            save(1, i).start()

    mine = pl.ds(pl.multiple_of(c * split, 16), split)
    last_col = small_copy(out.at[pl.ds(0, split), pl.ds(0, 256)], state_out.at[mine, :], 9, to_col)
    done = []

    def save_chunk(n):
        rows_n = pl.ds(*bounds[n])
        copy = pltpu.make_async_copy(out.at[rows_n, :], sums_out.at[rows_n, :], out_sem.at[n])
        copy.start()
        done.append(copy)

    for n in firsts[0::2]:
        save_chunk(n)
    for level in range(2 * bits):
        if level == min(3, 2 * bits - 1):
            for index in range(len(parts_of[0])):
                arrive(0, index)
            write_result((0, blocks))
            rs_col.wait()
            rs_out[...] = rs_out[...] + rs_land[1]
        if level == min(5, 2 * bits - 1):
            for index in range(len(dn_parts) - 1):
                arrive(1, index)
                write_hidden(dn_parts[index])
        if level == 0:
            for n in firsts[1::2]:
                end_level(n, 2 * bits - 1)
                save_chunk(n)
        if level == 2 * bits - 1:
            end_level(misc, level)
            last_col.start()
            save_chunk(misc)
            state_out[mine, :] = out[0:split, 0:256]
        for n in values:
            end_level(n, level)
            if level == 2 * bits - 1:
                save_chunk(n)
        if level < 2 * bits - 1:
            end_level(misc, level)
    arrive(1, len(dn_parts) - 1)
    write_hidden(dn_parts[-1])
    for copy in done:
        copy.wait()
    last_col.wait()
    for i in range(blocks):
        for n in range(2):
            save(n, i).wait()


def layer(seq_len, dp, hidden, cot, gate_w, value_w, state_w, out_w, *params):
    tokens, half = hidden.shape
    chan = params[1].shape[1]
    wide = chan + 384
    bits = dp.bit_length() - 1
    size = big_rows(dp, 2 * half)
    tail = misc_rows(dp, half // 2 + 64)
    total = tail + 3 * size
    blocks = tokens // STEP
    vmem = pl.BlockSpec(memory_space=pltpu.VMEM)
    hbm = pl.BlockSpec(memory_space=pl.ANY)

    def act(cols=half, dtype=BF16):
        return jax.ShapeDtypeStruct((tokens, cols), dtype)

    def room(*shape, dtype=BF16):
        return pltpu.VMEM(shape, dtype)

    def flags(*shape):
        return pltpu.SemaphoreType.DMA(shape)

    return pl.pallas_call(
        functools.partial(layer_kernel, seq_len, dp, 4 * chan),
        in_specs=[hbm] * 6 + [vmem] * len(params),
        out_specs=[hbm] * 5 + [vmem],
        out_shape=[
            jax.ShapeDtypeStruct((total, chan), BF16),
            act(),
            act(),
            act(),
            act(),
            jax.ShapeDtypeStruct((half, 256), BF16),
        ],
        scratch_shapes=[
            room(16, tokens, dtype=F32),
            room(8, tokens, dtype=F32),
            room(half, chan + wide),
            room(half, chan + wide),
            room(chan, half),
            room(chan, half),
            room(8, chan, dtype=F32),
            room(8, 256, dtype=F32),
            room(16, 128, dtype=F32),
            room(8, 128, dtype=F32),
            room(8, half, dtype=F32),
            room(8, half, dtype=F32),
            room(16, chan),
            room(tokens, half),
            room(tokens, half),
            room(tokens, half),
            room(tokens, half),
            room(tokens, chan, dtype=F32),
            room(tokens, chan),
            room(tokens, chan, dtype=F32),
            room(tokens, 256),
            room(tokens, 256, dtype=F32),
            room(tokens, chan, dtype=F32),
            room(tokens, chan),
            room(tokens, chan),
            room(24, tokens, dtype=F32),
            room(2 * half, tokens),
            room(tokens, chan),
            room(tokens, wide),
            room(tokens, chan),
            room(8, tokens, dtype=F32),
            room(128, chan, dtype=F32),
            room(STEP + 8, chan, dtype=F32),
            room(STEP + 8, 256, dtype=F32),
            room(STEP, chan, dtype=F32),
            room(STEP, 256, dtype=F32),
            room(tokens, half),
            room(tokens, half),
            room(tokens, half),
            room(tokens, half),
            room(tokens, half),
            room(blocks, 8, STEP, dtype=F32),
            room(3, blocks, 8, STEP, dtype=F32),
            room(chan, half, dtype=F32),
            room(2, half, chan),
            room(2, half, chan),
            room(16, 256, dtype=F32),
            room(2, 16, 256, dtype=F32),
            room(16, 256, dtype=F32),
            room(half, 256),
            room(half // 2, 256),
            room(2, 8, tokens, dtype=F32),
            room(56, chan, dtype=F32),
            room(40, 256, dtype=F32),
            room(16, 128, dtype=F32),
            room(16, half, dtype=F32),
            room(total, chan, dtype=F32),
            room(total, chan),
            room(total, chan),
            room(total, chan),
            flags(2, blocks),
            flags(2, 2, blocks),
            flags(3, 6),
            flags(2, blocks),
            flags(2, blocks),
            flags(2, blocks),
            flags(2, blocks),
            flags(2, 2, 3),
            flags(2, 3, blocks),
            flags(2, 10),
            flags(3 * AR_SPLIT + 1, 2 * bits),
            flags(3 * AR_SPLIT + 1, 2 * bits),
            flags(3 * AR_SPLIT + 1),
        ],
        compiler_params=pltpu.CompilerParams(
            collective_id=0, has_side_effects=True, vmem_limit_bytes=67_000_000
        ),
        name="layer",
    )(hidden, cot, gate_w, value_w, state_w, out_w, *params)


def finish_kernel(
    out_rows,
    gate_a,
    gate_b,
    value_a,
    value_b,
    misc,
    state,
    result_in,
    hidden_in,
    result,
    hidden_grad,
    g_gate,
    g_value,
    g_step,
    g_state,
    g_filter,
    g_shift,
    g_kernel,
    g_offset,
    g_decay,
    g_bias,
    g_skip,
    g_norm,
    g_gated,
    g_output,
):
    half = result.shape[1]
    result[...] = result_in[...]
    hidden_grad[...] = hidden_in[...].astype(F32)

    @pl.when(pl.program_id(0) < half // 128)
    def _():
        g_output[...] = out_rows[...].astype(F32)
        g_gate[:, 0:half] = gate_a[...].astype(F32)
        g_gate[:, half : 2 * half] = gate_b[...].astype(F32)
        g_value[:, 0:half] = value_a[...].astype(F32)
        g_value[:, half : 2 * half] = value_b[...].astype(F32)

    @pl.when(pl.program_id(0) == 0)
    def _():
        g_state[...] = state[...].astype(F32)
        small = misc[half // 2 : half // 2 + 64, :].astype(F32)
        heads = g_step.shape[0] // 2
        g_step[...] = small[40 : 40 + 2 * heads]
        g_kernel[...] = small[0:4, 0:256]
        g_offset[...] = small[4, 0:256]
        g_norm[0:256] = small[8, 0:256]
        g_norm[256:half] = small[9, 0 : half - 256]
        g_filter[...] = small[16:20]
        g_shift[...] = small[20]
        g_gated[...] = small[22]
        head = jnp.transpose(small[24:40, 0:128])[0:8]
        g_decay[...] = head[0, 0:heads]
        g_bias[...] = head[0, 8 : 8 + heads]
        sel = (iota((16, half), 0) == iota((16, half), 1) // (half // heads)).astype(F32).astype(BF16)
        skip = dot_nt(small[16:32].astype(BF16), sel)
        g_skip[...] = skip[5, 0:heads]


def finish(size, heads, out, state, result, hidden_grad):
    tokens, half = result.shape
    chan = out.shape[1]
    size_f = tokens // 4
    grid = 4

    def blk(cols):
        return pl.BlockSpec((size_f, cols), lambda i: (i, 0))

    def whole(shape):
        return pl.BlockSpec(shape, lambda i: (0,) * len(shape))

    parts = half // 128
    tail = out.shape[0] - 3 * size

    def part(start):
        return pl.BlockSpec((128, chan), lambda i: (start // 128 + jnp.minimum(i, parts - 1), 0))

    def streamed(rows, cols):
        return pl.BlockSpec((rows // parts, cols), lambda i: (jnp.minimum(i, parts - 1), 0))

    small = [
        (2 * heads, half),
        (half, 256),
        (4, chan),
        (chan,),
        (4, 256),
        (256,),
        (heads,),
        (heads,),
        (heads,),
        (half,),
        (chan,),
    ]
    big = (half, 2 * chan)
    shapes = [big, big] + small + [(2 * chan, half)]
    return pl.pallas_call(
        finish_kernel,
        grid=(grid,),
        in_specs=[
            pl.BlockSpec((256, half), lambda i: (tail // 256 + jnp.minimum(i, parts - 1), 0)),
            part(tail + size),
            part(tail + size + half),
            part(tail + 2 * size),
            part(tail + 2 * size + half),
            whole((tail, chan)),
            whole(state.shape),
            blk(half),
            blk(half),
        ],
        out_specs=[blk(half), blk(half), streamed(*big), streamed(*big)]
        + [whole(shape) for shape in small]
        + [streamed(2 * chan, half)],
        out_shape=[
            jax.ShapeDtypeStruct((tokens, half), BF16),
            jax.ShapeDtypeStruct((tokens, half), F32),
        ]
        + [jax.ShapeDtypeStruct(shape, F32) for shape in shapes],
        cost_estimate=pl.CostEstimate(flops=20_000_000, bytes_accessed=20_000_000, transcendentals=0),
        name="finish",
    )(
        out,
        out,
        out,
        out,
        out,
        out,
        state,
        result,
        hidden_grad,
    )


def body(
    hidden,
    gate_proj,
    value_proj,
    step_proj,
    state_proj,
    value_filter,
    value_shift,
    shared_kernel,
    shared_offset,
    decay_log,
    step_bias,
    skip_gain,
    input_gain,
    gated_gain,
    output_proj,
    cotangent,
):
    tokens, half = hidden.shape
    width = 2 * half
    chan = gated_gain.shape[0]
    heads = decay_log.shape[0]
    dp = lax.axis_size("dp")
    seq_len = min(LEN, tokens)

    out, result, hidden_grad, _, _, g_state = layer(
        seq_len,
        dp,
        hidden,
        cotangent,
        gate_proj,
        value_proj,
        state_proj,
        output_proj,
        step_proj.T,
        value_filter,
        value_shift,
        shared_kernel,
        shared_offset,
        decay_log,
        step_bias,
        skip_gain,
        input_gain,
        gated_gain,
    )
    outs = finish(big_rows(dp, width), heads, out, g_state, result, hidden_grad)
    return tuple(outs[0:4]) + (outs[4].T,) + tuple(outs[5:])


def solution(mesh):
    in_specs = (
        P("dp", "row"),
        P("row", "col"),
        P("row", "col"),
        P("row", "col"),
        P("row", None),
        P(None, ("col", "row")),
        P(("col", "row")),
        P(),
        P(),
        P(("col", "row")),
        P(("col", "row")),
        P(("col", "row")),
        P("row"),
        P(("col", "row")),
        P("col", "row"),
        P("dp", "row"),
    )
    out_specs = (
        P("dp", "row"),
        P("dp", "row"),
        P("row", "col"),
        P("row", "col"),
        P("row", "col"),
        P("row", None),
        P(None, ("col", "row")),
        P(("col", "row")),
        P(),
        P(),
        P(("col", "row")),
        P(("col", "row")),
        P(("col", "row")),
        P("row"),
        P(("col", "row")),
        P("col", "row"),
    )
    return jax.shard_map(body, mesh=mesh, in_specs=in_specs, out_specs=out_specs, check_vma=False)
```
